256 devices in a mesh: tp: 256 (over z, y, x, core).
Axes of the slice: x: 4, y: 4, z: 8, core: 2. Of those that a mesh axis runs over, the one named last changes fastest.
Arguments:
- hidden_in: bfloat16 [1, 2048, 2048], P(None, 'tp')
- lengths: int32 [1], replicated
- attn_norm: bfloat16 [2, 2048], replicated
- w_query: bfloat16 [2, 2048, 32, 64], replicated
- w_key: bfloat16 [2, 2048, 8, 64], replicated
- w_value: bfloat16 [2, 2048, 8, 64], replicated
- w_out: bfloat16 [2, 32, 64, 2048], replicated
- mlp_norm: bfloat16 [2, 2048], replicated
- w_gate: bfloat16 [2, 2048, 8192], P(None, None, 'tp')
- w_up: bfloat16 [2, 2048, 8192], P(None, None, 'tp')
- w_down: bfloat16 [2, 8192, 2048], P(None, 'tp')
- final_norm: bfloat16 [2048], replicated
Outputs:
- output: bfloat16 [1, 2048, 2048], P(None, 'tp')
All inputs are finite; a program needn't handle non-finite values.
Results may differ from the reference program's by a relative error of at most 0.019148.
Values are sent between devices in bfloat16 or wider.
A program may use at most 768 MiB of HBM per device.

```python
import jax
import jax.numpy as jnp
from jax import lax

BATCH = 1
SEQ_DEV = 8
TP_SIZE = 256
SEQ_LEN = 2048
D_MODEL = 2048
HEADS = 32
KV_HEADS = 8
HEAD_DIM = 64
FF_DIM = 8192
LAYERS = 2

NORM_EPS = 1e-5
ROPE_BASE = 500000.0


def setup_inputs(seed: int = 0) -> dict:
    keys = jax.random.split(jax.random.key(seed), 12)
    d_scale = D_MODEL ** -0.5
    hidden_in = jax.random.normal(keys[0], (BATCH, SEQ_LEN, D_MODEL), jnp.float32)
    lengths = jax.random.randint(keys[1], (BATCH,), 1, SEQ_LEN + 1, jnp.int32)
    attn_norm = 1.0 + 0.25 * jax.random.normal(keys[2], (LAYERS, D_MODEL), jnp.float32)
    w_query = 1.4 * d_scale * jax.random.normal(keys[3], (LAYERS, D_MODEL, HEADS, HEAD_DIM), jnp.float32)
    w_key = 1.4 * d_scale * jax.random.normal(keys[4], (LAYERS, D_MODEL, KV_HEADS, HEAD_DIM), jnp.float32)
    w_value = d_scale * jax.random.normal(keys[5], (LAYERS, D_MODEL, KV_HEADS, HEAD_DIM), jnp.float32)
    w_out = (HEADS * HEAD_DIM) ** -0.5 * jax.random.normal(keys[6], (LAYERS, HEADS, HEAD_DIM, D_MODEL), jnp.float32)
    mlp_norm = 1.0 + 0.25 * jax.random.normal(keys[7], (LAYERS, D_MODEL), jnp.float32)
    w_gate = d_scale * jax.random.normal(keys[8], (LAYERS, D_MODEL, FF_DIM), jnp.float32)
    w_up = d_scale * jax.random.normal(keys[9], (LAYERS, D_MODEL, FF_DIM), jnp.float32)
    w_down = FF_DIM ** -0.5 * jax.random.normal(keys[10], (LAYERS, FF_DIM, D_MODEL), jnp.float32)
    final_norm = 1.0 + 0.25 * jax.random.normal(keys[11], (D_MODEL,), jnp.float32)
    return {
        'hidden_in': hidden_in.astype(jnp.bfloat16),
        'lengths': lengths,
        'attn_norm': attn_norm.astype(jnp.bfloat16),
        'w_query': w_query.astype(jnp.bfloat16),
        'w_key': w_key.astype(jnp.bfloat16),
        'w_value': w_value.astype(jnp.bfloat16),
        'w_out': w_out.astype(jnp.bfloat16),
        'mlp_norm': mlp_norm.astype(jnp.bfloat16),
        'w_gate': w_gate.astype(jnp.bfloat16),
        'w_up': w_up.astype(jnp.bfloat16),
        'w_down': w_down.astype(jnp.bfloat16),
        'final_norm': final_norm.astype(jnp.bfloat16),
    }


def rms_norm(hidden, gain):
    h_wide = hidden.astype(jnp.float32)
    inv_rms = lax.rsqrt(jnp.mean(h_wide * h_wide, axis=-1, keepdims=True) + NORM_EPS)
    return (h_wide * inv_rms * gain.astype(jnp.float32)).astype(jnp.bfloat16)


def rotate(proj, cos_tab, sin_tab):
    half_dim = proj.shape[-1] // 2
    first = proj[..., :half_dim]
    second = proj[..., half_dim:]
    return jnp.concatenate([first * cos_tab - second * sin_tab, second * cos_tab + first * sin_tab], axis=-1)


def reference(hidden_in, lengths, attn_norm, w_query, w_key, w_value, w_out, mlp_norm, w_gate, w_up, w_down, final_norm):
    groups = HEADS // KV_HEADS
    ff_shard = FF_DIM // TP_SIZE
    half_dim = HEAD_DIM // 2
    positions = jnp.arange(SEQ_LEN)
    inv_freq = ROPE_BASE ** (-2.0 * jnp.arange(half_dim).astype(jnp.float32) / HEAD_DIM)
    angles = positions.astype(jnp.float32)[:, None, None] * inv_freq[None, None, :]
    cos_tab = jnp.cos(angles)
    sin_tab = jnp.sin(angles)
    score_scale = HEAD_DIM ** -0.5
    key_ok = positions[None, :] < lengths[:, None]

    def layer_fn(hidden, layer_w):
        g_attn, w_q, w_k, w_v, w_o, g_mlp, w_g, w_u, w_d = layer_w
        normed = rms_norm(hidden, g_attn).astype(jnp.float32)
        q_proj = jnp.einsum('bsd,dhe->bshe', normed, w_q.astype(jnp.float32))
        key_proj = jnp.einsum('bsd,dhe->bshe', normed, w_k.astype(jnp.float32))
        v_proj = jnp.einsum('bsd,dhe->bshe', normed, w_v.astype(jnp.float32)).astype(jnp.bfloat16)
        q_rot = rotate(q_proj, cos_tab, sin_tab).astype(jnp.bfloat16)
        k_rot = rotate(key_proj, cos_tab, sin_tab).astype(jnp.bfloat16)
        q_blocks = jnp.moveaxis(q_rot.reshape(BATCH, TP_SIZE, SEQ_DEV, KV_HEADS, groups, HEAD_DIM), 1, 0)
        k_wide = k_rot.astype(jnp.float32)
        v_wide = v_proj.astype(jnp.float32)

        def block_fn(blk_args):
            q_blk, blk_idx = blk_args
            q_pos = blk_idx * SEQ_DEV + jnp.arange(SEQ_DEV)
            scores = jnp.einsum('bqkgd,bskd->bkgqs', q_blk.astype(jnp.float32), k_wide) * score_scale
            allowed = (positions[None, None, :] <= q_pos[None, :, None]) & key_ok[:, None, :]
            scores = jnp.where(allowed[:, None, None, :, :], scores, -1e30)
            prob_mat = jax.nn.softmax(scores, axis=-1).astype(jnp.bfloat16)
            context = jnp.einsum('bkgqs,bskd->bqkgd', prob_mat.astype(jnp.float32), v_wide)
            return context.astype(jnp.bfloat16)

        context = lax.map(block_fn, (q_blocks, jnp.arange(TP_SIZE)))
        context = jnp.moveaxis(context, 0, 1).reshape(BATCH, SEQ_LEN, HEADS, HEAD_DIM)
        attn_out = jnp.einsum('bshe,hed->bsd', context.astype(jnp.float32), w_o.astype(jnp.float32))
        hidden = (hidden.astype(jnp.float32) + attn_out).astype(jnp.bfloat16)
        normed = rms_norm(hidden, g_mlp).reshape(BATCH * SEQ_LEN, D_MODEL)
        wg_shards = jnp.moveaxis(w_g.reshape(D_MODEL, TP_SIZE, ff_shard), 1, 0)
        wu_shards = jnp.moveaxis(w_u.reshape(D_MODEL, TP_SIZE, ff_shard), 1, 0)
        wd_shards = w_d.reshape(TP_SIZE, ff_shard, D_MODEL)

        def shard_fn(acc_sum, shard_w):
            g_w, u_w, d_w = shard_w
            gate_proj = jnp.dot(normed, g_w, preferred_element_type=jnp.float32)
            up_proj = jnp.dot(normed, u_w, preferred_element_type=jnp.float32)
            gated_act = (jax.nn.silu(gate_proj) * up_proj).astype(jnp.bfloat16)
            part_out = jnp.dot(gated_act, d_w, preferred_element_type=jnp.float32).astype(jnp.bfloat16)
            return acc_sum + part_out.astype(jnp.float32), None

        mlp_out, unused = lax.scan(shard_fn, jnp.zeros((BATCH * SEQ_LEN, D_MODEL), jnp.float32), (wg_shards, wu_shards, wd_shards))
        hidden = (hidden.astype(jnp.float32) + mlp_out.reshape(BATCH, SEQ_LEN, D_MODEL)).astype(jnp.bfloat16)
        return hidden, None

    hidden, unused = lax.scan(layer_fn, hidden_in, (attn_norm, w_query, w_key, w_value, w_out, mlp_norm, w_gate, w_up, w_down))
    return rms_norm(hidden, final_norm)
```

```python
import functools

import jax
import jax.numpy as jnp
from jax import lax
from jax.experimental import pallas as pl
from jax.experimental.pallas import tpu as pltpu
from jax.sharding import PartitionSpec as P

NORM_EPS = 1e-5
ROPE_BASE = 500000.0
NX = 4
PLANE = NX * NX
LANES = 128
CHUNK = 256
NT = (((1,), (1,)), ((), ()))
F32, BF16 = jnp.float32, jnp.bfloat16


def remote(src, dst, send_sem, recv_sem, device):
    return pltpu.make_async_remote_copy(
        src_ref=src, dst_ref=dst, send_sem=send_sem, recv_sem=recv_sem,
        device_id=(device,), device_id_type=pl.DeviceIdType.MESH)


def kernel(nz, h_ref, len_ref, cos_ref, sin_ref, gain_ref, wq_ref, wk_ref, wv_ref, wo_ref, wg_ref, wu_ref, wd_ref,
           out_ref, w_all, wo_v, wqkv, h_all, c_mat, kv_all, rs, ps, hres, zb, qbuf, bd,
           local_sem, w_recv, w_send, d_recv, d_send, h_recv, h_send, kv_recv, kv_send, kvd_recv, kvd_send,
           c_recv, c_send, rs_recv, rs_send):
    layers = wo_ref.shape[0]
    seq_dev, d_model = h_ref.shape
    units = wg_ref.shape[1]
    pack = 3 * units
    half = pack // 2
    rows = nz * seq_dev
    hq = wq_ref.shape[1] // nz
    hd = wk_ref.shape[1] // nz
    nch = d_model // CHUNK
    me = lax.axis_index('tp')
    core = me % 2
    px = (me // 2) % NX
    py = (me // (2 * NX)) % NX
    mp = (me // 2) % PLANE
    mz = me // (2 * PLANE)
    base = mz * (2 * PLANE)
    partner = base + mp * 2 + (1 - core)

    def z_peer(i):
        return ((mz + i) % nz) * (2 * PLANE) + mp * 2 + core

    def pack_copies(l):
        mine = w_all.at[l, core, mp]
        return [pltpu.make_async_copy(ref.at[l], mine.at[pl.ds(i * units, units)], local_sem.at[l, i])
                for i, ref in enumerate((wg_ref, wu_ref, wd_ref))]

    def qkv_copies(l):
        return [
            pltpu.make_async_copy(wq_ref.at[l, pl.ds(mz * hq, hq)], wqkv.at[l, pl.ds(0, hq)], local_sem.at[l, 3]),
            pltpu.make_async_copy(wk_ref.at[l, pl.ds(mz * hd, hd)], wqkv.at[l, pl.ds(hq, hd)], local_sem.at[l, 4]),
            pltpu.make_async_copy(wv_ref.at[l, pl.ds(mz * hd, hd)], wqkv.at[l, pl.ds(hq + hd, hd)], local_sem.at[l, 5]),
        ]

    def wo_copy(l):
        return pltpu.make_async_copy(wo_ref.at[l], wo_v.at[l], local_sem.at[l, 6])

    for l in range(layers):
        for c in pack_copies(l) + qkv_copies(l):
            c.start()
        wo_copy(l).start()

    barrier = pltpu.get_barrier_semaphore()

    def signal(device):
        pl.semaphore_signal(barrier, inc=1, device_id=(device,), device_id_type=pl.DeviceIdType.MESH)

    signal(partner)
    for i in range(1, nz):
        signal(z_peer(i))

    @pl.loop(1, PLANE)
    def _(i):
        signal(base + ((mp + i) % PLANE) * 2 + core)

    pl.semaphore_wait(barrier, 1 + (nz - 1) + (PLANE - 1))

    def slot(h, a1, a2):
        return a2 % NX * NX + a1 % NX if h == 0 else a1 % NX * NX + a2 % NX

    def where_am_i(h):
        return (px, py) if h == 0 else (py, px)

    def at(h, a1, a2):
        return base + slot(h, a1, a2) * 2 + core

    third = half // 3
    SPAN = ((0, half), (half, half))
    FROM_MINUS = ((0, 2 * third), (half, third))
    FROM_PLUS = ((2 * third, third), (half + third, 2 * third))

    def piece(l, c, p, span):
        return w_all.at[l, c, p, pl.ds(*span)]

    def w_copy(l, h, p, span, idx, device):
        ref = piece(l, core, p, span)
        return remote(ref, ref, w_send.at[l], w_recv.at[l, h, idx], device)

    def to_partner(l, p, span):
        ref = piece(l, core, p, span)
        remote(ref, ref, d_send.at[l], d_recv.at[l], partner).start()

    def p1(l):
        for c in pack_copies(l):
            c.wait()
        for h in range(2):
            a1, a2 = where_am_i(h)
            w_copy(l, h, mp, SPAN[h], 0, at(h, a1 + 1, a2)).start()
            w_copy(l, h, mp, SPAN[h], 1, at(h, a1 + NX - 1, a2)).start()
        to_partner(l, mp, (0, pack))

    def p2(l):
        for h in range(2):
            a1, a2 = where_am_i(h)
            low, high = slot(h, a1 + NX - 1, a2), slot(h, a1 + 1, a2)
            w_copy(l, h, low, SPAN[h], 0, me).wait_recv()
            w_copy(l, h, low, FROM_MINUS[h], 2, at(h, a1 + 1, a2)).start()
            w_copy(l, h, high, SPAN[h], 1, me).wait_recv()
            w_copy(l, h, high, FROM_PLUS[h], 3, at(h, a1 + NX - 1, a2)).start()
            to_partner(l, low, SPAN[h])
            to_partner(l, high, SPAN[h])

    def p3(l):
        for h in range(2):
            a1, a2 = where_am_i(h)
            for k in (0, 1, 3, 2):
                p = slot(h, a1 + k, a2)
                if k == 2:
                    w_copy(l, h, p, FROM_MINUS[h], 2, me).wait_recv()
                    w_copy(l, h, p, FROM_PLUS[h], 3, me).wait_recv()
                    to_partner(l, p, SPAN[h])
                w_copy(l, h, p, SPAN[h], 4 + k, at(h, a1, a2 + 1)).start()
                w_copy(l, h, p, SPAN[h], 8 + k, at(h, a1, a2 + NX - 1)).start()

    def p4(l):
        for k in (0, 1, 3, 2):
            for h in range(2):
                a1, a2 = where_am_i(h)
                low, high = slot(h, a1 + k, a2 + NX - 1), slot(h, a1 + k, a2 + 1)
                w_copy(l, h, low, SPAN[h], 4 + k, me).wait_recv()
                w_copy(l, h, low, FROM_MINUS[h], 12 + k, at(h, a1, a2 + 1)).start()
                w_copy(l, h, high, SPAN[h], 8 + k, me).wait_recv()
                w_copy(l, h, high, FROM_PLUS[h], 16 + k, at(h, a1, a2 + NX - 1)).start()
                to_partner(l, low, SPAN[h])
                to_partner(l, high, SPAN[h])

    def p5(l):
        for k in (0, 1, 3, 2):
            for h in range(2):
                a1, a2 = where_am_i(h)
                p = slot(h, a1 + k, a2 + 2)
                w_copy(l, h, p, FROM_MINUS[h], 12 + k, me).wait_recv()
                w_copy(l, h, p, FROM_PLUS[h], 16 + k, me).wait_recv()
                to_partner(l, p, SPAN[h])

    def w_done(l):
        ref = w_all.at[l, 1 - core]
        remote(ref, ref, d_send.at[l], d_recv.at[l], partner).wait_recv()

    def h_copy(l, device):
        ref = h_all.at[l, mz]
        return remote(h_ref if l == 0 else ref, ref, h_send.at[l], h_recv.at[l], device)

    def h_start(l):
        for i in range(1, nz):
            h_copy(l, z_peer(i)).start()

    def h_wait(l):
        if nz > 1:
            ref = h_all.at[l, pl.ds(0, nz - 1)]
            remote(ref, ref, h_send.at[l], h_recv.at[l], me).wait_recv()
        for i in range(nz):
            hres[pl.ds(i * seq_dev, seq_dev)] = h_all[l, i].astype(F32)

    def norm_to_zb(g):
        gain = gain_ref[pl.ds(g, 1)]
        step = min(16, rows)

        @pl.loop(0, rows // step)
        def _(i):
            r = pl.ds(pl.multiple_of(i * step, step), step)
            x = hres[r]
            inv = lax.rsqrt(jnp.mean(x * x, axis=-1, keepdims=True) + NORM_EPS)
            zb[r] = (x * inv * gain).astype(BF16)

    lane = lax.broadcasted_iota(jnp.int32, (rows, LANES), 1)
    low_half = lane < hd

    def rotate(x):
        first = (lane % hd) < hd // 2
        swapped = jnp.where(first, pltpu.roll(x, LANES - hd // 2, 1), pltpu.roll(x, hd // 2, 1))
        return x * cos_ref[...] + swapped * sin_ref[...]

    def kv_copy(l, device):
        ref = kv_all.at[l, core, mp]
        return remote(ref, ref, kv_send.at[l], kv_recv.at[l], device)

    def qkv(l):
        for c in qkv_copies(l):
            c.wait()
        proj = lax.dot_general(zb[...], wqkv[l], NT, preferred_element_type=F32)
        kv = proj[:, hq:hq + 2 * hd]
        kv_all[l, core, mp] = jnp.where(low_half, rotate(kv), kv).astype(BF16)

        @pl.loop(1, PLANE)
        def _(i):
            kv_copy(l, base + ((mp + i) % PLANE) * 2 + core).start()

        for j in range(hq // LANES):
            q = rotate(proj[:, j * LANES:(j + 1) * LANES])
            qbuf[2 * j] = jnp.where(low_half, q, 0.0).astype(BF16)
            qbuf[2 * j + 1] = jnp.where(low_half, pltpu.roll(q, LANES - hd, 1), 0.0).astype(BF16)

    def kv_wait(l):
        ref = kv_all.at[l, core, pl.ds(0, PLANE - 1)]
        remote(ref, ref, kv_send.at[l], kv_recv.at[l], me).wait_recv()
        ref = kv_all.at[l, core]
        remote(ref, ref, kvd_send.at[l], kvd_recv.at[l], partner).start()
        ref = kv_all.at[l, 1 - core]
        remote(ref, ref, kvd_send.at[l], kvd_recv.at[l], partner).wait_recv()

    def c_columns(j):
        return pl.ds(pl.multiple_of(mz * hq + j * LANES, LANES), LANES)

    def attention(l):
        keys = 2 * PLANE * rows
        j = lax.broadcasted_iota(jnp.int32, (1, keys), 1)
        key_pos = ((j // seq_dev) % nz) * (2 * PLANE * seq_dev) + ((j // rows) % PLANE) * (2 * seq_dev) \
            + (j // (PLANE * rows)) * seq_dev + j % seq_dev
        i = lax.broadcasted_iota(jnp.int32, (rows, 1), 0)
        q_pos = (i // seq_dev) * (2 * PLANE * seq_dev) + (mp * 2 + core) * seq_dev + i % seq_dev
        allowed = key_pos <= jnp.minimum(q_pos, len_ref[0] - 1)
        for pair in range(hq // LANES):
            outs = []
            for head in (2 * pair, 2 * pair + 1):
                kv = kv_all[l].reshape(keys, LANES)
                s = lax.dot_general(qbuf[head], kv, NT, preferred_element_type=F32) * (hd ** -0.5)
                s = jnp.where(allowed, s, -1e30)
                e = jnp.exp(s - jnp.max(s, axis=-1, keepdims=True))
                p = (e * (1.0 / jnp.sum(e, axis=-1, keepdims=True))).astype(BF16)
                outs.append(jnp.dot(p, kv, preferred_element_type=F32))
            c = jnp.where(low_half, pltpu.roll(outs[0], LANES - hd, 1), outs[1]).astype(BF16)
            c_mat[l, :, c_columns(pair)] = c
            ref = c_mat.at[l, :, c_columns(pair)]
            for i in range(1, nz):
                remote(ref, ref, c_send.at[l], c_recv.at[l], z_peer(i)).start()

    def out_proj(l):
        if nz > 1:
            ref = c_mat.at[l, :, pl.ds(0, (nz - 1) * hq)]
            remote(ref, ref, c_send.at[l], c_recv.at[l], me).wait_recv()
        wo_copy(l).wait()

        @pl.loop(0, nch)
        def _(n):
            cols = pl.ds(pl.multiple_of(n * CHUNK, CHUNK), CHUNK)
            acc = jnp.dot(c_mat[l], wo_v[l, :, cols], preferred_element_type=F32)
            hres[:, cols] = (hres[:, cols] + acc).astype(BF16).astype(F32)

    group = CHUNK // units
    n_groups = 2 * PLANE // group

    def slab(l, g, first, cols):
        per = PLANE // group
        return w_all[l, g // per, pl.ds((g % per) * group, group), pl.ds(first, units), cols]

    def mlp_units(l):
        block = lax.broadcasted_iota(jnp.int32, (rows, CHUNK), 1) // units

        @pl.loop(0, n_groups)
        def _(g):
            every = pl.ds(0, d_model)
            gate = lax.dot_general(zb[...], slab(l, g, 0, every).reshape(CHUNK, d_model), NT, preferred_element_type=F32)
            up = lax.dot_general(zb[...], slab(l, g, units, every).reshape(CHUNK, d_model), NT, preferred_element_type=F32)
            act = gate * (1.0 / (1.0 + jnp.exp(-gate))) * up
            for b in range(group):
                bd[g, pl.ds(b * rows, rows)] = jnp.where(block == b, act, 0.0).astype(BF16)

    def rs_copy(l, n, i):
        return remote(ps.at[l, n, (mz + i) % nz], rs.at[l, mz, n], rs_send.at[l], rs_recv.at[l], z_peer(i))

    def mlp_down(l):
        @pl.loop(0, nch)
        def _(n):
            cols = pl.ds(pl.multiple_of(n * CHUNK, CHUNK), CHUNK)
            acc = jnp.zeros((rows, CHUNK), F32)
            for g in range(n_groups):
                y = jnp.dot(bd[g], slab(l, g, 2 * units, cols).reshape(CHUNK, CHUNK), preferred_element_type=F32)
                y = y.astype(BF16).astype(F32)
                for b in range(group):
                    acc = acc + y[b * rows:(b + 1) * rows]
            ps[l, n] = acc.reshape(nz, seq_dev, CHUNK)
            for i in range(1, nz):
                rs_copy(l, n, i).start()

    def rs_finish(l, store):
        if nz > 1:
            ref = rs.at[l, pl.ds(0, nz - 1)]
            remote(ref, ref, rs_send.at[l], rs_recv.at[l], me).wait_recv()
        mine = pl.ds(pl.multiple_of(mz * seq_dev, seq_dev), seq_dev)
        for n in range(nch):
            rs[l, mz, n] = ps[l, n, mz]
        for n in range(nch):
            total = rs[l, 0, n]
            for i in range(1, nz):
                total = total + rs[l, i, n]
            cols = pl.ds(n * CHUNK, CHUNK)
            store(cols, (hres[mine, cols] + total).astype(BF16))

    def store_next(l):
        def store(cols, x):
            h_all[l + 1, mz, :, cols] = x
        return store

    def store_last(cols, x):
        hres[pl.ds(0, seq_dev), cols] = x.astype(F32)

    h_all[0, mz] = h_ref[...]
    h_start(0)
    p1(0)
    for l in range(layers):
        last = l == layers - 1
        h_wait(l)
        if l == 0:
            p2(0)
        norm_to_zb(l)
        qkv(l)
        if l == 0:
            p3(0)
        kv_wait(l)
        attention(l)
        p4(l)
        out_proj(l)
        norm_to_zb(layers + l)
        if not last:
            p1(l + 1)
        p5(l)
        w_done(l)
        mlp_units(l)
        mlp_down(l)
        if not last:
            p2(l + 1)
            p3(l + 1)
            rs_finish(l, store_next(l))
            h_start(l + 1)
    rs_finish_rows(rs_finish, layers - 1, hres, mz, seq_dev, out_ref, gain_ref, 2 * layers)

    for l in range(layers):
        ref = w_all.at[l, 0, pl.ds(0, PLANE - 1)]
        remote(ref, ref, w_send.at[l], w_recv.at[l, 0, 0], me).wait_send()
        ref = w_all.at[l, 0]
        remote(ref, ref, d_send.at[l], d_recv.at[l], me).wait_send()
        ref = kv_all.at[l, 0, pl.ds(0, PLANE - 1)]
        remote(ref, ref, kv_send.at[l], kv_recv.at[l], me).wait_send()
        ref = kv_all.at[l, 0]
        remote(ref, ref, kvd_send.at[l], kvd_recv.at[l], me).wait_send()
        if nz > 1:
            ref = h_all.at[l, pl.ds(0, nz - 1)]
            remote(ref, ref, h_send.at[l], h_recv.at[l], me).wait_send()
            ref = c_mat.at[l, :, pl.ds(0, (nz - 1) * hq)]
            remote(ref, ref, c_send.at[l], c_recv.at[l], me).wait_send()
            ref = rs.at[l, pl.ds(0, nz - 1)]
            remote(ref, ref, rs_send.at[l], rs_recv.at[l], me).wait_send()


def rs_finish_rows(rs_finish, l, hres, mz, seq_dev, out_ref, gain_ref, g):
    pieces = []
    rs_finish(l, lambda cols, x: pieces.append(x.astype(F32)))
    x = jnp.concatenate(pieces, axis=1)
    inv = lax.rsqrt(jnp.mean(x * x, axis=-1, keepdims=True) + NORM_EPS)
    out_ref[...] = (x * inv * gain_ref[pl.ds(g, 1)]).astype(BF16)


def solution(mesh):
    nz = mesh.shape['tp'] // (2 * PLANE)

    def device_fn(hidden_in, lengths, attn_norm, w_query, w_key, w_value, w_out, mlp_norm, w_gate, w_up, w_down, final_norm):
        seq_dev, d_model = hidden_in.shape[1:]
        layers, _, heads, hd = w_query.shape
        kv_heads = w_key.shape[2]
        units = w_gate.shape[2]
        assert kv_heads == nz and 2 * hd == LANES and heads % nz == 0
        hq = heads // nz * hd
        rows = nz * seq_dev
        nch = d_model // CHUNK
        n_groups = 2 * PLANE * units // CHUNK
        i, lane = jnp.arange(rows), jnp.arange(LANES)
        pos = (i // seq_dev) * (2 * PLANE * seq_dev) + (lax.axis_index('tp') % (2 * PLANE)) * seq_dev + i % seq_dev
        inv_freq = ROPE_BASE ** (-2.0 * (lane % (hd // 2)).astype(F32) / hd)
        angles = pos.astype(F32)[:, None] * inv_freq[None, :]
        cos = jnp.cos(angles)
        sin = jnp.where(lane % hd < hd // 2, -1.0, 1.0) * jnp.sin(angles)
        gains = jnp.concatenate([attn_norm, mlp_norm, final_norm[None]], axis=0).astype(F32)
        by_rows = lambda w: jnp.transpose(w, (0, 2, 3, 1)).reshape(layers, -1, d_model)
        units_first = lambda w: jnp.transpose(w, (0, 2, 1))
        any_spec, vmem, smem = (pl.BlockSpec(memory_space=s) for s in (pl.ANY, pltpu.VMEM, pltpu.SMEM))
        dma = pltpu.SemaphoreType.DMA
        out = pl.pallas_call(
            functools.partial(kernel, nz),
            name='decoder',
            out_shape=jax.ShapeDtypeStruct((seq_dev, d_model), BF16),
            in_specs=[vmem, smem, vmem, vmem, vmem] + [any_spec] * 7,
            out_specs=vmem,
            scratch_shapes=[
                pltpu.VMEM((layers, 2, PLANE, 3 * units, d_model), BF16),
                pltpu.VMEM((layers, heads * hd, d_model), BF16),
                pltpu.VMEM((layers, hq + 2 * hd, d_model), BF16),
                pltpu.VMEM((layers, nz, seq_dev, d_model), BF16),
                pltpu.VMEM((layers, rows, heads * hd), BF16),
                pltpu.VMEM((layers, 2, PLANE, rows, LANES), BF16),
                pltpu.VMEM((layers, nz, nch, seq_dev, CHUNK), F32),
                pltpu.VMEM((layers, nch, nz, seq_dev, CHUNK), F32),
                pltpu.VMEM((rows, d_model), F32),
                pltpu.VMEM((rows, d_model), BF16),
                pltpu.VMEM((hq // hd, rows, LANES), BF16),
                pltpu.VMEM((n_groups, CHUNK // units * rows, CHUNK), BF16),
                dma((layers, 7)), dma((layers, 2, 20)), dma((layers,)), dma((layers,)), dma((layers,)),
            ] + [dma((layers,))] * 10,
            compiler_params=pltpu.CompilerParams(
                collective_id=0, has_side_effects=True, vmem_limit_bytes=67_043_328),
        )(hidden_in[0], lengths, cos, sin, gains, by_rows(w_query), by_rows(w_key), by_rows(w_value),
          w_out.reshape(layers, heads * hd, d_model), units_first(w_gate), units_first(w_up), w_down)
        return out[None]

    seq_part = P(None, 'tp', None)
    in_specs = (seq_part, P(), P(), P(), P(), P(), P(), P(), P(None, None, 'tp'), P(None, None, 'tp'), P(None, 'tp', None), P())
    return jax.shard_map(device_fn, mesh=mesh, in_specs=in_specs, out_specs=seq_part, check_vma=False)
```

```python
import functools

import jax
import jax.numpy as jnp
import numpy as np
from jax import lax
from jax.experimental import pallas as pl
from jax.experimental.pallas import tpu as pltpu
from jax.sharding import PartitionSpec as P

NORM_EPS = 1e-5
ROPE_BASE = 500000.0
NX = 4
PLANE = NX * NX
LANES = 128
CHUNK = 256
NT = (((1,), (1,)), ((), ()))
F32, BF16 = jnp.float32, jnp.bfloat16


def remote(src, dst, send_sem, recv_sem, device):
    return pltpu.make_async_remote_copy(
        src_ref=src, dst_ref=dst, send_sem=send_sem, recv_sem=recv_sem,
        device_id=(device,), device_id_type=pl.DeviceIdType.MESH)


def scoped(f):
    @functools.wraps(f)
    def wrapped(*args):
        with jax.named_scope(f.__name__ + ('#l=%d' % args[0])):
            return f(*args)
    return wrapped


def kernel(nz, h_ref, len_ref, rope_ref, ga_ref, gm_ref, gf_ref, wq_ref, wk_ref, wv_ref, wo_ref, wg_ref, wu_ref, wd_ref,
           out_ref, w_all, wo_v, wqkv, h_all, c_mat, kv_all, rs, ps, hres, zb, qbuf, bd, rope, cos_t, sin_t, ga, gm, gf, len_s,
           local_sem, in_sem, w_recv, w_send, d_recv, d_send, h_recv, h_send, kv_recv, kv_send, kvd_recv, kvd_send,
           c_recv, c_send, rs_recv, rs_send):
    layers = wo_ref.shape[0]
    seq_dev, d_model = h_ref.shape
    units = wg_ref.shape[1]
    pack = 3 * units
    half = pack // 2
    rows = nz * seq_dev
    hq = wq_ref.shape[1] // nz
    hd = wk_ref.shape[1] // nz
    nch = d_model // CHUNK
    me = lax.axis_index('tp')
    core = me % 2
    px = (me // 2) % NX
    py = (me // (2 * NX)) % NX
    mp = (me // 2) % PLANE
    mz = me // (2 * PLANE)
    base = mz * (2 * PLANE)
    partner = base + mp * 2 + (1 - core)

    def z_peer(i):
        return ((mz + i) % nz) * (2 * PLANE) + mp * 2 + core

    far_z = sorted(range(1, nz), key=lambda i: -min(i, nz - i))

    def plane_peer(dy, dx):
        return base + ((py + dy) % NX * NX + (px + dx) % NX) * 2 + core

    far_plane = sorted(((dy, dx) for dy in range(NX) for dx in range(NX) if dy or dx),
                       key=lambda d: -sum(min(i, NX - i) for i in d))

    barrier = pltpu.get_barrier_semaphore()

    def signal(device):
        pl.semaphore_signal(barrier, inc=1, device_id=(device,), device_id_type=pl.DeviceIdType.MESH)

    for i in far_z:
        signal(z_peer(i))
    for d in far_plane:
        signal(plane_peer(*d))
    signal(partner)

    def pack_copies(l):
        mine = w_all.at[l, core, mp]
        return [pltpu.make_async_copy(ref.at[l], mine.at[pl.ds(i * units, units)], local_sem.at[l, i])
                for i, ref in enumerate((wg_ref, wu_ref, wd_ref))]

    def qkv_copies(l):
        return [
            pltpu.make_async_copy(wq_ref.at[l, pl.ds(mz * hq, hq)], wqkv.at[l, pl.ds(0, hq)], local_sem.at[l, 3]),
            pltpu.make_async_copy(wk_ref.at[l, pl.ds(mz * hd, hd)], wqkv.at[l, pl.ds(hq, hd)], local_sem.at[l, 4]),
            pltpu.make_async_copy(wv_ref.at[l, pl.ds(mz * hd, hd)], wqkv.at[l, pl.ds(hq + hd, hd)], local_sem.at[l, 5]),
        ]

    def wo_copy(l):
        return pltpu.make_async_copy(wo_ref.at[l], wo_v.at[l], local_sem.at[l, 6])

    small = [pltpu.make_async_copy(src, dst, in_sem.at[i]) for i, (src, dst) in enumerate((
        (h_ref, h_all.at[0, mz]), (rope_ref.at[mp * 2 + core], rope), (ga_ref, ga), (gm_ref, gm), (gf_ref, gf), (len_ref, len_s)))]
    for c in small:
        c.start()
    for l in range(layers):
        for c in pack_copies(l) + qkv_copies(l):
            c.start()
        wo_copy(l).start()

    def barrier_wait():
        pl.semaphore_wait(barrier, 1 + (nz - 1) + (PLANE - 1))

    def slot(h, a1, a2):
        return a2 % NX * NX + a1 % NX if h == 0 else a1 % NX * NX + a2 % NX

    def where_am_i(h):
        return (px, py) if h == 0 else (py, px)

    def at(h, a1, a2):
        return base + slot(h, a1, a2) * 2 + core

    third = half // 3
    SPAN = ((0, half), (half, half))
    FROM_MINUS = ((0, 2 * third), (half, third))
    FROM_PLUS = ((2 * third, third), (half + third, 2 * third))

    def piece(l, c, p, span):
        return w_all.at[l, c, p, pl.ds(*span)]

    def w_copy(l, h, p, span, idx, device):
        ref = piece(l, core, p, span)
        return remote(ref, ref, w_send.at[l], w_recv.at[l, h, idx], device)

    def to_partner(l, p, span):
        ref = piece(l, core, p, span)
        remote(ref, ref, d_send.at[l], d_recv.at[l], partner).start()

    @scoped
    def p1(l):
        for c in pack_copies(l):
            c.wait()
        for h in range(2):
            a1, a2 = where_am_i(h)
            w_copy(l, h, mp, SPAN[h], 0, at(h, a1 + 1, a2)).start()
            w_copy(l, h, mp, SPAN[h], 1, at(h, a1 + NX - 1, a2)).start()
        to_partner(l, mp, (0, pack))

    @scoped
    def p2(l):
        for h in range(2):
            a1, a2 = where_am_i(h)
            low, high = slot(h, a1 + NX - 1, a2), slot(h, a1 + 1, a2)
            w_copy(l, h, low, SPAN[h], 0, me).wait_recv()
            w_copy(l, h, low, FROM_MINUS[h], 2, at(h, a1 + 1, a2)).start()
            w_copy(l, h, high, SPAN[h], 1, me).wait_recv()
            w_copy(l, h, high, FROM_PLUS[h], 3, at(h, a1 + NX - 1, a2)).start()
            to_partner(l, low, SPAN[h])
            to_partner(l, high, SPAN[h])

    @scoped
    def p3(l, ks):
        for k in ks:
            for h in range(2):
                a1, a2 = where_am_i(h)
                p = slot(h, a1 + k, a2)
                if k == 2:
                    w_copy(l, h, p, FROM_MINUS[h], 2, me).wait_recv()
                    w_copy(l, h, p, FROM_PLUS[h], 3, me).wait_recv()
                    to_partner(l, p, SPAN[h])
                w_copy(l, h, p, SPAN[h], 4 + k, at(h, a1, a2 + 1)).start()
                w_copy(l, h, p, SPAN[h], 8 + k, at(h, a1, a2 + NX - 1)).start()

    @scoped
    def p4(l, ks):
        for k in ks:
            for h in range(2):
                a1, a2 = where_am_i(h)
                low, high = slot(h, a1 + k, a2 + NX - 1), slot(h, a1 + k, a2 + 1)
                w_copy(l, h, low, SPAN[h], 4 + k, me).wait_recv()
                w_copy(l, h, low, FROM_MINUS[h], 12 + k, at(h, a1, a2 + 1)).start()
                w_copy(l, h, high, SPAN[h], 8 + k, me).wait_recv()
                w_copy(l, h, high, FROM_PLUS[h], 16 + k, at(h, a1, a2 + NX - 1)).start()
                to_partner(l, low, SPAN[h])
                to_partner(l, high, SPAN[h])

    @scoped
    def p5(l):
        for k in (0, 1, 3, 2):
            for h in range(2):
                a1, a2 = where_am_i(h)
                p = slot(h, a1 + k, a2 + 2)
                w_copy(l, h, p, FROM_MINUS[h], 12 + k, me).wait_recv()
                w_copy(l, h, p, FROM_PLUS[h], 16 + k, me).wait_recv()
                to_partner(l, p, SPAN[h])

    @scoped
    def w_done(l):
        ref = w_all.at[l, 1 - core]
        remote(ref, ref, d_send.at[l], d_recv.at[l], partner).wait_recv()

    def h_copy(l, device):
        ref = h_all.at[l, mz]
        return remote(ref, ref, h_send.at[l], h_recv.at[l], device)

    @scoped
    def h_start(l):
        for i in far_z:
            h_copy(l, z_peer(i)).start()

    @scoped
    def h_wait(l):
        if nz > 1:
            ref = h_all.at[l, pl.ds(0, nz - 1)]
            with jax.named_scope('h_recv'):
                remote(ref, ref, h_send.at[l], h_recv.at[l], me).wait_recv()
        for i in range(nz):
            hres[pl.ds(i * seq_dev, seq_dev)] = h_all[l, i].astype(F32)

    @scoped
    def norm_to_zb(l, gains):
        gain = gains[...].astype(F32)[l:l + 1]
        step = min(16, rows)

        @pl.loop(0, rows // step)
        def _(i):
            r = pl.ds(pl.multiple_of(i * step, step), step)
            x = hres[r]
            inv = lax.rsqrt(jnp.mean(x * x, axis=-1, keepdims=True) + NORM_EPS)
            zb[r] = (x * inv * gain).astype(BF16)

    lane = lax.broadcasted_iota(jnp.int32, (rows, LANES), 1)
    low_half = lane < hd

    def rotate(x):
        first = (lane % hd) < hd // 2
        swapped = jnp.where(first, pltpu.roll(x, LANES - hd // 2, 1), pltpu.roll(x, hd // 2, 1))
        return x * cos_t[...] + swapped * sin_t[...]

    def rope_tables():
        first = (lane % hd) < hd // 2
        t = rope[...]
        cos_t[...] = jnp.where(first, t, pltpu.roll(t, hd // 2, 1))
        sin_t[...] = jnp.where(first, -pltpu.roll(t, LANES - hd // 2, 1), t)

    def kv_copy(l, device):
        ref = kv_all.at[l, core, mp]
        return remote(ref, ref, kv_send.at[l], kv_recv.at[l], device)

    @scoped
    def qkv(l):
        for c in qkv_copies(l):
            c.wait()
        proj = lax.dot_general(zb[...], wqkv[l], NT, preferred_element_type=F32)
        kv = proj[:, hq:hq + 2 * hd]
        kv_all[l, core, mp] = jnp.where(low_half, rotate(kv), kv).astype(BF16)

        for d in far_plane:
            kv_copy(l, plane_peer(*d)).start()

        for j in range(hq // LANES):
            q = rotate(proj[:, j * LANES:(j + 1) * LANES])
            qbuf[2 * j] = jnp.where(low_half, q, 0.0).astype(BF16)
            qbuf[2 * j + 1] = jnp.where(low_half, pltpu.roll(q, LANES - hd, 1), 0.0).astype(BF16)

    @scoped
    def kv_wait(l):
        ref = kv_all.at[l, core, pl.ds(0, PLANE - 1)]
        remote(ref, ref, kv_send.at[l], kv_recv.at[l], me).wait_recv()
        ref = kv_all.at[l, core]
        remote(ref, ref, kvd_send.at[l], kvd_recv.at[l], partner).start()
        ref = kv_all.at[l, 1 - core]
        remote(ref, ref, kvd_send.at[l], kvd_recv.at[l], partner).wait_recv()

    def c_columns(j):
        return pl.ds(pl.multiple_of(mz * hq + j * LANES, LANES), LANES)

    @scoped
    def attention(l):
        keys = 2 * PLANE * rows
        j = lax.broadcasted_iota(jnp.int32, (1, keys), 1)
        key_pos = ((j // seq_dev) % nz) * (2 * PLANE * seq_dev) + ((j // rows) % PLANE) * (2 * seq_dev) \
            + (j // (PLANE * rows)) * seq_dev + j % seq_dev
        i = lax.broadcasted_iota(jnp.int32, (rows, 1), 0)
        q_pos = (i // seq_dev) * (2 * PLANE * seq_dev) + (mp * 2 + core) * seq_dev + i % seq_dev
        allowed = key_pos <= jnp.minimum(q_pos, len_s[0] - 1)
        for pair in range(hq // LANES):
            outs = []
            for head in (2 * pair, 2 * pair + 1):
                kv = kv_all[l].reshape(keys, LANES)
                s = lax.dot_general(qbuf[head], kv, NT, preferred_element_type=F32) * (hd ** -0.5)
                s = jnp.where(allowed, s, -1e30)
                e = jnp.exp(s - jnp.max(s, axis=-1, keepdims=True))
                p = (e * (1.0 / jnp.sum(e, axis=-1, keepdims=True))).astype(BF16)
                outs.append(jnp.dot(p, kv, preferred_element_type=F32))
            c = jnp.where(low_half, pltpu.roll(outs[0], LANES - hd, 1), outs[1]).astype(BF16)
            c_mat[l, :, c_columns(pair)] = c
            ref = c_mat.at[l, :, c_columns(pair)]
            for i in far_z:
                remote(ref, ref, c_send.at[l], c_recv.at[l], z_peer(i)).start()

    @scoped
    def out_proj(l):
        if nz > 1:
            ref = c_mat.at[l, :, pl.ds(0, (nz - 1) * hq)]
            with jax.named_scope('c_wait'):
                remote(ref, ref, c_send.at[l], c_recv.at[l], me).wait_recv()
        with jax.named_scope('wo_wait'):
            wo_copy(l).wait()

        @pl.loop(0, nch)
        def _(n):
            cols = pl.ds(pl.multiple_of(n * CHUNK, CHUNK), CHUNK)
            acc = jnp.dot(c_mat[l], wo_v[l, :, cols], preferred_element_type=F32)
            hres[:, cols] = (hres[:, cols] + acc).astype(BF16).astype(F32)

    group = CHUNK // units
    n_groups = 2 * PLANE // group

    def slab(l, g, first, cols):
        per = PLANE // group
        return w_all[l, g // per, pl.ds((g % per) * group, group), pl.ds(first, units), cols]

    @scoped
    def mlp_units(l):
        block = lax.broadcasted_iota(jnp.int32, (rows, CHUNK), 1) // units

        @pl.loop(0, n_groups)
        def _(g):
            every = pl.ds(0, d_model)
            gate = lax.dot_general(zb[...], slab(l, g, 0, every).reshape(CHUNK, d_model), NT, preferred_element_type=F32)
            up = lax.dot_general(zb[...], slab(l, g, units, every).reshape(CHUNK, d_model), NT, preferred_element_type=F32)
            act = gate * (1.0 / (1.0 + jnp.exp(-gate))) * up
            for b in range(group):
                bd[g, pl.ds(b * rows, rows)] = jnp.where(block == b, act, 0.0).astype(BF16)

    def rs_copy(l, n, i):
        return remote(ps.at[l, n, (mz + i) % nz], rs.at[l, mz, n], rs_send.at[l], rs_recv.at[l], z_peer(i))

    @scoped
    def mlp_down(l):
        @pl.loop(0, nch)
        def _(n):
            cols = pl.ds(pl.multiple_of(n * CHUNK, CHUNK), CHUNK)
            acc = jnp.zeros((rows, CHUNK), F32)
            for g in range(n_groups):
                y = jnp.dot(bd[g], slab(l, g, 2 * units, cols).reshape(CHUNK, CHUNK), preferred_element_type=F32)
                y = y.astype(BF16).astype(F32)
                for b in range(group):
                    acc = acc + y[b * rows:(b + 1) * rows]
            ps[l, n] = acc.reshape(nz, seq_dev, CHUNK)
            for i in far_z:
                rs_copy(l, n, i).start()

    @scoped
    def rs_finish(l, store):
        if nz > 1:
            ref = rs.at[l, pl.ds(0, nz - 1)]
            with jax.named_scope('rs_wait'):
                remote(ref, ref, rs_send.at[l], rs_recv.at[l], me).wait_recv()
        mine = pl.ds(pl.multiple_of(mz * seq_dev, seq_dev), seq_dev)
        for n in range(nch):
            rs[l, mz, n] = ps[l, n, mz]
        for n in range(nch):
            total = rs[l, 0, n]
            for i in range(1, nz):
                total = total + rs[l, i, n]
            cols = pl.ds(n * CHUNK, CHUNK)
            store(cols, (hres[mine, cols] + total).astype(BF16))

    def store_next(l):
        def store(cols, x):
            h_all[l + 1, mz, :, cols] = x
        return store

    with jax.named_scope('small'):
        for c in small:
            c.wait()
        rope_tables()
    with jax.named_scope('barrier'):
        barrier_wait()
    h_start(0)
    p1(0)
    p3(0, (0,))
    p2(0)
    for l in range(layers):
        more = l + 1 < layers
        h_wait(l)
        norm_to_zb(l, ga)
        qkv(l)
        if l == 0:
            p3(0, (1, 3, 2))
            p4(0, (0,))
        else:
            p5(l)
        kv_wait(l)
        attention(l)
        if l == 0:
            p4(0, (1, 3, 2))
        if more:
            p1(l + 1)
            p3(l + 1, (0,))
        out_proj(l)
        norm_to_zb(l, gm)
        if l == 0:
            p5(l)
        w_done(l)
        mlp_units(l)
        if more:
            p2(l + 1)
            p3(l + 1, (1, 3))
        mlp_down(l)
        if more:
            p3(l + 1, (2,))
            p4(l + 1, (0,))
            rs_finish(l, store_next(l))
            h_start(l + 1)
            p4(l + 1, (1, 3, 2))
    pieces = []
    rs_finish(layers - 1, lambda cols, x: pieces.append(x.astype(F32)))
    x = jnp.concatenate(pieces, axis=1)
    inv = lax.rsqrt(jnp.mean(x * x, axis=-1, keepdims=True) + NORM_EPS)
    gain = gf[...].astype(F32)
    for i in range(d_model // LANES):
        cols = slice(i * LANES, (i + 1) * LANES)
        out_ref[:, cols] = x[:, cols] * inv * gain[i:i + 1]

    with jax.named_scope('drain'):
      for l in range(layers):
          ref = w_all.at[l, 0, pl.ds(0, PLANE - 1)]
          remote(ref, ref, w_send.at[l], w_recv.at[l, 0, 0], me).wait_send()
          ref = w_all.at[l, 0]
          remote(ref, ref, d_send.at[l], d_recv.at[l], me).wait_send()
          ref = kv_all.at[l, 0, pl.ds(0, PLANE - 1)]
          remote(ref, ref, kv_send.at[l], kv_recv.at[l], me).wait_send()
          ref = kv_all.at[l, 0]
          remote(ref, ref, kvd_send.at[l], kvd_recv.at[l], me).wait_send()
          if nz > 1:
              ref = h_all.at[l, pl.ds(0, nz - 1)]
              remote(ref, ref, h_send.at[l], h_recv.at[l], me).wait_send()
              ref = c_mat.at[l, :, pl.ds(0, (nz - 1) * hq)]
              remote(ref, ref, c_send.at[l], c_recv.at[l], me).wait_send()
              ref = rs.at[l, pl.ds(0, nz - 1)]
              remote(ref, ref, rs_send.at[l], rs_recv.at[l], me).wait_send()


def solution(mesh):
    nz = mesh.shape['tp'] // (2 * PLANE)

    def device_fn(hidden_in, lengths, attn_norm, w_query, w_key, w_value, w_out, mlp_norm, w_gate, w_up, w_down, final_norm):
        seq_dev, d_model = hidden_in.shape[1:]
        layers, _, heads, hd = w_query.shape
        kv_heads = w_key.shape[2]
        units = w_gate.shape[2]
        assert kv_heads == nz and 2 * hd == LANES and heads % nz == 0
        hq = heads // nz * hd
        rows = nz * seq_dev
        nch = d_model // CHUNK
        n_groups = 2 * PLANE * units // CHUNK
        dev, row = np.arange(2 * PLANE)[:, None], np.arange(rows)[None, :]
        pos = (row // seq_dev) * (2 * PLANE * seq_dev) + dev * seq_dev + row % seq_dev
        freq = np.float32(ROPE_BASE) ** (np.float32(-2.0) * np.arange(hd // 2, dtype=np.float32) / np.float32(hd))
        angles = (pos[..., None].astype(np.float32) * freq).astype(np.float64)
        rope = np.tile(np.concatenate([np.cos(angles), np.sin(angles)], axis=-1), (1, 1, 2)).astype(np.float32)
        by_rows = lambda w: jnp.transpose(w, (0, 2, 3, 1)).reshape(layers, -1, d_model)
        units_first = lambda w: jnp.transpose(w, (0, 2, 1))
        hbm, vmem = (pl.BlockSpec(memory_space=s) for s in (pltpu.HBM, pltpu.VMEM))
        dma = pltpu.SemaphoreType.DMA
        out = pl.pallas_call(
            functools.partial(kernel, nz),
            name='decoder',
            out_shape=jax.ShapeDtypeStruct((seq_dev, d_model), F32),
            in_specs=[hbm] * 13,
            out_specs=vmem,
            scratch_shapes=[
                pltpu.VMEM((layers, 2, PLANE, 3 * units, d_model), BF16),
                pltpu.VMEM((layers, heads * hd, d_model), BF16),
                pltpu.VMEM((layers, hq + 2 * hd, d_model), BF16),
                pltpu.VMEM((layers, nz, seq_dev, d_model), BF16),
                pltpu.VMEM((layers, rows, heads * hd), BF16),
                pltpu.VMEM((layers, 2, PLANE, rows, LANES), BF16),
                pltpu.VMEM((layers, nz, nch, seq_dev, CHUNK), F32),
                pltpu.VMEM((layers, nch, nz, seq_dev, CHUNK), F32),
                pltpu.VMEM((rows, d_model), F32),
                pltpu.VMEM((rows, d_model), BF16),
                pltpu.VMEM((hq // hd, rows, LANES), BF16),
                pltpu.VMEM((n_groups, CHUNK // units * rows, CHUNK), BF16),
                pltpu.VMEM((rows, LANES), F32), pltpu.VMEM((rows, LANES), F32), pltpu.VMEM((rows, LANES), F32),
                pltpu.VMEM((layers, d_model), BF16), pltpu.VMEM((layers, d_model), BF16),
                pltpu.VMEM((d_model // LANES, LANES), BF16),
                pltpu.SMEM((1,), jnp.int32),
                dma((layers, 7)), dma((6,)), dma((layers, 2, 20)), dma((layers,)), dma((layers,)), dma((layers,)),
            ] + [dma((layers,))] * 10,
            compiler_params=pltpu.CompilerParams(
                collective_id=0, has_side_effects=True, vmem_limit_bytes=67_043_328),
        )(hidden_in[0], lengths, jnp.asarray(rope), attn_norm, mlp_norm, final_norm.reshape(-1, LANES), by_rows(w_query), by_rows(w_key), by_rows(w_value),
          w_out.reshape(layers, heads * hd, d_model), units_first(w_gate), units_first(w_up), w_down)
        return out.astype(BF16)[None]

    seq_part = P(None, 'tp', None)
    in_specs = (seq_part, P(), P(), P(), P(), P(), P(), P(), P(None, None, 'tp'), P(None, None, 'tp'), P(None, 'tp', None), P())
    return jax.shard_map(device_fn, mesh=mesh, in_specs=in_specs, out_specs=seq_part, check_vma=False)
```

```python
import functools

import jax
import jax.numpy as jnp
import numpy as np
from jax import lax
from jax.experimental import pallas as pl
from jax.experimental.pallas import tpu as pltpu
from jax.sharding import PartitionSpec as P

NORM_EPS = 1e-5
ROPE_BASE = 500000.0
NX = 4
PLANE = NX * NX
LANES = 128
CHUNK = 256
NT = (((1,), (1,)), ((), ()))
F32, BF16 = jnp.float32, jnp.bfloat16


def remote(src, dst, send_sem, recv_sem, device):
    return pltpu.make_async_remote_copy(
        src_ref=src, dst_ref=dst, send_sem=send_sem, recv_sem=recv_sem,
        device_id=(device,), device_id_type=pl.DeviceIdType.MESH)


def scoped(f):
    @functools.wraps(f)
    def wrapped(*args):
        with jax.named_scope(f.__name__ + ('#l=%d' % args[0])):
            return f(*args)
    return wrapped


def kernel(nz, h_ref, len_ref, rope_ref, ga_ref, gm_ref, gf_ref, wq_ref, wk_ref, wv_ref, wo_ref, wg_ref, wu_ref, wd_ref,
           out_ref, w_all, wo_v, wqkv, h_all, c_mat, kv_all, rs, ra, sb, ps, acc, hres, zb, qbuf, bd, rope, cos_t, sin_t, ga, gm, gf, len_s,
           local_sem, in_sem, w_recv, w_send, d_recv, d_send, h_recv, h_send, kv_recv, kv_send, kvd_recv, kvd_send,
           c_recv, c_send, rs_recv, ra_recv, rs_send):
    layers = wo_ref.shape[0]
    seq_dev, d_model = h_ref.shape
    units = wg_ref.shape[1]
    pack = 3 * units
    half = pack // 2
    rows = nz * seq_dev
    hq = wq_ref.shape[1] // nz
    hd = wk_ref.shape[1] // nz
    nch = d_model // CHUNK
    me = lax.axis_index('tp')
    core = me % 2
    px = (me // 2) % NX
    py = (me // (2 * NX)) % NX
    mp = (me // 2) % PLANE
    mz = me // (2 * PLANE)
    base = mz * (2 * PLANE)
    partner = base + mp * 2 + (1 - core)

    def z_peer(i):
        return ((mz + i) % nz) * (2 * PLANE) + mp * 2 + core

    far_z = sorted(range(1, nz), key=lambda i: -min(i, nz - i))
    near_z = far_z[::-1]

    def plane_peer(dy, dx):
        return base + ((py + dy) % NX * NX + (px + dx) % NX) * 2 + core

    far_plane = sorted(((dy, dx) for dy in range(NX) for dx in range(NX) if dy or dx),
                       key=lambda d: -sum(min(i, NX - i) for i in d))

    barrier = pltpu.get_barrier_semaphore()

    def signal(device):
        pl.semaphore_signal(barrier, inc=1, device_id=(device,), device_id_type=pl.DeviceIdType.MESH)

    for i in far_z:
        signal(z_peer(i))
    for d in far_plane:
        signal(plane_peer(*d))
    signal(partner)

    def pack_copies(l):
        mine = w_all.at[l, core, mp]
        return [pltpu.make_async_copy(ref.at[l], mine.at[pl.ds(i * units, units)], local_sem.at[l, i])
                for i, ref in enumerate((wg_ref, wu_ref, wd_ref))]

    def qkv_copies(l):
        return [
            pltpu.make_async_copy(wq_ref.at[l, pl.ds(mz * hq, hq)], wqkv.at[l, pl.ds(0, hq)], local_sem.at[l, 3]),
            pltpu.make_async_copy(wk_ref.at[l, pl.ds(mz * hd, hd)], wqkv.at[l, pl.ds(hq, hd)], local_sem.at[l, 4]),
            pltpu.make_async_copy(wv_ref.at[l, pl.ds(mz * hd, hd)], wqkv.at[l, pl.ds(hq + hd, hd)], local_sem.at[l, 5]),
        ]

    def wo_copy(l):
        return pltpu.make_async_copy(wo_ref.at[l], wo_v.at[l], local_sem.at[l, 6])

    small = [pltpu.make_async_copy(src, dst, in_sem.at[i]) for i, (src, dst) in enumerate((
        (h_ref, h_all.at[0, mz]), (rope_ref.at[mp * 2 + core], rope), (ga_ref, ga), (gm_ref, gm), (gf_ref, gf), (len_ref, len_s)))]
    for c in small:
        c.start()
    for c in pack_copies(0) + qkv_copies(0):
        c.start()

    def start_later_copies():
        wo_copy(0).start()
        for l in range(1, layers):
            for c in pack_copies(l) + qkv_copies(l):
                c.start()
            wo_copy(l).start()

    def barrier_wait():
        pl.semaphore_wait(barrier, 1 + (nz - 1) + (PLANE - 1))

    def slot(h, a1, a2):
        return a2 % NX * NX + a1 % NX if h == 0 else a1 % NX * NX + a2 % NX

    def where_am_i(h):
        return (px, py) if h == 0 else (py, px)

    def at(h, a1, a2):
        return base + slot(h, a1, a2) * 2 + core

    third = half // 3
    SPAN = ((0, half), (half, half))
    FROM_MINUS = ((0, 2 * third), (half, third))
    FROM_PLUS = ((2 * third, third), (half + third, 2 * third))

    def piece(l, c, p, span):
        return w_all.at[l, c, p, pl.ds(*span)]

    def w_copy(l, h, p, span, idx, device):
        ref = piece(l, core, p, span)
        return remote(ref, ref, w_send.at[l], w_recv.at[l, h, idx], device)

    GROUPS = (((0, 0), (1, 0), (3, 0), (0, 1)), ((0, 3), (2, 0), (0, 2), (1, 1)),
              ((1, 3), (3, 1), (3, 3), (2, 1)), ((2, 3), (1, 2), (3, 2), (2, 2)))
    GROUP_OF = {d: g for g, ds in enumerate(GROUPS) for d in ds}

    def to_partner(l, h, k1, k2, span):
        a1, a2 = where_am_i(h)
        ref = piece(l, core, slot(h, a1 + k1, a2 + k2), span)
        g = GROUP_OF[(k1, k2) if h == 0 else (k2, k1)]
        remote(ref, ref, d_send.at[l], d_recv.at[l, g], partner).start()

    @scoped
    def p1(l):
        for c in pack_copies(l):
            c.wait()
        for h in range(2):
            a1, a2 = where_am_i(h)
            w_copy(l, h, mp, SPAN[h], 0, at(h, a1 + 1, a2)).start()
            w_copy(l, h, mp, SPAN[h], 1, at(h, a1 + NX - 1, a2)).start()
        to_partner(l, 0, 0, 0, (0, pack))

    @scoped
    def p2(l):
        for h in range(2):
            a1, a2 = where_am_i(h)
            low, high = slot(h, a1 + NX - 1, a2), slot(h, a1 + 1, a2)
            w_copy(l, h, low, SPAN[h], 0, me).wait_recv()
            w_copy(l, h, low, FROM_MINUS[h], 2, at(h, a1 + 1, a2)).start()
            w_copy(l, h, high, SPAN[h], 1, me).wait_recv()
            w_copy(l, h, high, FROM_PLUS[h], 3, at(h, a1 + NX - 1, a2)).start()
            to_partner(l, h, NX - 1, 0, SPAN[h])
            to_partner(l, h, 1, 0, SPAN[h])

    @scoped
    def p3(l, ks):
        for k in ks:
            for h in range(2):
                a1, a2 = where_am_i(h)
                p = slot(h, a1 + k, a2)
                if k == 2:
                    w_copy(l, h, p, FROM_MINUS[h], 2, me).wait_recv()
                    w_copy(l, h, p, FROM_PLUS[h], 3, me).wait_recv()
                    to_partner(l, h, k, 0, SPAN[h])
                w_copy(l, h, p, SPAN[h], 4 + k, at(h, a1, a2 + 1)).start()
                w_copy(l, h, p, SPAN[h], 8 + k, at(h, a1, a2 + NX - 1)).start()

    @scoped
    def p4(l, ks):
        for k in ks:
            for h in range(2):
                a1, a2 = where_am_i(h)
                low, high = slot(h, a1 + k, a2 + NX - 1), slot(h, a1 + k, a2 + 1)
                w_copy(l, h, low, SPAN[h], 4 + k, me).wait_recv()
                w_copy(l, h, low, FROM_MINUS[h], 12 + k, at(h, a1, a2 + 1)).start()
                w_copy(l, h, high, SPAN[h], 8 + k, me).wait_recv()
                w_copy(l, h, high, FROM_PLUS[h], 16 + k, at(h, a1, a2 + NX - 1)).start()
                to_partner(l, h, k, NX - 1, SPAN[h])
                to_partner(l, h, k, 1, SPAN[h])

    @scoped
    def p5(l, ks):
        for k in ks:
            for h in range(2):
                a1, a2 = where_am_i(h)
                p = slot(h, a1 + k, a2 + 2)
                w_copy(l, h, p, FROM_MINUS[h], 12 + k, me).wait_recv()
                w_copy(l, h, p, FROM_PLUS[h], 16 + k, me).wait_recv()
                to_partner(l, h, k, 2, SPAN[h])

    @scoped
    def w_done(l, gs):
        for g in gs:
            ref = w_all.at[l, 1 - core, pl.ds(0, len(GROUPS[g]))]
            remote(ref, ref, d_send.at[l], d_recv.at[l, g], partner).wait_recv()

    def h_copy(l, first, size, device):
        ref = h_all.at[l, mz, :, pl.ds(first, size)]
        return remote(ref, ref, h_send.at[l], h_recv.at[l], device)

    def h_start(l, first, size):
        for i in far_z:
            h_copy(l, first, size, z_peer(i)).start()

    @scoped
    def h_wait(l):
        if nz > 1:
            ref = h_all.at[l, pl.ds(0, nz - 1)]
            with jax.named_scope('h_recv'):
                remote(ref, ref, h_send.at[l], h_recv.at[l], me).wait_recv()
        for i in range(nz):
            hres[pl.ds(i * seq_dev, seq_dev)] = h_all[l, i].astype(F32)

    @scoped
    def norm_to_zb(l, gains):
        gain = gains[...].astype(F32)[l:l + 1]
        step = min(16, rows)

        @pl.loop(0, rows // step)
        def _(i):
            r = pl.ds(pl.multiple_of(i * step, step), step)
            x = hres[r]
            inv = lax.rsqrt(jnp.mean(x * x, axis=-1, keepdims=True) + NORM_EPS)
            zb[r] = (x * inv * gain).astype(BF16)

    lane = lax.broadcasted_iota(jnp.int32, (rows, LANES), 1)
    low_half = lane < hd

    def rotate(x):
        first = (lane % hd) < hd // 2
        swapped = jnp.where(first, pltpu.roll(x, LANES - hd // 2, 1), pltpu.roll(x, hd // 2, 1))
        return x * cos_t[...] + swapped * sin_t[...]

    def rope_tables():
        first = (lane % hd) < hd // 2
        t = rope[...]
        cos_t[...] = jnp.where(first, t, pltpu.roll(t, hd // 2, 1))
        sin_t[...] = jnp.where(first, -pltpu.roll(t, LANES - hd // 2, 1), t)

    def kv_copy(l, device):
        ref = kv_all.at[l, core, mp]
        return remote(ref, ref, kv_send.at[l], kv_recv.at[l], device)

    @scoped
    def qkv(l):
        for c in qkv_copies(l):
            c.wait()
        proj = lax.dot_general(zb[...], wqkv[l], NT, preferred_element_type=F32)
        kv = proj[:, hq:hq + 2 * hd]
        kv_all[l, core, mp] = jnp.where(low_half, rotate(kv), kv).astype(BF16)

        for d in far_plane:
            kv_copy(l, plane_peer(*d)).start()

        for j in range(hq // LANES):
            q = rotate(proj[:, j * LANES:(j + 1) * LANES]) * (hd ** -0.5)
            qbuf[2 * j] = jnp.where(low_half, q, 0.0).astype(BF16)
            qbuf[2 * j + 1] = jnp.where(low_half, pltpu.roll(q, LANES - hd, 1), 0.0).astype(BF16)

    @scoped
    def kv_wait(l):
        ref = kv_all.at[l, core, pl.ds(0, PLANE - 1)]
        remote(ref, ref, kv_send.at[l], kv_recv.at[l], me).wait_recv()
        ref = kv_all.at[l, core]
        remote(ref, ref, kvd_send.at[l], kvd_recv.at[l], partner).start()
        ref = kv_all.at[l, 1 - core]
        remote(ref, ref, kvd_send.at[l], kvd_recv.at[l], partner).wait_recv()

    def c_columns(j):
        return pl.ds(pl.multiple_of(mz * hq + j * LANES, LANES), LANES)

    @scoped
    def attention(l):
        keys = 2 * PLANE * rows
        j = lax.broadcasted_iota(jnp.int32, (1, keys), 1)
        key_pos = ((j // seq_dev) % nz) * (2 * PLANE * seq_dev) + ((j // rows) % PLANE) * (2 * seq_dev) \
            + (j // (PLANE * rows)) * seq_dev + j % seq_dev
        i = lax.broadcasted_iota(jnp.int32, (rows, 1), 0)
        q_pos = (i // seq_dev) * (2 * PLANE * seq_dev) + (mp * 2 + core) * seq_dev + i % seq_dev
        allowed = key_pos <= jnp.minimum(q_pos, len_s[0] - 1)
        for pair in range(hq // LANES):
            outs = []
            for head in (2 * pair, 2 * pair + 1):
                kv = kv_all[l].reshape(keys, LANES)
                s = lax.dot_general(qbuf[head], kv, NT, preferred_element_type=F32)
                s = jnp.where(allowed, s, -1e30)
                e = jnp.exp(s - jnp.max(s, axis=-1, keepdims=True))
                p = (e * (1.0 / jnp.sum(e, axis=-1, keepdims=True))).astype(BF16)
                outs.append(jnp.dot(p, kv, preferred_element_type=F32))
            c = jnp.where(low_half, pltpu.roll(outs[0], LANES - hd, 1), outs[1]).astype(BF16)
            c_mat[l, :, c_columns(pair)] = c
            ref = c_mat.at[l, :, c_columns(pair)]
            for i in near_z:
                remote(ref, ref, c_send.at[l], c_recv.at[l, i], z_peer(i)).start()

    @scoped
    def out_proj(l):
        with jax.named_scope('wo_wait'):
            wo_copy(l).wait()
        for i in [0] + near_z:
            src = (mz + nz - i) % nz
            cols = pl.ds(pl.multiple_of(src * hq, hq), hq)
            if i:
                ref = c_mat.at[l, :, cols]
                with jax.named_scope('c_wait'):
                    remote(ref, ref, c_send.at[l], c_recv.at[l, i], me).wait_recv()
            part = jnp.dot(c_mat[l, :, cols], wo_v[l, cols, :], preferred_element_type=F32)
            acc[...] = acc[...] + part if i else part
        step = min(16, rows)

        @pl.loop(0, rows // step)
        def _(i):
            r = pl.ds(pl.multiple_of(i * step, step), step)
            hres[r] = (hres[r] + acc[r]).astype(BF16).astype(F32)

    group = CHUNK // units
    n_groups = len(GROUPS)
    assert group == 2 * len(GROUPS[0])

    def slab(l, g, first, cols):
        parts = [w_all[l, c, slot(0, px + dx, py + dy), pl.ds(first, units), cols] for c in range(2) for dx, dy in GROUPS[g]]
        return jnp.concatenate(parts, axis=0)

    @scoped
    def mlp_units(l, gs):
        block = lax.broadcasted_iota(jnp.int32, (rows, CHUNK), 1) // units
        for g in gs:
            every = pl.ds(0, d_model)
            gate = lax.dot_general(zb[...], slab(l, g, 0, every), NT, preferred_element_type=F32)
            up = lax.dot_general(zb[...], slab(l, g, units, every), NT, preferred_element_type=F32)
            act = gate * (1.0 / (1.0 + jnp.exp(-gate))) * up
            for b in range(group):
                bd[g, pl.ds(b * rows, rows)] = jnp.where(block == b, act, 0.0).astype(BF16)

    two_step = nz == 8

    def ps_of(l, n, i):
        return ps.at[l, n, (mz + i + nz) % nz]

    def rs_start(l, n):
        if not two_step:
            for k, i in enumerate(far_z):
                remote(ps_of(l, n, i), rs.at[l, n, k], rs_send.at[l], rs_recv.at[l, n], z_peer(i)).start()
            return
        for side, to in ((0, nz - 2), (1, 2)):
            cols = pl.ds(side * LANES, LANES)
            remote(ps.at[l, n, (mz + 4) % nz, :, cols], ra.at[l, n, 2, :, cols], rs_send.at[l], ra_recv.at[l, n], z_peer(to)).start()
        for side, to in ((0, nz - 1), (1, 1)):
            remote(ps_of(l, n, 3 * (to if to == 1 else -1)), ra.at[l, n, side], rs_send.at[l], ra_recv.at[l, n], z_peer(to)).start()
        for side, to in ((0, nz - 1), (1, 1)):
            remote(ps_of(l, n, to), rs.at[l, n, side], rs_send.at[l], rs_recv.at[l, n], z_peer(to)).start()

    @scoped
    def rs_middle(l):
        if not two_step:
            return

        @pl.loop(0, nch)
        def _(n):
            ref = ra.at[l, n]
            remote(ref, ref, rs_send.at[l], ra_recv.at[l, n], me).wait_recv()
            for side, to in ((0, nz - 2), (1, 2)):
                cols = pl.ds(side * LANES, LANES)
                sb[l, n, side] = ps[l, n, (mz + to) % nz] + ra[l, n, side]
                sb[l, n, side, :, cols] = sb[l, n, side, :, cols] + ra[l, n, 2, :, cols]
                remote(sb.at[l, n, side], rs.at[l, n, 2 + side], rs_send.at[l], rs_recv.at[l, n], z_peer(to)).start()

    @scoped
    def mlp_down(l):
        @pl.loop(0, nch)
        def _(n):
            cols = pl.ds(pl.multiple_of(n * CHUNK, CHUNK), CHUNK)
            total = jnp.zeros((rows, CHUNK), F32)
            for g in range(n_groups):
                y = jnp.dot(bd[g], slab(l, g, 2 * units, cols), preferred_element_type=F32)
                y = y.astype(BF16).astype(F32)
                for b in range(group):
                    total = total + y[b * rows:(b + 1) * rows]
            ps[l, n] = total.reshape(nz, seq_dev, CHUNK)
            rs_start(l, n)

    n_in = 4 if two_step else nz - 1

    @scoped
    def rs_finish(l, store):
        mine = pl.ds(pl.multiple_of(mz * seq_dev, seq_dev), seq_dev)
        for n in range(nch):
            if n_in:
                ref = rs.at[l, n]
                remote(ref, ref, rs_send.at[l], rs_recv.at[l, n], me).wait_recv()
            total = ps[l, n, mz]
            for k in range(n_in):
                total = total + rs[l, n, k]
            store(n, (hres[mine, n * CHUNK:(n + 1) * CHUNK] + total).astype(BF16))

    def store_next(l):
        def store(n, x):
            h_all[l + 1, mz, :, n * CHUNK:(n + 1) * CHUNK] = x
            if n % 2 or nch == 1:
                first = max(n - 1, 0) * CHUNK
                h_start(l + 1, first, (n + 1) * CHUNK - first)
        return store

    with jax.named_scope('small'):
        for c in small:
            c.wait()
        rope_tables()
    with jax.named_scope('barrier'):
        barrier_wait()
    h_start(0, 0, d_model)
    p1(0)
    p3(0, (0,))
    start_later_copies()
    p2(0)
    for l in range(layers):
        more = l + 1 < layers
        h_wait(l)
        norm_to_zb(l, ga)
        qkv(l)
        if l == 0:
            p3(0, (1, 3, 2))
            p4(0, (0,))
        else:
            p5(l, (0, 1, 3, 2))
        kv_wait(l)
        attention(l)
        if l == 0:
            p4(0, (1, 3, 2))
        if more:
            p1(l + 1)
            p3(l + 1, (0,))
        out_proj(l)
        norm_to_zb(l, gm)
        if l == 0:
            w_done(l, (0,))
            mlp_units(l, (0,))
            p5(l, (0,))
            w_done(l, (1,))
            mlp_units(l, (1,))
            p5(l, (1, 3))
            w_done(l, (2,))
            mlp_units(l, (2,))
            p5(l, (2,))
            w_done(l, (3,))
            mlp_units(l, (3,))
        else:
            w_done(l, range(n_groups))
            mlp_units(l, range(n_groups))
        if more:
            p2(l + 1)
            p3(l + 1, (1, 3))
        mlp_down(l)
        rs_middle(l)
        if more:
            rs_finish(l, store_next(l))
            p3(l + 1, (2,))
            p4(l + 1, (0, 1, 3, 2))
    pieces = []
    rs_finish(layers - 1, lambda n, x: pieces.append(x.astype(F32)))
    x = jnp.concatenate(pieces, axis=1)
    inv = lax.rsqrt(jnp.mean(x * x, axis=-1, keepdims=True) + NORM_EPS)
    gain = gf[...].astype(F32)
    for i in range(d_model // LANES):
        cols = slice(i * LANES, (i + 1) * LANES)
        out_ref[:, cols] = x[:, cols] * inv * gain[i:i + 1]

    with jax.named_scope('drain'):
      for l in range(layers):
          ref = w_all.at[l, 0, pl.ds(0, PLANE - 1)]
          remote(ref, ref, w_send.at[l], w_recv.at[l, 0, 0], me).wait_send()
          ref = w_all.at[l, 0]
          remote(ref, ref, d_send.at[l], d_recv.at[l, 0], me).wait_send()
          ref = kv_all.at[l, 0, pl.ds(0, PLANE - 1)]
          remote(ref, ref, kv_send.at[l], kv_recv.at[l], me).wait_send()
          ref = kv_all.at[l, 0]
          remote(ref, ref, kvd_send.at[l], kvd_recv.at[l], me).wait_send()
          if nz > 1:
              ref = h_all.at[l, pl.ds(0, nz - 1)]
              remote(ref, ref, h_send.at[l], h_recv.at[l], me).wait_send()
              ref = c_mat.at[l, :, pl.ds(0, (nz - 1) * hq)]
              remote(ref, ref, c_send.at[l], c_recv.at[l, 0], me).wait_send()
              ref = ps.at[l, :, pl.ds(0, nz - 1)]
              remote(ref, ref, rs_send.at[l], rs_recv.at[l, 0], me).wait_send()


def solution(mesh):
    nz = mesh.shape['tp'] // (2 * PLANE)

    def device_fn(hidden_in, lengths, attn_norm, w_query, w_key, w_value, w_out, mlp_norm, w_gate, w_up, w_down, final_norm):
        seq_dev, d_model = hidden_in.shape[1:]
        layers, _, heads, hd = w_query.shape
        kv_heads = w_key.shape[2]
        units = w_gate.shape[2]
        assert kv_heads == nz and 2 * hd == LANES and heads % nz == 0
        hq = heads // nz * hd
        rows = nz * seq_dev
        nch = d_model // CHUNK
        n_groups = 2 * PLANE * units // CHUNK
        dev, row = np.arange(2 * PLANE)[:, None], np.arange(rows)[None, :]
        pos = (row // seq_dev) * (2 * PLANE * seq_dev) + dev * seq_dev + row % seq_dev
        freq = np.float32(ROPE_BASE) ** (np.float32(-2.0) * np.arange(hd // 2, dtype=np.float32) / np.float32(hd))
        angles = (pos[..., None].astype(np.float32) * freq).astype(np.float64)
        rope = np.tile(np.concatenate([np.cos(angles), np.sin(angles)], axis=-1), (1, 1, 2)).astype(np.float32)
        by_rows = lambda w: jnp.transpose(w, (0, 2, 3, 1)).reshape(layers, -1, d_model)
        units_first = lambda w: jnp.transpose(w, (0, 2, 1))
        hbm, vmem = (pl.BlockSpec(memory_space=s) for s in (pltpu.HBM, pltpu.VMEM))
        dma = pltpu.SemaphoreType.DMA
        out = pl.pallas_call(
            functools.partial(kernel, nz),
            name='decoder',
            out_shape=jax.ShapeDtypeStruct((seq_dev, d_model), F32),
            in_specs=[hbm] * 13,
            out_specs=vmem,
            scratch_shapes=[
                pltpu.VMEM((layers, 2, PLANE, 3 * units, d_model), BF16),
                pltpu.VMEM((layers, heads * hd, d_model), BF16),
                pltpu.VMEM((layers, hq + 2 * hd, d_model), BF16),
                pltpu.VMEM((layers, nz, seq_dev, d_model), BF16),
                pltpu.VMEM((layers, rows, heads * hd), BF16),
                pltpu.VMEM((layers, 2, PLANE, rows, LANES), BF16),
                pltpu.VMEM((layers, nch, 4 if nz == 8 else max(nz - 1, 1), seq_dev, CHUNK), F32),
                pltpu.VMEM((layers, nch, 3, seq_dev, CHUNK), F32),
                pltpu.VMEM((layers, nch, 2, seq_dev, CHUNK), F32),
                pltpu.VMEM((layers, nch, nz, seq_dev, CHUNK), F32),
                pltpu.VMEM((rows, d_model), F32),
                pltpu.VMEM((rows, d_model), F32),
                pltpu.VMEM((rows, d_model), BF16),
                pltpu.VMEM((hq // hd, rows, LANES), BF16),
                pltpu.VMEM((n_groups, CHUNK // units * rows, CHUNK), BF16),
                pltpu.VMEM((rows, LANES), F32), pltpu.VMEM((rows, LANES), F32), pltpu.VMEM((rows, LANES), F32),
                pltpu.VMEM((layers, d_model), BF16), pltpu.VMEM((layers, d_model), BF16),
                pltpu.VMEM((d_model // LANES, LANES), BF16),
                pltpu.SMEM((1,), jnp.int32),
                dma((layers, 7)), dma((6,)), dma((layers, 2, 20)), dma((layers,)),
                dma((layers, 4)), dma((layers,)),
                dma((layers,)), dma((layers,)), dma((layers,)), dma((layers,)), dma((layers,)), dma((layers,)),
                dma((layers, nz)), dma((layers,)), dma((layers, nch)), dma((layers, nch)), dma((layers,)),
            ],
            compiler_params=pltpu.CompilerParams(
                collective_id=0, has_side_effects=True, vmem_limit_bytes=67_043_328),
        )(hidden_in[0], lengths, jnp.asarray(rope), attn_norm, mlp_norm, final_norm.reshape(-1, LANES), by_rows(w_query), by_rows(w_key), by_rows(w_value),
          w_out.reshape(layers, heads * hd, d_model), units_first(w_gate), units_first(w_up), w_down)
        return out.astype(BF16)[None]

    seq_part = P(None, 'tp', None)
    in_specs = (seq_part, P(), P(), P(), P(), P(), P(), P(), P(None, None, 'tp'), P(None, None, 'tp'), P(None, 'tp', None), P())
    return jax.shard_map(device_fn, mesh=mesh, in_specs=in_specs, out_specs=seq_part, check_vma=False)
```

```python
import functools

import jax
import jax.numpy as jnp
import numpy as np
from jax import lax
from jax.experimental import pallas as pl
from jax.experimental.pallas import tpu as pltpu
from jax.sharding import PartitionSpec as P

NORM_EPS = 1e-5
ROPE_BASE = 500000.0
NX = 4
PLANE = NX * NX
LANES = 128
CHUNK = 256
NT = (((1,), (1,)), ((), ()))
F32, BF16 = jnp.float32, jnp.bfloat16


def remote(src, dst, send_sem, recv_sem, device):
    return pltpu.make_async_remote_copy(
        src_ref=src, dst_ref=dst, send_sem=send_sem, recv_sem=recv_sem,
        device_id=(device,), device_id_type=pl.DeviceIdType.MESH)


def scoped(f):
    @functools.wraps(f)
    def wrapped(*args):
        with jax.named_scope(f.__name__ + ('#l=%d' % args[0])):
            return f(*args)
    return wrapped


def kernel(nz, h_ref, len_ref, rope_ref, ga_ref, gm_ref, gf_ref, wq_ref, wk_ref, wv_ref, wo_ref, wg_ref, wu_ref, wd_ref,
           out_ref, w_all, wo_v, wqkv, h_all, c_mat, kv_all, rs, ra, sb, ps, acc, hres, zb, qbuf, bd, rope, cos_t, sin_t, ga, gm, gf, len_s,
           local_sem, in_sem, w_recv, w_send, d_recv, d_send, h_recv, h_send, kv_recv, kv_send, kvd_recv, kvd_send,
           c_recv, c_send, rs_recv, ra_recv, rs_send):
    layers = wo_ref.shape[0]
    seq_dev, d_model = h_ref.shape
    units = wg_ref.shape[1]
    pack = 3 * units
    half = pack // 2
    rows = nz * seq_dev
    hq = wq_ref.shape[1] // nz
    hd = wk_ref.shape[1] // nz
    nch = d_model // CHUNK
    me = lax.axis_index('tp')
    core = me % 2
    px = (me // 2) % NX
    py = (me // (2 * NX)) % NX
    mp = (me // 2) % PLANE
    mz = me // (2 * PLANE)
    base = mz * (2 * PLANE)
    partner = base + mp * 2 + (1 - core)

    def z_peer(i):
        return ((mz + i) % nz) * (2 * PLANE) + mp * 2 + core

    far_z = sorted(range(1, nz), key=lambda i: -min(i, nz - i))
    near_z = far_z[::-1]

    def plane_peer(dy, dx):
        return base + ((py + dy) % NX * NX + (px + dx) % NX) * 2 + core

    far_plane = sorted(((dy, dx) for dy in range(NX) for dx in range(NX) if dy or dx),
                       key=lambda d: -sum(min(i, NX - i) for i in d))

    barrier = pltpu.get_barrier_semaphore()

    def signal(device):
        pl.semaphore_signal(barrier, inc=1, device_id=(device,), device_id_type=pl.DeviceIdType.MESH)

    for i in far_z:
        signal(z_peer(i))
    for d in far_plane:
        signal(plane_peer(*d))
    signal(partner)

    def pack_copies(l):
        mine = w_all.at[l, core, mp]
        return [pltpu.make_async_copy(ref.at[l], mine.at[pl.ds(i * units, units)], local_sem.at[l, i])
                for i, ref in enumerate((wg_ref, wu_ref, wd_ref))]

    def qkv_copies(l):
        return [
            pltpu.make_async_copy(wq_ref.at[l, pl.ds(mz * hq, hq)], wqkv.at[l, pl.ds(0, hq)], local_sem.at[l, 3]),
            pltpu.make_async_copy(wk_ref.at[l, pl.ds(mz * hd, hd)], wqkv.at[l, pl.ds(hq, hd)], local_sem.at[l, 4]),
            pltpu.make_async_copy(wv_ref.at[l, pl.ds(mz * hd, hd)], wqkv.at[l, pl.ds(hq + hd, hd)], local_sem.at[l, 5]),
        ]

    def wo_copy(l):
        return pltpu.make_async_copy(wo_ref.at[l], wo_v.at[l], local_sem.at[l, 6])

    small = [pltpu.make_async_copy(src, dst, in_sem.at[i]) for i, (src, dst) in enumerate((
        (h_ref, h_all.at[0, mz]), (rope_ref.at[mp * 2 + core], rope), (ga_ref, ga), (gm_ref, gm), (gf_ref, gf), (len_ref, len_s)))]
    for c in small:
        c.start()
    for c in pack_copies(0) + qkv_copies(0):
        c.start()

    def start_later_copies():
        wo_copy(0).start()
        for l in range(1, layers):
            for c in pack_copies(l) + qkv_copies(l):
                c.start()
            wo_copy(l).start()

    def barrier_wait():
        pl.semaphore_wait(barrier, 1 + (nz - 1) + (PLANE - 1))

    def slot(h, a1, a2):
        return a2 % NX * NX + a1 % NX if h == 0 else a1 % NX * NX + a2 % NX

    def where_am_i(h):
        return (px, py) if h == 0 else (py, px)

    def at(h, a1, a2):
        return base + slot(h, a1, a2) * 2 + core

    third = half // 3
    SPAN = ((0, half), (half, half))
    FROM_MINUS = ((0, 2 * third), (half, third))
    FROM_PLUS = ((2 * third, third), (half + third, 2 * third))

    def piece(l, c, p, span):
        return w_all.at[l, c, p, pl.ds(*span)]

    def w_copy(l, h, p, span, idx, device):
        ref = piece(l, core, p, span)
        return remote(ref, ref, w_send.at[l], w_recv.at[l, h, idx], device)

    GROUPS = (((0, 0), (1, 0), (3, 0), (0, 1)), ((0, 3), (2, 0), (0, 2), (1, 1)),
              ((1, 3), (3, 1), (3, 3), (2, 1)), ((2, 3), (1, 2), (3, 2), (2, 2)))
    GROUP_OF = {d: g for g, ds in enumerate(GROUPS) for d in ds}

    def to_partner(l, h, k1, k2, span):
        a1, a2 = where_am_i(h)
        ref = piece(l, core, slot(h, a1 + k1, a2 + k2), span)
        g = GROUP_OF[(k1, k2) if h == 0 else (k2, k1)]
        remote(ref, ref, d_send.at[l], d_recv.at[l, g], partner).start()

    @scoped
    def p1(l):
        for c in pack_copies(l):
            c.wait()
        for h in range(2):
            a1, a2 = where_am_i(h)
            w_copy(l, h, mp, SPAN[h], 0, at(h, a1 + 1, a2)).start()
            w_copy(l, h, mp, SPAN[h], 1, at(h, a1 + NX - 1, a2)).start()
        to_partner(l, 0, 0, 0, (0, pack))

    @scoped
    def p2(l):
        for h in range(2):
            a1, a2 = where_am_i(h)
            low, high = slot(h, a1 + NX - 1, a2), slot(h, a1 + 1, a2)
            w_copy(l, h, low, SPAN[h], 0, me).wait_recv()
            w_copy(l, h, low, FROM_MINUS[h], 2, at(h, a1 + 1, a2)).start()
            w_copy(l, h, high, SPAN[h], 1, me).wait_recv()
            w_copy(l, h, high, FROM_PLUS[h], 3, at(h, a1 + NX - 1, a2)).start()
            to_partner(l, h, NX - 1, 0, SPAN[h])
            to_partner(l, h, 1, 0, SPAN[h])

    @scoped
    def p3(l, ks):
        for k in ks:
            for h in range(2):
                a1, a2 = where_am_i(h)
                p = slot(h, a1 + k, a2)
                if k == 2:
                    w_copy(l, h, p, FROM_MINUS[h], 2, me).wait_recv()
                    w_copy(l, h, p, FROM_PLUS[h], 3, me).wait_recv()
                    to_partner(l, h, k, 0, SPAN[h])
                w_copy(l, h, p, SPAN[h], 4 + k, at(h, a1, a2 + 1)).start()
                w_copy(l, h, p, SPAN[h], 8 + k, at(h, a1, a2 + NX - 1)).start()

    @scoped
    def p4(l, ks):
        for k in ks:
            for h in range(2):
                a1, a2 = where_am_i(h)
                low, high = slot(h, a1 + k, a2 + NX - 1), slot(h, a1 + k, a2 + 1)
                w_copy(l, h, low, SPAN[h], 4 + k, me).wait_recv()
                w_copy(l, h, low, FROM_MINUS[h], 12 + k, at(h, a1, a2 + 1)).start()
                w_copy(l, h, high, SPAN[h], 8 + k, me).wait_recv()
                w_copy(l, h, high, FROM_PLUS[h], 16 + k, at(h, a1, a2 + NX - 1)).start()
                to_partner(l, h, k, NX - 1, SPAN[h])
                to_partner(l, h, k, 1, SPAN[h])

    @scoped
    def p5(l, ks):
        for k in ks:
            for h in range(2):
                a1, a2 = where_am_i(h)
                p = slot(h, a1 + k, a2 + 2)
                w_copy(l, h, p, FROM_MINUS[h], 12 + k, me).wait_recv()
                w_copy(l, h, p, FROM_PLUS[h], 16 + k, me).wait_recv()
                to_partner(l, h, k, 2, SPAN[h])

    @scoped
    def w_done(l, gs):
        for g in gs:
            ref = w_all.at[l, 1 - core, pl.ds(0, len(GROUPS[g]))]
            remote(ref, ref, d_send.at[l], d_recv.at[l, g], partner).wait_recv()

    def h_copy(l, first, size, device):
        ref = h_all.at[l, mz, :, pl.ds(first, size)]
        return remote(ref, ref, h_send.at[l], h_recv.at[l], device)

    def h_start(l, first, size):
        for i in far_z:
            h_copy(l, first, size, z_peer(i)).start()

    @scoped
    def h_wait(l):
        if nz > 1:
            ref = h_all.at[l, pl.ds(0, nz - 1)]
            with jax.named_scope('h_recv'):
                remote(ref, ref, h_send.at[l], h_recv.at[l], me).wait_recv()
        for i in range(nz):
            hres[pl.ds(i * seq_dev, seq_dev)] = h_all[l, i].astype(F32)

    @scoped
    def norm_to_zb(l, gains):
        gain = gains[...].astype(F32)[l:l + 1]
        step = min(16, rows)

        @pl.loop(0, rows // step)
        def _(i):
            r = pl.ds(pl.multiple_of(i * step, step), step)
            x = hres[r]
            inv = lax.rsqrt(jnp.mean(x * x, axis=-1, keepdims=True) + NORM_EPS)
            zb[r] = (x * inv * gain).astype(BF16)

    lane = lax.broadcasted_iota(jnp.int32, (rows, LANES), 1)
    low_half = lane < hd

    def rotate(x):
        first = (lane % hd) < hd // 2
        swapped = jnp.where(first, pltpu.roll(x, LANES - hd // 2, 1), pltpu.roll(x, hd // 2, 1))
        return x * cos_t[...] + swapped * sin_t[...]

    def rope_tables():
        first = (lane % hd) < hd // 2
        t = rope[...]
        cos_t[...] = jnp.where(first, t, pltpu.roll(t, hd // 2, 1))
        sin_t[...] = jnp.where(first, -pltpu.roll(t, LANES - hd // 2, 1), t)

    def kv_copy(l, device):
        ref = kv_all.at[l, core, mp]
        return remote(ref, ref, kv_send.at[l], kv_recv.at[l], device)

    @scoped
    def qkv(l):
        for c in qkv_copies(l):
            c.wait()
        kv = lax.dot_general(zb[...], wqkv[l, pl.ds(hq, 2 * hd), :], NT, preferred_element_type=F32)
        kv_all[l, core, mp] = jnp.where(low_half, rotate(kv), kv).astype(BF16)
        for d in far_plane:
            kv_copy(l, plane_peer(*d)).start()
        proj = lax.dot_general(zb[...], wqkv[l, pl.ds(0, hq), :], NT, preferred_element_type=F32)
        for j in range(hq // LANES):
            q = rotate(proj[:, j * LANES:(j + 1) * LANES]) * (hd ** -0.5)
            for half_head, x in enumerate((q, pltpu.roll(q, LANES - hd, 1))):
                head = 2 * j + half_head
                qbuf[pl.ds(head * rows, rows)] = jnp.where(low_half, x, 0.0).astype(BF16)

    @scoped
    def kv_wait(l):
        ref = kv_all.at[l, core, pl.ds(0, PLANE - 1)]
        remote(ref, ref, kv_send.at[l], kv_recv.at[l], me).wait_recv()
        ref = kv_all.at[l, core]
        remote(ref, ref, kvd_send.at[l], kvd_recv.at[l], partner).start()
        ref = kv_all.at[l, 1 - core]
        remote(ref, ref, kvd_send.at[l], kvd_recv.at[l], partner).wait_recv()

    def c_columns(j):
        return pl.ds(pl.multiple_of(mz * hq + j * LANES, LANES), LANES)

    @scoped
    def attention(l):
        keys = 2 * PLANE * rows
        j = lax.broadcasted_iota(jnp.int32, (1, keys), 1)
        key_pos = ((j // seq_dev) % nz) * (2 * PLANE * seq_dev) + ((j // rows) % PLANE) * (2 * seq_dev) \
            + (j // (PLANE * rows)) * seq_dev + j % seq_dev
        i = lax.broadcasted_iota(jnp.int32, (hq // hd * rows, 1), 0) % rows
        q_pos = (i // seq_dev) * (2 * PLANE * seq_dev) + (mp * 2 + core) * seq_dev + i % seq_dev
        allowed = key_pos <= jnp.minimum(q_pos, len_s[0] - 1)
        kv = kv_all[l].reshape(keys, LANES)
        s = lax.dot_general(qbuf[...], kv, NT, preferred_element_type=F32)
        s = jnp.where(allowed, s, -1e30)
        e = jnp.exp(s - jnp.max(s, axis=-1, keepdims=True))
        p = (e * (1.0 / jnp.sum(e, axis=-1, keepdims=True))).astype(BF16)
        o = jnp.dot(p, kv, preferred_element_type=F32)
        for pair in range(hq // LANES):
            even, odd = (o[h * rows:(h + 1) * rows] for h in (2 * pair, 2 * pair + 1))
            c_mat[l, :, c_columns(pair)] = jnp.where(low_half, pltpu.roll(even, LANES - hd, 1), odd).astype(BF16)
        ref = c_mat.at[l, :, pl.ds(pl.multiple_of(mz * hq, hq), hq)]
        for i in near_z:
            remote(ref, ref, c_send.at[l], c_recv.at[l, i], z_peer(i)).start()

    @scoped
    def out_proj(l):
        with jax.named_scope('wo_wait'):
            wo_copy(l).wait()
        for i in [0] + near_z:
            src = (mz + nz - i) % nz
            cols = pl.ds(pl.multiple_of(src * hq, hq), hq)
            if i:
                ref = c_mat.at[l, :, cols]
                with jax.named_scope('c_wait'):
                    remote(ref, ref, c_send.at[l], c_recv.at[l, i], me).wait_recv()
            part = jnp.dot(c_mat[l, :, cols], wo_v[l, cols, :], preferred_element_type=F32)
            acc[...] = acc[...] + part if i else part
        step = min(16, rows)

        @pl.loop(0, rows // step)
        def _(i):
            r = pl.ds(pl.multiple_of(i * step, step), step)
            hres[r] = (hres[r] + acc[r]).astype(BF16).astype(F32)

    group = CHUNK // units
    n_groups = len(GROUPS)
    assert group == 2 * len(GROUPS[0])

    def slab(l, g, first, cols):
        parts = [w_all[l, c, slot(0, px + dx, py + dy), pl.ds(first, units), cols] for c in range(2) for dx, dy in GROUPS[g]]
        return jnp.concatenate(parts, axis=0)

    @scoped
    def mlp_units(l, gs):
        block = lax.broadcasted_iota(jnp.int32, (rows, CHUNK), 1) // units
        for g in gs:
            every = pl.ds(0, d_model)
            gate = lax.dot_general(zb[...], slab(l, g, 0, every), NT, preferred_element_type=F32)
            up = lax.dot_general(zb[...], slab(l, g, units, every), NT, preferred_element_type=F32)
            act = gate * (1.0 / (1.0 + jnp.exp(-gate))) * up
            for b in range(group):
                bd[g, pl.ds(b * rows, rows)] = jnp.where(block == b, act, 0.0).astype(BF16)

    two_step = nz == 8

    def ps_of(l, n, i):
        return ps.at[l, n, (mz + i + nz) % nz]

    def rs_start(l, n):
        if not two_step:
            for k, i in enumerate(far_z):
                remote(ps_of(l, n, i), rs.at[l, n, k], rs_send.at[l], rs_recv.at[l, n], z_peer(i)).start()
            return
        for side, to in ((0, nz - 2), (1, 2)):
            cols = pl.ds(side * LANES, LANES)
            remote(ps.at[l, n, (mz + 4) % nz, :, cols], ra.at[l, n, 2, :, cols], rs_send.at[l], ra_recv.at[l, n], z_peer(to)).start()
        for side, to in ((0, nz - 1), (1, 1)):
            remote(ps_of(l, n, 3 * (to if to == 1 else -1)), ra.at[l, n, side], rs_send.at[l], ra_recv.at[l, n], z_peer(to)).start()
        for side, to in ((0, nz - 1), (1, 1)):
            remote(ps_of(l, n, to), rs.at[l, n, side], rs_send.at[l], rs_recv.at[l, n], z_peer(to)).start()

    @scoped
    def rs_middle(l):
        if not two_step:
            return

        @pl.loop(0, nch)
        def _(n):
            ref = ra.at[l, n]
            remote(ref, ref, rs_send.at[l], ra_recv.at[l, n], me).wait_recv()
            for side, to in ((0, nz - 2), (1, 2)):
                cols = pl.ds(side * LANES, LANES)
                sb[l, n, side] = ps[l, n, (mz + to) % nz] + ra[l, n, side]
                sb[l, n, side, :, cols] = sb[l, n, side, :, cols] + ra[l, n, 2, :, cols]
                remote(sb.at[l, n, side], rs.at[l, n, 2 + side], rs_send.at[l], rs_recv.at[l, n], z_peer(to)).start()

    @scoped
    def mlp_down(l):
        @pl.loop(0, nch)
        def _(n):
            cols = pl.ds(pl.multiple_of(n * CHUNK, CHUNK), CHUNK)
            total = jnp.zeros((rows, CHUNK), F32)
            for g in range(n_groups):
                y = jnp.dot(bd[g], slab(l, g, 2 * units, cols), preferred_element_type=F32)
                y = y.astype(BF16).astype(F32)
                for b in range(group):
                    total = total + y[b * rows:(b + 1) * rows]
            ps[l, n] = total.reshape(nz, seq_dev, CHUNK)
            rs_start(l, n)

    n_in = 4 if two_step else nz - 1

    @scoped
    def rs_finish(l, store):
        mine = pl.ds(pl.multiple_of(mz * seq_dev, seq_dev), seq_dev)
        for n in range(nch):
            if n_in:
                ref = rs.at[l, n]
                remote(ref, ref, rs_send.at[l], rs_recv.at[l, n], me).wait_recv()
            total = ps[l, n, mz]
            for k in range(n_in):
                total = total + rs[l, n, k]
            store(n, (hres[mine, n * CHUNK:(n + 1) * CHUNK] + total).astype(BF16))

    def store_next(l):
        def store(n, x):
            h_all[l + 1, mz, :, n * CHUNK:(n + 1) * CHUNK] = x
            if n % 2 or nch == 1:
                first = max(n - 1, 0) * CHUNK
                h_start(l + 1, first, (n + 1) * CHUNK - first)
        return store

    with jax.named_scope('small'):
        for c in small:
            c.wait()
        rope_tables()
    with jax.named_scope('barrier'):
        barrier_wait()
    h_start(0, 0, d_model)
    p1(0)
    p3(0, (0,))
    start_later_copies()
    p2(0)
    for l in range(layers):
        more = l + 1 < layers
        h_wait(l)
        norm_to_zb(l, ga)
        qkv(l)
        if l == 0:
            p3(0, (1, 3, 2))
            p4(0, (0,))
        else:
            p4(l, (2,))
        kv_wait(l)
        attention(l)
        if l == 0:
            p4(0, (1, 3, 2))
        else:
            p5(l, (0, 1, 3, 2))
        if more:
            p1(l + 1)
            p3(l + 1, (0,))
        out_proj(l)
        norm_to_zb(l, gm)
        if l == 0:
            w_done(l, (0,))
            mlp_units(l, (0,))
            p5(l, (0,))
            w_done(l, (1,))
            mlp_units(l, (1,))
            p5(l, (1, 3))
            w_done(l, (2,))
            mlp_units(l, (2,))
            p5(l, (2,))
            w_done(l, (3,))
            mlp_units(l, (3,))
        else:
            w_done(l, range(n_groups))
            mlp_units(l, range(n_groups))
        mlp_down(l)
        if more:
            p2(l + 1)
            p3(l + 1, (1, 3))
        rs_middle(l)
        if more:
            p3(l + 1, (2,))
            p4(l + 1, (0,))
            rs_finish(l, store_next(l))
            p4(l + 1, (1, 3))
    pieces = []
    rs_finish(layers - 1, lambda n, x: pieces.append(x.astype(F32)))
    x = jnp.concatenate(pieces, axis=1)
    inv = lax.rsqrt(jnp.mean(x * x, axis=-1, keepdims=True) + NORM_EPS)
    gain = gf[...].astype(F32)
    for i in range(d_model // LANES):
        cols = slice(i * LANES, (i + 1) * LANES)
        out_ref[:, cols] = x[:, cols] * inv * gain[i:i + 1]

    with jax.named_scope('drain'):
      for l in range(layers):
          ref = w_all.at[l, 0, pl.ds(0, PLANE - 1)]
          remote(ref, ref, w_send.at[l], w_recv.at[l, 0, 0], me).wait_send()
          ref = w_all.at[l, 0]
          remote(ref, ref, d_send.at[l], d_recv.at[l, 0], me).wait_send()
          ref = kv_all.at[l, 0, pl.ds(0, PLANE - 1)]
          remote(ref, ref, kv_send.at[l], kv_recv.at[l], me).wait_send()
          ref = kv_all.at[l, 0]
          remote(ref, ref, kvd_send.at[l], kvd_recv.at[l], me).wait_send()
          if nz > 1:
              ref = h_all.at[l, pl.ds(0, nz - 1)]
              remote(ref, ref, h_send.at[l], h_recv.at[l], me).wait_send()
              ref = c_mat.at[l, :, pl.ds(0, (nz - 1) * hq)]
              remote(ref, ref, c_send.at[l], c_recv.at[l, 0], me).wait_send()
              ref = ps.at[l, :, pl.ds(0, nz - 1)]
              remote(ref, ref, rs_send.at[l], rs_recv.at[l, 0], me).wait_send()


def solution(mesh):
    nz = mesh.shape['tp'] // (2 * PLANE)

    def device_fn(hidden_in, lengths, attn_norm, w_query, w_key, w_value, w_out, mlp_norm, w_gate, w_up, w_down, final_norm):
        seq_dev, d_model = hidden_in.shape[1:]
        layers, _, heads, hd = w_query.shape
        kv_heads = w_key.shape[2]
        units = w_gate.shape[2]
        assert kv_heads == nz and 2 * hd == LANES and heads % nz == 0
        hq = heads // nz * hd
        rows = nz * seq_dev
        nch = d_model // CHUNK
        n_groups = 2 * PLANE * units // CHUNK
        dev, row = np.arange(2 * PLANE)[:, None], np.arange(rows)[None, :]
        pos = (row // seq_dev) * (2 * PLANE * seq_dev) + dev * seq_dev + row % seq_dev
        freq = np.float32(ROPE_BASE) ** (np.float32(-2.0) * np.arange(hd // 2, dtype=np.float32) / np.float32(hd))
        angles = (pos[..., None].astype(np.float32) * freq).astype(np.float64)
        rope = np.tile(np.concatenate([np.cos(angles), np.sin(angles)], axis=-1), (1, 1, 2)).astype(np.float32)
        by_rows = lambda w: jnp.transpose(w, (0, 2, 3, 1)).reshape(layers, -1, d_model)
        units_first = lambda w: jnp.transpose(w, (0, 2, 1))
        hbm, vmem = (pl.BlockSpec(memory_space=s) for s in (pltpu.HBM, pltpu.VMEM))
        dma = pltpu.SemaphoreType.DMA
        out = pl.pallas_call(
            functools.partial(kernel, nz),
            name='decoder',
            out_shape=jax.ShapeDtypeStruct((seq_dev, d_model), F32),
            in_specs=[hbm] * 13,
            out_specs=vmem,
            scratch_shapes=[
                pltpu.VMEM((layers, 2, PLANE, 3 * units, d_model), BF16),
                pltpu.VMEM((layers, heads * hd, d_model), BF16),
                pltpu.VMEM((layers, hq + 2 * hd, d_model), BF16),
                pltpu.VMEM((layers, nz, seq_dev, d_model), BF16),
                pltpu.VMEM((layers, rows, heads * hd), BF16),
                pltpu.VMEM((layers, 2, PLANE, rows, LANES), BF16),
                pltpu.VMEM((layers, nch, 4 if nz == 8 else max(nz - 1, 1), seq_dev, CHUNK), F32),
                pltpu.VMEM((layers, nch, 3, seq_dev, CHUNK), F32),
                pltpu.VMEM((layers, nch, 2, seq_dev, CHUNK), F32),
                pltpu.VMEM((layers, nch, nz, seq_dev, CHUNK), F32),
                pltpu.VMEM((rows, d_model), F32),
                pltpu.VMEM((rows, d_model), F32),
                pltpu.VMEM((rows, d_model), BF16),
                pltpu.VMEM((hq // hd * rows, LANES), BF16),
                pltpu.VMEM((n_groups, CHUNK // units * rows, CHUNK), BF16),
                pltpu.VMEM((rows, LANES), F32), pltpu.VMEM((rows, LANES), F32), pltpu.VMEM((rows, LANES), F32),
                pltpu.VMEM((layers, d_model), BF16), pltpu.VMEM((layers, d_model), BF16),
                pltpu.VMEM((d_model // LANES, LANES), BF16),
                pltpu.SMEM((1,), jnp.int32),
                dma((layers, 7)), dma((6,)), dma((layers, 2, 20)), dma((layers,)),
                dma((layers, 4)), dma((layers,)),
                dma((layers,)), dma((layers,)), dma((layers,)), dma((layers,)), dma((layers,)), dma((layers,)),
                dma((layers, nz)), dma((layers,)), dma((layers, nch)), dma((layers, nch)), dma((layers,)),
            ],
            compiler_params=pltpu.CompilerParams(
                collective_id=0, has_side_effects=True, vmem_limit_bytes=67_043_328),
        )(hidden_in[0], lengths, jnp.asarray(rope), attn_norm, mlp_norm, final_norm.reshape(-1, LANES), by_rows(w_query), by_rows(w_key), by_rows(w_value),
          w_out.reshape(layers, heads * hd, d_model), units_first(w_gate), units_first(w_up), w_down)
        return out.astype(BF16)[None]

    seq_part = P(None, 'tp', None)
    in_specs = (seq_part, P(), P(), P(), P(), P(), P(), P(), P(None, None, 'tp'), P(None, None, 'tp'), P(None, 'tp', None), P())
    return jax.shard_map(device_fn, mesh=mesh, in_specs=in_specs, out_specs=seq_part, check_vma=False)
```

```python
import functools

import jax
import jax.numpy as jnp
import numpy as np
from jax import lax
from jax.experimental import pallas as pl
from jax.experimental.pallas import tpu as pltpu
from jax.sharding import PartitionSpec as P

NORM_EPS = 1e-5
ROPE_BASE = 500000.0
NX = 4
PLANE = NX * NX
LANES = 128
CHUNK = 256
NT = (((1,), (1,)), ((), ()))
F32, BF16 = jnp.float32, jnp.bfloat16


def remote(src, dst, send_sem, recv_sem, device):
    return pltpu.make_async_remote_copy(
        src_ref=src, dst_ref=dst, send_sem=send_sem, recv_sem=recv_sem,
        device_id=(device,), device_id_type=pl.DeviceIdType.MESH)


def scoped(f):
    @functools.wraps(f)
    def wrapped(*args):
        with jax.named_scope(f.__name__ + ('#l=%d' % args[0])):
            return f(*args)
    return wrapped


def kernel(nz, h_ref, len_ref, rope_ref, ga_ref, gm_ref, gf_ref, wq_ref, wk_ref, wv_ref, wo_ref, wg_ref, wu_ref, wd_ref,
           out_ref, w_all, wo_v, wqkv, h_all, c_mat, kv_all, rs, ra, sb, ps, acc, hres, zb, qbuf, bd, rope, cos_t, sin_t, ga, gm, gf, len_s,
           local_sem, in_sem, w_recv, w_send, d_recv, d_send, h_recv, h_send, kv_recv, kv_send, kvd_recv, kvd_send,
           c_recv, c_send, rs_recv, ra_recv, rs_send):
    layers = wo_ref.shape[0]
    seq_dev, d_model = h_ref.shape
    units = wg_ref.shape[1]
    pack = 3 * units
    half = pack // 2
    rows = nz * seq_dev
    hq = wq_ref.shape[1] // nz
    hd = wk_ref.shape[1] // nz
    nch = d_model // CHUNK
    me = lax.axis_index('tp')
    core = me % 2
    px = (me // 2) % NX
    py = (me // (2 * NX)) % NX
    mp = (me // 2) % PLANE
    mz = me // (2 * PLANE)
    base = mz * (2 * PLANE)
    partner = base + mp * 2 + (1 - core)

    def z_peer(i):
        return ((mz + i) % nz) * (2 * PLANE) + mp * 2 + core

    far_z = sorted(range(1, nz), key=lambda i: -min(i, nz - i))
    tied = nz == 8
    send_z = [1, 7, 3, 5, 2, 6] if tied else far_z
    take_z = [1, 7, 2, 6, 3, 5, 4] if tied else far_z[::-1]

    def plane_peer(dy, dx):
        return base + ((py + dy) % NX * NX + (px + dx) % NX) * 2 + core

    far_plane = sorted(((dy, dx) for dy in range(NX) for dx in range(NX) if dy or dx),
                       key=lambda d: -sum(min(i, NX - i) for i in d))

    barrier = pltpu.get_barrier_semaphore()

    def signal(device):
        pl.semaphore_signal(barrier, inc=1, device_id=(device,), device_id_type=pl.DeviceIdType.MESH)

    for i in far_z:
        signal(z_peer(i))
    for d in far_plane:
        signal(plane_peer(*d))
    signal(partner)

    def pack_copies(l):
        mine = w_all.at[l, core, mp]
        return [pltpu.make_async_copy(ref.at[l], mine.at[pl.ds(i * units, units)], local_sem.at[l, i])
                for i, ref in enumerate((wg_ref, wu_ref, wd_ref))]

    def qkv_copies(l):
        return [
            pltpu.make_async_copy(wq_ref.at[l, pl.ds(mz * hq, hq)], wqkv.at[l, pl.ds(0, hq)], local_sem.at[l, 3]),
            pltpu.make_async_copy(wk_ref.at[l, pl.ds(mz * hd, hd)], wqkv.at[l, pl.ds(hq, hd)], local_sem.at[l, 4]),
            pltpu.make_async_copy(wv_ref.at[l, pl.ds(mz * hd, hd)], wqkv.at[l, pl.ds(hq + hd, hd)], local_sem.at[l, 5]),
        ]

    def wo_copy(l):
        return pltpu.make_async_copy(wo_ref.at[l], wo_v.at[l], local_sem.at[l, 6])

    small = [pltpu.make_async_copy(src, dst, in_sem.at[i]) for i, (src, dst) in enumerate((
        (h_ref, h_all.at[0, mz]), (rope_ref.at[mp * 2 + core], rope), (ga_ref, ga), (gm_ref, gm), (gf_ref, gf), (len_ref, len_s)))]
    for c in small:
        c.start()
    for c in pack_copies(0) + qkv_copies(0):
        c.start()

    def start_later_copies():
        wo_copy(0).start()
        for l in range(1, layers):
            for c in pack_copies(l) + qkv_copies(l):
                c.start()
            wo_copy(l).start()

    def barrier_wait():
        pl.semaphore_wait(barrier, 1 + (nz - 1) + (PLANE - 1))

    def slot(h, a1, a2):
        return a2 % NX * NX + a1 % NX if h == 0 else a1 % NX * NX + a2 % NX

    def where_am_i(h):
        return (px, py) if h == 0 else (py, px)

    def at(h, a1, a2):
        return base + slot(h, a1, a2) * 2 + core

    third = half // 3
    SPAN = ((0, half), (half, half))

    def from_minus(h, k):
        return (h * half, 2 * third if k == 2 else third)

    def from_plus(h, k):
        first, size = from_minus(h, k)
        return (first + size, half - size)

    def piece(l, c, p, span):
        return w_all.at[l, c, p, pl.ds(*span)]

    def w_copy(l, h, p, span, idx, device):
        ref = piece(l, core, p, span)
        return remote(ref, ref, w_send.at[l], w_recv.at[l, h, idx], device)

    GROUPS = (((0, 0), (1, 0), (3, 0), (0, 1)), ((0, 3), (2, 0), (0, 2), (1, 1)),
              ((1, 3), (3, 1), (3, 3), (2, 1)), ((2, 3), (1, 2), (3, 2), (2, 2)))
    GROUP_OF = {d: g for g, ds in enumerate(GROUPS) for d in ds}

    def to_partner(l, h, k1, k2, span):
        a1, a2 = where_am_i(h)
        ref = piece(l, core, slot(h, a1 + k1, a2 + k2), span)
        g = GROUP_OF[(k1, k2) if h == 0 else (k2, k1)]
        remote(ref, ref, d_send.at[l], d_recv.at[l, g], partner).start()

    @scoped
    def p1(l):
        for c in pack_copies(l):
            c.wait()
        for h in range(2):
            a1, a2 = where_am_i(h)
            w_copy(l, h, mp, SPAN[h], 0, at(h, a1 + 1, a2)).start()
            w_copy(l, h, mp, SPAN[h], 1, at(h, a1 + NX - 1, a2)).start()
        to_partner(l, 0, 0, 0, (0, pack))

    @scoped
    def p2(l):
        for h in range(2):
            a1, a2 = where_am_i(h)
            low, high = slot(h, a1 + NX - 1, a2), slot(h, a1 + 1, a2)
            w_copy(l, h, low, SPAN[h], 0, me).wait_recv()
            w_copy(l, h, low, from_minus(h, 0), 2, at(h, a1 + 1, a2)).start()
            w_copy(l, h, high, SPAN[h], 1, me).wait_recv()
            w_copy(l, h, high, from_plus(h, 0), 3, at(h, a1 + NX - 1, a2)).start()
            to_partner(l, h, NX - 1, 0, SPAN[h])
            to_partner(l, h, 1, 0, SPAN[h])

    @scoped
    def p3(l, ks):
        for k in ks:
            for h in range(2):
                a1, a2 = where_am_i(h)
                p = slot(h, a1 + k, a2)
                if k == 2:
                    w_copy(l, h, p, from_minus(h, 0), 2, me).wait_recv()
                    w_copy(l, h, p, from_plus(h, 0), 3, me).wait_recv()
                    to_partner(l, h, k, 0, SPAN[h])
                w_copy(l, h, p, SPAN[h], 4 + k, at(h, a1, a2 + 1)).start()
                w_copy(l, h, p, SPAN[h], 8 + k, at(h, a1, a2 + NX - 1)).start()

    @scoped
    def p4(l, ks):
        for k in ks:
            for h in range(2):
                a1, a2 = where_am_i(h)
                low, high = slot(h, a1 + k, a2 + NX - 1), slot(h, a1 + k, a2 + 1)
                w_copy(l, h, low, SPAN[h], 4 + k, me).wait_recv()
                w_copy(l, h, low, from_minus(h, k), 12 + k, at(h, a1, a2 + 1)).start()
                w_copy(l, h, high, SPAN[h], 8 + k, me).wait_recv()
                w_copy(l, h, high, from_plus(h, k), 16 + k, at(h, a1, a2 + NX - 1)).start()
                to_partner(l, h, k, NX - 1, SPAN[h])
                to_partner(l, h, k, 1, SPAN[h])

    @scoped
    def p5(l, ks):
        for k in ks:
            for h in range(2):
                a1, a2 = where_am_i(h)
                p = slot(h, a1 + k, a2 + 2)
                w_copy(l, h, p, from_minus(h, k), 12 + k, me).wait_recv()
                w_copy(l, h, p, from_plus(h, k), 16 + k, me).wait_recv()
                to_partner(l, h, k, 2, SPAN[h])

    @scoped
    def w_done(l, gs):
        for g in gs:
            ref = w_all.at[l, 1 - core, pl.ds(0, len(GROUPS[g]))]
            remote(ref, ref, d_send.at[l], d_recv.at[l, g], partner).wait_recv()

    def h_copy(l, src, first, size, i, device):
        ref = h_all.at[l, src, :, pl.ds(first, size)]
        return remote(ref, ref, h_send.at[l], h_recv.at[l, i], device)

    def h_start(l, first, size):
        for i in send_z:
            h_copy(l, mz, first, size, i, z_peer(i)).start()

    def h_take(l, i):
        h_copy(l, (mz + nz - i) % nz, 0, d_model, i, me).wait_recv()

    @scoped
    def h_relay(l):
        if tied:
            for i, first, to in ((1, 0, 3), (7, d_model // 2, 5)):
                h_take(l, i)
                h_copy(l, (mz + nz - i) % nz, first, d_model // 2, 4, z_peer(to)).start()

    @scoped
    def h_wait(l):
        for i in take_z:
            if not (tied and i in (1, 7)):
                h_take(l, i)
        for i in range(nz):
            hres[pl.ds(i * seq_dev, seq_dev)] = h_all[l, i].astype(F32)

    @scoped
    def norm_to_zb(l, gains, residual=False):
        gain = gains[...].astype(F32)[l:l + 1]
        step = min(16, rows)
        for first in range(0, rows, step):
            r = pl.ds(first, step)
            x = hres[r]
            if residual:
                x = (x + acc[r]).astype(BF16).astype(F32)
                hres[r] = x
            inv = lax.rsqrt(jnp.mean(x * x, axis=-1, keepdims=True) + NORM_EPS)
            zb[r] = (x * inv * gain).astype(BF16)

    lane = lax.broadcasted_iota(jnp.int32, (rows, LANES), 1)
    low_half = lane < hd

    def rotate(x):
        first = (lane % hd) < hd // 2
        swapped = jnp.where(first, pltpu.roll(x, LANES - hd // 2, 1), pltpu.roll(x, hd // 2, 1))
        return x * cos_t[...] + swapped * sin_t[...]

    def rope_tables():
        first = (lane % hd) < hd // 2
        t = rope[...]
        cos_t[...] = jnp.where(first, t, pltpu.roll(t, hd // 2, 1))
        sin_t[...] = jnp.where(first, -pltpu.roll(t, LANES - hd // 2, 1), t)

    def kv_copy(l, device):
        ref = kv_all.at[l, core, mp]
        return remote(ref, ref, kv_send.at[l], kv_recv.at[l], device)

    @scoped
    def qkv(l):
        for c in qkv_copies(l):
            c.wait()
        kv = lax.dot_general(zb[...], wqkv[l, pl.ds(hq, 2 * hd), :], NT, preferred_element_type=F32)
        kv_all[l, core, mp] = jnp.where(low_half, rotate(kv), kv).astype(BF16)
        for d in far_plane:
            kv_copy(l, plane_peer(*d)).start()
        proj = lax.dot_general(zb[...], wqkv[l, pl.ds(0, hq), :], NT, preferred_element_type=F32)
        for j in range(hq // LANES):
            q = rotate(proj[:, j * LANES:(j + 1) * LANES]) * (hd ** -0.5)
            for half_head, x in enumerate((q, pltpu.roll(q, LANES - hd, 1))):
                head = 2 * j + half_head
                qbuf[pl.ds(head * rows, rows)] = jnp.where(low_half, x, 0.0).astype(BF16)

    @scoped
    def kv_wait(l):
        ref = kv_all.at[l, core, pl.ds(0, PLANE - 1)]
        remote(ref, ref, kv_send.at[l], kv_recv.at[l], me).wait_recv()
        ref = kv_all.at[l, core]
        remote(ref, ref, kvd_send.at[l], kvd_recv.at[l], partner).start()
        ref = kv_all.at[l, 1 - core]
        remote(ref, ref, kvd_send.at[l], kvd_recv.at[l], partner).wait_recv()

    def c_columns(j):
        return pl.ds(pl.multiple_of(mz * hq + j * LANES, LANES), LANES)

    def c_copy(l, src, r, i, device):
        ref = c_mat.at[l, r, pl.ds(pl.multiple_of(src * hq, hq), hq)]
        return remote(ref, ref, c_send.at[l], c_recv.at[l, i], device)

    @scoped
    def attention(l):
        keys = 2 * PLANE * rows
        j = lax.broadcasted_iota(jnp.int32, (1, keys), 1)
        key_pos = ((j // seq_dev) % nz) * (2 * PLANE * seq_dev) + ((j // rows) % PLANE) * (2 * seq_dev) \
            + (j // (PLANE * rows)) * seq_dev + j % seq_dev
        i = lax.broadcasted_iota(jnp.int32, (hq // hd * rows, 1), 0) % rows
        q_pos = (i // seq_dev) * (2 * PLANE * seq_dev) + (mp * 2 + core) * seq_dev + i % seq_dev
        allowed = key_pos <= jnp.minimum(q_pos, len_s[0] - 1)
        kv = kv_all[l].reshape(keys, LANES)
        s = lax.dot_general(qbuf[...], kv, NT, preferred_element_type=F32)
        s = jnp.where(allowed, s, -1e30)
        e = jnp.exp(s - jnp.max(s, axis=-1, keepdims=True))
        p = (e * (1.0 / jnp.sum(e, axis=-1, keepdims=True))).astype(BF16)
        o = jnp.dot(p, kv, preferred_element_type=F32)
        for pair in range(hq // LANES):
            even, odd = (o[h * rows:(h + 1) * rows] for h in (2 * pair, 2 * pair + 1))
            c_mat[l, :, c_columns(pair)] = jnp.where(low_half, pltpu.roll(even, LANES - hd, 1), odd).astype(BF16)
        for i in send_z:
            c_copy(l, mz, pl.ds(0, rows), i, z_peer(i)).start()

    @scoped
    def out_proj(l):
        with jax.named_scope('wo_wait'):
            wo_copy(l).wait()
        for i in [0] + take_z:
            src = (mz + nz - i) % nz
            cols = pl.ds(pl.multiple_of(src * hq, hq), hq)
            if i:
                with jax.named_scope('c_wait'):
                    c_copy(l, src, pl.ds(0, rows), i, me).wait_recv()
            if tied and i in (1, 7):
                first, to = (0, 3) if i == 1 else (rows // 2, 5)
                c_copy(l, src, pl.ds(first, rows // 2), 4, z_peer(to)).start()
            part = jnp.dot(c_mat[l, :, cols], wo_v[l, cols, :], preferred_element_type=F32)
            acc[...] = acc[...] + part if i else part

    group = CHUNK // units
    n_groups = len(GROUPS)
    assert group == 2 * len(GROUPS[0])

    def slab(l, g, first, cols):
        parts = [w_all[l, c, slot(0, px + dx, py + dy), pl.ds(first, units), cols] for c in range(2) for dx, dy in GROUPS[g]]
        return jnp.concatenate(parts, axis=0)

    @scoped
    def mlp_units(l, gs):
        block = lax.broadcasted_iota(jnp.int32, (rows, CHUNK), 1) // units
        for g in gs:
            every = pl.ds(0, d_model)
            gate = lax.dot_general(zb[...], slab(l, g, 0, every), NT, preferred_element_type=F32)
            up = lax.dot_general(zb[...], slab(l, g, units, every), NT, preferred_element_type=F32)
            act = gate * (1.0 / (1.0 + jnp.exp(-gate))) * up
            for b in range(group):
                bd[g, pl.ds(b * rows, rows)] = jnp.where(block == b, act, 0.0).astype(BF16)

    two_step = nz == 8

    def ps_of(l, n, i):
        return ps.at[l, n, (mz + i + nz) % nz]

    def rs_start(l, n):
        if not two_step:
            for k, i in enumerate(far_z):
                remote(ps_of(l, n, i), rs.at[l, n, k], rs_send.at[l], rs_recv.at[l, n], z_peer(i)).start()
            return
        for side, to in ((0, nz - 2), (1, 2)):
            cols = pl.ds(side * LANES, LANES)
            remote(ps.at[l, n, (mz + 4) % nz, :, cols], ra.at[l, n, 2, :, cols], rs_send.at[l], ra_recv.at[l, n], z_peer(to)).start()
        for side, to in ((0, nz - 1), (1, 1)):
            remote(ps_of(l, n, 3 * (to if to == 1 else -1)), ra.at[l, n, side], rs_send.at[l], ra_recv.at[l, n], z_peer(to)).start()
        for side, to in ((0, nz - 1), (1, 1)):
            remote(ps_of(l, n, to), rs.at[l, n, side], rs_send.at[l], rs_recv.at[l, n], z_peer(to)).start()

    @scoped
    def rs_middle(l):
        if not two_step:
            return

        @pl.loop(0, nch)
        def _(n):
            ref = ra.at[l, n]
            remote(ref, ref, rs_send.at[l], ra_recv.at[l, n], me).wait_recv()
            for side, to in ((0, nz - 2), (1, 2)):
                cols = pl.ds(side * LANES, LANES)
                sb[l, n, side] = ps[l, n, (mz + to) % nz] + ra[l, n, side]
                sb[l, n, side, :, cols] = sb[l, n, side, :, cols] + ra[l, n, 2, :, cols]
                remote(sb.at[l, n, side], rs.at[l, n, 2 + side], rs_send.at[l], rs_recv.at[l, n], z_peer(to)).start()

    @scoped
    def mlp_down(l):
        @pl.loop(0, nch)
        def _(n):
            cols = pl.ds(pl.multiple_of(n * CHUNK, CHUNK), CHUNK)
            total = jnp.zeros((rows, CHUNK), F32)
            for g in range(n_groups):
                y = jnp.dot(bd[g], slab(l, g, 2 * units, cols), preferred_element_type=F32)
                y = y.astype(BF16).astype(F32)
                for b in range(group):
                    total = total + y[b * rows:(b + 1) * rows]
            ps[l, n] = total.reshape(nz, seq_dev, CHUNK)
            rs_start(l, n)

    n_in = 4 if two_step else nz - 1

    @scoped
    def rs_finish(l, store):
        mine = pl.ds(pl.multiple_of(mz * seq_dev, seq_dev), seq_dev)
        for n in range(nch):
            if n_in:
                ref = rs.at[l, n]
                remote(ref, ref, rs_send.at[l], rs_recv.at[l, n], me).wait_recv()
            total = ps[l, n, mz]
            for k in range(n_in):
                total = total + rs[l, n, k]
            store(n, (hres[mine, n * CHUNK:(n + 1) * CHUNK] + total).astype(BF16))

    def store_next(l):
        def store(n, x):
            h_all[l + 1, mz, :, n * CHUNK:(n + 1) * CHUNK] = x
            if n % 2 or nch == 1:
                first = max(n - 1, 0) * CHUNK
                h_start(l + 1, first, (n + 1) * CHUNK - first)
        return store

    with jax.named_scope('small'):
        for c in small:
            c.wait()
        rope_tables()
    with jax.named_scope('barrier'):
        barrier_wait()
    h_start(0, 0, d_model)
    p1(0)
    p3(0, (0,))
    start_later_copies()
    h_relay(0)
    p2(0)
    for l in range(layers):
        more = l + 1 < layers
        if l:
            h_relay(l)
        h_wait(l)
        norm_to_zb(l, ga)
        qkv(l)
        if l == 0:
            p3(0, (1, 3, 2))
            p4(0, (0,))
        else:
            p4(l, (1, 3, 2))
        kv_wait(l)
        attention(l)
        if l == 0:
            p4(0, (1, 3, 2))
        else:
            p5(l, (0, 1, 3, 2))
        if more:
            p1(l + 1)
            p3(l + 1, (0,))
        out_proj(l)
        norm_to_zb(l, gm, True)
        if l == 0:
            w_done(l, (0,))
            mlp_units(l, (0,))
            p5(l, (0,))
            w_done(l, (1,))
            mlp_units(l, (1,))
            p5(l, (1, 3))
            w_done(l, (2,))
            mlp_units(l, (2,))
            p5(l, (2,))
            w_done(l, (3,))
            mlp_units(l, (3,))
        else:
            w_done(l, range(n_groups))
            mlp_units(l, range(n_groups))
        mlp_down(l)
        if more:
            p2(l + 1)
            p3(l + 1, (1, 3))
        rs_middle(l)
        if more:
            p3(l + 1, (2,))
            p4(l + 1, (0,))
            rs_finish(l, store_next(l))
    pieces = []
    rs_finish(layers - 1, lambda n, x: pieces.append(x.astype(F32)))
    x = jnp.concatenate(pieces, axis=1)
    inv = lax.rsqrt(jnp.mean(x * x, axis=-1, keepdims=True) + NORM_EPS)
    gain = gf[...].astype(F32)
    for i in range(d_model // LANES):
        cols = slice(i * LANES, (i + 1) * LANES)
        out_ref[:, cols] = x[:, cols] * inv * gain[i:i + 1]

    with jax.named_scope('drain'):
      for l in range(layers):
          ref = w_all.at[l, 0, pl.ds(0, PLANE - 1)]
          remote(ref, ref, w_send.at[l], w_recv.at[l, 0, 0], me).wait_send()
          ref = w_all.at[l, 0]
          remote(ref, ref, d_send.at[l], d_recv.at[l, 0], me).wait_send()
          ref = kv_all.at[l, 0, pl.ds(0, PLANE - 1)]
          remote(ref, ref, kv_send.at[l], kv_recv.at[l], me).wait_send()
          ref = kv_all.at[l, 0]
          remote(ref, ref, kvd_send.at[l], kvd_recv.at[l], me).wait_send()
          if nz > 1:
              ref = h_all.at[l, pl.ds(0, nz - 1)]
              remote(ref, ref, h_send.at[l], h_recv.at[l, 0], me).wait_send()
              ref = c_mat.at[l, :, pl.ds(0, (nz - 1) * hq)]
              remote(ref, ref, c_send.at[l], c_recv.at[l, 0], me).wait_send()
              ref = ps.at[l, :, pl.ds(0, nz - 1)]
              remote(ref, ref, rs_send.at[l], rs_recv.at[l, 0], me).wait_send()


def solution(mesh):
    nz = mesh.shape['tp'] // (2 * PLANE)

    def device_fn(hidden_in, lengths, attn_norm, w_query, w_key, w_value, w_out, mlp_norm, w_gate, w_up, w_down, final_norm):
        seq_dev, d_model = hidden_in.shape[1:]
        layers, _, heads, hd = w_query.shape
        kv_heads = w_key.shape[2]
        units = w_gate.shape[2]
        assert kv_heads == nz and 2 * hd == LANES and heads % nz == 0
        hq = heads // nz * hd
        rows = nz * seq_dev
        nch = d_model // CHUNK
        n_groups = 2 * PLANE * units // CHUNK
        dev, row = np.arange(2 * PLANE)[:, None], np.arange(rows)[None, :]
        pos = (row // seq_dev) * (2 * PLANE * seq_dev) + dev * seq_dev + row % seq_dev
        freq = np.float32(ROPE_BASE) ** (np.float32(-2.0) * np.arange(hd // 2, dtype=np.float32) / np.float32(hd))
        angles = (pos[..., None].astype(np.float32) * freq).astype(np.float64)
        rope = np.tile(np.concatenate([np.cos(angles), np.sin(angles)], axis=-1), (1, 1, 2)).astype(np.float32)
        by_rows = lambda w: jnp.transpose(w, (0, 2, 3, 1)).reshape(layers, -1, d_model)
        units_first = lambda w: jnp.transpose(w, (0, 2, 1))
        hbm, vmem = (pl.BlockSpec(memory_space=s) for s in (pltpu.HBM, pltpu.VMEM))
        dma = pltpu.SemaphoreType.DMA
        out = pl.pallas_call(
            functools.partial(kernel, nz),
            name='decoder',
            out_shape=jax.ShapeDtypeStruct((seq_dev, d_model), F32),
            in_specs=[hbm] * 13,
            out_specs=vmem,
            scratch_shapes=[
                pltpu.VMEM((layers, 2, PLANE, 3 * units, d_model), BF16),
                pltpu.VMEM((layers, heads * hd, d_model), BF16),
                pltpu.VMEM((layers, hq + 2 * hd, d_model), BF16),
                pltpu.VMEM((layers, nz, seq_dev, d_model), BF16),
                pltpu.VMEM((layers, rows, heads * hd), BF16),
                pltpu.VMEM((layers, 2, PLANE, rows, LANES), BF16),
                pltpu.VMEM((layers, nch, 4 if nz == 8 else max(nz - 1, 1), seq_dev, CHUNK), F32),
                pltpu.VMEM((layers, nch, 3, seq_dev, CHUNK), F32),
                pltpu.VMEM((layers, nch, 2, seq_dev, CHUNK), F32),
                pltpu.VMEM((layers, nch, nz, seq_dev, CHUNK), F32),
                pltpu.VMEM((rows, d_model), F32),
                pltpu.VMEM((rows, d_model), F32),
                pltpu.VMEM((rows, d_model), BF16),
                pltpu.VMEM((hq // hd * rows, LANES), BF16),
                pltpu.VMEM((n_groups, CHUNK // units * rows, CHUNK), BF16),
                pltpu.VMEM((rows, LANES), F32), pltpu.VMEM((rows, LANES), F32), pltpu.VMEM((rows, LANES), F32),
                pltpu.VMEM((layers, d_model), BF16), pltpu.VMEM((layers, d_model), BF16),
                pltpu.VMEM((d_model // LANES, LANES), BF16),
                pltpu.SMEM((1,), jnp.int32),
                dma((layers, 7)), dma((6,)), dma((layers, 2, 20)), dma((layers,)),
                dma((layers, 4)), dma((layers,)),
                dma((layers, nz)), dma((layers,)), dma((layers,)), dma((layers,)), dma((layers,)), dma((layers,)),
                dma((layers, nz)), dma((layers,)), dma((layers, nch)), dma((layers, nch)), dma((layers,)),
            ],
            compiler_params=pltpu.CompilerParams(
                collective_id=0, has_side_effects=True, vmem_limit_bytes=67_043_328),
        )(hidden_in[0], lengths, jnp.asarray(rope), attn_norm, mlp_norm, final_norm.reshape(-1, LANES), by_rows(w_query), by_rows(w_key), by_rows(w_value),
          w_out.reshape(layers, heads * hd, d_model), units_first(w_gate), units_first(w_up), w_down)
        return out.astype(BF16)[None]

    seq_part = P(None, 'tp', None)
    in_specs = (seq_part, P(), P(), P(), P(), P(), P(), P(), P(None, None, 'tp'), P(None, None, 'tp'), P(None, 'tp', None), P())
    return jax.shard_map(device_fn, mesh=mesh, in_specs=in_specs, out_specs=seq_part, check_vma=False)
```

```python
import functools

import jax
import jax.numpy as jnp
import numpy as np
from jax import lax
from jax.experimental import pallas as pl
from jax.experimental.pallas import tpu as pltpu
from jax.sharding import PartitionSpec as P

NORM_EPS = 1e-5
ROPE_BASE = 500000.0
NX = 4
PLANE = NX * NX
LANES = 128
CHUNK = 256
NT = (((1,), (1,)), ((), ()))
F32, BF16 = jnp.float32, jnp.bfloat16


def remote(src, dst, send_sem, recv_sem, device):
    return pltpu.make_async_remote_copy(
        src_ref=src, dst_ref=dst, send_sem=send_sem, recv_sem=recv_sem,
        device_id=(device,), device_id_type=pl.DeviceIdType.MESH)


def scoped(f):
    @functools.wraps(f)
    def wrapped(*args):
        with jax.named_scope(f.__name__ + ('#l=%d' % args[0])):
            return f(*args)
    return wrapped


def kernel(nz, h_ref, len_ref, rope_ref, ga_ref, gm_ref, gf_ref, wq_ref, wk_ref, wv_ref, wo_ref, wg_ref, wu_ref, wd_ref,
           out_ref, w_all, wo_v, wqkv, h_all, c_mat, kv_all, rs, ra, sb, ps, acc, hres, zb, qbuf, bd, rope, cos_t, sin_t, ga, gm, gf, len_s,
           local_sem, in_sem, w_recv, w_send, d_recv, d_send, h_recv, h_send, kv_recv, kv_send, kvd_recv, kvd_send,
           c_recv, c_send, rs_recv, ra_recv, rs_send):
    layers = wo_ref.shape[0]
    seq_dev, d_model = h_ref.shape
    units = wg_ref.shape[1]
    pack = 3 * units
    half = pack // 2
    rows = nz * seq_dev
    hq = wq_ref.shape[1] // nz
    hd = wk_ref.shape[1] // nz
    nch = d_model // CHUNK
    me = lax.axis_index('tp')
    core = me % 2
    px = (me // 2) % NX
    py = (me // (2 * NX)) % NX
    mp = (me // 2) % PLANE
    mz = me // (2 * PLANE)
    base = mz * (2 * PLANE)
    partner = base + mp * 2 + (1 - core)

    def z_peer(i):
        return ((mz + i) % nz) * (2 * PLANE) + mp * 2 + core

    far_z = sorted(range(1, nz), key=lambda i: -min(i, nz - i))
    def plane_peer(dy, dx):
        return base + ((py + dy) % NX * NX + (px + dx) % NX) * 2 + core

    far_plane = sorted(((dy, dx) for dy in range(NX) for dx in range(NX) if dy or dx),
                       key=lambda d: -sum(min(i, NX - i) for i in d))

    barrier = pltpu.get_barrier_semaphore()

    def signal(device):
        pl.semaphore_signal(barrier, inc=1, device_id=(device,), device_id_type=pl.DeviceIdType.MESH)

    for i in far_z:
        signal(z_peer(i))
    for d in far_plane:
        signal(plane_peer(*d))
    signal(partner)

    def pack_copies(l):
        mine = w_all.at[l, core, mp]
        return [pltpu.make_async_copy(ref.at[l], mine.at[pl.ds(i * units, units)], local_sem.at[l, i])
                for i, ref in enumerate((wg_ref, wu_ref, wd_ref))]

    def qkv_copies(l):
        return [
            pltpu.make_async_copy(wq_ref.at[l, pl.ds(mz * hq, hq)], wqkv.at[l, pl.ds(0, hq)], local_sem.at[l, 3]),
            pltpu.make_async_copy(wk_ref.at[l, pl.ds(mz * hd, hd)], wqkv.at[l, pl.ds(hq, hd)], local_sem.at[l, 4]),
            pltpu.make_async_copy(wv_ref.at[l, pl.ds(mz * hd, hd)], wqkv.at[l, pl.ds(hq + hd, hd)], local_sem.at[l, 5]),
        ]

    def wo_copy(l):
        return pltpu.make_async_copy(wo_ref.at[l], wo_v.at[l], local_sem.at[l, 6])

    small = [pltpu.make_async_copy(src, dst, in_sem.at[i]) for i, (src, dst) in enumerate((
        (h_ref, h_all.at[0, mz]), (rope_ref.at[mp * 2 + core], rope), (ga_ref, ga), (gm_ref, gm), (gf_ref, gf), (len_ref, len_s)))]
    for c in small:
        c.start()
    for c in pack_copies(0) + qkv_copies(0):
        c.start()

    def start_later_copies():
        wo_copy(0).start()
        for l in range(1, layers):
            for c in pack_copies(l) + qkv_copies(l):
                c.start()
            wo_copy(l).start()

    def barrier_wait():
        pl.semaphore_wait(barrier, 1 + (nz - 1) + (PLANE - 1))

    def slot(h, a1, a2):
        return a2 % NX * NX + a1 % NX if h == 0 else a1 % NX * NX + a2 % NX

    def where_am_i(h):
        return (px, py) if h == 0 else (py, px)

    def at(h, a1, a2):
        return base + slot(h, a1, a2) * 2 + core

    third = half // 3
    SPAN = ((0, half), (half, half))

    def from_minus(h, k):
        return (h * half, 2 * third if (k in (1, 2)) != (h == 1) else third)

    def from_plus(h, k):
        first, size = from_minus(h, k)
        return (first + size, half - size)

    def piece(l, c, p, span):
        return w_all.at[l, c, p, pl.ds(*span)]

    def w_copy(l, h, p, span, idx, device):
        ref = piece(l, core, p, span)
        return remote(ref, ref, w_send.at[l], w_recv.at[l, h, idx], device)

    GROUPS = (((0, 0), (1, 0), (3, 0), (0, 1)), ((0, 3), (2, 0), (0, 2), (1, 1)),
              ((1, 3), (3, 1), (3, 3), (2, 1)), ((2, 3), (1, 2), (3, 2), (2, 2)))
    GROUP_OF = {d: g for g, ds in enumerate(GROUPS) for d in ds}

    def to_partner(l, h, k1, k2, span):
        a1, a2 = where_am_i(h)
        ref = piece(l, core, slot(h, a1 + k1, a2 + k2), span)
        g = GROUP_OF[(k1, k2) if h == 0 else (k2, k1)]
        remote(ref, ref, d_send.at[l], d_recv.at[l, g], partner).start()

    @scoped
    def p1(l):
        for c in pack_copies(l):
            c.wait()
        for h in range(2):
            a1, a2 = where_am_i(h)
            w_copy(l, h, mp, SPAN[h], 0, at(h, a1 + 1, a2)).start()
            w_copy(l, h, mp, SPAN[h], 1, at(h, a1 + NX - 1, a2)).start()
        to_partner(l, 0, 0, 0, (0, pack))

    @scoped
    def p2(l):
        for h in range(2):
            a1, a2 = where_am_i(h)
            low, high = slot(h, a1 + NX - 1, a2), slot(h, a1 + 1, a2)
            w_copy(l, h, low, SPAN[h], 0, me).wait_recv()
            w_copy(l, h, low, from_minus(h, 0), 2, at(h, a1 + 1, a2)).start()
            w_copy(l, h, high, SPAN[h], 1, me).wait_recv()
            w_copy(l, h, high, from_plus(h, 0), 3, at(h, a1 + NX - 1, a2)).start()
            to_partner(l, h, NX - 1, 0, SPAN[h])
            to_partner(l, h, 1, 0, SPAN[h])

    @scoped
    def p3(l, ks):
        for k in ks:
            for h in range(2):
                a1, a2 = where_am_i(h)
                p = slot(h, a1 + k, a2)
                if k == 2:
                    w_copy(l, h, p, from_minus(h, 0), 2, me).wait_recv()
                    w_copy(l, h, p, from_plus(h, 0), 3, me).wait_recv()
                    to_partner(l, h, k, 0, SPAN[h])
                w_copy(l, h, p, SPAN[h], 4 + k, at(h, a1, a2 + 1)).start()
                w_copy(l, h, p, SPAN[h], 8 + k, at(h, a1, a2 + NX - 1)).start()

    @scoped
    def p4(l, ks):
        for k in ks:
            for h in range(2):
                a1, a2 = where_am_i(h)
                low, high = slot(h, a1 + k, a2 + NX - 1), slot(h, a1 + k, a2 + 1)
                w_copy(l, h, low, SPAN[h], 4 + k, me).wait_recv()
                w_copy(l, h, low, from_minus(h, k), 12 + k, at(h, a1, a2 + 1)).start()
                w_copy(l, h, high, SPAN[h], 8 + k, me).wait_recv()
                w_copy(l, h, high, from_plus(h, k), 16 + k, at(h, a1, a2 + NX - 1)).start()
                to_partner(l, h, k, NX - 1, SPAN[h])
                to_partner(l, h, k, 1, SPAN[h])

    @scoped
    def p5(l, ks):
        for k in ks:
            for h in range(2):
                a1, a2 = where_am_i(h)
                p = slot(h, a1 + k, a2 + 2)
                w_copy(l, h, p, from_minus(h, k), 12 + k, me).wait_recv()
                w_copy(l, h, p, from_plus(h, k), 16 + k, me).wait_recv()
                to_partner(l, h, k, 2, SPAN[h])

    @scoped
    def w_done(l, gs):
        for g in gs:
            ref = w_all.at[l, 1 - core, pl.ds(0, len(GROUPS[g]))]
            remote(ref, ref, d_send.at[l], d_recv.at[l, g], partner).wait_recv()

    def h_copy(l, src, first, size, i, device):
        ref = h_all.at[l, src, :, pl.ds(first, size)]
        return remote(ref, ref, h_send.at[l], h_recv.at[l, i], device)

    def h_start(l, first, size):
        for i in far_z:
            h_copy(l, mz, first, size, i, z_peer(i)).start()

    def h_take(l, i):
        h_copy(l, (mz + nz - i) % nz, 0, d_model, i, me).wait_recv()

    @scoped
    def h_wait(l):
        for i in far_z:
            h_take(l, i)
        for i in range(nz):
            hres[pl.ds(i * seq_dev, seq_dev)] = h_all[l, i].astype(F32)

    @scoped
    def norm_to_zb(l, gains, residual=False):
        gain = gains[...].astype(F32)[l:l + 1]
        step = min(16, rows)
        for first in range(0, rows, step):
            r = pl.ds(first, step)
            x = hres[r]
            if residual:
                x = (x + acc[r]).astype(BF16).astype(F32)
                hres[r] = x
            inv = lax.rsqrt(jnp.mean(x * x, axis=-1, keepdims=True) + NORM_EPS)
            zb[r] = (x * inv * gain).astype(BF16)

    lane = lax.broadcasted_iota(jnp.int32, (rows, LANES), 1)
    low_half = lane < hd

    def rotate(x):
        first = (lane % hd) < hd // 2
        swapped = jnp.where(first, pltpu.roll(x, LANES - hd // 2, 1), pltpu.roll(x, hd // 2, 1))
        return x * cos_t[...] + swapped * sin_t[...]

    def rope_tables():
        first = (lane % hd) < hd // 2
        t = rope[...]
        cos_t[...] = jnp.where(first, t, pltpu.roll(t, hd // 2, 1))
        sin_t[...] = jnp.where(first, -pltpu.roll(t, LANES - hd // 2, 1), t)

    def kv_copy(l, device):
        ref = kv_all.at[l, core, mp]
        return remote(ref, ref, kv_send.at[l], kv_recv.at[l], device)

    @scoped
    def qkv(l):
        for c in qkv_copies(l):
            c.wait()
        kv = lax.dot_general(zb[...], wqkv[l, pl.ds(hq, 2 * hd), :], NT, preferred_element_type=F32)
        kv_all[l, core, mp] = jnp.where(low_half, rotate(kv), kv).astype(BF16)
        for d in far_plane:
            kv_copy(l, plane_peer(*d)).start()
        proj = lax.dot_general(zb[...], wqkv[l, pl.ds(0, hq), :], NT, preferred_element_type=F32)
        for j in range(hq // LANES):
            q = rotate(proj[:, j * LANES:(j + 1) * LANES]) * (hd ** -0.5)
            for half_head, x in enumerate((q, pltpu.roll(q, LANES - hd, 1))):
                head = 2 * j + half_head
                qbuf[pl.ds(head * rows, rows)] = jnp.where(low_half, x, 0.0).astype(BF16)

    @scoped
    def kv_wait(l):
        ref = kv_all.at[l, core, pl.ds(0, PLANE - 1)]
        remote(ref, ref, kv_send.at[l], kv_recv.at[l], me).wait_recv()
        ref = kv_all.at[l, core]
        remote(ref, ref, kvd_send.at[l], kvd_recv.at[l], partner).start()
        ref = kv_all.at[l, 1 - core]
        remote(ref, ref, kvd_send.at[l], kvd_recv.at[l], partner).wait_recv()

    def c_columns(j):
        return pl.ds(pl.multiple_of(mz * hq + j * LANES, LANES), LANES)

    def c_copy(l, src, r, i, device):
        ref = c_mat.at[l, r, pl.ds(pl.multiple_of(src * hq, hq), hq)]
        return remote(ref, ref, c_send.at[l], c_recv.at[l, i], device)

    @scoped
    def attention(l):
        keys = 2 * PLANE * rows
        j = lax.broadcasted_iota(jnp.int32, (1, keys), 1)
        key_pos = ((j // seq_dev) % nz) * (2 * PLANE * seq_dev) + ((j // rows) % PLANE) * (2 * seq_dev) \
            + (j // (PLANE * rows)) * seq_dev + j % seq_dev
        i = lax.broadcasted_iota(jnp.int32, (hq // hd * rows, 1), 0) % rows
        q_pos = (i // seq_dev) * (2 * PLANE * seq_dev) + (mp * 2 + core) * seq_dev + i % seq_dev
        allowed = key_pos <= jnp.minimum(q_pos, len_s[0] - 1)
        kv = kv_all[l].reshape(keys, LANES)
        s = lax.dot_general(qbuf[...], kv, NT, preferred_element_type=F32)
        s = jnp.where(allowed, s, -1e30)
        e = jnp.exp(s - jnp.max(s, axis=-1, keepdims=True))
        p = (e * (1.0 / jnp.sum(e, axis=-1, keepdims=True))).astype(BF16)
        o = jnp.dot(p, kv, preferred_element_type=F32)
        for pair in range(hq // LANES):
            even, odd = (o[h * rows:(h + 1) * rows] for h in (2 * pair, 2 * pair + 1))
            c_mat[l, :, c_columns(pair)] = jnp.where(low_half, pltpu.roll(even, LANES - hd, 1), odd).astype(BF16)
        for i in far_z:
            c_copy(l, mz, pl.ds(0, rows), i, z_peer(i)).start()

    @scoped
    def out_proj(l):
        with jax.named_scope('wo_wait'):
            wo_copy(l).wait()
        for i in [0] + far_z:
            src = (mz + nz - i) % nz
            cols = pl.ds(pl.multiple_of(src * hq, hq), hq)
            if i:
                with jax.named_scope('c_wait'):
                    c_copy(l, src, pl.ds(0, rows), i, me).wait_recv()
            part = jnp.dot(c_mat[l, :, cols], wo_v[l, cols, :], preferred_element_type=F32)
            acc[...] = acc[...] + part if i else part

    group = CHUNK // units
    n_groups = len(GROUPS)
    assert group == 2 * len(GROUPS[0])

    def slab(l, g, first, cols):
        parts = [w_all[l, c, slot(0, px + dx, py + dy), pl.ds(first, units), cols] for c in range(2) for dx, dy in GROUPS[g]]
        return jnp.concatenate(parts, axis=0)

    @scoped
    def mlp_units(l, gs):
        block = lax.broadcasted_iota(jnp.int32, (rows, CHUNK), 1) // units
        for g in gs:
            every = pl.ds(0, d_model)
            gate = lax.dot_general(zb[...], slab(l, g, 0, every), NT, preferred_element_type=F32)
            up = lax.dot_general(zb[...], slab(l, g, units, every), NT, preferred_element_type=F32)
            act = gate * (1.0 / (1.0 + jnp.exp(-gate))) * up
            for b in range(group):
                bd[g, pl.ds(b * rows, rows)] = jnp.where(block == b, act, 0.0).astype(BF16)

    two_step = nz == 8

    def ps_of(l, n, i):
        return ps.at[l, n, (mz + i + nz) % nz]

    def rs_start(l, n):
        if not two_step:
            for k, i in enumerate(far_z):
                remote(ps_of(l, n, i), rs.at[l, n, k], rs_send.at[l], rs_recv.at[l, n], z_peer(i)).start()
            return
        for side, to in ((0, nz - 2), (1, 2)):
            cols = pl.ds(side * LANES, LANES)
            remote(ps.at[l, n, (mz + 4) % nz, :, cols], ra.at[l, n, 2, :, cols], rs_send.at[l], ra_recv.at[l, n], z_peer(to)).start()
        for side, to in ((0, nz - 1), (1, 1)):
            remote(ps_of(l, n, 3 * (to if to == 1 else -1)), ra.at[l, n, side], rs_send.at[l], ra_recv.at[l, n], z_peer(to)).start()
        for side, to in ((0, nz - 1), (1, 1)):
            remote(ps_of(l, n, to), rs.at[l, n, side], rs_send.at[l], rs_recv.at[l, n], z_peer(to)).start()

    @scoped
    def rs_middle(l):
        if not two_step:
            return

        @pl.loop(0, nch)
        def _(n):
            ref = ra.at[l, n]
            remote(ref, ref, rs_send.at[l], ra_recv.at[l, n], me).wait_recv()
            for side, to in ((0, nz - 2), (1, 2)):
                cols = pl.ds(side * LANES, LANES)
                sb[l, n, side] = ps[l, n, (mz + to) % nz] + ra[l, n, side]
                sb[l, n, side, :, cols] = sb[l, n, side, :, cols] + ra[l, n, 2, :, cols]
                remote(sb.at[l, n, side], rs.at[l, n, 2 + side], rs_send.at[l], rs_recv.at[l, n], z_peer(to)).start()

    @scoped
    def mlp_down(l):
        @pl.loop(0, nch)
        def _(n):
            cols = pl.ds(pl.multiple_of(n * CHUNK, CHUNK), CHUNK)
            total = jnp.zeros((rows, CHUNK), F32)
            for g in range(n_groups):
                y = jnp.dot(bd[g], slab(l, g, 2 * units, cols), preferred_element_type=F32)
                y = y.astype(BF16).astype(F32)
                for b in range(group):
                    total = total + y[b * rows:(b + 1) * rows]
            ps[l, n] = total.reshape(nz, seq_dev, CHUNK)
            rs_start(l, n)

    n_in = 4 if two_step else nz - 1

    @scoped
    def rs_finish(l, store):
        mine = pl.ds(pl.multiple_of(mz * seq_dev, seq_dev), seq_dev)
        for n in range(nch):
            if n_in:
                ref = rs.at[l, n]
                remote(ref, ref, rs_send.at[l], rs_recv.at[l, n], me).wait_recv()
            total = ps[l, n, mz]
            for k in range(n_in):
                total = total + rs[l, n, k]
            store(n, (hres[mine, n * CHUNK:(n + 1) * CHUNK] + total).astype(BF16))

    def store_next(l):
        def store(n, x):
            h_all[l + 1, mz, :, n * CHUNK:(n + 1) * CHUNK] = x
            if n % 2 or nch == 1:
                first = max(n - 1, 0) * CHUNK
                h_start(l + 1, first, (n + 1) * CHUNK - first)
        return store

    with jax.named_scope('small'):
        for c in small:
            c.wait()
        rope_tables()
    with jax.named_scope('barrier'):
        barrier_wait()
    h_start(0, 0, d_model)
    p1(0)
    p3(0, (0,))
    start_later_copies()
    p2(0)
    for l in range(layers):
        more = l + 1 < layers
        h_wait(l)
        norm_to_zb(l, ga)
        qkv(l)
        if l == 0:
            p3(0, (1, 3, 2))
            p4(0, (0,))
        else:
            p4(l, (3, 2))
        kv_wait(l)
        attention(l)
        if l == 0:
            p4(0, (1, 3))
            p5(0, (0,))
            p4(0, (2,))
        else:
            p5(l, (0, 1, 3, 2))
        if more:
            p1(l + 1)
            p3(l + 1, (0,))
        out_proj(l)
        norm_to_zb(l, gm, True)
        if l == 0:
            w_done(l, (0,))
            mlp_units(l, (0,))
            w_done(l, (1,))
            mlp_units(l, (1,))
            p5(l, (1, 3))
            w_done(l, (2,))
            mlp_units(l, (2,))
            p5(l, (2,))
            w_done(l, (3,))
            mlp_units(l, (3,))
        else:
            w_done(l, range(n_groups))
            mlp_units(l, range(n_groups))
        mlp_down(l)
        if more:
            p2(l + 1)
            p3(l + 1, (1, 3))
        rs_middle(l)
        if more:
            p3(l + 1, (2,))
            p4(l + 1, (0,))
            rs_finish(l, store_next(l))
            p4(l + 1, (1,))
    pieces = []
    rs_finish(layers - 1, lambda n, x: pieces.append(x.astype(F32)))
    x = jnp.concatenate(pieces, axis=1)
    inv = lax.rsqrt(jnp.mean(x * x, axis=-1, keepdims=True) + NORM_EPS)
    gain = gf[...].astype(F32)
    for i in range(d_model // LANES):
        cols = slice(i * LANES, (i + 1) * LANES)
        out_ref[:, cols] = x[:, cols] * inv * gain[i:i + 1]

    with jax.named_scope('drain'):
      for l in range(layers):
          ref = w_all.at[l, 0, pl.ds(0, PLANE - 1)]
          remote(ref, ref, w_send.at[l], w_recv.at[l, 0, 0], me).wait_send()
          ref = w_all.at[l, 0]
          remote(ref, ref, d_send.at[l], d_recv.at[l, 0], me).wait_send()
          ref = kv_all.at[l, 0, pl.ds(0, PLANE - 1)]
          remote(ref, ref, kv_send.at[l], kv_recv.at[l], me).wait_send()
          ref = kv_all.at[l, 0]
          remote(ref, ref, kvd_send.at[l], kvd_recv.at[l], me).wait_send()
          if nz > 1:
              ref = h_all.at[l, pl.ds(0, nz - 1)]
              remote(ref, ref, h_send.at[l], h_recv.at[l, 0], me).wait_send()
              ref = c_mat.at[l, :, pl.ds(0, (nz - 1) * hq)]
              remote(ref, ref, c_send.at[l], c_recv.at[l, 0], me).wait_send()
              ref = ps.at[l, :, pl.ds(0, nz - 1)]
              remote(ref, ref, rs_send.at[l], rs_recv.at[l, 0], me).wait_send()


def solution(mesh):
    nz = mesh.shape['tp'] // (2 * PLANE)

    def device_fn(hidden_in, lengths, attn_norm, w_query, w_key, w_value, w_out, mlp_norm, w_gate, w_up, w_down, final_norm):
        seq_dev, d_model = hidden_in.shape[1:]
        layers, _, heads, hd = w_query.shape
        kv_heads = w_key.shape[2]
        units = w_gate.shape[2]
        assert kv_heads == nz and 2 * hd == LANES and heads % nz == 0
        hq = heads // nz * hd
        rows = nz * seq_dev
        nch = d_model // CHUNK
        n_groups = 2 * PLANE * units // CHUNK
        dev, row = np.arange(2 * PLANE)[:, None], np.arange(rows)[None, :]
        pos = (row // seq_dev) * (2 * PLANE * seq_dev) + dev * seq_dev + row % seq_dev
        freq = np.float32(ROPE_BASE) ** (np.float32(-2.0) * np.arange(hd // 2, dtype=np.float32) / np.float32(hd))
        angles = (pos[..., None].astype(np.float32) * freq).astype(np.float64)
        rope = np.tile(np.concatenate([np.cos(angles), np.sin(angles)], axis=-1), (1, 1, 2)).astype(np.float32)
        by_rows = lambda w: jnp.transpose(w, (0, 2, 3, 1)).reshape(layers, -1, d_model)
        units_first = lambda w: jnp.transpose(w, (0, 2, 1))
        hbm, vmem = (pl.BlockSpec(memory_space=s) for s in (pltpu.HBM, pltpu.VMEM))
        dma = pltpu.SemaphoreType.DMA
        out = pl.pallas_call(
            functools.partial(kernel, nz),
            name='decoder',
            out_shape=jax.ShapeDtypeStruct((seq_dev, d_model), F32),
            in_specs=[hbm] * 13,
            out_specs=vmem,
            scratch_shapes=[
                pltpu.VMEM((layers, 2, PLANE, 3 * units, d_model), BF16),
                pltpu.VMEM((layers, heads * hd, d_model), BF16),
                pltpu.VMEM((layers, hq + 2 * hd, d_model), BF16),
                pltpu.VMEM((layers, nz, seq_dev, d_model), BF16),
                pltpu.VMEM((layers, rows, heads * hd), BF16),
                pltpu.VMEM((layers, 2, PLANE, rows, LANES), BF16),
                pltpu.VMEM((layers, nch, 4 if nz == 8 else max(nz - 1, 1), seq_dev, CHUNK), F32),
                pltpu.VMEM((layers, nch, 3, seq_dev, CHUNK), F32),
                pltpu.VMEM((layers, nch, 2, seq_dev, CHUNK), F32),
                pltpu.VMEM((layers, nch, nz, seq_dev, CHUNK), F32),
                pltpu.VMEM((rows, d_model), F32),
                pltpu.VMEM((rows, d_model), F32),
                pltpu.VMEM((rows, d_model), BF16),
                pltpu.VMEM((hq // hd * rows, LANES), BF16),
                pltpu.VMEM((n_groups, CHUNK // units * rows, CHUNK), BF16),
                pltpu.VMEM((rows, LANES), F32), pltpu.VMEM((rows, LANES), F32), pltpu.VMEM((rows, LANES), F32),
                pltpu.VMEM((layers, d_model), BF16), pltpu.VMEM((layers, d_model), BF16),
                pltpu.VMEM((d_model // LANES, LANES), BF16),
                pltpu.SMEM((1,), jnp.int32),
                dma((layers, 7)), dma((6,)), dma((layers, 2, 20)), dma((layers,)),
                dma((layers, 4)), dma((layers,)),
                dma((layers, nz)), dma((layers,)), dma((layers,)), dma((layers,)), dma((layers,)), dma((layers,)),
                dma((layers, nz)), dma((layers,)), dma((layers, nch)), dma((layers, nch)), dma((layers,)),
            ],
            compiler_params=pltpu.CompilerParams(
                collective_id=0, has_side_effects=True, vmem_limit_bytes=67_043_328),
        )(hidden_in[0], lengths, jnp.asarray(rope), attn_norm, mlp_norm, final_norm.reshape(-1, LANES), by_rows(w_query), by_rows(w_key), by_rows(w_value),
          w_out.reshape(layers, heads * hd, d_model), units_first(w_gate), units_first(w_up), w_down)
        return out.astype(BF16)[None]

    seq_part = P(None, 'tp', None)
    in_specs = (seq_part, P(), P(), P(), P(), P(), P(), P(), P(None, None, 'tp'), P(None, None, 'tp'), P(None, 'tp', None), P())
    return jax.shard_map(device_fn, mesh=mesh, in_specs=in_specs, out_specs=seq_part, check_vma=False)
```

```python
import functools

import jax
import jax.numpy as jnp
import numpy as np
from jax import lax
from jax.experimental import pallas as pl
from jax.experimental.pallas import tpu as pltpu
from jax.sharding import PartitionSpec as P

NORM_EPS = 1e-5
ROPE_BASE = 500000.0
NX = 4
PLANE = NX * NX
LANES = 128
CHUNK = 256
NT = (((1,), (1,)), ((), ()))
F32, BF16 = jnp.float32, jnp.bfloat16


def remote(src, dst, send_sem, recv_sem, device):
    return pltpu.make_async_remote_copy(
        src_ref=src, dst_ref=dst, send_sem=send_sem, recv_sem=recv_sem,
        device_id=(device,), device_id_type=pl.DeviceIdType.MESH)


def scoped(f):
    @functools.wraps(f)
    def wrapped(*args):
        with jax.named_scope(f.__name__ + ('#l=%d' % args[0])):
            return f(*args)
    return wrapped


def kernel(nz, h_ref, len_ref, rope_ref, ga_ref, gm_ref, gf_ref, wq_ref, wk_ref, wv_ref, wo_ref, wg_ref, wu_ref, wd_ref,
           out_ref, w_all, wo_v, wqkv, h_all, c_mat, kv_all, rs, ra, sb, ps, acc, hres, zb, qbuf, bd, rope, cos_t, sin_t, ga, gm, gf, len_s,
           local_sem, in_sem, w_recv, w_send, d_recv, d_send, h_recv, h_send, kv_recv, kv_send, kvd_recv, kvd_send,
           c_recv, c_send, rs_recv, ra_recv, rs_send):
    layers = wo_ref.shape[0]
    seq_dev, d_model = h_ref.shape
    units = wg_ref.shape[1]
    pack = 3 * units
    half = pack // 2
    rows = nz * seq_dev
    hq = wq_ref.shape[1] // nz
    hd = wk_ref.shape[1] // nz
    nch = d_model // CHUNK
    me = lax.axis_index('tp')
    core = me % 2
    px = (me // 2) % NX
    py = (me // (2 * NX)) % NX
    mp = (me // 2) % PLANE
    mz = me // (2 * PLANE)
    base = mz * (2 * PLANE)
    partner = base + mp * 2 + (1 - core)

    def z_peer(i):
        return ((mz + i) % nz) * (2 * PLANE) + mp * 2 + core

    far_z = sorted(range(1, nz), key=lambda i: -min(i, nz - i))
    def plane_peer(dy, dx):
        return base + ((py + dy) % NX * NX + (px + dx) % NX) * 2 + core

    far_plane = sorted(((dy, dx) for dy in range(NX) for dx in range(NX) if dy or dx),
                       key=lambda d: -sum(min(i, NX - i) for i in d))

    barrier = pltpu.get_barrier_semaphore()

    def signal(device):
        pl.semaphore_signal(barrier, inc=1, device_id=(device,), device_id_type=pl.DeviceIdType.MESH)

    for i in far_z:
        signal(z_peer(i))
    for d in far_plane:
        signal(plane_peer(*d))
    signal(partner)

    def pack_copies(l):
        mine = w_all.at[l, core, mp]
        return [pltpu.make_async_copy(ref.at[l], mine.at[pl.ds(i * units, units)], local_sem.at[l, i])
                for i, ref in enumerate((wg_ref, wu_ref, wd_ref))]

    def qkv_copies(l):
        return [
            pltpu.make_async_copy(wq_ref.at[l, pl.ds(mz * hq, hq)], wqkv.at[l, pl.ds(0, hq)], local_sem.at[l, 3]),
            pltpu.make_async_copy(wk_ref.at[l, pl.ds(mz * hd, hd)], wqkv.at[l, pl.ds(hq, hd)], local_sem.at[l, 4]),
            pltpu.make_async_copy(wv_ref.at[l, pl.ds(mz * hd, hd)], wqkv.at[l, pl.ds(hq + hd, hd)], local_sem.at[l, 5]),
        ]

    def wo_copy(l):
        return pltpu.make_async_copy(wo_ref.at[l], wo_v.at[l], local_sem.at[l, 6])

    small = [pltpu.make_async_copy(src, dst, in_sem.at[i]) for i, (src, dst) in enumerate((
        (h_ref, h_all.at[0, mz]), (rope_ref.at[mp * 2 + core], rope), (ga_ref, ga), (gm_ref, gm), (gf_ref, gf), (len_ref, len_s)))]
    for c in small:
        c.start()
    for c in pack_copies(0) + qkv_copies(0):
        c.start()

    def start_later_copies():
        wo_copy(0).start()
        for l in range(1, layers):
            for c in pack_copies(l) + qkv_copies(l):
                c.start()
            wo_copy(l).start()

    def barrier_wait():
        pl.semaphore_wait(barrier, 1 + (nz - 1) + (PLANE - 1))

    def slot(h, a1, a2):
        return a2 % NX * NX + a1 % NX if h == 0 else a1 % NX * NX + a2 % NX

    def where_am_i(h):
        return (px, py) if h == 0 else (py, px)

    def at(h, a1, a2):
        return base + slot(h, a1, a2) * 2 + core

    third = half // 3
    SPAN = ((0, half), (half, half))

    def from_minus(h, k):
        return (h * half, 2 * third if (k in (1, 2)) != (h == 1) else third)

    def from_plus(h, k):
        first, size = from_minus(h, k)
        return (first + size, half - size)

    def piece(l, c, p, span):
        return w_all.at[l, c, p, pl.ds(*span)]

    def w_copy(l, h, p, span, idx, device):
        ref = piece(l, core, p, span)
        return remote(ref, ref, w_send.at[l], w_recv.at[l, h, idx], device)

    GROUPS = (((0, 0), (1, 0), (3, 0), (0, 1)), ((0, 3), (2, 0), (0, 2), (1, 1)),
              ((1, 3), (3, 1), (3, 3), (2, 1)), ((2, 3), (1, 2), (3, 2), (2, 2)))
    GROUP_OF = {d: g for g, ds in enumerate(GROUPS) for d in ds}

    def to_partner(l, h, k1, k2, span):
        a1, a2 = where_am_i(h)
        ref = piece(l, core, slot(h, a1 + k1, a2 + k2), span)
        g = GROUP_OF[(k1, k2) if h == 0 else (k2, k1)]
        remote(ref, ref, d_send.at[l], d_recv.at[l, g], partner).start()

    @scoped
    def p1(l):
        for c in pack_copies(l):
            c.wait()
        for h in range(2):
            a1, a2 = where_am_i(h)
            w_copy(l, h, mp, SPAN[h], 0, at(h, a1 + 1, a2)).start()
            w_copy(l, h, mp, SPAN[h], 1, at(h, a1 + NX - 1, a2)).start()
        to_partner(l, 0, 0, 0, (0, pack))

    @scoped
    def p2(l):
        for h in range(2):
            a1, a2 = where_am_i(h)
            low, high = slot(h, a1 + NX - 1, a2), slot(h, a1 + 1, a2)
            w_copy(l, h, low, SPAN[h], 0, me).wait_recv()
            w_copy(l, h, low, from_minus(h, 0), 2, at(h, a1 + 1, a2)).start()
            w_copy(l, h, high, SPAN[h], 1, me).wait_recv()
            w_copy(l, h, high, from_plus(h, 0), 3, at(h, a1 + NX - 1, a2)).start()
            to_partner(l, h, NX - 1, 0, SPAN[h])
            to_partner(l, h, 1, 0, SPAN[h])

    @scoped
    def p3(l, ks):
        for k in ks:
            for h in range(2):
                a1, a2 = where_am_i(h)
                p = slot(h, a1 + k, a2)
                if k == 2:
                    w_copy(l, h, p, from_minus(h, 0), 2, me).wait_recv()
                    w_copy(l, h, p, from_plus(h, 0), 3, me).wait_recv()
                    to_partner(l, h, k, 0, SPAN[h])
                w_copy(l, h, p, SPAN[h], 4 + k, at(h, a1, a2 + 1)).start()
                w_copy(l, h, p, SPAN[h], 8 + k, at(h, a1, a2 + NX - 1)).start()

    @scoped
    def p4(l, ks):
        for k in ks:
            for h in range(2):
                a1, a2 = where_am_i(h)
                low, high = slot(h, a1 + k, a2 + NX - 1), slot(h, a1 + k, a2 + 1)
                w_copy(l, h, low, SPAN[h], 4 + k, me).wait_recv()
                w_copy(l, h, low, from_minus(h, k), 12 + k, at(h, a1, a2 + 1)).start()
                w_copy(l, h, high, SPAN[h], 8 + k, me).wait_recv()
                w_copy(l, h, high, from_plus(h, k), 16 + k, at(h, a1, a2 + NX - 1)).start()
                to_partner(l, h, k, NX - 1, SPAN[h])
                to_partner(l, h, k, 1, SPAN[h])

    @scoped
    def p5(l, ks):
        for k in ks:
            for h in range(2):
                a1, a2 = where_am_i(h)
                p = slot(h, a1 + k, a2 + 2)
                w_copy(l, h, p, from_minus(h, k), 12 + k, me).wait_recv()
                w_copy(l, h, p, from_plus(h, k), 16 + k, me).wait_recv()
                to_partner(l, h, k, 2, SPAN[h])

    @scoped
    def w_done(l, gs):
        for g in gs:
            ref = w_all.at[l, 1 - core, pl.ds(0, len(GROUPS[g]))]
            remote(ref, ref, d_send.at[l], d_recv.at[l, g], partner).wait_recv()

    def h_copy(l, src, first, size, i, device):
        ref = h_all.at[l, src, :, pl.ds(first, size)]
        return remote(ref, ref, h_send.at[l], h_recv.at[l, i], device)

    def h_start(l, first, size):
        for i in far_z:
            h_copy(l, mz, first, size, i, z_peer(i)).start()

    def h_take(l, i):
        h_copy(l, (mz + nz - i) % nz, 0, d_model, i, me).wait_recv()

    @scoped
    def h_wait(l):
        for i in far_z:
            h_take(l, i)
        for i in range(nz):
            hres[pl.ds(i * seq_dev, seq_dev)] = h_all[l, i].astype(F32)

    @scoped
    def norm_to_zb(l, gains, residual=False):
        gain = gains[...].astype(F32)[l:l + 1]
        step = min(16, rows)
        for first in range(0, rows, step):
            r = pl.ds(first, step)
            x = hres[r]
            if residual:
                x = (x + acc[r]).astype(BF16).astype(F32)
                hres[r] = x
            inv = lax.rsqrt(jnp.mean(x * x, axis=-1, keepdims=True) + NORM_EPS)
            zb[r] = (x * inv * gain).astype(BF16)

    lane = lax.broadcasted_iota(jnp.int32, (rows, LANES), 1)
    low_half = lane < hd

    def rotate(x):
        first = (lane % hd) < hd // 2
        swapped = jnp.where(first, pltpu.roll(x, LANES - hd // 2, 1), pltpu.roll(x, hd // 2, 1))
        return x * cos_t[...] + swapped * sin_t[...]

    def rope_tables():
        first = (lane % hd) < hd // 2
        t = rope[...]
        cos_t[...] = jnp.where(first, t, pltpu.roll(t, hd // 2, 1))
        sin_t[...] = jnp.where(first, -pltpu.roll(t, LANES - hd // 2, 1), t)

    def kv_copy(l, device):
        ref = kv_all.at[l, core, mp]
        return remote(ref, ref, kv_send.at[l], kv_recv.at[l], device)

    @scoped
    def qkv(l):
        for c in qkv_copies(l):
            c.wait()
        kv = lax.dot_general(zb[...], wqkv[l, pl.ds(hq, 2 * hd), :], NT, preferred_element_type=F32)
        kv_all[l, core, mp] = jnp.where(low_half, rotate(kv), kv).astype(BF16)
        for d in far_plane:
            kv_copy(l, plane_peer(*d)).start()
        proj = lax.dot_general(zb[...], wqkv[l, pl.ds(0, hq), :], NT, preferred_element_type=F32)
        for j in range(hq // LANES):
            q = rotate(proj[:, j * LANES:(j + 1) * LANES]) * (hd ** -0.5)
            for half_head, x in enumerate((q, pltpu.roll(q, LANES - hd, 1))):
                head = 2 * j + half_head
                qbuf[pl.ds(head * rows, rows)] = jnp.where(low_half, x, 0.0).astype(BF16)

    @scoped
    def kv_wait(l):
        ref = kv_all.at[l, core, pl.ds(0, PLANE - 1)]
        remote(ref, ref, kv_send.at[l], kv_recv.at[l], me).wait_recv()
        ref = kv_all.at[l, core]
        remote(ref, ref, kvd_send.at[l], kvd_recv.at[l], partner).start()
        ref = kv_all.at[l, 1 - core]
        remote(ref, ref, kvd_send.at[l], kvd_recv.at[l], partner).wait_recv()

    def c_columns(j):
        return pl.ds(pl.multiple_of(mz * hq + j * LANES, LANES), LANES)

    def c_copy(l, src, r, i, device):
        ref = c_mat.at[l, r, pl.ds(pl.multiple_of(src * hq, hq), hq)]
        return remote(ref, ref, c_send.at[l], c_recv.at[l, i], device)

    @scoped
    def attention(l):
        keys = 2 * PLANE * rows
        j = lax.broadcasted_iota(jnp.int32, (1, keys), 1)
        key_pos = ((j // seq_dev) % nz) * (2 * PLANE * seq_dev) + ((j // rows) % PLANE) * (2 * seq_dev) \
            + (j // (PLANE * rows)) * seq_dev + j % seq_dev
        i = lax.broadcasted_iota(jnp.int32, (hq // hd * rows, 1), 0) % rows
        q_pos = (i // seq_dev) * (2 * PLANE * seq_dev) + (mp * 2 + core) * seq_dev + i % seq_dev
        allowed = key_pos <= jnp.minimum(q_pos, len_s[0] - 1)
        kv = kv_all[l].reshape(keys, LANES)
        s = lax.dot_general(qbuf[...], kv, NT, preferred_element_type=F32)
        s = jnp.where(allowed, s, -1e30)
        e = jnp.exp(s - jnp.max(s, axis=-1, keepdims=True))
        p = (e * (1.0 / jnp.sum(e, axis=-1, keepdims=True))).astype(BF16)
        o = jnp.dot(p, kv, preferred_element_type=F32)
        for pair in range(hq // LANES):
            even, odd = (o[h * rows:(h + 1) * rows] for h in (2 * pair, 2 * pair + 1))
            c_mat[l, :, c_columns(pair)] = jnp.where(low_half, pltpu.roll(even, LANES - hd, 1), odd).astype(BF16)
        for i in far_z:
            c_copy(l, mz, pl.ds(0, rows), i, z_peer(i)).start()

    @scoped
    def out_proj(l):
        with jax.named_scope('wo_wait'):
            wo_copy(l).wait()
        for i in [0] + far_z[::-1]:
            src = (mz + nz - i) % nz
            cols = pl.ds(pl.multiple_of(src * hq, hq), hq)
            if i:
                with jax.named_scope('c_wait'):
                    c_copy(l, src, pl.ds(0, rows), i, me).wait_recv()
            part = jnp.dot(c_mat[l, :, cols], wo_v[l, cols, :], preferred_element_type=F32)
            acc[...] = acc[...] + part if i else part

    group = CHUNK // units
    n_groups = len(GROUPS)
    assert group == 2 * len(GROUPS[0])

    def slab(l, g, first, cols):
        parts = [w_all[l, c, slot(0, px + dx, py + dy), pl.ds(first, units), cols] for c in range(2) for dx, dy in GROUPS[g]]
        return jnp.concatenate(parts, axis=0)

    @scoped
    def mlp_units(l, gs):
        block = lax.broadcasted_iota(jnp.int32, (rows, CHUNK), 1) // units
        for g in gs:
            every = pl.ds(0, d_model)
            gate = lax.dot_general(zb[...], slab(l, g, 0, every), NT, preferred_element_type=F32)
            up = lax.dot_general(zb[...], slab(l, g, units, every), NT, preferred_element_type=F32)
            act = gate * (1.0 / (1.0 + jnp.exp(-gate))) * up
            for b in range(group):
                bd[g, pl.ds(b * rows, rows)] = jnp.where(block == b, act, 0.0).astype(BF16)

    two_step = nz == 8

    def ps_of(l, n, i):
        return ps.at[l, n, (mz + i + nz) % nz]

    def rs_start(l, n):
        if not two_step:
            for k, i in enumerate(far_z):
                remote(ps_of(l, n, i), rs.at[l, n, k], rs_send.at[l], rs_recv.at[l, n], z_peer(i)).start()
            return
        for side, to in ((0, nz - 2), (1, 2)):
            cols = pl.ds(side * LANES, LANES)
            remote(ps.at[l, n, (mz + 4) % nz, :, cols], ra.at[l, n, 2, :, cols], rs_send.at[l], ra_recv.at[l, n], z_peer(to)).start()
        for side, to in ((0, nz - 1), (1, 1)):
            remote(ps_of(l, n, 3 * (to if to == 1 else -1)), ra.at[l, n, side], rs_send.at[l], ra_recv.at[l, n], z_peer(to)).start()

    @scoped
    def rs_middle(l):
        if not two_step:
            return

        @pl.loop(0, nch)
        def _(n):
            ref = ra.at[l, n]
            remote(ref, ref, rs_send.at[l], ra_recv.at[l, n], me).wait_recv()
            for side, to in ((0, nz - 2), (1, 2)):
                cols = pl.ds(side * LANES, LANES)
                sb[l, n, side] = ps[l, n, (mz + to) % nz] + ra[l, n, side]
                sb[l, n, side, :, cols] = sb[l, n, side, :, cols] + ra[l, n, 2, :, cols]
                remote(sb.at[l, n, side], rs.at[l, n, 2 + side], rs_send.at[l], rs_recv.at[l, n], z_peer(to)).start()
            for side, to in ((0, nz - 1), (1, 1)):
                remote(ps_of(l, n, to), rs.at[l, n, side], rs_send.at[l], rs_recv.at[l, n], z_peer(to)).start()

    @scoped
    def mlp_down(l):
        @pl.loop(0, nch)
        def _(n):
            cols = pl.ds(pl.multiple_of(n * CHUNK, CHUNK), CHUNK)
            total = jnp.zeros((rows, CHUNK), F32)
            for g in range(n_groups):
                y = jnp.dot(bd[g], slab(l, g, 2 * units, cols), preferred_element_type=F32)
                y = y.astype(BF16).astype(F32)
                for b in range(group):
                    total = total + y[b * rows:(b + 1) * rows]
            ps[l, n] = total.reshape(nz, seq_dev, CHUNK)
            rs_start(l, n)

    n_in = 4 if two_step else nz - 1

    @scoped
    def rs_finish(l, store):
        mine = pl.ds(pl.multiple_of(mz * seq_dev, seq_dev), seq_dev)
        for n in range(nch):
            if n_in:
                ref = rs.at[l, n]
                remote(ref, ref, rs_send.at[l], rs_recv.at[l, n], me).wait_recv()
            total = ps[l, n, mz]
            for k in range(n_in):
                total = total + rs[l, n, k]
            store(n, (hres[mine, n * CHUNK:(n + 1) * CHUNK] + total).astype(BF16))

    def store_next(l):
        def store(n, x):
            h_all[l + 1, mz, :, n * CHUNK:(n + 1) * CHUNK] = x
            if n % 2 or nch == 1:
                first = max(n - 1, 0) * CHUNK
                h_start(l + 1, first, (n + 1) * CHUNK - first)
        return store

    with jax.named_scope('small'):
        for c in small:
            c.wait()
        rope_tables()
    with jax.named_scope('barrier'):
        barrier_wait()
    h_start(0, 0, d_model)
    p1(0)
    p3(0, (0,))
    start_later_copies()
    p2(0)
    for l in range(layers):
        more = l + 1 < layers
        h_wait(l)
        norm_to_zb(l, ga)
        qkv(l)
        if l == 0:
            p3(0, (1, 3, 2))
            p4(0, (0,))
        else:
            p4(l, (0, 1, 3, 2))
        kv_wait(l)
        attention(l)
        if l == 0:
            p4(0, (1, 3, 2))
            p5(0, (0,))
        else:
            p5(l, (0, 1, 3, 2))
        if more:
            p1(l + 1)
            p3(l + 1, (0,))
        out_proj(l)
        norm_to_zb(l, gm, True)
        if l == 0:
            w_done(l, (0,))
            mlp_units(l, (0,))
            w_done(l, (1,))
            mlp_units(l, (1,))
            p5(l, (1, 3))
            w_done(l, (2,))
            mlp_units(l, (2,))
            p5(l, (2,))
            w_done(l, (3,))
            mlp_units(l, (3,))
        else:
            w_done(l, range(n_groups))
            mlp_units(l, range(n_groups))
        mlp_down(l)
        if more:
            p2(l + 1)
            p3(l + 1, (1, 3))
        rs_middle(l)
        if more:
            rs_finish(l, store_next(l))
            p3(l + 1, (2,))
    pieces = []
    rs_finish(layers - 1, lambda n, x: pieces.append(x.astype(F32)))
    x = jnp.concatenate(pieces, axis=1)
    inv = lax.rsqrt(jnp.mean(x * x, axis=-1, keepdims=True) + NORM_EPS)
    gain = gf[...].astype(F32)
    for i in range(d_model // LANES):
        cols = slice(i * LANES, (i + 1) * LANES)
        out_ref[:, cols] = x[:, cols] * inv * gain[i:i + 1]

    with jax.named_scope('drain'):
      for l in range(layers):
          ref = w_all.at[l, 0, pl.ds(0, PLANE - 1)]
          remote(ref, ref, w_send.at[l], w_recv.at[l, 0, 0], me).wait_send()
          ref = w_all.at[l, 0]
          remote(ref, ref, d_send.at[l], d_recv.at[l, 0], me).wait_send()
          ref = kv_all.at[l, 0, pl.ds(0, PLANE - 1)]
          remote(ref, ref, kv_send.at[l], kv_recv.at[l], me).wait_send()
          ref = kv_all.at[l, 0]
          remote(ref, ref, kvd_send.at[l], kvd_recv.at[l], me).wait_send()
          if nz > 1:
              ref = h_all.at[l, pl.ds(0, nz - 1)]
              remote(ref, ref, h_send.at[l], h_recv.at[l, 0], me).wait_send()
              ref = c_mat.at[l, :, pl.ds(0, (nz - 1) * hq)]
              remote(ref, ref, c_send.at[l], c_recv.at[l, 0], me).wait_send()
              ref = ps.at[l, :, pl.ds(0, nz - 1)]
              remote(ref, ref, rs_send.at[l], rs_recv.at[l, 0], me).wait_send()


def solution(mesh):
    nz = mesh.shape['tp'] // (2 * PLANE)

    def device_fn(hidden_in, lengths, attn_norm, w_query, w_key, w_value, w_out, mlp_norm, w_gate, w_up, w_down, final_norm):
        seq_dev, d_model = hidden_in.shape[1:]
        layers, _, heads, hd = w_query.shape
        kv_heads = w_key.shape[2]
        units = w_gate.shape[2]
        assert kv_heads == nz and 2 * hd == LANES and heads % nz == 0
        hq = heads // nz * hd
        rows = nz * seq_dev
        nch = d_model // CHUNK
        n_groups = 2 * PLANE * units // CHUNK
        dev, row = np.arange(2 * PLANE)[:, None], np.arange(rows)[None, :]
        pos = (row // seq_dev) * (2 * PLANE * seq_dev) + dev * seq_dev + row % seq_dev
        freq = np.float32(ROPE_BASE) ** (np.float32(-2.0) * np.arange(hd // 2, dtype=np.float32) / np.float32(hd))
        angles = (pos[..., None].astype(np.float32) * freq).astype(np.float64)
        rope = np.tile(np.concatenate([np.cos(angles), np.sin(angles)], axis=-1), (1, 1, 2)).astype(np.float32)
        by_rows = lambda w: jnp.transpose(w, (0, 2, 3, 1)).reshape(layers, -1, d_model)
        units_first = lambda w: jnp.transpose(w, (0, 2, 1))
        hbm, vmem = (pl.BlockSpec(memory_space=s) for s in (pltpu.HBM, pltpu.VMEM))
        dma = pltpu.SemaphoreType.DMA
        out = pl.pallas_call(
            functools.partial(kernel, nz),
            name='decoder',
            out_shape=jax.ShapeDtypeStruct((seq_dev, d_model), F32),
            in_specs=[hbm] * 13,
            out_specs=vmem,
            scratch_shapes=[
                pltpu.VMEM((layers, 2, PLANE, 3 * units, d_model), BF16),
                pltpu.VMEM((layers, heads * hd, d_model), BF16),
                pltpu.VMEM((layers, hq + 2 * hd, d_model), BF16),
                pltpu.VMEM((layers, nz, seq_dev, d_model), BF16),
                pltpu.VMEM((layers, rows, heads * hd), BF16),
                pltpu.VMEM((layers, 2, PLANE, rows, LANES), BF16),
                pltpu.VMEM((layers, nch, 4 if nz == 8 else max(nz - 1, 1), seq_dev, CHUNK), F32),
                pltpu.VMEM((layers, nch, 3, seq_dev, CHUNK), F32),
                pltpu.VMEM((layers, nch, 2, seq_dev, CHUNK), F32),
                pltpu.VMEM((layers, nch, nz, seq_dev, CHUNK), F32),
                pltpu.VMEM((rows, d_model), F32),
                pltpu.VMEM((rows, d_model), F32),
                pltpu.VMEM((rows, d_model), BF16),
                pltpu.VMEM((hq // hd * rows, LANES), BF16),
                pltpu.VMEM((n_groups, CHUNK // units * rows, CHUNK), BF16),
                pltpu.VMEM((rows, LANES), F32), pltpu.VMEM((rows, LANES), F32), pltpu.VMEM((rows, LANES), F32),
                pltpu.VMEM((layers, d_model), BF16), pltpu.VMEM((layers, d_model), BF16),
                pltpu.VMEM((d_model // LANES, LANES), BF16),
                pltpu.SMEM((1,), jnp.int32),
                dma((layers, 7)), dma((6,)), dma((layers, 2, 20)), dma((layers,)),
                dma((layers, 4)), dma((layers,)),
                dma((layers, nz)), dma((layers,)), dma((layers,)), dma((layers,)), dma((layers,)), dma((layers,)),
                dma((layers, nz)), dma((layers,)), dma((layers, nch)), dma((layers, nch)), dma((layers,)),
            ],
            compiler_params=pltpu.CompilerParams(
                collective_id=0, has_side_effects=True, vmem_limit_bytes=67_043_328),
        )(hidden_in[0], lengths, jnp.asarray(rope), attn_norm, mlp_norm, final_norm.reshape(-1, LANES), by_rows(w_query), by_rows(w_key), by_rows(w_value),
          w_out.reshape(layers, heads * hd, d_model), units_first(w_gate), units_first(w_up), w_down)
        return out.astype(BF16)[None]

    seq_part = P(None, 'tp', None)
    in_specs = (seq_part, P(), P(), P(), P(), P(), P(), P(), P(None, None, 'tp'), P(None, None, 'tp'), P(None, 'tp', None), P())
    return jax.shard_map(device_fn, mesh=mesh, in_specs=in_specs, out_specs=seq_part, check_vma=False)
```

```python
import functools

import jax
import jax.numpy as jnp
import numpy as np
from jax import lax
from jax.experimental import pallas as pl
from jax.experimental.pallas import tpu as pltpu
from jax.sharding import PartitionSpec as P

NORM_EPS = 1e-5
ROPE_BASE = 500000.0
NX = 4
PLANE = NX * NX
LANES = 128
CHUNK = 256
NT = (((1,), (1,)), ((), ()))
F32, BF16 = jnp.float32, jnp.bfloat16


def remote(src, dst, send_sem, recv_sem, device):
    return pltpu.make_async_remote_copy(
        src_ref=src, dst_ref=dst, send_sem=send_sem, recv_sem=recv_sem,
        device_id=(device,), device_id_type=pl.DeviceIdType.MESH)


def scoped(f):
    @functools.wraps(f)
    def wrapped(*args):
        with jax.named_scope(f.__name__ + ('#l=%d' % args[0])):
            return f(*args)
    return wrapped


def kernel(nz, h_ref, len_ref, rope_ref, ga_ref, gm_ref, gf_ref, wq_ref, wk_ref, wv_ref, wo_ref, wg_ref, wu_ref, wd_ref,
           out_ref, w_all, wo_v, wqkv, h_all, c_mat, kv_all, rs, ra, sb, ps, acc, hres, zb, qbuf, bd, rope, cos_t, sin_t, ga, gm, gf, len_s,
           local_sem, in_sem, w_recv, w_send, d_recv, d_send, h_recv, h_send, kv_recv, kv_send, kvd_recv, kvd_send,
           c_recv, c_send, rs_recv, ra_recv, rs_send):
    layers = wo_ref.shape[0]
    seq_dev, d_model = h_ref.shape
    units = wg_ref.shape[1]
    pack = 3 * units
    half = pack // 2
    rows = nz * seq_dev
    hq = wq_ref.shape[1] // nz
    hd = wk_ref.shape[1] // nz
    me = lax.axis_index('tp')
    core = me % 2
    px = (me // 2) % NX
    py = (me // (2 * NX)) % NX
    mp = (me // 2) % PLANE
    mz = me // (2 * PLANE)
    base = mz * (2 * PLANE)
    partner = base + mp * 2 + (1 - core)

    def z_peer(i):
        return ((mz + i) % nz) * (2 * PLANE) + mp * 2 + core

    far_z = sorted(range(1, nz), key=lambda i: -min(i, nz - i))
    next_z = far_z[-2:]
    def plane_peer(dy, dx):
        return base + ((py + dy) % NX * NX + (px + dx) % NX) * 2 + core

    far_plane = sorted(((dy, dx) for dy in range(NX) for dx in range(NX) if dy or dx),
                       key=lambda d: -sum(min(i, NX - i) for i in d))

    barrier = pltpu.get_barrier_semaphore()

    def signal(device):
        pl.semaphore_signal(barrier, inc=1, device_id=(device,), device_id_type=pl.DeviceIdType.MESH)

    for i in far_z:
        signal(z_peer(i))
    for d in far_plane:
        signal(plane_peer(*d))
    signal(partner)

    def pack_copies(l):
        mine = w_all.at[l, core, mp]
        return [pltpu.make_async_copy(ref.at[l], mine.at[pl.ds(i * units, units)], local_sem.at[l, 0])
                for i, ref in enumerate((wg_ref, wu_ref, wd_ref))]

    def qkv_copies(l):
        return [pltpu.make_async_copy(ref.at[l, pl.ds(mz * n, n)], wqkv.at[l, pl.ds(first, n)], local_sem.at[l, 1])
                for ref, first, n in ((wq_ref, 0, hq), (wk_ref, hq, hd), (wv_ref, hq + hd, hd))]

    def wo_copy(l):
        return pltpu.make_async_copy(wo_ref.at[l], wo_v.at[l], local_sem.at[l, 2])

    def take(ref, sem):
        remote(ref, ref, w_send.at[0], sem, me).wait_recv()

    def pack_wait(l):
        mine = w_all.at[l, core, mp]
        pltpu.make_async_copy(mine, mine, local_sem.at[l, 0]).wait()

    def qkv_wait(l):
        pltpu.make_async_copy(wqkv.at[l], wqkv.at[l], local_sem.at[l, 1]).wait()

    small = [pltpu.make_async_copy(src, dst, in_sem.at[i]) for i, (src, dst) in enumerate((
        (h_ref, h_all.at[0, mz]), (rope_ref.at[mp * 2 + core], rope), (ga_ref, ga), (gm_ref, gm), (gf_ref, gf), (len_ref, len_s)))]
    for c in small:
        c.start()
    for c in pack_copies(0) + qkv_copies(0):
        c.start()

    def start_later_copies():
        wo_copy(0).start()
        for l in range(1, layers):
            for c in pack_copies(l) + qkv_copies(l):
                c.start()
            wo_copy(l).start()

    def barrier_wait():
        pl.semaphore_wait(barrier, 1 + (nz - 1) + (PLANE - 1))

    def slot(h, a1, a2):
        return a2 % NX * NX + a1 % NX if h == 0 else a1 % NX * NX + a2 % NX

    def where_am_i(h):
        return (px, py) if h == 0 else (py, px)

    def at(h, a1, a2):
        return base + slot(h, a1, a2) * 2 + core

    third = half // 3
    SPAN = ((0, half), (half, half))

    def from_minus(h, k):
        return (h * half, 2 * third if (k in (1, 2)) != (h == 1) else third)

    def from_plus(h, k):
        first, size = from_minus(h, k)
        return (first + size, half - size)

    def piece(l, c, p, span):
        return w_all.at[l, c, p, pl.ds(*span)]

    def w_start(l, p, span, idx, device):
        ref = piece(l, core, p, span)
        remote(ref, ref, w_send.at[l], w_recv.at[l, idx], device).start()

    def w_take(l, idx, packs):
        take(w_all.at[l, core, pl.ds(0, packs)], w_recv.at[l, idx])

    GROUPS = (((0, 0), (1, 0), (3, 0), (0, 1)), ((0, 3), (2, 0), (0, 2), (1, 1)),
              ((1, 3), (3, 1), (3, 3), (2, 1)), ((2, 3), (1, 2), (3, 2), (2, 2)))
    GROUP_OF = {d: g for g, ds in enumerate(GROUPS) for d in ds}

    def to_partner(l, h, k1, k2, span):
        a1, a2 = where_am_i(h)
        ref = piece(l, core, slot(h, a1 + k1, a2 + k2), span)
        g = GROUP_OF[(k1, k2) if h == 0 else (k2, k1)]
        remote(ref, ref, d_send.at[l], d_recv.at[l, g], partner).start()

    @scoped
    def p1(l):
        pack_wait(l)
        for h in range(2):
            a1, a2 = where_am_i(h)
            w_start(l, mp, SPAN[h], 0, at(h, a1 + 1, a2))
            w_start(l, mp, SPAN[h], 0, at(h, a1 + NX - 1, a2))
        to_partner(l, 0, 0, 0, (0, pack))

    @scoped
    def p2(l):
        w_take(l, 0, 2)
        for h in range(2):
            a1, a2 = where_am_i(h)
            w_start(l, slot(h, a1 + NX - 1, a2), from_minus(h, 0), 1, at(h, a1 + 1, a2))
            w_start(l, slot(h, a1 + 1, a2), from_plus(h, 0), 1, at(h, a1 + NX - 1, a2))
            to_partner(l, h, NX - 1, 0, SPAN[h])
            to_partner(l, h, 1, 0, SPAN[h])

    @scoped
    def p3(l, ks):
        for k in ks:
            if k == 2:
                w_take(l, 1, 1)
            for h in range(2):
                a1, a2 = where_am_i(h)
                p = slot(h, a1 + k, a2)
                w_start(l, p, SPAN[h], 2 + k, at(h, a1, a2 + 1))
                w_start(l, p, SPAN[h], 2 + k, at(h, a1, a2 + NX - 1))
                if k == 2:
                    to_partner(l, h, k, 0, SPAN[h])

    @scoped
    def p4(l, ks):
        for k in ks:
            w_take(l, 2 + k, 2)
            for h in range(2):
                a1, a2 = where_am_i(h)
                w_start(l, slot(h, a1 + k, a2 + NX - 1), from_minus(h, k), 6 + k, at(h, a1, a2 + 1))
                w_start(l, slot(h, a1 + k, a2 + 1), from_plus(h, k), 6 + k, at(h, a1, a2 + NX - 1))
                to_partner(l, h, k, NX - 1, SPAN[h])
                to_partner(l, h, k, 1, SPAN[h])

    @scoped
    def p5(l, ks):
        for k in ks:
            w_take(l, 6 + k, 1)
            for h in range(2):
                to_partner(l, h, k, 2, SPAN[h])

    @scoped
    def w_done(l, gs):
        for g in gs:
            take(w_all.at[l, 1 - core, pl.ds(0, len(GROUPS[g]))], d_recv.at[l, g])

    def h_start(l, first, size):
        for i in far_z:
            ref = h_all.at[l, mz, :, pl.ds(first, size)]
            remote(ref, ref, h_send.at[l], h_recv.at[l], z_peer(i)).start()

    @scoped
    def h_wait(l):
        if nz > 1:
            take(h_all.at[l, pl.ds(0, nz - 1)], h_recv.at[l])
        for i in range(nz):
            hres[pl.ds(i * seq_dev, seq_dev)] = h_all[l, i].astype(F32)

    @scoped
    def norm_to_zb(l, gains, residual=False):
        gain = gains[...].astype(F32)[l:l + 1]
        step = min(16, rows)
        for first in range(0, rows, step):
            r = pl.ds(first, step)
            x = hres[r]
            if residual:
                x = (x + acc[r]).astype(BF16).astype(F32)
                hres[r] = x
            inv = lax.rsqrt(jnp.mean(x * x, axis=-1, keepdims=True) + NORM_EPS)
            zb[r] = (x * inv * gain).astype(BF16)

    lane = lax.broadcasted_iota(jnp.int32, (rows, LANES), 1)
    low_half = lane < hd

    def rotate(x):
        first = (lane % hd) < hd // 2
        swapped = jnp.where(first, pltpu.roll(x, LANES - hd // 2, 1), pltpu.roll(x, hd // 2, 1))
        return x * cos_t[...] + swapped * sin_t[...]

    def rope_tables():
        first = (lane % hd) < hd // 2
        t = rope[...]
        cos_t[...] = jnp.where(first, t, pltpu.roll(t, hd // 2, 1))
        sin_t[...] = jnp.where(first, -pltpu.roll(t, LANES - hd // 2, 1), t)

    def kv_copy(l, device):
        ref = kv_all.at[l, core, mp]
        return remote(ref, ref, kv_send.at[l], kv_recv.at[l], device)

    @scoped
    def qkv(l):
        qkv_wait(l)
        kv = lax.dot_general(zb[...], wqkv[l, pl.ds(hq, 2 * hd), :], NT, preferred_element_type=F32)
        kv_all[l, core, mp] = jnp.where(low_half, rotate(kv), kv).astype(BF16)
        for d in far_plane:
            kv_copy(l, plane_peer(*d)).start()
        proj = lax.dot_general(zb[...], wqkv[l, pl.ds(0, hq), :], NT, preferred_element_type=F32)
        for j in range(hq // LANES):
            q = rotate(proj[:, j * LANES:(j + 1) * LANES]) * (hd ** -0.5)
            for half_head, x in enumerate((q, pltpu.roll(q, LANES - hd, 1))):
                head = 2 * j + half_head
                qbuf[pl.ds(head * rows, rows)] = jnp.where(low_half, x, 0.0).astype(BF16)

    @scoped
    def kv_wait(l):
        take(kv_all.at[l, core, pl.ds(0, PLANE - 1)], kv_recv.at[l])
        ref = kv_all.at[l, core]
        remote(ref, ref, kvd_send.at[l], kvd_recv.at[l], partner).start()
        take(kv_all.at[l, 1 - core], kvd_recv.at[l])

    def c_columns(z):
        return pl.ds(pl.multiple_of(z * hq, hq), hq)

    @scoped
    def attention(l):
        keys = 2 * PLANE * rows
        j = lax.broadcasted_iota(jnp.int32, (1, keys), 1)
        key_pos = ((j // seq_dev) % nz) * (2 * PLANE * seq_dev) + ((j // rows) % PLANE) * (2 * seq_dev) \
            + (j // (PLANE * rows)) * seq_dev + j % seq_dev
        i = lax.broadcasted_iota(jnp.int32, (hq // hd * rows, 1), 0) % rows
        q_pos = (i // seq_dev) * (2 * PLANE * seq_dev) + (mp * 2 + core) * seq_dev + i % seq_dev
        allowed = key_pos <= jnp.minimum(q_pos, len_s[0] - 1)
        kv = kv_all[l].reshape(keys, LANES)
        s = lax.dot_general(qbuf[...], kv, NT, preferred_element_type=F32)
        s = jnp.where(allowed, s, -1e30)
        e = jnp.exp(s - jnp.max(s, axis=-1, keepdims=True))
        p = (e * (1.0 / jnp.sum(e, axis=-1, keepdims=True))).astype(BF16)
        o = jnp.dot(p, kv, preferred_element_type=F32)
        for pair in range(hq // LANES):
            even, odd = (o[h * rows:(h + 1) * rows] for h in (2 * pair, 2 * pair + 1))
            c_mat[l, :, pl.ds(pl.multiple_of(mz * hq + pair * LANES, LANES), LANES)] = jnp.where(low_half, pltpu.roll(even, LANES - hd, 1), odd).astype(BF16)
        ref = c_mat.at[l, :, c_columns(mz)]
        for i in far_z:
            remote(ref, ref, c_send.at[l], c_recv.at[l, int(i in next_z)], z_peer(i)).start()

    @scoped
    def out_proj(l):
        with jax.named_scope('wo_wait'):
            wo_copy(l).wait()
        for i in [0] + far_z:
            if i and i in (far_z[0], far_z[-len(next_z)]):
                near = i in next_z
                n = len(next_z) if near else nz - 1 - len(next_z)
                with jax.named_scope('c_wait'):
                    take(c_mat.at[l, :, pl.ds(0, n * hq)], c_recv.at[l, int(near)])
            cols = c_columns((mz + nz - i) % nz)
            part = jnp.dot(c_mat[l, :, cols], wo_v[l, cols, :], preferred_element_type=F32)
            acc[...] = acc[...] + part if i else part

    group = CHUNK // units
    n_groups = len(GROUPS)
    assert group == 2 * len(GROUPS[0])

    def slab(l, g, first, cols):
        parts = [w_all[l, c, slot(0, px + dx, py + dy), pl.ds(first, units), cols] for c in range(2) for dx, dy in GROUPS[g]]
        return jnp.concatenate(parts, axis=0)

    @scoped
    def mlp_units(l, gs):
        block = lax.broadcasted_iota(jnp.int32, (rows, CHUNK), 1) // units
        for g in gs:
            every = pl.ds(0, d_model)
            gate = lax.dot_general(zb[...], slab(l, g, 0, every), NT, preferred_element_type=F32)
            up = lax.dot_general(zb[...], slab(l, g, units, every), NT, preferred_element_type=F32)
            act = gate * (1.0 / (1.0 + jnp.exp(-gate))) * up
            for b in range(group):
                bd[g, pl.ds(b * rows, rows)] = jnp.where(block == b, act, 0.0).astype(BF16)

    two_step = nz == 8
    wide = min(2 * CHUNK, d_model)
    n_sums = d_model // wide

    def ps_of(l, n, i):
        return ps.at[l, n, (mz + i + nz) % nz]

    def rs_start(l, n):
        if not two_step:
            for k, i in enumerate(far_z):
                remote(ps_of(l, n, i), rs.at[l, n, k], rs_send.at[l], rs_recv.at[l, n], z_peer(i)).start()
            return
        for side, to in ((0, nz - 2), (1, 2)):
            cols = pl.ds(side * (wide // 2), wide // 2)
            remote(ps.at[l, n, (mz + 4) % nz, :, cols], ra.at[l, n, 2, :, cols], rs_send.at[l], ra_recv.at[l, n], z_peer(to)).start()
        for side, to in ((0, -1), (1, 1)):
            remote(ps_of(l, n, 3 * to), ra.at[l, n, side], rs_send.at[l], ra_recv.at[l, n], z_peer(nz + to)).start()

    @scoped
    def rs_middle(l):
        if not two_step:
            return

        @pl.loop(0, n_sums)
        def _(n):
            take(ra.at[l, n], ra_recv.at[l, n])
            for side, to in ((0, -2), (1, 2)):
                cols = pl.ds(side * (wide // 2), wide // 2)
                sb[l, n, side] = ps[l, n, (mz + nz + to) % nz] + ra[l, n, side]
                sb[l, n, side, :, cols] = sb[l, n, side, :, cols] + ra[l, n, 2, :, cols]
                remote(sb.at[l, n, side], rs.at[l, n, 2 + side], rs_send.at[l], rs_recv.at[l, n], z_peer(nz + to)).start()
            for side, to in ((0, -1), (1, 1)):
                remote(ps_of(l, n, to), rs.at[l, n, side], rs_send.at[l], rs_recv.at[l, n], z_peer(nz + to)).start()

    @scoped
    def mlp_down(l):
        @pl.loop(0, n_sums)
        def _(n):
            cols = pl.ds(pl.multiple_of(n * wide, wide), wide)
            total = jnp.zeros((rows, wide), F32)
            for g in range(n_groups):
                y = jnp.dot(bd[g], slab(l, g, 2 * units, cols), preferred_element_type=F32)
                y = y.astype(BF16).astype(F32)
                for b in range(group):
                    total = total + y[b * rows:(b + 1) * rows]
            ps[l, n] = total.reshape(nz, seq_dev, wide)
            rs_start(l, n)

    n_in = 4 if two_step else nz - 1

    @scoped
    def rs_finish(l, store):
        mine = pl.ds(pl.multiple_of(mz * seq_dev, seq_dev), seq_dev)
        for n in range(n_sums):
            if n_in:
                take(rs.at[l, n], rs_recv.at[l, n])
            total = ps[l, n, mz]
            for k in range(n_in):
                total = total + rs[l, n, k]
            store(n, (hres[mine, n * wide:(n + 1) * wide] + total).astype(BF16))

    def store_next(l):
        def store(n, x):
            h_all[l + 1, mz, :, n * wide:(n + 1) * wide] = x
            h_start(l + 1, n * wide, wide)
        return store

    with jax.named_scope('small'):
        for c in small:
            c.wait()
        rope_tables()
    with jax.named_scope('barrier'):
        barrier_wait()
    h_start(0, 0, d_model)
    p1(0)
    p3(0, (0,))
    start_later_copies()
    p2(0)
    for l in range(layers):
        more = l + 1 < layers
        h_wait(l)
        norm_to_zb(l, ga)
        qkv(l)
        if l == 0:
            p3(0, (1, 3, 2))
            p4(0, (0,))
        else:
            p4(l, (0, 1, 3, 2))
        kv_wait(l)
        attention(l)
        if l == 0:
            p4(0, (1, 3, 2))
            p5(0, (0,))
        else:
            p5(l, (0, 1, 3, 2))
        if more:
            p1(l + 1)
            p3(l + 1, (0,))
        out_proj(l)
        norm_to_zb(l, gm, True)
        if l == 0:
            w_done(l, (0,))
            mlp_units(l, (0,))
            w_done(l, (1,))
            mlp_units(l, (1,))
            p5(l, (1, 3))
            w_done(l, (2,))
            mlp_units(l, (2,))
            p5(l, (2,))
            w_done(l, (3,))
            mlp_units(l, (3,))
        else:
            w_done(l, range(n_groups))
            mlp_units(l, range(n_groups))
        mlp_down(l)
        if more:
            p2(l + 1)
            p3(l + 1, (1, 3))
        rs_middle(l)
        if more:
            rs_finish(l, store_next(l))
            p3(l + 1, (2,))
    pieces = []
    rs_finish(layers - 1, lambda n, x: pieces.append(x.astype(F32)))
    x = jnp.concatenate(pieces, axis=1)
    inv = lax.rsqrt(jnp.mean(x * x, axis=-1, keepdims=True) + NORM_EPS)
    gain = gf[...].astype(F32)
    for i in range(d_model // LANES):
        cols = slice(i * LANES, (i + 1) * LANES)
        out_ref[:, cols] = x[:, cols] * inv * gain[i:i + 1]

    with jax.named_scope('drain'):
      for l in range(layers):
          ref = w_all.at[l, 0, pl.ds(0, PLANE - 1)]
          remote(ref, ref, w_send.at[l], w_recv.at[l, 0], me).wait_send()
          ref = w_all.at[l, 0]
          remote(ref, ref, d_send.at[l], d_recv.at[l, 0], me).wait_send()
          ref = kv_all.at[l, 0, pl.ds(0, PLANE - 1)]
          remote(ref, ref, kv_send.at[l], kv_recv.at[l], me).wait_send()
          ref = kv_all.at[l, 0]
          remote(ref, ref, kvd_send.at[l], kvd_recv.at[l], me).wait_send()
          if nz > 1:
              ref = h_all.at[l, pl.ds(0, nz - 1)]
              remote(ref, ref, h_send.at[l], h_recv.at[l], me).wait_send()
              ref = c_mat.at[l, :, pl.ds(0, (nz - 1) * hq)]
              remote(ref, ref, c_send.at[l], c_recv.at[l, 0], me).wait_send()
              ref = ps.at[l, :, pl.ds(0, nz - 1)]
              remote(ref, ref, rs_send.at[l], rs_recv.at[l, 0], me).wait_send()


def solution(mesh):
    nz = mesh.shape['tp'] // (2 * PLANE)

    def device_fn(hidden_in, lengths, attn_norm, w_query, w_key, w_value, w_out, mlp_norm, w_gate, w_up, w_down, final_norm):
        seq_dev, d_model = hidden_in.shape[1:]
        layers, _, heads, hd = w_query.shape
        kv_heads = w_key.shape[2]
        units = w_gate.shape[2]
        assert kv_heads == nz and 2 * hd == LANES and heads % nz == 0
        hq = heads // nz * hd
        rows = nz * seq_dev
        wide = min(2 * CHUNK, d_model)
        n_sums = d_model // wide
        n_groups = 2 * PLANE * units // CHUNK
        dev, row = np.arange(2 * PLANE)[:, None], np.arange(rows)[None, :]
        pos = (row // seq_dev) * (2 * PLANE * seq_dev) + dev * seq_dev + row % seq_dev
        freq = np.float32(ROPE_BASE) ** (np.float32(-2.0) * np.arange(hd // 2, dtype=np.float32) / np.float32(hd))
        angles = (pos[..., None].astype(np.float32) * freq).astype(np.float64)
        rope = np.tile(np.concatenate([np.cos(angles), np.sin(angles)], axis=-1), (1, 1, 2)).astype(np.float32)
        by_rows = lambda w: jnp.transpose(w, (0, 2, 3, 1)).reshape(layers, -1, d_model)
        units_first = lambda w: jnp.transpose(w, (0, 2, 1))
        hbm, vmem = (pl.BlockSpec(memory_space=s) for s in (pltpu.HBM, pltpu.VMEM))
        dma = pltpu.SemaphoreType.DMA
        out = pl.pallas_call(
            functools.partial(kernel, nz),
            name='decoder',
            out_shape=jax.ShapeDtypeStruct((seq_dev, d_model), F32),
            in_specs=[hbm] * 13,
            out_specs=vmem,
            scratch_shapes=[
                pltpu.VMEM((layers, 2, PLANE, 3 * units, d_model), BF16),
                pltpu.VMEM((layers, heads * hd, d_model), BF16),
                pltpu.VMEM((layers, hq + 2 * hd, d_model), BF16),
                pltpu.VMEM((layers, nz, seq_dev, d_model), BF16),
                pltpu.VMEM((layers, rows, heads * hd), BF16),
                pltpu.VMEM((layers, 2, PLANE, rows, LANES), BF16),
                pltpu.VMEM((layers, n_sums, 4 if nz == 8 else max(nz - 1, 1), seq_dev, wide), F32),
                pltpu.VMEM((layers, n_sums, 3, seq_dev, wide), F32),
                pltpu.VMEM((layers, n_sums, 2, seq_dev, wide), F32),
                pltpu.VMEM((layers, n_sums, nz, seq_dev, wide), F32),
                pltpu.VMEM((rows, d_model), F32),
                pltpu.VMEM((rows, d_model), F32),
                pltpu.VMEM((rows, d_model), BF16),
                pltpu.VMEM((hq // hd * rows, LANES), BF16),
                pltpu.VMEM((n_groups, CHUNK // units * rows, CHUNK), BF16),
                pltpu.VMEM((rows, LANES), F32), pltpu.VMEM((rows, LANES), F32), pltpu.VMEM((rows, LANES), F32),
                pltpu.VMEM((layers, d_model), BF16), pltpu.VMEM((layers, d_model), BF16),
                pltpu.VMEM((d_model // LANES, LANES), BF16),
                pltpu.SMEM((1,), jnp.int32),
                dma((layers, 3)), dma((6,)), dma((layers, 10)), dma((layers,)),
                dma((layers, n_groups)), dma((layers,)),
                dma((layers,)), dma((layers,)), dma((layers,)), dma((layers,)), dma((layers,)), dma((layers,)),
                dma((layers, 2)), dma((layers,)), dma((layers, n_sums)), dma((layers, n_sums)), dma((layers,)),
            ],
            compiler_params=pltpu.CompilerParams(
                collective_id=0, has_side_effects=True, vmem_limit_bytes=67_043_328),
        )(hidden_in[0], lengths, jnp.asarray(rope), attn_norm, mlp_norm, final_norm.reshape(-1, LANES), by_rows(w_query), by_rows(w_key), by_rows(w_value),
          w_out.reshape(layers, heads * hd, d_model), units_first(w_gate), units_first(w_up), w_down)
        return out.astype(BF16)[None]

    seq_part = P(None, 'tp', None)
    in_specs = (seq_part, P(), P(), P(), P(), P(), P(), P(), P(None, None, 'tp'), P(None, None, 'tp'), P(None, 'tp', None), P())
    return jax.shard_map(device_fn, mesh=mesh, in_specs=in_specs, out_specs=seq_part, check_vma=False)
```

```python
import functools

import jax
import jax.numpy as jnp
import numpy as np
from jax import lax
from jax.experimental import pallas as pl
from jax.experimental.pallas import tpu as pltpu
from jax.sharding import PartitionSpec as P

NORM_EPS = 1e-5
ROPE_BASE = 500000.0
NX = 4
PLANE = NX * NX
LANES = 128
CHUNK = 256
NT = (((1,), (1,)), ((), ()))
F32, BF16 = jnp.float32, jnp.bfloat16


def remote(src, dst, send_sem, recv_sem, device):
    return pltpu.make_async_remote_copy(
        src_ref=src, dst_ref=dst, send_sem=send_sem, recv_sem=recv_sem,
        device_id=(device,), device_id_type=pl.DeviceIdType.MESH)


def scoped(f):
    @functools.wraps(f)
    def wrapped(*args):
        with jax.named_scope(f.__name__ + ('#l=%d' % args[0])):
            return f(*args)
    return wrapped


def kernel(nz, h_ref, len_ref, rope_ref, ga_ref, gm_ref, gf_ref, wq_ref, wk_ref, wv_ref, wo_ref, wg_ref, wu_ref, wd_ref,
           out_ref, w_all, wo_v, wqkv, h_all, c_mat, kv_all, rs, ra, sb, ps, acc, hres, zb, qbuf, bd, rope, cos_t, sin_t, ga, gm, gf, len_s,
           local_sem, in_sem, w_recv, w_send, d_recv, d_send, rounds, h_recv, h_send, kv_recv, kv_send, kvd_recv, kvd_send,
           c_recv, c_send, rs_recv, ra_recv, rs_send):
    layers = wo_ref.shape[0]
    seq_dev, d_model = h_ref.shape
    units = wg_ref.shape[1]
    pack = 3 * units
    half = pack // 2
    rows = nz * seq_dev
    hq = wq_ref.shape[1] // nz
    hd = wk_ref.shape[1] // nz
    me = lax.axis_index('tp')
    core = me % 2
    px = (me // 2) % NX
    py = (me // (2 * NX)) % NX
    mp = (me // 2) % PLANE
    mz = me // (2 * PLANE)
    base = mz * (2 * PLANE)
    partner = base + mp * 2 + (1 - core)

    def z_peer(i):
        return ((mz + i) % nz) * (2 * PLANE) + mp * 2 + core

    far_z = sorted(range(1, nz), key=lambda i: -min(i, nz - i))
    next_z = [i for i in far_z if min(i, nz - i) == 1]
    def plane_peer(dy, dx):
        return base + ((py + dy) % NX * NX + (px + dx) % NX) * 2 + core

    far_plane = sorted(((dy, dx) for dy in range(NX) for dx in range(NX) if dy or dx),
                       key=lambda d: -sum(min(i, NX - i) for i in d))

    barrier = pltpu.get_barrier_semaphore()
    next_devices = [plane_peer(0, 1), plane_peer(0, NX - 1), plane_peer(1, 0), plane_peer(NX - 1, 0)]
    next_devices += [z_peer(i) for i in next_z]

    def signal(sem, device):
        pl.semaphore_signal(sem, inc=1, device_id=(device,), device_id_type=pl.DeviceIdType.MESH)

    signal(barrier, partner)
    for d in next_devices:
        signal(barrier, d)

    def round_start(r):
        for d in next_devices:
            signal(rounds.at[r], d)

    def round_wait(r):
        pl.semaphore_wait(rounds.at[r], len(next_devices))

    def pack_copies(l):
        mine = w_all.at[l, core, mp]
        return [pltpu.make_async_copy(ref.at[l], mine.at[pl.ds(i * units, units)], local_sem.at[l, 0])
                for i, ref in enumerate((wg_ref, wu_ref, wd_ref))]

    def qkv_copies(l):
        return [pltpu.make_async_copy(ref.at[l, pl.ds(mz * n, n)], wqkv.at[l, pl.ds(first, n)], local_sem.at[l, 1])
                for ref, first, n in ((wq_ref, 0, hq), (wk_ref, hq, hd), (wv_ref, hq + hd, hd))]

    def wo_copy(l):
        return pltpu.make_async_copy(wo_ref.at[l], wo_v.at[l], local_sem.at[l, 2])

    def take(ref, sem):
        remote(ref, ref, w_send.at[0], sem, me).wait_recv()

    def pack_wait(l):
        mine = w_all.at[l, core, mp]
        pltpu.make_async_copy(mine, mine, local_sem.at[l, 0]).wait()

    def qkv_wait(l):
        pltpu.make_async_copy(wqkv.at[l], wqkv.at[l], local_sem.at[l, 1]).wait()

    small = [pltpu.make_async_copy(src, dst, in_sem.at[i]) for i, (src, dst) in enumerate((
        (h_ref, h_all.at[0, mz]), (rope_ref.at[mp * 2 + core], rope), (ga_ref, ga), (gm_ref, gm), (gf_ref, gf), (len_ref, len_s)))]
    for c in pack_copies(0) + small + qkv_copies(0):
        c.start()

    def start_later_copies():
        wo_copy(0).start()
        for l in range(1, layers):
            for c in pack_copies(l) + qkv_copies(l):
                c.start()
            wo_copy(l).start()

    def slot(h, a1, a2):
        return a2 % NX * NX + a1 % NX if h == 0 else a1 % NX * NX + a2 % NX

    def where_am_i(h):
        return (px, py) if h == 0 else (py, px)

    def at(h, a1, a2):
        return base + slot(h, a1, a2) * 2 + core

    third = half // 3
    SPAN = ((0, half), (half, half))

    def from_minus(h, k):
        return (h * half, 2 * third if (k in (1, 2)) != (h == 1) else third)

    def from_plus(h, k):
        first, size = from_minus(h, k)
        return (first + size, half - size)

    def piece(l, c, p, span):
        return w_all.at[l, c, p, pl.ds(*span)]

    def w_start(l, p, span, idx, device):
        ref = piece(l, core, p, span)
        remote(ref, ref, w_send.at[l], w_recv.at[l, idx], device).start()

    def w_take(l, idx, packs):
        take(w_all.at[l, core, pl.ds(0, packs)], w_recv.at[l, idx])

    GROUPS = (((0, 0), (1, 0), (3, 0), (0, 1)), ((0, 3), (2, 0), (0, 2), (1, 1)),
              ((1, 3), (3, 1), (3, 3), (2, 1)), ((2, 3), (1, 2), (3, 2), (2, 2)))
    GROUP_OF = {d: g for g, ds in enumerate(GROUPS) for d in ds}

    def to_partner(l, h, k1, k2, span):
        a1, a2 = where_am_i(h)
        ref = piece(l, core, slot(h, a1 + k1, a2 + k2), span)
        g = GROUP_OF[(k1, k2) if h == 0 else (k2, k1)]
        remote(ref, ref, d_send.at[l], d_recv.at[l, g], partner).start()

    @scoped
    def p1(l):
        pack_wait(l)
        for h in range(2):
            a1, a2 = where_am_i(h)
            w_start(l, mp, SPAN[h], 0, at(h, a1 + 1, a2))
            w_start(l, mp, SPAN[h], 0, at(h, a1 + NX - 1, a2))
        to_partner(l, 0, 0, 0, (0, pack))

    @scoped
    def p2(l):
        w_take(l, 0, 2)
        for h in range(2):
            a1, a2 = where_am_i(h)
            w_start(l, slot(h, a1 + NX - 1, a2), from_minus(h, 0), 1, at(h, a1 + 1, a2))
            w_start(l, slot(h, a1 + 1, a2), from_plus(h, 0), 1, at(h, a1 + NX - 1, a2))
            to_partner(l, h, NX - 1, 0, SPAN[h])
            to_partner(l, h, 1, 0, SPAN[h])

    @scoped
    def p3(l, ks):
        for k in ks:
            if k == 2:
                w_take(l, 1, 1)
            for h in range(2):
                a1, a2 = where_am_i(h)
                p = slot(h, a1 + k, a2)
                w_start(l, p, SPAN[h], 2 + k, at(h, a1, a2 + 1))
                w_start(l, p, SPAN[h], 2 + k, at(h, a1, a2 + NX - 1))
                if k == 2:
                    to_partner(l, h, k, 0, SPAN[h])

    @scoped
    def p4(l, ks):
        for k in ks:
            w_take(l, 2 + k, 2)
            for h in range(2):
                a1, a2 = where_am_i(h)
                w_start(l, slot(h, a1 + k, a2 + NX - 1), from_minus(h, k), 6 + k, at(h, a1, a2 + 1))
                w_start(l, slot(h, a1 + k, a2 + 1), from_plus(h, k), 6 + k, at(h, a1, a2 + NX - 1))
                to_partner(l, h, k, NX - 1, SPAN[h])
                to_partner(l, h, k, 1, SPAN[h])

    @scoped
    def p5(l, ks):
        for k in ks:
            w_take(l, 6 + k, 1)
            for h in range(2):
                to_partner(l, h, k, 2, SPAN[h])

    @scoped
    def w_done(l, gs):
        for g in gs:
            take(w_all.at[l, 1 - core, pl.ds(0, len(GROUPS[g]))], d_recv.at[l, g])

    def h_start(l, first, size, peers):
        for i in peers:
            ref = h_all.at[l, mz, :, pl.ds(first, size)]
            remote(ref, ref, h_send.at[l], h_recv.at[l], z_peer(i)).start()

    @scoped
    def h_wait(l):
        if nz > 1:
            take(h_all.at[l, pl.ds(0, nz - 1)], h_recv.at[l])
        for i in range(nz):
            hres[pl.ds(i * seq_dev, seq_dev)] = h_all[l, i].astype(F32)

    @scoped
    def norm_to_zb(l, gains, residual=False):
        gain = gains[...].astype(F32)[l:l + 1]
        step = min(16, rows)
        for first in range(0, rows, step):
            r = pl.ds(first, step)
            x = hres[r]
            if residual:
                x = (x + acc[r]).astype(BF16).astype(F32)
                hres[r] = x
            inv = lax.rsqrt(jnp.mean(x * x, axis=-1, keepdims=True) + NORM_EPS)
            zb[r] = (x * inv * gain).astype(BF16)

    lane = lax.broadcasted_iota(jnp.int32, (rows, LANES), 1)
    low_half = lane < hd

    def rotate(x):
        first = (lane % hd) < hd // 2
        swapped = jnp.where(first, pltpu.roll(x, LANES - hd // 2, 1), pltpu.roll(x, hd // 2, 1))
        return x * cos_t[...] + swapped * sin_t[...]

    def rope_tables():
        first = (lane % hd) < hd // 2
        t = rope[...]
        cos_t[...] = jnp.where(first, t, pltpu.roll(t, hd // 2, 1))
        sin_t[...] = jnp.where(first, -pltpu.roll(t, LANES - hd // 2, 1), t)

    def kv_copy(l, device):
        ref = kv_all.at[l, core, mp]
        return remote(ref, ref, kv_send.at[l], kv_recv.at[l], device)

    @scoped
    def qkv(l):
        qkv_wait(l)
        kv = lax.dot_general(zb[...], wqkv[l, pl.ds(hq, 2 * hd), :], NT, preferred_element_type=F32)
        kv_all[l, core, mp] = jnp.where(low_half, rotate(kv), kv).astype(BF16)
        for d in far_plane:
            kv_copy(l, plane_peer(*d)).start()
        proj = lax.dot_general(zb[...], wqkv[l, pl.ds(0, hq), :], NT, preferred_element_type=F32)
        for j in range(hq // LANES):
            q = rotate(proj[:, j * LANES:(j + 1) * LANES]) * (hd ** -0.5)
            for half_head, x in enumerate((q, pltpu.roll(q, LANES - hd, 1))):
                head = 2 * j + half_head
                qbuf[pl.ds(head * rows, rows)] = jnp.where(low_half, x, 0.0).astype(BF16)

    @scoped
    def kv_wait(l):
        take(kv_all.at[l, core, pl.ds(0, PLANE - 1)], kv_recv.at[l])
        ref = kv_all.at[l, core]
        remote(ref, ref, kvd_send.at[l], kvd_recv.at[l], partner).start()
        take(kv_all.at[l, 1 - core], kvd_recv.at[l])

    def c_columns(z):
        return pl.ds(pl.multiple_of(z * hq, hq), hq)

    @scoped
    def attention(l):
        keys = 2 * PLANE * rows
        j = lax.broadcasted_iota(jnp.int32, (1, keys), 1)
        key_pos = ((j // seq_dev) % nz) * (2 * PLANE * seq_dev) + ((j // rows) % PLANE) * (2 * seq_dev) \
            + (j // (PLANE * rows)) * seq_dev + j % seq_dev
        i = lax.broadcasted_iota(jnp.int32, (hq // hd * rows, 1), 0) % rows
        q_pos = (i // seq_dev) * (2 * PLANE * seq_dev) + (mp * 2 + core) * seq_dev + i % seq_dev
        allowed = key_pos <= jnp.minimum(q_pos, len_s[0] - 1)
        kv = kv_all[l].reshape(keys, LANES)
        s = lax.dot_general(qbuf[...], kv, NT, preferred_element_type=F32)
        s = jnp.where(allowed, s, -1e30)
        e = jnp.exp(s - jnp.max(s, axis=-1, keepdims=True))
        p = (e * (1.0 / jnp.sum(e, axis=-1, keepdims=True))).astype(BF16)
        o = jnp.dot(p, kv, preferred_element_type=F32)
        for pair in range(hq // LANES):
            even, odd = (o[h * rows:(h + 1) * rows] for h in (2 * pair, 2 * pair + 1))
            c_mat[l, :, pl.ds(pl.multiple_of(mz * hq + pair * LANES, LANES), LANES)] = jnp.where(low_half, pltpu.roll(even, LANES - hd, 1), odd).astype(BF16)
        ref = c_mat.at[l, :, c_columns(mz)]
        for i in far_z:
            remote(ref, ref, c_send.at[l], c_recv.at[l, int(i in next_z)], z_peer(i)).start()

    @scoped
    def out_proj(l):
        with jax.named_scope('wo_wait'):
            wo_copy(l).wait()
        for i in [0] + far_z:
            if i and i in (far_z[0], far_z[-len(next_z)]):
                near = i in next_z
                n = len(next_z) if near else nz - 1 - len(next_z)
                with jax.named_scope('c_wait'):
                    take(c_mat.at[l, :, pl.ds(0, n * hq)], c_recv.at[l, int(near)])
            cols = c_columns((mz + nz - i) % nz)
            part = jnp.dot(c_mat[l, :, cols], wo_v[l, cols, :], preferred_element_type=F32)
            acc[...] = acc[...] + part if i else part

    group = CHUNK // units
    n_groups = len(GROUPS)
    assert group == 2 * len(GROUPS[0])

    def slab(l, g, first, cols):
        parts = [w_all[l, c, slot(0, px + dx, py + dy), pl.ds(first, units), cols] for c in range(2) for dx, dy in GROUPS[g]]
        return jnp.concatenate(parts, axis=0)

    @scoped
    def mlp_units(l, gs):
        block = lax.broadcasted_iota(jnp.int32, (rows, CHUNK), 1) // units
        for g in gs:
            every = pl.ds(0, d_model)
            gate = lax.dot_general(zb[...], slab(l, g, 0, every), NT, preferred_element_type=F32)
            up = lax.dot_general(zb[...], slab(l, g, units, every), NT, preferred_element_type=F32)
            act = gate * (1.0 / (1.0 + jnp.exp(-gate))) * up
            for b in range(group):
                bd[g, pl.ds(b * rows, rows)] = jnp.where(block == b, act, 0.0).astype(BF16)

    two_step = nz == 8
    wide = min(2 * CHUNK, d_model)
    n_sums = d_model // wide

    def ps_of(l, n, i):
        return ps.at[l, n, (mz + i + nz) % nz]

    def rs_start(l, n):
        if not two_step:
            for k, i in enumerate(far_z):
                remote(ps_of(l, n, i), rs.at[l, n, k], rs_send.at[l], rs_recv.at[l, n], z_peer(i)).start()
            return
        for side, to in ((0, nz - 2), (1, 2)):
            cols = pl.ds(side * (wide // 2), wide // 2)
            remote(ps.at[l, n, (mz + 4) % nz, :, cols], ra.at[l, n, 2, :, cols], rs_send.at[l], ra_recv.at[l, n], z_peer(to)).start()
        for side, to in ((0, -1), (1, 1)):
            remote(ps_of(l, n, 3 * to), ra.at[l, n, side], rs_send.at[l], ra_recv.at[l, n], z_peer(nz + to)).start()

    @scoped
    def rs_middle(l):
        if not two_step:
            return

        @pl.loop(0, n_sums)
        def _(n):
            take(ra.at[l, n], ra_recv.at[l, n])
            for side, to in ((0, -2), (1, 2)):
                cols = pl.ds(side * (wide // 2), wide // 2)
                sb[l, n, side] = ps[l, n, (mz + nz + to) % nz] + ra[l, n, side]
                sb[l, n, side, :, cols] = sb[l, n, side, :, cols] + ra[l, n, 2, :, cols]
                remote(sb.at[l, n, side], rs.at[l, n, 2 + side], rs_send.at[l], rs_recv.at[l, n], z_peer(nz + to)).start()
            for side, to in ((0, -1), (1, 1)):
                remote(ps_of(l, n, to), rs.at[l, n, side], rs_send.at[l], rs_recv.at[l, n], z_peer(nz + to)).start()

    @scoped
    def mlp_down(l):
        @pl.loop(0, n_sums)
        def _(n):
            cols = pl.ds(pl.multiple_of(n * wide, wide), wide)
            total = jnp.zeros((rows, wide), F32)
            for g in range(n_groups):
                y = jnp.dot(bd[g], slab(l, g, 2 * units, cols), preferred_element_type=F32)
                y = y.astype(BF16).astype(F32)
                for b in range(group):
                    total = total + y[b * rows:(b + 1) * rows]
            ps[l, n] = total.reshape(nz, seq_dev, wide)
            rs_start(l, n)

    n_in = 4 if two_step else nz - 1

    @scoped
    def rs_finish(l, store):
        mine = pl.ds(pl.multiple_of(mz * seq_dev, seq_dev), seq_dev)
        for n in range(n_sums):
            if n_in:
                take(rs.at[l, n], rs_recv.at[l, n])
            total = ps[l, n, mz]
            for k in range(n_in):
                total = total + rs[l, n, k]
            store(n, (hres[mine, n * wide:(n + 1) * wide] + total).astype(BF16))

    def store_next(l):
        def store(n, x):
            h_all[l + 1, mz, :, n * wide:(n + 1) * wide] = x
            h_start(l + 1, n * wide, wide, far_z)
        return store

    with jax.named_scope('barrier'):
        pl.semaphore_wait(barrier, 1 + len(next_devices))
    round_start(0)
    p1(0)
    p3(0, (0,))
    with jax.named_scope('rounds'):
        small[0].wait()
        for r in range(4):
            if r:
                round_wait(r - 1)
                if r < 3:
                    round_start(r)
            h_start(0, 0, d_model, [i for i in far_z if min(i, nz - i) == r + 1])
    start_later_copies()
    with jax.named_scope('small'):
        for c in small[1:]:
            c.wait()
        rope_tables()
    p2(0)
    for l in range(layers):
        more = l + 1 < layers
        h_wait(l)
        norm_to_zb(l, ga)
        qkv(l)
        if l == 0:
            p3(0, (1, 3, 2))
            p4(0, (0,))
        else:
            p4(l, (0, 1, 3, 2))
        kv_wait(l)
        attention(l)
        if l == 0:
            p4(0, (1, 3, 2))
            p5(0, (0,))
        else:
            p5(l, (0, 1, 3, 2))
        if more:
            p1(l + 1)
            p3(l + 1, (0,))
        out_proj(l)
        norm_to_zb(l, gm, True)
        if l == 0:
            w_done(l, (0,))
            mlp_units(l, (0,))
            w_done(l, (1,))
            mlp_units(l, (1,))
            p5(l, (1, 3))
            w_done(l, (2,))
            mlp_units(l, (2,))
            p5(l, (2,))
            w_done(l, (3,))
            mlp_units(l, (3,))
        else:
            w_done(l, range(n_groups))
            mlp_units(l, range(n_groups))
        mlp_down(l)
        if more:
            p2(l + 1)
            p3(l + 1, (1, 3))
        rs_middle(l)
        if more:
            rs_finish(l, store_next(l))
            p3(l + 1, (2,))
    pieces = []
    rs_finish(layers - 1, lambda n, x: pieces.append(x.astype(F32)))
    x = jnp.concatenate(pieces, axis=1)
    inv = lax.rsqrt(jnp.mean(x * x, axis=-1, keepdims=True) + NORM_EPS)
    gain = gf[...].astype(F32)
    for i in range(d_model // LANES):
        cols = slice(i * LANES, (i + 1) * LANES)
        out_ref[:, cols] = x[:, cols] * inv * gain[i:i + 1]

    with jax.named_scope('drain'):
      for l in range(layers):
          ref = w_all.at[l, 0, pl.ds(0, PLANE - 1)]
          remote(ref, ref, w_send.at[l], w_recv.at[l, 0], me).wait_send()
          ref = w_all.at[l, 0]
          remote(ref, ref, d_send.at[l], d_recv.at[l, 0], me).wait_send()
          ref = kv_all.at[l, 0, pl.ds(0, PLANE - 1)]
          remote(ref, ref, kv_send.at[l], kv_recv.at[l], me).wait_send()
          ref = kv_all.at[l, 0]
          remote(ref, ref, kvd_send.at[l], kvd_recv.at[l], me).wait_send()
          if nz > 1:
              ref = h_all.at[l, pl.ds(0, nz - 1)]
              remote(ref, ref, h_send.at[l], h_recv.at[l], me).wait_send()
              ref = c_mat.at[l, :, pl.ds(0, (nz - 1) * hq)]
              remote(ref, ref, c_send.at[l], c_recv.at[l, 0], me).wait_send()
              ref = ps.at[l, :, pl.ds(0, nz - 1)]
              remote(ref, ref, rs_send.at[l], rs_recv.at[l, 0], me).wait_send()


def solution(mesh):
    nz = mesh.shape['tp'] // (2 * PLANE)

    def device_fn(hidden_in, lengths, attn_norm, w_query, w_key, w_value, w_out, mlp_norm, w_gate, w_up, w_down, final_norm):
        seq_dev, d_model = hidden_in.shape[1:]
        layers, _, heads, hd = w_query.shape
        kv_heads = w_key.shape[2]
        units = w_gate.shape[2]
        assert kv_heads == nz and 2 * hd == LANES and heads % nz == 0
        hq = heads // nz * hd
        rows = nz * seq_dev
        wide = min(2 * CHUNK, d_model)
        n_sums = d_model // wide
        n_groups = 2 * PLANE * units // CHUNK
        dev, row = np.arange(2 * PLANE)[:, None], np.arange(rows)[None, :]
        pos = (row // seq_dev) * (2 * PLANE * seq_dev) + dev * seq_dev + row % seq_dev
        freq = np.float32(ROPE_BASE) ** (np.float32(-2.0) * np.arange(hd // 2, dtype=np.float32) / np.float32(hd))
        angles = (pos[..., None].astype(np.float32) * freq).astype(np.float64)
        rope = np.tile(np.concatenate([np.cos(angles), np.sin(angles)], axis=-1), (1, 1, 2)).astype(np.float32)
        by_rows = lambda w: jnp.transpose(w, (0, 2, 3, 1)).reshape(layers, -1, d_model)
        units_first = lambda w: jnp.transpose(w, (0, 2, 1))
        hbm, vmem = (pl.BlockSpec(memory_space=s) for s in (pltpu.HBM, pltpu.VMEM))
        dma = pltpu.SemaphoreType.DMA
        out = pl.pallas_call(
            functools.partial(kernel, nz),
            name='decoder',
            out_shape=jax.ShapeDtypeStruct((seq_dev, d_model), F32),
            in_specs=[hbm] * 13,
            out_specs=vmem,
            scratch_shapes=[
                pltpu.VMEM((layers, 2, PLANE, 3 * units, d_model), BF16),
                pltpu.VMEM((layers, heads * hd, d_model), BF16),
                pltpu.VMEM((layers, hq + 2 * hd, d_model), BF16),
                pltpu.VMEM((layers, nz, seq_dev, d_model), BF16),
                pltpu.VMEM((layers, rows, heads * hd), BF16),
                pltpu.VMEM((layers, 2, PLANE, rows, LANES), BF16),
                pltpu.VMEM((layers, n_sums, 4 if nz == 8 else max(nz - 1, 1), seq_dev, wide), F32),
                pltpu.VMEM((layers, n_sums, 3, seq_dev, wide), F32),
                pltpu.VMEM((layers, n_sums, 2, seq_dev, wide), F32),
                pltpu.VMEM((layers, n_sums, nz, seq_dev, wide), F32),
                pltpu.VMEM((rows, d_model), F32),
                pltpu.VMEM((rows, d_model), F32),
                pltpu.VMEM((rows, d_model), BF16),
                pltpu.VMEM((hq // hd * rows, LANES), BF16),
                pltpu.VMEM((n_groups, CHUNK // units * rows, CHUNK), BF16),
                pltpu.VMEM((rows, LANES), F32), pltpu.VMEM((rows, LANES), F32), pltpu.VMEM((rows, LANES), F32),
                pltpu.VMEM((layers, d_model), BF16), pltpu.VMEM((layers, d_model), BF16),
                pltpu.VMEM((d_model // LANES, LANES), BF16),
                pltpu.SMEM((1,), jnp.int32),
                dma((layers, 3)), dma((6,)), dma((layers, 10)), dma((layers,)),
                dma((layers, n_groups)), dma((layers,)),
                pltpu.SemaphoreType.REGULAR((3,)),
                dma((layers,)), dma((layers,)), dma((layers,)), dma((layers,)), dma((layers,)), dma((layers,)),
                dma((layers, 2)), dma((layers,)), dma((layers, n_sums)), dma((layers, n_sums)), dma((layers,)),
            ],
            compiler_params=pltpu.CompilerParams(
                collective_id=0, has_side_effects=True, vmem_limit_bytes=56_400_000),
        )(hidden_in[0], lengths, jnp.asarray(rope), attn_norm, mlp_norm, final_norm.reshape(-1, LANES), by_rows(w_query), by_rows(w_key), by_rows(w_value),
          w_out.reshape(layers, heads * hd, d_model), units_first(w_gate), units_first(w_up), w_down)
        return out.astype(BF16)[None]

    seq_part = P(None, 'tp', None)
    in_specs = (seq_part, P(), P(), P(), P(), P(), P(), P(), P(None, None, 'tp'), P(None, None, 'tp'), P(None, 'tp', None), P())
    return jax.shard_map(device_fn, mesh=mesh, in_specs=in_specs, out_specs=seq_part, check_vma=False)
```

```python
import functools

import jax
import jax.numpy as jnp
import numpy as np
from jax import lax
from jax.experimental import pallas as pl
from jax.experimental.pallas import tpu as pltpu
from jax.sharding import PartitionSpec as P

NORM_EPS = 1e-5
ROPE_BASE = 500000.0
NX = 4
PLANE = NX * NX
LANES = 128
CHUNK = 256
NT = (((1,), (1,)), ((), ()))
F32, BF16 = jnp.float32, jnp.bfloat16


def remote(src, dst, send_sem, recv_sem, device):
    return pltpu.make_async_remote_copy(
        src_ref=src, dst_ref=dst, send_sem=send_sem, recv_sem=recv_sem,
        device_id=(device,), device_id_type=pl.DeviceIdType.MESH)


def scoped(f):
    @functools.wraps(f)
    def wrapped(*args):
        with jax.named_scope(f.__name__ + ('#l=%d' % args[0])):
            return f(*args)
    return wrapped


def kernel(nz, h_ref, len_ref, rope_ref, ga_ref, gm_ref, gf_ref, wq_ref, wk_ref, wv_ref, wo_ref, wg_ref, wu_ref, wd_ref,
           out_ref, w_all, wo_v, wqkv, h_all, c_mat, kv_all, rs, ra, sb, ps, acc, hres, zb, qbuf, bd, rope, cos_t, sin_t, ga, gm, gf, len_s,
           local_sem, in_sem, w_recv, w_send, d_recv, d_send, rounds, h_recv, h_send, kv_recv, kv_send, kvd_recv, kvd_send,
           c_recv, c_send, rs_recv, ra_recv, rs_send):
    layers = wo_ref.shape[0]
    seq_dev, d_model = h_ref.shape
    units = wg_ref.shape[1]
    pack = 3 * units
    half = pack // 2
    rows = nz * seq_dev
    hq = wq_ref.shape[1] // nz
    hd = wk_ref.shape[1] // nz
    me = lax.axis_index('tp')
    core = me % 2
    px = (me // 2) % NX
    py = (me // (2 * NX)) % NX
    mp = (me // 2) % PLANE
    mz = me // (2 * PLANE)
    base = mz * (2 * PLANE)
    partner = base + mp * 2 + (1 - core)

    def z_peer(i):
        return ((mz + i) % nz) * (2 * PLANE) + mp * 2 + core

    far_z = sorted(range(1, nz), key=lambda i: -min(i, nz - i))
    next_z = [i for i in far_z if min(i, nz - i) == 1]
    def plane_peer(dy, dx):
        return base + ((py + dy) % NX * NX + (px + dx) % NX) * 2 + core

    far_plane = sorted(((dy, dx) for dy in range(NX) for dx in range(NX) if dy or dx),
                       key=lambda d: -sum(min(i, NX - i) for i in d))

    barrier = pltpu.get_barrier_semaphore()
    next_devices = [plane_peer(0, 1), plane_peer(0, NX - 1), plane_peer(1, 0), plane_peer(NX - 1, 0)]
    next_devices += [z_peer(i) for i in next_z]

    def signal(sem, device):
        pl.semaphore_signal(sem, inc=1, device_id=(device,), device_id_type=pl.DeviceIdType.MESH)

    signal(barrier, partner)
    for d in next_devices:
        signal(barrier, d)

    def round_start(r):
        for d in next_devices:
            signal(rounds.at[r], d)

    def round_wait(r):
        pl.semaphore_wait(rounds.at[r], len(next_devices))

    def pack_copies(l):
        mine = w_all.at[l, core, mp]
        return [pltpu.make_async_copy(ref.at[l], mine.at[pl.ds(i * units, units)], local_sem.at[l, 0])
                for i, ref in enumerate((wg_ref, wu_ref, wd_ref))]

    def qkv_copies(l):
        return [pltpu.make_async_copy(ref.at[l, pl.ds(mz * n, n)], wqkv.at[l, pl.ds(first, n)], local_sem.at[l, 1])
                for ref, first, n in ((wq_ref, 0, hq), (wk_ref, hq, hd), (wv_ref, hq + hd, hd))]

    def wo_copy(l):
        return pltpu.make_async_copy(wo_ref.at[l], wo_v.at[l], local_sem.at[l, 2])

    def take(ref, sem):
        remote(ref, ref, w_send.at[0], sem, me).wait_recv()

    def pack_wait(l):
        mine = w_all.at[l, core, mp]
        pltpu.make_async_copy(mine, mine, local_sem.at[l, 0]).wait()

    def qkv_wait(l):
        pltpu.make_async_copy(wqkv.at[l], wqkv.at[l], local_sem.at[l, 1]).wait()

    small = [pltpu.make_async_copy(src, dst, in_sem.at[i]) for i, (src, dst) in enumerate((
        (h_ref, h_all.at[0, mz]), (rope_ref.at[mp * 2 + core], rope), (ga_ref, ga), (gm_ref, gm), (gf_ref, gf), (len_ref, len_s)))]
    for c in pack_copies(0) + small + qkv_copies(0):
        c.start()

    def start_later_copies():
        wo_copy(0).start()
        for l in range(1, layers):
            for c in pack_copies(l) + qkv_copies(l):
                c.start()
            wo_copy(l).start()

    def slot(h, a1, a2):
        return a2 % NX * NX + a1 % NX if h == 0 else a1 % NX * NX + a2 % NX

    def where_am_i(h):
        return (px, py) if h == 0 else (py, px)

    def at(h, a1, a2):
        return base + slot(h, a1, a2) * 2 + core

    third = half // 3
    SPAN = ((0, half), (half, half))

    def from_minus(h, k):
        return (h * half, 2 * third if (k in (1, 2)) != (h == 1) else third)

    def from_plus(h, k):
        first, size = from_minus(h, k)
        return (first + size, half - size)

    def piece(l, c, p, span):
        return w_all.at[l, c, p, pl.ds(*span)]

    def w_start(l, p, span, idx, device):
        ref = piece(l, core, p, span)
        remote(ref, ref, w_send.at[l], w_recv.at[l, idx], device).start()

    def w_take(l, idx, packs):
        take(w_all.at[l, core, pl.ds(0, packs)], w_recv.at[l, idx])

    GROUPS = (((0, 0), (1, 0), (3, 0), (0, 1)), ((0, 3), (2, 0), (0, 2), (1, 1)),
              ((1, 3), (3, 1), (3, 3), (2, 1)), ((2, 3), (1, 2), (3, 2), (2, 2)))
    GROUP_OF = {d: g for g, ds in enumerate(GROUPS) for d in ds}

    def to_partner(l, h, k1, k2, span):
        a1, a2 = where_am_i(h)
        ref = piece(l, core, slot(h, a1 + k1, a2 + k2), span)
        g = GROUP_OF[(k1, k2) if h == 0 else (k2, k1)]
        remote(ref, ref, d_send.at[l], d_recv.at[l, g], partner).start()

    @scoped
    def p1(l):
        pack_wait(l)
        for h in range(2):
            a1, a2 = where_am_i(h)
            w_start(l, mp, SPAN[h], 0, at(h, a1 + 1, a2))
            w_start(l, mp, SPAN[h], 0, at(h, a1 + NX - 1, a2))
        to_partner(l, 0, 0, 0, (0, pack))

    @scoped
    def p2(l):
        w_take(l, 0, 2)
        for h in range(2):
            a1, a2 = where_am_i(h)
            w_start(l, slot(h, a1 + NX - 1, a2), from_minus(h, 0), 1, at(h, a1 + 1, a2))
            w_start(l, slot(h, a1 + 1, a2), from_plus(h, 0), 1, at(h, a1 + NX - 1, a2))
            to_partner(l, h, NX - 1, 0, SPAN[h])
            to_partner(l, h, 1, 0, SPAN[h])

    @scoped
    def p3(l, ks):
        for k in ks:
            if k == 2:
                w_take(l, 1, 1)
            for h in range(2):
                a1, a2 = where_am_i(h)
                p = slot(h, a1 + k, a2)
                w_start(l, p, SPAN[h], 2 + k, at(h, a1, a2 + 1))
                w_start(l, p, SPAN[h], 2 + k, at(h, a1, a2 + NX - 1))
                if k == 2:
                    to_partner(l, h, k, 0, SPAN[h])

    @scoped
    def p4(l, ks):
        for k in ks:
            w_take(l, 2 + k, 2)
            for h in range(2):
                a1, a2 = where_am_i(h)
                w_start(l, slot(h, a1 + k, a2 + NX - 1), from_minus(h, k), 6 + k, at(h, a1, a2 + 1))
                w_start(l, slot(h, a1 + k, a2 + 1), from_plus(h, k), 6 + k, at(h, a1, a2 + NX - 1))
                to_partner(l, h, k, NX - 1, SPAN[h])
                to_partner(l, h, k, 1, SPAN[h])

    @scoped
    def p5(l, ks):
        for k in ks:
            w_take(l, 6 + k, 1)
            for h in range(2):
                to_partner(l, h, k, 2, SPAN[h])

    @scoped
    def w_done(l, gs):
        for g in gs:
            take(w_all.at[l, 1 - core, pl.ds(0, len(GROUPS[g]))], d_recv.at[l, g])

    def h_start(l, first, size, peers):
        for i in peers:
            ref = h_all.at[l, mz, :, pl.ds(first, size)]
            remote(ref, ref, h_send.at[l], h_recv.at[l], z_peer(i)).start()

    @scoped
    def h_wait(l):
        if nz > 1:
            take(h_all.at[l, pl.ds(0, nz - 1)], h_recv.at[l])
        for i in range(nz):
            hres[pl.ds(i * seq_dev, seq_dev)] = h_all[l, i].astype(F32)

    @scoped
    def norm_to_zb(l, gains, residual=False):
        gain = gains[...].astype(F32)[l:l + 1]
        step = min(16, rows)
        for first in range(0, rows, step):
            r = pl.ds(first, step)
            x = hres[r]
            if residual:
                x = (x + acc[r]).astype(BF16).astype(F32)
                hres[r] = x
            inv = lax.rsqrt(jnp.mean(x * x, axis=-1, keepdims=True) + NORM_EPS)
            zb[r] = (x * inv * gain).astype(BF16)

    lane = lax.broadcasted_iota(jnp.int32, (rows, LANES), 1)
    low_half = lane < hd

    def rotate(x):
        first = (lane % hd) < hd // 2
        swapped = jnp.where(first, pltpu.roll(x, LANES - hd // 2, 1), pltpu.roll(x, hd // 2, 1))
        return x * cos_t[...] + swapped * sin_t[...]

    def rope_tables():
        first = (lane % hd) < hd // 2
        t = rope[...]
        cos_t[...] = jnp.where(first, t, pltpu.roll(t, hd // 2, 1))
        sin_t[...] = jnp.where(first, -pltpu.roll(t, LANES - hd // 2, 1), t)

    def kv_copy(l, device):
        ref = kv_all.at[l, core, mp]
        return remote(ref, ref, kv_send.at[l], kv_recv.at[l], device)

    @scoped
    def qkv(l):
        qkv_wait(l)
        kv = lax.dot_general(zb[...], wqkv[l, pl.ds(hq, 2 * hd), :], NT, preferred_element_type=F32)
        kv_all[l, core, mp] = jnp.where(low_half, rotate(kv), kv).astype(BF16)
        for d in far_plane:
            kv_copy(l, plane_peer(*d)).start()
        proj = lax.dot_general(zb[...], wqkv[l, pl.ds(0, hq), :], NT, preferred_element_type=F32)
        for j in range(hq // LANES):
            q = rotate(proj[:, j * LANES:(j + 1) * LANES]) * (hd ** -0.5)
            for half_head, x in enumerate((q, pltpu.roll(q, LANES - hd, 1))):
                head = 2 * j + half_head
                qbuf[pl.ds(head * rows, rows)] = jnp.where(low_half, x, 0.0).astype(BF16)

    @scoped
    def kv_wait(l):
        take(kv_all.at[l, core, pl.ds(0, PLANE - 1)], kv_recv.at[l])
        ref = kv_all.at[l, core]
        remote(ref, ref, kvd_send.at[l], kvd_recv.at[l], partner).start()
        take(kv_all.at[l, 1 - core], kvd_recv.at[l])

    def c_columns(z):
        return pl.ds(pl.multiple_of(z * hq, hq), hq)

    @scoped
    def attention(l):
        keys = 2 * PLANE * rows
        j = lax.broadcasted_iota(jnp.int32, (1, keys), 1)
        key_pos = ((j // seq_dev) % nz) * (2 * PLANE * seq_dev) + ((j // rows) % PLANE) * (2 * seq_dev) \
            + (j // (PLANE * rows)) * seq_dev + j % seq_dev
        i = lax.broadcasted_iota(jnp.int32, (hq // hd * rows, 1), 0) % rows
        q_pos = (i // seq_dev) * (2 * PLANE * seq_dev) + (mp * 2 + core) * seq_dev + i % seq_dev
        allowed = key_pos <= jnp.minimum(q_pos, len_s[0] - 1)
        kv = kv_all[l].reshape(keys, LANES)
        s = lax.dot_general(qbuf[...], kv, NT, preferred_element_type=F32)
        s = jnp.where(allowed, s, -1e30)
        e = jnp.exp(s - jnp.max(s, axis=-1, keepdims=True))
        p = (e * (1.0 / jnp.sum(e, axis=-1, keepdims=True))).astype(BF16)
        o = jnp.dot(p, kv, preferred_element_type=F32)
        for pair in range(hq // LANES):
            even, odd = (o[h * rows:(h + 1) * rows] for h in (2 * pair, 2 * pair + 1))
            c_mat[l, :, pl.ds(pl.multiple_of(mz * hq + pair * LANES, LANES), LANES)] = jnp.where(low_half, pltpu.roll(even, LANES - hd, 1), odd).astype(BF16)
        ref = c_mat.at[l, :, c_columns(mz)]
        for i in far_z:
            remote(ref, ref, c_send.at[l], c_recv.at[l, int(i in next_z)], z_peer(i)).start()

    @scoped
    def out_proj(l):
        with jax.named_scope('wo_wait'):
            wo_copy(l).wait()
        for i in [0] + far_z:
            if i and i in (far_z[0], far_z[-len(next_z)]):
                near = i in next_z
                n = len(next_z) if near else nz - 1 - len(next_z)
                with jax.named_scope('c_wait'):
                    take(c_mat.at[l, :, pl.ds(0, n * hq)], c_recv.at[l, int(near)])
            cols = c_columns((mz + nz - i) % nz)
            part = jnp.dot(c_mat[l, :, cols], wo_v[l, cols, :], preferred_element_type=F32)
            acc[...] = acc[...] + part if i else part

    group = CHUNK // units
    n_groups = len(GROUPS)
    assert group == 2 * len(GROUPS[0])

    def slab(l, g, first, cols):
        parts = [w_all[l, c, slot(0, px + dx, py + dy), pl.ds(first, units), cols] for c in range(2) for dx, dy in GROUPS[g]]
        return jnp.concatenate(parts, axis=0)

    @scoped
    def mlp_units(l, gs):
        block = lax.broadcasted_iota(jnp.int32, (rows, CHUNK), 1) // units
        for g in gs:
            every = pl.ds(0, d_model)
            gate = lax.dot_general(zb[...], slab(l, g, 0, every), NT, preferred_element_type=F32)
            up = lax.dot_general(zb[...], slab(l, g, units, every), NT, preferred_element_type=F32)
            act = gate * (1.0 / (1.0 + jnp.exp(-gate))) * up
            for b in range(group):
                bd[g, pl.ds(b * rows, rows)] = jnp.where(block == b, act, 0.0).astype(BF16)

    two_step = nz == 8
    wide = min(2 * CHUNK, d_model)
    n_sums = d_model // wide

    def ps_of(l, n, i):
        return ps.at[l, n, (mz + i + nz) % nz]

    def rs_start(l, n):
        if not two_step:
            for k, i in enumerate(far_z):
                remote(ps_of(l, n, i), rs.at[l, n, k], rs_send.at[l], rs_recv.at[l, n], z_peer(i)).start()
            return
        for side, to in ((0, nz - 2), (1, 2)):
            cols = pl.ds(side * (wide // 2), wide // 2)
            remote(ps.at[l, n, (mz + 4) % nz, :, cols], ra.at[l, n, 2, :, cols], rs_send.at[l], ra_recv.at[l, n], z_peer(to)).start()
        for side, to in ((0, -1), (1, 1)):
            remote(ps_of(l, n, 3 * to), ra.at[l, n, side], rs_send.at[l], ra_recv.at[l, n], z_peer(nz + to)).start()

    @scoped
    def rs_middle(l):
        if not two_step:
            return

        @pl.loop(0, n_sums)
        def _(n):
            take(ra.at[l, n], ra_recv.at[l, n])
            for side, to in ((0, -2), (1, 2)):
                cols = pl.ds(side * (wide // 2), wide // 2)
                sb[l, n, side] = ps[l, n, (mz + nz + to) % nz] + ra[l, n, side]
                sb[l, n, side, :, cols] = sb[l, n, side, :, cols] + ra[l, n, 2, :, cols]
                remote(sb.at[l, n, side], rs.at[l, n, 2 + side], rs_send.at[l], rs_recv.at[l, n], z_peer(nz + to)).start()
            for side, to in ((0, -1), (1, 1)):
                remote(ps_of(l, n, to), rs.at[l, n, side], rs_send.at[l], rs_recv.at[l, n], z_peer(nz + to)).start()

    @scoped
    def mlp_down(l):
        @pl.loop(0, n_sums)
        def _(n):
            cols = pl.ds(pl.multiple_of(n * wide, wide), wide)
            total = jnp.zeros((rows, wide), F32)
            for g in range(n_groups):
                y = jnp.dot(bd[g], slab(l, g, 2 * units, cols), preferred_element_type=F32)
                y = y.astype(BF16).astype(F32)
                for b in range(group):
                    total = total + y[b * rows:(b + 1) * rows]
            ps[l, n] = total.reshape(nz, seq_dev, wide)
            rs_start(l, n)

    n_in = 4 if two_step else nz - 1

    @scoped
    def rs_finish(l, store):
        mine = pl.ds(pl.multiple_of(mz * seq_dev, seq_dev), seq_dev)
        for n in range(n_sums):
            if n_in:
                take(rs.at[l, n], rs_recv.at[l, n])
            total = ps[l, n, mz]
            for k in range(n_in):
                total = total + rs[l, n, k]
            store(n, (hres[mine, n * wide:(n + 1) * wide] + total).astype(BF16))

    def store_next(l):
        def store(n, x):
            h_all[l + 1, mz, :, n * wide:(n + 1) * wide] = x
            h_start(l + 1, n * wide, wide, far_z)
        return store

    with jax.named_scope('barrier'):
        pl.semaphore_wait(barrier, 1 + len(next_devices))
    round_start(0)
    p1(0)
    p3(0, (0,))
    with jax.named_scope('rounds'):
        small[0].wait()
        for r in range(4):
            if r:
                round_wait(r - 1)
                if r < 3:
                    round_start(r)
            h_start(0, 0, d_model, [i for i in far_z if min(i, nz - i) == r + 1])
    start_later_copies()
    with jax.named_scope('small'):
        for c in small[1:]:
            c.wait()
        rope_tables()
    p2(0)
    for l in range(layers):
        more = l + 1 < layers
        h_wait(l)
        norm_to_zb(l, ga)
        qkv(l)
        if l == 0:
            p3(0, (1, 3, 2))
            p4(0, (0,))
        else:
            p4(l, (0, 1, 3, 2))
        kv_wait(l)
        attention(l)
        if l == 0:
            p4(0, (1, 3, 2))
            p5(0, (0,))
        else:
            p5(l, (0, 1, 3, 2))
        if more:
            p1(l + 1)
            p3(l + 1, (0,))
        out_proj(l)
        norm_to_zb(l, gm, True)
        if l == 0:
            w_done(l, (0,))
            mlp_units(l, (0,))
            w_done(l, (1,))
            mlp_units(l, (1,))
            p5(l, (1, 3))
            w_done(l, (2,))
            mlp_units(l, (2,))
            p5(l, (2,))
            w_done(l, (3,))
            mlp_units(l, (3,))
        else:
            w_done(l, range(n_groups))
            mlp_units(l, range(n_groups))
        mlp_down(l)
        if more:
            p2(l + 1)
            p3(l + 1, (1, 3))
        rs_middle(l)
        if more:
            rs_finish(l, store_next(l))
            p3(l + 1, (2,))
    pieces = []
    rs_finish(layers - 1, lambda n, x: pieces.append(x.astype(F32)))
    x = jnp.concatenate(pieces, axis=1)
    inv = lax.rsqrt(jnp.mean(x * x, axis=-1, keepdims=True) + NORM_EPS)
    gain = gf[...].astype(F32)
    for i in range(d_model // LANES):
        cols = slice(i * LANES, (i + 1) * LANES)
        out_ref[:, cols] = x[:, cols] * inv * gain[i:i + 1]

    with jax.named_scope('drain'):
      for l in range(layers):
          ref = w_all.at[l, 0, pl.ds(0, PLANE - 1)]
          remote(ref, ref, w_send.at[l], w_recv.at[l, 0], me).wait_send()
          ref = w_all.at[l, 0]
          remote(ref, ref, d_send.at[l], d_recv.at[l, 0], me).wait_send()
          ref = kv_all.at[l, 0, pl.ds(0, PLANE - 1)]
          remote(ref, ref, kv_send.at[l], kv_recv.at[l], me).wait_send()
          ref = kv_all.at[l, 0]
          remote(ref, ref, kvd_send.at[l], kvd_recv.at[l], me).wait_send()
          if nz > 1:
              ref = h_all.at[l, pl.ds(0, nz - 1)]
              remote(ref, ref, h_send.at[l], h_recv.at[l], me).wait_send()
              ref = c_mat.at[l, :, pl.ds(0, (nz - 1) * hq)]
              remote(ref, ref, c_send.at[l], c_recv.at[l, 0], me).wait_send()
              ref = ps.at[l, :, pl.ds(0, nz - 1)]
              remote(ref, ref, rs_send.at[l], rs_recv.at[l, 0], me).wait_send()


def solution(mesh):
    nz = mesh.shape['tp'] // (2 * PLANE)

    def device_fn(hidden_in, lengths, attn_norm, w_query, w_key, w_value, w_out, mlp_norm, w_gate, w_up, w_down, final_norm):
        seq_dev, d_model = hidden_in.shape[1:]
        layers, _, heads, hd = w_query.shape
        kv_heads = w_key.shape[2]
        units = w_gate.shape[2]
        assert kv_heads == nz and 2 * hd == LANES and heads % nz == 0
        hq = heads // nz * hd
        rows = nz * seq_dev
        wide = min(2 * CHUNK, d_model)
        n_sums = d_model // wide
        n_groups = 2 * PLANE * units // CHUNK
        dev, row = np.arange(2 * PLANE)[:, None], np.arange(rows)[None, :]
        pos = (row // seq_dev) * (2 * PLANE * seq_dev) + dev * seq_dev + row % seq_dev
        freq = np.float32(ROPE_BASE) ** (np.float32(-2.0) * np.arange(hd // 2, dtype=np.float32) / np.float32(hd))
        angles = (pos[..., None].astype(np.float32) * freq).astype(np.float64)
        rope = np.tile(np.concatenate([np.cos(angles), np.sin(angles)], axis=-1), (1, 1, 2)).astype(np.float32)
        by_rows = lambda w: jnp.transpose(w, (0, 2, 3, 1)).reshape(layers, -1, d_model)
        units_first = lambda w: jnp.transpose(w, (0, 2, 1))
        pinned = lambda x: pltpu.with_memory_space_constraint(x, pltpu.HBM)
        hbm, vmem = (pl.BlockSpec(memory_space=s) for s in (pltpu.HBM, pltpu.VMEM))
        dma = pltpu.SemaphoreType.DMA
        out = pl.pallas_call(
            functools.partial(kernel, nz),
            name='decoder',
            out_shape=pltpu.VMEM((seq_dev, d_model), F32),
            in_specs=[hbm] * 13,
            out_specs=vmem,
            scratch_shapes=[
                pltpu.VMEM((layers, 2, PLANE, 3 * units, d_model), BF16),
                pltpu.VMEM((layers, heads * hd, d_model), BF16),
                pltpu.VMEM((layers, hq + 2 * hd, d_model), BF16),
                pltpu.VMEM((layers, nz, seq_dev, d_model), BF16),
                pltpu.VMEM((layers, rows, heads * hd), BF16),
                pltpu.VMEM((layers, 2, PLANE, rows, LANES), BF16),
                pltpu.VMEM((layers, n_sums, 4 if nz == 8 else max(nz - 1, 1), seq_dev, wide), F32),
                pltpu.VMEM((layers, n_sums, 3, seq_dev, wide), F32),
                pltpu.VMEM((layers, n_sums, 2, seq_dev, wide), F32),
                pltpu.VMEM((layers, n_sums, nz, seq_dev, wide), F32),
                pltpu.VMEM((rows, d_model), F32),
                pltpu.VMEM((rows, d_model), F32),
                pltpu.VMEM((rows, d_model), BF16),
                pltpu.VMEM((hq // hd * rows, LANES), BF16),
                pltpu.VMEM((n_groups, CHUNK // units * rows, CHUNK), BF16),
                pltpu.VMEM((rows, LANES), F32), pltpu.VMEM((rows, LANES), F32), pltpu.VMEM((rows, LANES), F32),
                pltpu.VMEM((layers, d_model), BF16), pltpu.VMEM((layers, d_model), BF16),
                pltpu.VMEM((d_model // LANES, LANES), BF16),
                pltpu.SMEM((1,), jnp.int32),
                dma((layers, 3)), dma((6,)), dma((layers, 10)), dma((layers,)),
                dma((layers, n_groups)), dma((layers,)),
                pltpu.SemaphoreType.REGULAR((3,)),
                dma((layers,)), dma((layers,)), dma((layers,)), dma((layers,)), dma((layers,)), dma((layers,)),
                dma((layers, 2)), dma((layers,)), dma((layers, n_sums)), dma((layers, n_sums)), dma((layers,)),
            ],
            compiler_params=pltpu.CompilerParams(
                collective_id=0, has_side_effects=True, vmem_limit_bytes=60_000_000),
        )(pinned(hidden_in[0]), lengths, *map(pinned, (
            jnp.asarray(rope), attn_norm, mlp_norm, final_norm.reshape(-1, LANES), by_rows(w_query), by_rows(w_key), by_rows(w_value),
            w_out.reshape(layers, heads * hd, d_model), units_first(w_gate), units_first(w_up), w_down)))
        return out.astype(BF16)[None]

    seq_part = P(None, 'tp', None)
    in_specs = (seq_part, P(), P(), P(), P(), P(), P(), P(), P(None, None, 'tp'), P(None, None, 'tp'), P(None, 'tp', None), P())
    return jax.shard_map(device_fn, mesh=mesh, in_specs=in_specs, out_specs=seq_part, check_vma=False)
```

```python
import functools

import jax
import jax.numpy as jnp
import numpy as np
from jax import lax
from jax.experimental import pallas as pl
from jax.experimental.pallas import tpu as pltpu
from jax.sharding import PartitionSpec as P

NORM_EPS = 1e-5
ROPE_BASE = 500000.0
NX = 4
PLANE = NX * NX
LANES = 128
CHUNK = 256
NT = (((1,), (1,)), ((), ()))
F32, BF16 = jnp.float32, jnp.bfloat16


def remote(src, dst, send_sem, recv_sem, device):
    return pltpu.make_async_remote_copy(
        src_ref=src, dst_ref=dst, send_sem=send_sem, recv_sem=recv_sem,
        device_id=(device,), device_id_type=pl.DeviceIdType.MESH)


def scoped(f):
    @functools.wraps(f)
    def wrapped(*args):
        with jax.named_scope(f.__name__ + ('#l=%d' % args[0])):
            return f(*args)
    return wrapped


def kernel(nz, h_ref, len_ref, rope_ref, ga_ref, gm_ref, gf_ref, wq_ref, wk_ref, wv_ref, wo_ref, wg_ref, wu_ref, wd_ref,
           out_ref, w_all, wo_v, wqkv, h_all, c_mat, kv_all, rs, ra, sb, ps, acc, hres, zb, qbuf, bd, rope, cos_t, sin_t, ga, gm, gf, len_s,
           local_sem, in_sem, w_recv, w_send, d_recv, d_send, rounds, h_recv, h_send, kv_recv, kv_send, kvd_recv, kvd_send,
           c_recv, c_send, rs_recv, ra_recv, rs_send):
    layers = wo_ref.shape[0]
    seq_dev, d_model = h_ref.shape
    units = wg_ref.shape[1]
    pack = 3 * units
    half = pack // 2
    rows = nz * seq_dev
    hq = wq_ref.shape[1] // nz
    hd = wk_ref.shape[1] // nz
    me = lax.axis_index('tp')
    core = me % 2
    px = (me // 2) % NX
    py = (me // (2 * NX)) % NX
    mp = (me // 2) % PLANE
    mz = me // (2 * PLANE)
    base = mz * (2 * PLANE)
    partner = base + mp * 2 + (1 - core)

    def z_peer(i):
        return ((mz + i) % nz) * (2 * PLANE) + mp * 2 + core

    far_z = sorted(range(1, nz), key=lambda i: -min(i, nz - i))
    next_z = [i for i in far_z if min(i, nz - i) == 1]
    def plane_peer(dy, dx):
        return base + ((py + dy) % NX * NX + (px + dx) % NX) * 2 + core

    far_plane = sorted(((dy, dx) for dy in range(NX) for dx in range(NX) if dy or dx),
                       key=lambda d: -sum(min(i, NX - i) for i in d))

    barrier = pltpu.get_barrier_semaphore()
    next_devices = [plane_peer(0, 1), plane_peer(0, NX - 1), plane_peer(1, 0), plane_peer(NX - 1, 0)]
    next_devices += [z_peer(i) for i in next_z]

    def signal(sem, device):
        pl.semaphore_signal(sem, inc=1, device_id=(device,), device_id_type=pl.DeviceIdType.MESH)

    signal(barrier, partner)
    for d in next_devices:
        signal(barrier, d)

    def round_start(r):
        for d in next_devices:
            signal(rounds.at[r], d)

    def round_wait(r):
        pl.semaphore_wait(rounds.at[r], len(next_devices))

    def pack_copies(l):
        mine = w_all.at[l, core, mp]
        return [pltpu.make_async_copy(ref.at[l], mine.at[pl.ds(i * units, units)], local_sem.at[l, 0])
                for i, ref in enumerate((wg_ref, wu_ref, wd_ref))]

    def qkv_copies(l):
        return [pltpu.make_async_copy(ref.at[l, pl.ds(mz * n, n)], wqkv.at[l, pl.ds(first, n)], local_sem.at[l, 1])
                for ref, first, n in ((wq_ref, 0, hq), (wk_ref, hq, hd), (wv_ref, hq + hd, hd))]

    def wo_copy(l):
        return pltpu.make_async_copy(wo_ref.at[l], wo_v.at[l], local_sem.at[l, 2])

    def take(ref, sem):
        remote(ref, ref, w_send.at[0], sem, me).wait_recv()

    def pack_wait(l):
        mine = w_all.at[l, core, mp]
        pltpu.make_async_copy(mine, mine, local_sem.at[l, 0]).wait()

    def qkv_wait(l):
        pltpu.make_async_copy(wqkv.at[l], wqkv.at[l], local_sem.at[l, 1]).wait()

    small = [pltpu.make_async_copy(src, dst, in_sem.at[i]) for i, (src, dst) in enumerate((
        (h_ref, h_all.at[0, mz]), (rope_ref.at[mp * 2 + core], rope), (ga_ref, ga), (gm_ref, gm), (gf_ref, gf), (len_ref, len_s)))]
    for c in pack_copies(0) + small + qkv_copies(0):
        c.start()

    def start_later_copies():
        wo_copy(0).start()
        for l in range(1, layers):
            for c in pack_copies(l) + qkv_copies(l):
                c.start()
            wo_copy(l).start()

    def slot(h, a1, a2):
        return a2 % NX * NX + a1 % NX if h == 0 else a1 % NX * NX + a2 % NX

    def where_am_i(h):
        return (px, py) if h == 0 else (py, px)

    def at(h, a1, a2):
        return base + slot(h, a1, a2) * 2 + core

    third = half // 3
    SPAN = ((0, half), (half, half))

    def from_minus(h, k):
        return (h * half, 2 * third if (k in (1, 2)) != (h == 1) else third)

    def from_plus(h, k):
        first, size = from_minus(h, k)
        return (first + size, half - size)

    def piece(l, c, p, span):
        return w_all.at[l, c, p, pl.ds(*span)]

    def w_start(l, p, span, idx, device):
        ref = piece(l, core, p, span)
        remote(ref, ref, w_send.at[l], w_recv.at[l, idx], device).start()

    def w_take(l, idx, packs):
        take(w_all.at[l, core, pl.ds(0, packs)], w_recv.at[l, idx])

    GROUPS = (((0, 0), (1, 0), (3, 0), (0, 1)), ((0, 3), (2, 0), (0, 2), (1, 1)),
              ((1, 3), (3, 1), (3, 3), (2, 1)), ((2, 3), (1, 2), (3, 2), (2, 2)))
    GROUP_OF = {d: g for g, ds in enumerate(GROUPS) for d in ds}

    def to_partner(l, h, k1, k2, span):
        a1, a2 = where_am_i(h)
        ref = piece(l, core, slot(h, a1 + k1, a2 + k2), span)
        g = GROUP_OF[(k1, k2) if h == 0 else (k2, k1)]
        remote(ref, ref, d_send.at[l], d_recv.at[l, g], partner).start()

    @scoped
    def p1(l):
        pack_wait(l)
        for h in range(2):
            a1, a2 = where_am_i(h)
            w_start(l, mp, SPAN[h], 0, at(h, a1 + 1, a2))
            w_start(l, mp, SPAN[h], 0, at(h, a1 + NX - 1, a2))
        to_partner(l, 0, 0, 0, (0, pack))

    @scoped
    def p2(l):
        w_take(l, 0, 2)
        for h in range(2):
            a1, a2 = where_am_i(h)
            w_start(l, slot(h, a1 + NX - 1, a2), from_minus(h, 0), 1, at(h, a1 + 1, a2))
            w_start(l, slot(h, a1 + 1, a2), from_plus(h, 0), 1, at(h, a1 + NX - 1, a2))
            to_partner(l, h, NX - 1, 0, SPAN[h])
            to_partner(l, h, 1, 0, SPAN[h])

    @scoped
    def p3(l, ks):
        for k in ks:
            if k == 2:
                w_take(l, 1, 1)
            for h in range(2):
                a1, a2 = where_am_i(h)
                p = slot(h, a1 + k, a2)
                w_start(l, p, SPAN[h], 2 + k, at(h, a1, a2 + 1))
                w_start(l, p, SPAN[h], 2 + k, at(h, a1, a2 + NX - 1))
                if k == 2:
                    to_partner(l, h, k, 0, SPAN[h])

    @scoped
    def p4(l, ks):
        for k in ks:
            w_take(l, 2 + k, 2)
            for h in range(2):
                a1, a2 = where_am_i(h)
                w_start(l, slot(h, a1 + k, a2 + NX - 1), from_minus(h, k), 6 + k, at(h, a1, a2 + 1))
                w_start(l, slot(h, a1 + k, a2 + 1), from_plus(h, k), 6 + k, at(h, a1, a2 + NX - 1))
                to_partner(l, h, k, NX - 1, SPAN[h])
                to_partner(l, h, k, 1, SPAN[h])

    @scoped
    def p5(l, ks):
        for k in ks:
            w_take(l, 6 + k, 1)
            for h in range(2):
                to_partner(l, h, k, 2, SPAN[h])

    @scoped
    def w_done(l, gs):
        for g in gs:
            take(w_all.at[l, 1 - core, pl.ds(0, len(GROUPS[g]))], d_recv.at[l, g])

    def h_start(l, first, size, peers):
        for i in peers:
            ref = h_all.at[l, mz, :, pl.ds(first, size)]
            remote(ref, ref, h_send.at[l], h_recv.at[l], z_peer(i)).start()

    @scoped
    def h_wait(l):
        if nz > 1:
            take(h_all.at[l, pl.ds(0, nz - 1)], h_recv.at[l])
        for i in range(nz):
            hres[pl.ds(i * seq_dev, seq_dev)] = h_all[l, i].astype(F32)

    @scoped
    def norm_to_zb(l, gains, residual=False):
        gain = gains[...].astype(F32)[l:l + 1]
        step = min(16, rows)
        for first in range(0, rows, step):
            r = pl.ds(first, step)
            x = hres[r]
            if residual:
                x = (x + acc[r]).astype(BF16).astype(F32)
                hres[r] = x
            inv = lax.rsqrt(jnp.mean(x * x, axis=-1, keepdims=True) + NORM_EPS)
            zb[r] = (x * inv * gain).astype(BF16)

    lane = lax.broadcasted_iota(jnp.int32, (rows, LANES), 1)
    low_half = lane < hd

    def rotate(x):
        first = (lane % hd) < hd // 2
        swapped = jnp.where(first, pltpu.roll(x, LANES - hd // 2, 1), pltpu.roll(x, hd // 2, 1))
        return x * cos_t[...] + swapped * sin_t[...]

    def rope_tables():
        first = (lane % hd) < hd // 2
        t = rope[...]
        cos_t[...] = jnp.where(first, t, pltpu.roll(t, hd // 2, 1))
        sin_t[...] = jnp.where(first, -pltpu.roll(t, LANES - hd // 2, 1), t)

    def kv_copy(l, device):
        ref = kv_all.at[l, core, mp]
        return remote(ref, ref, kv_send.at[l], kv_recv.at[l], device)

    @scoped
    def qkv(l):
        qkv_wait(l)
        kv = lax.dot_general(zb[...], wqkv[l, pl.ds(hq, 2 * hd), :], NT, preferred_element_type=F32)
        kv_all[l, core, mp] = jnp.where(low_half, rotate(kv), kv).astype(BF16)
        for d in far_plane:
            kv_copy(l, plane_peer(*d)).start()
        proj = lax.dot_general(zb[...], wqkv[l, pl.ds(0, hq), :], NT, preferred_element_type=F32)
        for j in range(hq // LANES):
            q = rotate(proj[:, j * LANES:(j + 1) * LANES]) * (hd ** -0.5)
            for half_head, x in enumerate((q, pltpu.roll(q, LANES - hd, 1))):
                head = 2 * j + half_head
                qbuf[pl.ds(head * rows, rows)] = jnp.where(low_half, x, 0.0).astype(BF16)

    @scoped
    def kv_wait(l):
        take(kv_all.at[l, core, pl.ds(0, PLANE - 1)], kv_recv.at[l])
        ref = kv_all.at[l, core]
        remote(ref, ref, kvd_send.at[l], kvd_recv.at[l], partner).start()
        take(kv_all.at[l, 1 - core], kvd_recv.at[l])

    def c_columns(z):
        return pl.ds(pl.multiple_of(z * hq, hq), hq)

    @scoped
    def attention(l):
        keys = 2 * PLANE * rows
        j = lax.broadcasted_iota(jnp.int32, (1, keys), 1)
        key_pos = ((j // seq_dev) % nz) * (2 * PLANE * seq_dev) + ((j // rows) % PLANE) * (2 * seq_dev) \
            + (j // (PLANE * rows)) * seq_dev + j % seq_dev
        i = lax.broadcasted_iota(jnp.int32, (hq // hd * rows, 1), 0) % rows
        q_pos = (i // seq_dev) * (2 * PLANE * seq_dev) + (mp * 2 + core) * seq_dev + i % seq_dev
        allowed = key_pos <= jnp.minimum(q_pos, len_s[0] - 1)
        kv = kv_all[l].reshape(keys, LANES)
        s = lax.dot_general(qbuf[...], kv, NT, preferred_element_type=F32)
        s = jnp.where(allowed, s, -1e30)
        e = jnp.exp(s - jnp.max(s, axis=-1, keepdims=True))
        p = (e * (1.0 / jnp.sum(e, axis=-1, keepdims=True))).astype(BF16)
        o = jnp.dot(p, kv, preferred_element_type=F32)
        for pair in range(hq // LANES):
            even, odd = (o[h * rows:(h + 1) * rows] for h in (2 * pair, 2 * pair + 1))
            c_mat[l, :, pl.ds(pl.multiple_of(mz * hq + pair * LANES, LANES), LANES)] = jnp.where(low_half, pltpu.roll(even, LANES - hd, 1), odd).astype(BF16)
        ref = c_mat.at[l, :, c_columns(mz)]
        for i in far_z:
            remote(ref, ref, c_send.at[l], c_recv.at[l, int(i in next_z)], z_peer(i)).start()

    @scoped
    def out_proj(l):
        with jax.named_scope('wo_wait'):
            wo_copy(l).wait()
        for i in [0] + far_z:
            if i and i in (far_z[0], far_z[-len(next_z)]):
                near = i in next_z
                n = len(next_z) if near else nz - 1 - len(next_z)
                with jax.named_scope('c_wait'):
                    take(c_mat.at[l, :, pl.ds(0, n * hq)], c_recv.at[l, int(near)])
            cols = c_columns((mz + nz - i) % nz)
            part = jnp.dot(c_mat[l, :, cols], wo_v[l, cols, :], preferred_element_type=F32)
            acc[...] = acc[...] + part if i else part

    group = CHUNK // units
    n_groups = len(GROUPS)
    assert group == 2 * len(GROUPS[0])

    def slab(l, g, first, cols):
        parts = [w_all[l, c, slot(0, px + dx, py + dy), pl.ds(first, units), cols] for c in range(2) for dx, dy in GROUPS[g]]
        return jnp.concatenate(parts, axis=0)

    @scoped
    def mlp_units(l, gs):
        block = lax.broadcasted_iota(jnp.int32, (rows, CHUNK), 1) // units
        for g in gs:
            every = pl.ds(0, d_model)
            gate = lax.dot_general(zb[...], slab(l, g, 0, every), NT, preferred_element_type=F32)
            up = lax.dot_general(zb[...], slab(l, g, units, every), NT, preferred_element_type=F32)
            act = gate * (1.0 / (1.0 + jnp.exp(-gate))) * up
            for b in range(group):
                bd[g, pl.ds(b * rows, rows)] = jnp.where(block == b, act, 0.0).astype(BF16)

    two_step = nz == 8
    wide = min(2 * CHUNK, d_model)
    n_sums = d_model // wide

    def ps_of(l, n, i):
        return ps.at[l, n, (mz + i + nz) % nz]

    def rs_start(l, n):
        if not two_step:
            for k, i in enumerate(far_z):
                remote(ps_of(l, n, i), rs.at[l, n, k], rs_send.at[l], rs_recv.at[l, n], z_peer(i)).start()
            return
        for side, to in ((0, nz - 2), (1, 2)):
            cols = pl.ds(side * (wide // 2), wide // 2)
            remote(ps.at[l, n, (mz + 4) % nz, :, cols], ra.at[l, n, 2, :, cols], rs_send.at[l], ra_recv.at[l, n], z_peer(to)).start()
        for side, to in ((0, -1), (1, 1)):
            remote(ps_of(l, n, 3 * to), ra.at[l, n, side], rs_send.at[l], ra_recv.at[l, n], z_peer(nz + to)).start()

    @scoped
    def rs_middle(l):
        if not two_step:
            return
        for n in range(n_sums):
            for side, to in ((0, -1), (1, 1)):
                remote(ps_of(l, n, to), rs.at[l, n, side], rs_send.at[l], rs_recv.at[l, n], z_peer(nz + to)).start()

        @pl.loop(0, n_sums)
        def _(n):
            take(ra.at[l, n], ra_recv.at[l, n])
            for side, to in ((0, -2), (1, 2)):
                cols = pl.ds(side * (wide // 2), wide // 2)
                sb[l, n, side] = ps[l, n, (mz + nz + to) % nz] + ra[l, n, side]
                sb[l, n, side, :, cols] = sb[l, n, side, :, cols] + ra[l, n, 2, :, cols]
                remote(sb.at[l, n, side], rs.at[l, n, 2 + side], rs_send.at[l], rs_recv.at[l, n], z_peer(nz + to)).start()

    @scoped
    def mlp_down(l):
        @pl.loop(0, n_sums)
        def _(n):
            cols = pl.ds(pl.multiple_of(n * wide, wide), wide)
            total = jnp.zeros((rows, wide), F32)
            for g in range(n_groups):
                y = jnp.dot(bd[g], slab(l, g, 2 * units, cols), preferred_element_type=F32)
                y = y.astype(BF16).astype(F32)
                for b in range(group):
                    total = total + y[b * rows:(b + 1) * rows]
            ps[l, n] = total.reshape(nz, seq_dev, wide)
            rs_start(l, n)

    n_in = 4 if two_step else nz - 1

    @scoped
    def rs_finish(l, store):
        mine = pl.ds(pl.multiple_of(mz * seq_dev, seq_dev), seq_dev)
        for n in range(n_sums):
            if n_in:
                take(rs.at[l, n], rs_recv.at[l, n])
            total = ps[l, n, mz]
            for k in range(n_in):
                total = total + rs[l, n, k]
            store(n, (hres[mine, n * wide:(n + 1) * wide] + total).astype(BF16))

    def store_next(l):
        def store(n, x):
            h_all[l + 1, mz, :, n * wide:(n + 1) * wide] = x
            h_start(l + 1, n * wide, wide, far_z)
        return store

    with jax.named_scope('barrier'):
        pl.semaphore_wait(barrier, 1 + len(next_devices))
    round_start(0)
    p1(0)
    p3(0, (0,))
    with jax.named_scope('rounds'):
        small[0].wait()
        for r in range(4):
            if r:
                round_wait(r - 1)
                if r < 3:
                    round_start(r)
            h_start(0, 0, d_model, [i for i in far_z if min(i, nz - i) == r + 1])
    start_later_copies()
    with jax.named_scope('small'):
        for c in small[1:]:
            c.wait()
        rope_tables()
    p2(0)
    p3(0, (1,))
    for l in range(layers):
        more = l + 1 < layers
        h_wait(l)
        norm_to_zb(l, ga)
        qkv(l)
        if l == 0:
            p3(0, (3, 2))
            p4(0, (0,))
        else:
            p4(l, (0, 1, 3, 2))
        kv_wait(l)
        attention(l)
        if l == 0:
            p4(0, (1, 3, 2))
            p5(0, (0,))
        else:
            p5(l, (0, 1, 3, 2))
        if more:
            p1(l + 1)
            p3(l + 1, (0,))
        out_proj(l)
        norm_to_zb(l, gm, True)
        if l == 0:
            w_done(l, (0,))
            mlp_units(l, (0,))
            w_done(l, (1,))
            mlp_units(l, (1,))
            p5(l, (1, 3))
            w_done(l, (2,))
            mlp_units(l, (2,))
            p5(l, (2,))
            w_done(l, (3,))
            mlp_units(l, (3,))
        else:
            w_done(l, range(n_groups))
            mlp_units(l, range(n_groups))
        mlp_down(l)
        if more:
            p2(l + 1)
            p3(l + 1, (1, 3))
        rs_middle(l)
        if more:
            rs_finish(l, store_next(l))
            p3(l + 1, (2,))
    pieces = []
    rs_finish(layers - 1, lambda n, x: pieces.append(x.astype(F32)))
    x = jnp.concatenate(pieces, axis=1)
    inv = lax.rsqrt(jnp.mean(x * x, axis=-1, keepdims=True) + NORM_EPS)
    gain = gf[...].astype(F32)
    for i in range(d_model // LANES):
        cols = slice(i * LANES, (i + 1) * LANES)
        out_ref[:, cols] = x[:, cols] * inv * gain[i:i + 1]

    with jax.named_scope('drain'):
      for l in range(layers):
          ref = w_all.at[l, 0, pl.ds(0, PLANE - 1)]
          remote(ref, ref, w_send.at[l], w_recv.at[l, 0], me).wait_send()
          ref = w_all.at[l, 0]
          remote(ref, ref, d_send.at[l], d_recv.at[l, 0], me).wait_send()
          ref = kv_all.at[l, 0, pl.ds(0, PLANE - 1)]
          remote(ref, ref, kv_send.at[l], kv_recv.at[l], me).wait_send()
          ref = kv_all.at[l, 0]
          remote(ref, ref, kvd_send.at[l], kvd_recv.at[l], me).wait_send()
          if nz > 1:
              ref = h_all.at[l, pl.ds(0, nz - 1)]
              remote(ref, ref, h_send.at[l], h_recv.at[l], me).wait_send()
              ref = c_mat.at[l, :, pl.ds(0, (nz - 1) * hq)]
              remote(ref, ref, c_send.at[l], c_recv.at[l, 0], me).wait_send()
              ref = ps.at[l, :, pl.ds(0, nz - 1)]
              remote(ref, ref, rs_send.at[l], rs_recv.at[l, 0], me).wait_send()


def solution(mesh):
    nz = mesh.shape['tp'] // (2 * PLANE)

    def device_fn(hidden_in, lengths, attn_norm, w_query, w_key, w_value, w_out, mlp_norm, w_gate, w_up, w_down, final_norm):
        seq_dev, d_model = hidden_in.shape[1:]
        layers, _, heads, hd = w_query.shape
        kv_heads = w_key.shape[2]
        units = w_gate.shape[2]
        assert kv_heads == nz and 2 * hd == LANES and heads % nz == 0
        hq = heads // nz * hd
        rows = nz * seq_dev
        wide = min(2 * CHUNK, d_model)
        n_sums = d_model // wide
        n_groups = 2 * PLANE * units // CHUNK
        dev, row = np.arange(2 * PLANE)[:, None], np.arange(rows)[None, :]
        pos = (row // seq_dev) * (2 * PLANE * seq_dev) + dev * seq_dev + row % seq_dev
        freq = np.float32(ROPE_BASE) ** (np.float32(-2.0) * np.arange(hd // 2, dtype=np.float32) / np.float32(hd))
        angles = (pos[..., None].astype(np.float32) * freq).astype(np.float64)
        rope = np.tile(np.concatenate([np.cos(angles), np.sin(angles)], axis=-1), (1, 1, 2)).astype(np.float32)
        by_rows = lambda w: jnp.transpose(w, (0, 2, 3, 1)).reshape(layers, -1, d_model)
        units_first = lambda w: jnp.transpose(w, (0, 2, 1))
        pinned = lambda x: pltpu.with_memory_space_constraint(x, pltpu.HBM)
        hbm, vmem = (pl.BlockSpec(memory_space=s) for s in (pltpu.HBM, pltpu.VMEM))
        dma = pltpu.SemaphoreType.DMA
        out = pl.pallas_call(
            functools.partial(kernel, nz),
            name='decoder',
            out_shape=pltpu.VMEM((seq_dev, d_model), F32),
            in_specs=[hbm] * 13,
            out_specs=vmem,
            scratch_shapes=[
                pltpu.VMEM((layers, 2, PLANE, 3 * units, d_model), BF16),
                pltpu.VMEM((layers, heads * hd, d_model), BF16),
                pltpu.VMEM((layers, hq + 2 * hd, d_model), BF16),
                pltpu.VMEM((layers, nz, seq_dev, d_model), BF16),
                pltpu.VMEM((layers, rows, heads * hd), BF16),
                pltpu.VMEM((layers, 2, PLANE, rows, LANES), BF16),
                pltpu.VMEM((layers, n_sums, 4 if nz == 8 else max(nz - 1, 1), seq_dev, wide), F32),
                pltpu.VMEM((layers, n_sums, 3, seq_dev, wide), F32),
                pltpu.VMEM((layers, n_sums, 2, seq_dev, wide), F32),
                pltpu.VMEM((layers, n_sums, nz, seq_dev, wide), F32),
                pltpu.VMEM((rows, d_model), F32),
                pltpu.VMEM((rows, d_model), F32),
                pltpu.VMEM((rows, d_model), BF16),
                pltpu.VMEM((hq // hd * rows, LANES), BF16),
                pltpu.VMEM((n_groups, CHUNK // units * rows, CHUNK), BF16),
                pltpu.VMEM((rows, LANES), F32), pltpu.VMEM((rows, LANES), F32), pltpu.VMEM((rows, LANES), F32),
                pltpu.VMEM((layers, d_model), BF16), pltpu.VMEM((layers, d_model), BF16),
                pltpu.VMEM((d_model // LANES, LANES), BF16),
                pltpu.SMEM((1,), jnp.int32),
                dma((layers, 3)), dma((6,)), dma((layers, 10)), dma((layers,)),
                dma((layers, n_groups)), dma((layers,)),
                pltpu.SemaphoreType.REGULAR((3,)),
                dma((layers,)), dma((layers,)), dma((layers,)), dma((layers,)), dma((layers,)), dma((layers,)),
                dma((layers, 2)), dma((layers,)), dma((layers, n_sums)), dma((layers, n_sums)), dma((layers,)),
            ],
            compiler_params=pltpu.CompilerParams(
                collective_id=0, has_side_effects=True, vmem_limit_bytes=60_000_000),
        )(pinned(hidden_in[0]), lengths, *map(pinned, (
            jnp.asarray(rope), attn_norm, mlp_norm, final_norm.reshape(-1, LANES), by_rows(w_query), by_rows(w_key), by_rows(w_value),
            w_out.reshape(layers, heads * hd, d_model), units_first(w_gate), units_first(w_up), w_down)))
        return out.astype(BF16)[None]

    seq_part = P(None, 'tp', None)
    in_specs = (seq_part, P(), P(), P(), P(), P(), P(), P(), P(None, None, 'tp'), P(None, None, 'tp'), P(None, 'tp', None), P())
    return jax.shard_map(device_fn, mesh=mesh, in_specs=in_specs, out_specs=seq_part, check_vma=False)
```

```python
import functools

import jax
import jax.numpy as jnp
import numpy as np
from jax import lax
from jax.experimental import pallas as pl
from jax.experimental.pallas import tpu as pltpu
from jax.sharding import PartitionSpec as P

NORM_EPS = 1e-5
ROPE_BASE = 500000.0
NX = 4
PLANE = NX * NX
LANES = 128
CHUNK = 256
NT = (((1,), (1,)), ((), ()))
F32, BF16 = jnp.float32, jnp.bfloat16


def remote(src, dst, send_sem, recv_sem, device):
    return pltpu.make_async_remote_copy(
        src_ref=src, dst_ref=dst, send_sem=send_sem, recv_sem=recv_sem,
        device_id=(device,), device_id_type=pl.DeviceIdType.MESH)


def scoped(f):
    @functools.wraps(f)
    def wrapped(*args):
        with jax.named_scope(f.__name__ + ('#l=%d' % args[0])):
            return f(*args)
    return wrapped


def kernel(nz, h_ref, len_ref, rope_ref, ga_ref, gm_ref, gf_ref, wq_ref, wk_ref, wv_ref, wo_ref, wg_ref, wu_ref, wd_ref,
           out_ref, w_all, wo_v, wqkv, h_all, c_mat, kv_all, rs, ra, sb, ps, acc, hres, zb, qbuf, bd, rope, cos_t, sin_t, ga, gm, gf, len_s,
           local_sem, in_sem, w_recv, w_send, d_recv, d_send, rounds, h_recv, h_send, kv_recv, kv_send, kvd_recv, kvd_send,
           c_recv, c_send, rs_recv, ra_recv, rs_send):
    layers = wo_ref.shape[0]
    seq_dev, d_model = h_ref.shape
    units = wg_ref.shape[1]
    pack = 3 * units
    half = pack // 2
    rows = nz * seq_dev
    hq = wq_ref.shape[1] // nz
    hd = wk_ref.shape[1] // nz
    me = lax.axis_index('tp')
    core = me % 2
    px = (me // 2) % NX
    py = (me // (2 * NX)) % NX
    mp = (me // 2) % PLANE
    mz = me // (2 * PLANE)
    base = mz * (2 * PLANE)
    partner = base + mp * 2 + (1 - core)

    def z_peer(i):
        return ((mz + i) % nz) * (2 * PLANE) + mp * 2 + core

    far_z = sorted(range(1, nz), key=lambda i: -min(i, nz - i))
    next_z = [i for i in far_z if min(i, nz - i) == 1]
    def plane_peer(dy, dx):
        return base + ((py + dy) % NX * NX + (px + dx) % NX) * 2 + core

    far_plane = sorted(((dy, dx) for dy in range(NX) for dx in range(NX) if dy or dx),
                       key=lambda d: -sum(min(i, NX - i) for i in d))

    barrier = pltpu.get_barrier_semaphore()
    next_devices = [plane_peer(0, 1), plane_peer(0, NX - 1), plane_peer(1, 0), plane_peer(NX - 1, 0)]
    next_devices += [z_peer(i) for i in next_z]

    def signal(sem, device):
        pl.semaphore_signal(sem, inc=1, device_id=(device,), device_id_type=pl.DeviceIdType.MESH)

    signal(barrier, partner)
    for d in next_devices:
        signal(barrier, d)

    def round_start(r):
        for d in next_devices:
            signal(rounds.at[r], d)

    def round_wait(r):
        pl.semaphore_wait(rounds.at[r], len(next_devices))

    def pack_copies(l):
        mine = w_all.at[l, core, mp]
        return [pltpu.make_async_copy(ref.at[l], mine.at[pl.ds(i * units, units)], local_sem.at[l, 0])
                for i, ref in enumerate((wg_ref, wu_ref, wd_ref))]

    def qkv_copies(l):
        return [pltpu.make_async_copy(ref.at[l, pl.ds(mz * n, n)], wqkv.at[l, pl.ds(first, n)], local_sem.at[l, 1])
                for ref, first, n in ((wq_ref, 0, hq), (wk_ref, hq, hd), (wv_ref, hq + hd, hd))]

    def wo_copy(l):
        return pltpu.make_async_copy(wo_ref.at[l], wo_v.at[l], local_sem.at[l, 2])

    def take(ref, sem):
        remote(ref, ref, w_send.at[0], sem, me).wait_recv()

    def pack_wait(l):
        mine = w_all.at[l, core, mp]
        pltpu.make_async_copy(mine, mine, local_sem.at[l, 0]).wait()

    def qkv_wait(l):
        pltpu.make_async_copy(wqkv.at[l], wqkv.at[l], local_sem.at[l, 1]).wait()

    small = [pltpu.make_async_copy(src, dst, in_sem.at[i]) for i, (src, dst) in enumerate((
        (h_ref, h_all.at[0, mz]), (rope_ref.at[mp * 2 + core], rope), (ga_ref, ga), (gm_ref, gm), (gf_ref, gf), (len_ref, len_s)))]
    for c in pack_copies(0) + small + qkv_copies(0):
        c.start()

    def start_later_copies():
        wo_copy(0).start()
        for l in range(1, layers):
            for c in pack_copies(l) + qkv_copies(l):
                c.start()
            wo_copy(l).start()

    def slot(h, a1, a2):
        return a2 % NX * NX + a1 % NX if h == 0 else a1 % NX * NX + a2 % NX

    def where_am_i(h):
        return (px, py) if h == 0 else (py, px)

    def at(h, a1, a2):
        return base + slot(h, a1, a2) * 2 + core

    third = half // 3
    SPAN = ((0, half), (half, half))

    def from_minus(h, k):
        return (h * half, 2 * third if (k in (1, 2)) != (h == 1) else third)

    def from_plus(h, k):
        first, size = from_minus(h, k)
        return (first + size, half - size)

    def piece(l, c, p, span):
        return w_all.at[l, c, p, pl.ds(*span)]

    def w_start(l, p, span, idx, device):
        ref = piece(l, core, p, span)
        remote(ref, ref, w_send.at[l], w_recv.at[l, idx], device).start()

    def w_take(l, idx, packs):
        take(w_all.at[l, core, pl.ds(0, packs)], w_recv.at[l, idx])

    GROUPS = (((0, 0), (1, 0), (3, 0), (0, 1)), ((0, 3), (2, 0), (0, 2), (1, 1)),
              ((1, 3), (3, 1), (3, 3), (2, 1)), ((2, 3), (1, 2), (3, 2), (2, 2)))
    ARRIVALS = (*GROUPS[:-1], GROUPS[-1][:-1], GROUPS[-1][-1:])
    ARRIVAL_OF = {d: g for g, ds in enumerate(ARRIVALS) for d in ds}

    def to_partner(l, h, k1, k2, span):
        a1, a2 = where_am_i(h)
        ref = piece(l, core, slot(h, a1 + k1, a2 + k2), span)
        g = ARRIVAL_OF[(k1, k2) if h == 0 else (k2, k1)]
        remote(ref, ref, d_send.at[l], d_recv.at[l, g], partner).start()

    @scoped
    def p1(l):
        pack_wait(l)
        for h in range(2):
            a1, a2 = where_am_i(h)
            w_start(l, mp, SPAN[h], 0, at(h, a1 + 1, a2))
            w_start(l, mp, SPAN[h], 0, at(h, a1 + NX - 1, a2))
        to_partner(l, 0, 0, 0, (0, pack))

    @scoped
    def p2(l):
        w_take(l, 0, 2)
        for h in range(2):
            a1, a2 = where_am_i(h)
            w_start(l, slot(h, a1 + NX - 1, a2), from_minus(h, 0), 1, at(h, a1 + 1, a2))
            w_start(l, slot(h, a1 + 1, a2), from_plus(h, 0), 1, at(h, a1 + NX - 1, a2))
            to_partner(l, h, NX - 1, 0, SPAN[h])
            to_partner(l, h, 1, 0, SPAN[h])

    @scoped
    def p3(l, ks):
        for k in ks:
            if k == 2:
                w_take(l, 1, 1)
            for h in range(2):
                a1, a2 = where_am_i(h)
                p = slot(h, a1 + k, a2)
                w_start(l, p, SPAN[h], 2 + k, at(h, a1, a2 + 1))
                w_start(l, p, SPAN[h], 2 + k, at(h, a1, a2 + NX - 1))
                if k == 2:
                    to_partner(l, h, k, 0, SPAN[h])

    @scoped
    def p4(l, ks):
        for k in ks:
            w_take(l, 2 + k, 2)
            for h in range(2):
                a1, a2 = where_am_i(h)
                w_start(l, slot(h, a1 + k, a2 + NX - 1), from_minus(h, k), 6 + k, at(h, a1, a2 + 1))
                w_start(l, slot(h, a1 + k, a2 + 1), from_plus(h, k), 6 + k, at(h, a1, a2 + NX - 1))
                to_partner(l, h, k, NX - 1, SPAN[h])
                to_partner(l, h, k, 1, SPAN[h])

    @scoped
    def p5(l, ks):
        for k in ks:
            w_take(l, 6 + k, 1)
            for h in range(2):
                to_partner(l, h, k, 2, SPAN[h])

    @scoped
    def w_done(l, gs):
        for g in gs:
            take(w_all.at[l, 1 - core, pl.ds(0, len(ARRIVALS[g]))], d_recv.at[l, g])

    def h_start(l, first, size, peers):
        for i in peers:
            ref = h_all.at[l, mz, :, pl.ds(first, size)]
            remote(ref, ref, h_send.at[l], h_recv.at[l], z_peer(i)).start()

    @scoped
    def h_wait(l):
        if nz > 1:
            take(h_all.at[l, pl.ds(0, nz - 1)], h_recv.at[l])
        for i in range(nz):
            hres[pl.ds(i * seq_dev, seq_dev)] = h_all[l, i].astype(F32)

    @scoped
    def norm_to_zb(l, gains, residual=False):
        gain = gains[...].astype(F32)[l:l + 1]
        step = min(16, rows)
        for first in range(0, rows, step):
            r = pl.ds(first, step)
            x = hres[r]
            if residual:
                x = (x + acc[r]).astype(BF16).astype(F32)
                hres[r] = x
            inv = lax.rsqrt(jnp.mean(x * x, axis=-1, keepdims=True) + NORM_EPS)
            zb[r] = (x * inv * gain).astype(BF16)

    lane = lax.broadcasted_iota(jnp.int32, (rows, LANES), 1)
    low_half = lane < hd

    def rotate(x):
        first = (lane % hd) < hd // 2
        swapped = jnp.where(first, pltpu.roll(x, LANES - hd // 2, 1), pltpu.roll(x, hd // 2, 1))
        return x * cos_t[...] + swapped * sin_t[...]

    def rope_tables():
        first = (lane % hd) < hd // 2
        t = rope[...]
        cos_t[...] = jnp.where(first, t, pltpu.roll(t, hd // 2, 1))
        sin_t[...] = jnp.where(first, -pltpu.roll(t, LANES - hd // 2, 1), t)

    def kv_copy(l, device):
        ref = kv_all.at[l, core, mp]
        return remote(ref, ref, kv_send.at[l], kv_recv.at[l], device)

    @scoped
    def qkv(l):
        qkv_wait(l)
        kv = lax.dot_general(zb[...], wqkv[l, pl.ds(hq, 2 * hd), :], NT, preferred_element_type=F32)
        kv_all[l, core, mp] = jnp.where(low_half, rotate(kv), kv).astype(BF16)
        for d in far_plane:
            kv_copy(l, plane_peer(*d)).start()
        proj = lax.dot_general(zb[...], wqkv[l, pl.ds(0, hq), :], NT, preferred_element_type=F32)
        for j in range(hq // LANES):
            q = rotate(proj[:, j * LANES:(j + 1) * LANES]) * (hd ** -0.5)
            for half_head, x in enumerate((q, pltpu.roll(q, LANES - hd, 1))):
                head = 2 * j + half_head
                qbuf[pl.ds(head * rows, rows)] = jnp.where(low_half, x, 0.0).astype(BF16)

    @scoped
    def kv_wait(l):
        take(kv_all.at[l, core, pl.ds(0, PLANE - 1)], kv_recv.at[l])
        ref = kv_all.at[l, core]
        remote(ref, ref, kvd_send.at[l], kvd_recv.at[l], partner).start()
        take(kv_all.at[l, 1 - core], kvd_recv.at[l])

    def c_columns(z):
        return pl.ds(pl.multiple_of(z * hq, hq), hq)

    @scoped
    def attention(l):
        keys = 2 * PLANE * rows
        j = lax.broadcasted_iota(jnp.int32, (1, keys), 1)
        key_pos = ((j // seq_dev) % nz) * (2 * PLANE * seq_dev) + ((j // rows) % PLANE) * (2 * seq_dev) \
            + (j // (PLANE * rows)) * seq_dev + j % seq_dev
        i = lax.broadcasted_iota(jnp.int32, (hq // hd * rows, 1), 0) % rows
        q_pos = (i // seq_dev) * (2 * PLANE * seq_dev) + (mp * 2 + core) * seq_dev + i % seq_dev
        allowed = key_pos <= jnp.minimum(q_pos, len_s[0] - 1)
        kv = kv_all[l].reshape(keys, LANES)
        s = lax.dot_general(qbuf[...], kv, NT, preferred_element_type=F32)
        s = jnp.where(allowed, s, -1e30)
        e = jnp.exp(s - jnp.max(s, axis=-1, keepdims=True))
        p = (e * (1.0 / jnp.sum(e, axis=-1, keepdims=True))).astype(BF16)
        o = jnp.dot(p, kv, preferred_element_type=F32)
        for pair in range(hq // LANES):
            even, odd = (o[h * rows:(h + 1) * rows] for h in (2 * pair, 2 * pair + 1))
            c_mat[l, :, pl.ds(pl.multiple_of(mz * hq + pair * LANES, LANES), LANES)] = jnp.where(low_half, pltpu.roll(even, LANES - hd, 1), odd).astype(BF16)
        ref = c_mat.at[l, :, c_columns(mz)]
        for i in far_z:
            remote(ref, ref, c_send.at[l], c_recv.at[l, int(i in next_z)], z_peer(i)).start()

    @scoped
    def out_proj(l):
        with jax.named_scope('wo_wait'):
            wo_copy(l).wait()
        for i in [0] + far_z:
            if i and i in (far_z[0], far_z[-len(next_z)]):
                near = i in next_z
                n = len(next_z) if near else nz - 1 - len(next_z)
                with jax.named_scope('c_wait'):
                    take(c_mat.at[l, :, pl.ds(0, n * hq)], c_recv.at[l, int(near)])
            cols = c_columns((mz + nz - i) % nz)
            part = jnp.dot(c_mat[l, :, cols], wo_v[l, cols, :], preferred_element_type=F32)
            acc[...] = acc[...] + part if i else part

    group = CHUNK // units
    n_groups = len(GROUPS)
    assert group == 2 * len(GROUPS[0])

    def slab(l, places, first, cols):
        parts = [w_all[l, c, slot(0, px + dx, py + dy), pl.ds(first, units), cols] for dx, dy in places for c in range(2)]
        return jnp.concatenate(parts, axis=0)

    block = lax.broadcasted_iota(jnp.int32, (rows, CHUNK), 1) // units
    every = pl.ds(0, d_model)

    def units_of(l, places):
        gate = lax.dot_general(zb[...], slab(l, places, 0, every), NT, preferred_element_type=F32)
        up = lax.dot_general(zb[...], slab(l, places, units, every), NT, preferred_element_type=F32)
        return gate * (1.0 / (1.0 + jnp.exp(-gate))) * up

    def spread(g, act, blocks):
        for b in blocks:
            bd[g, pl.ds(b * rows, rows)] = jnp.where(block == b, act, 0.0).astype(BF16)

    @scoped
    def mlp_units(l, gs):
        for g in gs:
            spread(g, units_of(l, GROUPS[g]), range(group))

    @scoped
    def mlp_units_but_last(l, g):
        places = GROUPS[g][:-1] + GROUPS[g][:1]
        spread(g, units_of(l, places), range(group - 2))

    @scoped
    def mlp_units_last(l, g):
        act = units_of(l, GROUPS[g][-2:])
        spread(g, jnp.concatenate([jnp.zeros_like(act), act], axis=1), range(group - 2, group))

    two_step = nz == 8
    wide = min(2 * CHUNK, d_model)
    n_sums = d_model // wide

    def ps_of(l, n, i):
        return ps.at[l, n, (mz + i + nz) % nz]

    def rs_start(l, n):
        if not two_step:
            for k, i in enumerate(far_z):
                remote(ps_of(l, n, i), rs.at[l, n, k], rs_send.at[l], rs_recv.at[l, n], z_peer(i)).start()
            return
        for side, to in ((0, nz - 2), (1, 2)):
            cols = pl.ds(side * (wide // 2), wide // 2)
            remote(ps.at[l, n, (mz + 4) % nz, :, cols], ra.at[l, n, 2, :, cols], rs_send.at[l], ra_recv.at[l, n], z_peer(to)).start()
        for side, to in ((0, -1), (1, 1)):
            remote(ps_of(l, n, 3 * to), ra.at[l, n, side], rs_send.at[l], ra_recv.at[l, n], z_peer(nz + to)).start()

    @scoped
    def rs_middle(l):
        if not two_step:
            return
        for n in range(n_sums):
            for side, to in ((0, -1), (1, 1)):
                remote(ps_of(l, n, to), rs.at[l, n, side], rs_send.at[l], rs_recv.at[l, n], z_peer(nz + to)).start()

        @pl.loop(0, n_sums)
        def _(n):
            take(ra.at[l, n], ra_recv.at[l, n])
            for side, to in ((0, -2), (1, 2)):
                cols = pl.ds(side * (wide // 2), wide // 2)
                sb[l, n, side] = ps[l, n, (mz + nz + to) % nz] + ra[l, n, side]
                sb[l, n, side, :, cols] = sb[l, n, side, :, cols] + ra[l, n, 2, :, cols]
                remote(sb.at[l, n, side], rs.at[l, n, 2 + side], rs_send.at[l], rs_recv.at[l, n], z_peer(nz + to)).start()

    def down(l, n, gs):
        cols = pl.ds(pl.multiple_of(n * wide, wide), wide)
        total = jnp.zeros((rows, wide), F32)
        for g in gs:
            y = jnp.dot(bd[g], slab(l, GROUPS[g], 2 * units, cols), preferred_element_type=F32)
            y = y.astype(BF16).astype(F32)
            for b in range(group):
                total = total + y[b * rows:(b + 1) * rows]
        return total

    @scoped
    def mlp_down_early(l, gs):
        @pl.loop(0, n_sums)
        def _(n):
            acc[:, pl.ds(pl.multiple_of(n * wide, wide), wide)] = down(l, n, gs)

    @scoped
    def mlp_down(l, gs, early):
        @pl.loop(0, n_sums)
        def _(n):
            total = down(l, n, gs)
            if early:
                total = total + acc[:, pl.ds(pl.multiple_of(n * wide, wide), wide)]
            ps[l, n] = total.reshape(nz, seq_dev, wide)
            rs_start(l, n)

    n_in = 4 if two_step else nz - 1

    @scoped
    def rs_finish(l, store):
        mine = pl.ds(pl.multiple_of(mz * seq_dev, seq_dev), seq_dev)
        for n in range(n_sums):
            if n_in:
                take(rs.at[l, n], rs_recv.at[l, n])
            total = ps[l, n, mz]
            for k in range(n_in):
                total = total + rs[l, n, k]
            store(n, (hres[mine, n * wide:(n + 1) * wide] + total).astype(BF16))

    def store_next(l):
        def store(n, x):
            h_all[l + 1, mz, :, n * wide:(n + 1) * wide] = x
            h_start(l + 1, n * wide, wide, far_z)
        return store

    with jax.named_scope('barrier'):
        pl.semaphore_wait(barrier, 1 + len(next_devices))
    round_start(0)
    p1(0)
    p3(0, (0,))
    with jax.named_scope('rounds'):
        small[0].wait()
        for r in range(4):
            if r:
                round_wait(r - 1)
                if r < 3:
                    round_start(r)
            h_start(0, 0, d_model, [i for i in far_z if min(i, nz - i) == r + 1])
    start_later_copies()
    with jax.named_scope('small'):
        for c in small[1:]:
            c.wait()
        rope_tables()
    p2(0)
    for l in range(layers):
        more = l + 1 < layers
        h_wait(l)
        norm_to_zb(l, ga)
        qkv(l)
        if l == 0:
            p3(0, (1, 3, 2))
            p4(0, (0,))
        else:
            p4(l, (0, 1, 3, 2))
        kv_wait(l)
        attention(l)
        if l == 0:
            p4(0, (1, 3, 2))
            p5(0, (0,))
        else:
            p5(l, (0, 1, 3, 2))
        if more:
            p1(l + 1)
            p3(l + 1, (0,))
        out_proj(l)
        norm_to_zb(l, gm, True)
        if l == 0:
            w_done(l, (0,))
            mlp_units(l, (0,))
            w_done(l, (1,))
            mlp_units(l, (1,))
            p5(l, (1, 3))
            mlp_down_early(l, (0, 1))
            w_done(l, (2,))
            mlp_units(l, (2,))
            w_done(l, (3,))
            mlp_units_but_last(l, 3)
            p5(l, (2,))
            w_done(l, (4,))
            mlp_units_last(l, 3)
        else:
            w_done(l, range(n_groups + 1))
            mlp_units(l, range(n_groups))
        mlp_down(l, (2, 3) if l == 0 else range(n_groups), l == 0)
        if more:
            p2(l + 1)
            p3(l + 1, (1, 3))
        rs_middle(l)
        if more:
            rs_finish(l, store_next(l))
            p3(l + 1, (2,))
    pieces = []
    rs_finish(layers - 1, lambda n, x: pieces.append(x.astype(F32)))
    x = jnp.concatenate(pieces, axis=1)
    inv = lax.rsqrt(jnp.mean(x * x, axis=-1, keepdims=True) + NORM_EPS)
    gain = gf[...].astype(F32)
    for i in range(d_model // LANES):
        cols = slice(i * LANES, (i + 1) * LANES)
        out_ref[:, cols] = x[:, cols] * inv * gain[i:i + 1]

    with jax.named_scope('drain'):
      for l in range(layers):
          ref = w_all.at[l, 0, pl.ds(0, PLANE - 1)]
          remote(ref, ref, w_send.at[l], w_recv.at[l, 0], me).wait_send()
          ref = w_all.at[l, 0]
          remote(ref, ref, d_send.at[l], d_recv.at[l, 0], me).wait_send()
          ref = kv_all.at[l, 0, pl.ds(0, PLANE - 1)]
          remote(ref, ref, kv_send.at[l], kv_recv.at[l], me).wait_send()
          ref = kv_all.at[l, 0]
          remote(ref, ref, kvd_send.at[l], kvd_recv.at[l], me).wait_send()
          if nz > 1:
              ref = h_all.at[l, pl.ds(0, nz - 1)]
              remote(ref, ref, h_send.at[l], h_recv.at[l], me).wait_send()
              ref = c_mat.at[l, :, pl.ds(0, (nz - 1) * hq)]
              remote(ref, ref, c_send.at[l], c_recv.at[l, 0], me).wait_send()
              ref = ps.at[l, :, pl.ds(0, nz - 1)]
              remote(ref, ref, rs_send.at[l], rs_recv.at[l, 0], me).wait_send()


def solution(mesh):
    nz = mesh.shape['tp'] // (2 * PLANE)

    def device_fn(hidden_in, lengths, attn_norm, w_query, w_key, w_value, w_out, mlp_norm, w_gate, w_up, w_down, final_norm):
        seq_dev, d_model = hidden_in.shape[1:]
        layers, _, heads, hd = w_query.shape
        kv_heads = w_key.shape[2]
        units = w_gate.shape[2]
        assert kv_heads == nz and 2 * hd == LANES and heads % nz == 0
        hq = heads // nz * hd
        rows = nz * seq_dev
        wide = min(2 * CHUNK, d_model)
        n_sums = d_model // wide
        n_groups = 2 * PLANE * units // CHUNK
        dev, row = np.arange(2 * PLANE)[:, None], np.arange(rows)[None, :]
        pos = (row // seq_dev) * (2 * PLANE * seq_dev) + dev * seq_dev + row % seq_dev
        freq = np.float32(ROPE_BASE) ** (np.float32(-2.0) * np.arange(hd // 2, dtype=np.float32) / np.float32(hd))
        angles = (pos[..., None].astype(np.float32) * freq).astype(np.float64)
        rope = np.tile(np.concatenate([np.cos(angles), np.sin(angles)], axis=-1), (1, 1, 2)).astype(np.float32)
        by_rows = lambda w: jnp.transpose(w, (0, 2, 3, 1)).reshape(layers, -1, d_model)
        units_first = lambda w: jnp.transpose(w, (0, 2, 1))
        pinned = lambda x: pltpu.with_memory_space_constraint(x, pltpu.HBM)
        hbm, vmem = (pl.BlockSpec(memory_space=s) for s in (pltpu.HBM, pltpu.VMEM))
        dma = pltpu.SemaphoreType.DMA
        out = pl.pallas_call(
            functools.partial(kernel, nz),
            name='decoder',
            out_shape=pltpu.VMEM((seq_dev, d_model), F32),
            in_specs=[hbm] * 13,
            out_specs=vmem,
            scratch_shapes=[
                pltpu.VMEM((layers, 2, PLANE, 3 * units, d_model), BF16),
                pltpu.VMEM((layers, heads * hd, d_model), BF16),
                pltpu.VMEM((layers, hq + 2 * hd, d_model), BF16),
                pltpu.VMEM((layers, nz, seq_dev, d_model), BF16),
                pltpu.VMEM((layers, rows, heads * hd), BF16),
                pltpu.VMEM((layers, 2, PLANE, rows, LANES), BF16),
                pltpu.VMEM((layers, n_sums, 4 if nz == 8 else max(nz - 1, 1), seq_dev, wide), F32),
                pltpu.VMEM((layers, n_sums, 3, seq_dev, wide), F32),
                pltpu.VMEM((layers, n_sums, 2, seq_dev, wide), F32),
                pltpu.VMEM((layers, n_sums, nz, seq_dev, wide), F32),
                pltpu.VMEM((rows, d_model), F32),
                pltpu.VMEM((rows, d_model), F32),
                pltpu.VMEM((rows, d_model), BF16),
                pltpu.VMEM((hq // hd * rows, LANES), BF16),
                pltpu.VMEM((n_groups, CHUNK // units * rows, CHUNK), BF16),
                pltpu.VMEM((rows, LANES), F32), pltpu.VMEM((rows, LANES), F32), pltpu.VMEM((rows, LANES), F32),
                pltpu.VMEM((layers, d_model), BF16), pltpu.VMEM((layers, d_model), BF16),
                pltpu.VMEM((d_model // LANES, LANES), BF16),
                pltpu.SMEM((1,), jnp.int32),
                dma((layers, 3)), dma((6,)), dma((layers, 10)), dma((layers,)),
                dma((layers, n_groups + 1)), dma((layers,)),
                pltpu.SemaphoreType.REGULAR((3,)),
                dma((layers,)), dma((layers,)), dma((layers,)), dma((layers,)), dma((layers,)), dma((layers,)),
                dma((layers, 2)), dma((layers,)), dma((layers, n_sums)), dma((layers, n_sums)), dma((layers,)),
            ],
            compiler_params=pltpu.CompilerParams(
                collective_id=0, has_side_effects=True, vmem_limit_bytes=60_000_000),
        )(pinned(hidden_in[0]), lengths, *map(pinned, (
            jnp.asarray(rope), attn_norm, mlp_norm, final_norm.reshape(-1, LANES), by_rows(w_query), by_rows(w_key), by_rows(w_value),
            w_out.reshape(layers, heads * hd, d_model), units_first(w_gate), units_first(w_up), w_down)))
        return out.astype(BF16)[None]

    seq_part = P(None, 'tp', None)
    in_specs = (seq_part, P(), P(), P(), P(), P(), P(), P(), P(None, None, 'tp'), P(None, None, 'tp'), P(None, 'tp', None), P())
    return jax.shard_map(device_fn, mesh=mesh, in_specs=in_specs, out_specs=seq_part, check_vma=False)
```

```python
import functools

import jax
import jax.numpy as jnp
import numpy as np
from jax import lax
from jax.experimental import pallas as pl
from jax.experimental.pallas import tpu as pltpu
from jax.sharding import PartitionSpec as P

NORM_EPS = 1e-5
ROPE_BASE = 500000.0
NX = 4
PLANE = NX * NX
LANES = 128
CHUNK = 256
NT = (((1,), (1,)), ((), ()))
F32, BF16 = jnp.float32, jnp.bfloat16


def remote(src, dst, send_sem, recv_sem, device):
    return pltpu.make_async_remote_copy(
        src_ref=src, dst_ref=dst, send_sem=send_sem, recv_sem=recv_sem,
        device_id=(device,), device_id_type=pl.DeviceIdType.MESH)


def scoped(f):
    @functools.wraps(f)
    def wrapped(*args):
        with jax.named_scope(f.__name__ + ('#l=%d' % args[0])):
            return f(*args)
    return wrapped


def kernel(nz, h_ref, len_ref, rope_ref, ga_ref, gm_ref, gf_ref, wq_ref, wk_ref, wv_ref, wo_ref, wg_ref, wu_ref, wd_ref,
           out_ref, w_all, wo_v, wqkv, wkv, kv_rows, h_all, c_mat, kv_all, rs, ra, sb, ps, acc, hres, zb, qbuf, bd, rope, cos_t, sin_t, ga, gm, gf, len_s,
           local_sem, in_sem, w_recv, w_send, d_recv, d_send, rounds, h_recv, h_send, kv_recv, kv_send, kvd_recv, kvd_send, kva_recv, kva_send,
           c_recv, c_send, rs_recv, ra_recv, rs_send):
    layers = wo_ref.shape[0]
    seq_dev, d_model = h_ref.shape
    units = wg_ref.shape[1]
    pack = 3 * units
    half = pack // 2
    rows = nz * seq_dev
    hq = wq_ref.shape[1] // nz
    hd = wk_ref.shape[1] // nz
    me = lax.axis_index('tp')
    core = me % 2
    px = (me // 2) % NX
    py = (me // (2 * NX)) % NX
    mp = (me // 2) % PLANE
    mz = me // (2 * PLANE)
    base = mz * (2 * PLANE)
    partner = base + mp * 2 + (1 - core)

    def z_peer(i):
        return ((mz + i) % nz) * (2 * PLANE) + mp * 2 + core

    far_z = sorted(range(1, nz), key=lambda i: -min(i, nz - i))
    next_z = [i for i in far_z if min(i, nz - i) == 1]
    def plane_peer(dy, dx):
        return base + ((py + dy) % NX * NX + (px + dx) % NX) * 2 + core

    far_plane = sorted(((dy, dx) for dy in range(NX) for dx in range(NX) if dy or dx),
                       key=lambda d: -sum(min(i, NX - i) for i in d))

    barrier = pltpu.get_barrier_semaphore()
    next_devices = [plane_peer(0, 1), plane_peer(0, NX - 1), plane_peer(1, 0), plane_peer(NX - 1, 0)]
    next_devices += [z_peer(i) for i in next_z]

    def signal(sem, device):
        pl.semaphore_signal(sem, inc=1, device_id=(device,), device_id_type=pl.DeviceIdType.MESH)

    signal(barrier, partner)
    for d in next_devices:
        signal(barrier, d)

    def round_start(r):
        for d in next_devices:
            signal(rounds.at[r], d)

    def round_wait(r):
        pl.semaphore_wait(rounds.at[r], len(next_devices))

    def pack_copies(l):
        mine = w_all.at[l, core, mp]
        return [pltpu.make_async_copy(ref.at[l], mine.at[pl.ds(i * units, units)], local_sem.at[l, 0])
                for i, ref in enumerate((wg_ref, wu_ref, wd_ref))]

    def qkv_copies(l):
        mine = [(wq_ref, 0, hq), (wk_ref, hq, hd), (wv_ref, hq + hd, hd)]
        return [pltpu.make_async_copy(ref.at[l, pl.ds(mz * n, n)], wqkv.at[l, pl.ds(first, n)], local_sem.at[l, 1])
                for ref, first, n in (mine[:1] if l else mine)]

    def kv_weight_copies(l):
        return [pltpu.make_async_copy(ref.at[l, pl.ds(z * hd, hd)], wkv.at[l - 1, pl.ds((2 * z + i) * hd, hd)], local_sem.at[l, 3])
                for z in range(nz) for i, ref in enumerate((wk_ref, wv_ref))]

    def wo_copy(l):
        return pltpu.make_async_copy(wo_ref.at[l], wo_v.at[l], local_sem.at[l, 2])

    def take(ref, sem):
        remote(ref, ref, w_send.at[0], sem, me).wait_recv()

    def pack_wait(l):
        mine = w_all.at[l, core, mp]
        pltpu.make_async_copy(mine, mine, local_sem.at[l, 0]).wait()

    def qkv_wait(l):
        ref = wqkv.at[l, pl.ds(0, hq)] if l else wqkv.at[l]
        pltpu.make_async_copy(ref, ref, local_sem.at[l, 1]).wait()

    small = [pltpu.make_async_copy(src, dst, in_sem.at[i]) for i, (src, dst) in enumerate((
        (h_ref, h_all.at[0, mz]), (rope_ref.at[mp * 2 + core], rope), (ga_ref, ga), (gm_ref, gm), (gf_ref, gf), (len_ref, len_s)))]
    for c in pack_copies(0) + small + qkv_copies(0):
        c.start()

    def start_later_copies():
        wo_copy(0).start()
        for l in range(1, layers):
            for c in pack_copies(l) + qkv_copies(l) + kv_weight_copies(l):
                c.start()
            wo_copy(l).start()

    def slot(h, a1, a2):
        return a2 % NX * NX + a1 % NX if h == 0 else a1 % NX * NX + a2 % NX

    def where_am_i(h):
        return (px, py) if h == 0 else (py, px)

    def at(h, a1, a2):
        return base + slot(h, a1, a2) * 2 + core

    third = half // 3
    SPAN = ((0, half), (half, half))

    def from_minus(h, k):
        return (h * half, 2 * third if (k in (1, 2)) != (h == 1) else third)

    def from_plus(h, k):
        first, size = from_minus(h, k)
        return (first + size, half - size)

    def piece(l, c, p, span):
        return w_all.at[l, c, p, pl.ds(*span)]

    def w_start(l, p, span, idx, device):
        ref = piece(l, core, p, span)
        remote(ref, ref, w_send.at[l], w_recv.at[l, idx], device).start()

    def w_take(l, idx, packs):
        take(w_all.at[l, core, pl.ds(0, packs)], w_recv.at[l, idx])

    GROUPS = (((0, 0), (1, 0), (3, 0), (0, 1)), ((0, 3), (2, 0), (0, 2), (1, 1)),
              ((1, 3), (3, 1), (3, 3), (2, 1)), ((2, 3), (1, 2), (3, 2), (2, 2)))
    ARRIVALS = (*GROUPS[:-1], GROUPS[-1][:-1], GROUPS[-1][-1:])
    ARRIVAL_OF = {d: g for g, ds in enumerate(ARRIVALS) for d in ds}

    def to_partner(l, h, k1, k2, span):
        a1, a2 = where_am_i(h)
        ref = piece(l, core, slot(h, a1 + k1, a2 + k2), span)
        g = ARRIVAL_OF[(k1, k2) if h == 0 else (k2, k1)]
        remote(ref, ref, d_send.at[l], d_recv.at[l, g], partner).start()

    @scoped
    def p1(l):
        pack_wait(l)
        for h in range(2):
            a1, a2 = where_am_i(h)
            w_start(l, mp, SPAN[h], 0, at(h, a1 + 1, a2))
            w_start(l, mp, SPAN[h], 0, at(h, a1 + NX - 1, a2))
        to_partner(l, 0, 0, 0, (0, pack))

    @scoped
    def p2(l):
        w_take(l, 0, 2)
        for h in range(2):
            a1, a2 = where_am_i(h)
            w_start(l, slot(h, a1 + NX - 1, a2), from_minus(h, 0), 1, at(h, a1 + 1, a2))
            w_start(l, slot(h, a1 + 1, a2), from_plus(h, 0), 1, at(h, a1 + NX - 1, a2))
            to_partner(l, h, NX - 1, 0, SPAN[h])
            to_partner(l, h, 1, 0, SPAN[h])

    @scoped
    def p3(l, ks):
        for k in ks:
            if k == 2:
                w_take(l, 1, 1)
            for h in range(2):
                a1, a2 = where_am_i(h)
                p = slot(h, a1 + k, a2)
                w_start(l, p, SPAN[h], 2 + k, at(h, a1, a2 + 1))
                w_start(l, p, SPAN[h], 2 + k, at(h, a1, a2 + NX - 1))
                if k == 2:
                    to_partner(l, h, k, 0, SPAN[h])

    @scoped
    def p4(l, ks):
        for k in ks:
            w_take(l, 2 + k, 2)
            for h in range(2):
                a1, a2 = where_am_i(h)
                w_start(l, slot(h, a1 + k, a2 + NX - 1), from_minus(h, k), 6 + k, at(h, a1, a2 + 1))
                w_start(l, slot(h, a1 + k, a2 + 1), from_plus(h, k), 6 + k, at(h, a1, a2 + NX - 1))
                to_partner(l, h, k, NX - 1, SPAN[h])
                to_partner(l, h, k, 1, SPAN[h])

    @scoped
    def p5(l, ks):
        for k in ks:
            w_take(l, 6 + k, 1)
            for h in range(2):
                to_partner(l, h, k, 2, SPAN[h])

    @scoped
    def w_done(l, gs):
        for g in gs:
            take(w_all.at[l, 1 - core, pl.ds(0, len(ARRIVALS[g]))], d_recv.at[l, g])

    def h_start(l, first, size, peers):
        for i in peers:
            ref = h_all.at[l, mz, :, pl.ds(first, size)]
            remote(ref, ref, h_send.at[l], h_recv.at[l], z_peer(i)).start()

    @scoped
    def h_wait(l):
        if nz > 1:
            take(h_all.at[l, pl.ds(0, nz - 1)], h_recv.at[l])
        for i in range(nz):
            hres[pl.ds(i * seq_dev, seq_dev)] = h_all[l, i].astype(F32)

    @scoped
    def norm_to_zb(l, gains, residual=False):
        gain = gains[...].astype(F32)[l:l + 1]
        step = min(16, rows)
        for first in range(0, rows, step):
            r = pl.ds(first, step)
            x = hres[r]
            if residual:
                x = (x + acc[r]).astype(BF16).astype(F32)
                hres[r] = x
            inv = lax.rsqrt(jnp.mean(x * x, axis=-1, keepdims=True) + NORM_EPS)
            zb[r] = (x * inv * gain).astype(BF16)

    lane = lax.broadcasted_iota(jnp.int32, (rows, LANES), 1)
    low_half = lane < hd

    def rotate(x, cos, sin):
        first = (lane[:x.shape[0]] % hd) < hd // 2
        swapped = jnp.where(first, pltpu.roll(x, LANES - hd // 2, 1), pltpu.roll(x, hd // 2, 1))
        return x * cos + swapped * sin

    def rope_tables():
        first = (lane % hd) < hd // 2
        t = rope[...]
        cos_t[...] = jnp.where(first, t, pltpu.roll(t, hd // 2, 1))
        sin_t[...] = jnp.where(first, -pltpu.roll(t, LANES - hd // 2, 1), t)

    def kv_copy(l, device):
        ref = kv_all.at[l, core, mp]
        return remote(ref, ref, kv_send.at[l], kv_recv.at[l], device)

    def kv_start(l):
        for d in far_plane:
            kv_copy(l, plane_peer(*d)).start()

    @scoped
    def kv_first(l):
        qkv_wait(l)
        kv = lax.dot_general(zb[...], wqkv[l, pl.ds(hq, 2 * hd), :], NT, preferred_element_type=F32)
        kv_all[l, core, mp] = jnp.where(low_half, rotate(kv, cos_t[...], sin_t[...]), kv).astype(BF16)
        kv_start(l)

    def kv_own(l):
        return kv_all.at[l, core, mp, pl.ds(pl.multiple_of(mz * seq_dev, seq_dev), seq_dev)]

    @scoped
    def kv_heads(l):
        ref = wkv.at[l - 1]
        pltpu.make_async_copy(ref, ref, local_sem.at[l, 3]).wait()
        x = h_all[l, mz].astype(F32)
        inv = lax.rsqrt(jnp.mean(x * x, axis=-1, keepdims=True) + NORM_EPS)
        z = x * inv * ga[...].astype(F32)[l:l + 1]
        z = jnp.concatenate([z, z], axis=0).astype(BF16)
        kv = lax.dot_general(z, wkv[l - 1], NT, preferred_element_type=F32)[:seq_dev]
        mine = pl.ds(pl.multiple_of(mz * seq_dev, seq_dev), seq_dev)
        for head in range(nz):
            part = kv[:, head * LANES:(head + 1) * LANES]
            kv_rows[l - 1, head] = jnp.where(low_half[:seq_dev], rotate(part, cos_t[mine], sin_t[mine]), part).astype(BF16)
        pltpu.make_async_copy(kv_rows.at[l - 1, mz], kv_own(l), local_sem.at[l, 0]).start()
        for i in far_z:
            remote(kv_rows.at[l - 1, (mz + i) % nz], kv_own(l), kva_send.at[l - 1], kva_recv.at[l - 1], z_peer(i)).start()

    @scoped
    def kv_heads_wait(l):
        pltpu.make_async_copy(kv_rows.at[l - 1, mz], kv_own(l), local_sem.at[l, 0]).wait()
        if nz > 1:
            take(kv_rows.at[l - 1, pl.ds(0, nz - 1)], kva_recv.at[l - 1])
        kv_start(l)

    @scoped
    def q_first(l):
        if l:
            qkv_wait(l)
        proj = lax.dot_general(zb[...], wqkv[l, pl.ds(0, hq), :], NT, preferred_element_type=F32)
        for j in range(hq // LANES):
            q = rotate(proj[:, j * LANES:(j + 1) * LANES], cos_t[...], sin_t[...]) * (hd ** -0.5)
            for half_head, x in enumerate((q, pltpu.roll(q, LANES - hd, 1))):
                head = 2 * j + half_head
                qbuf[pl.ds(head * rows, rows)] = jnp.where(low_half, x, 0.0).astype(BF16)

    @scoped
    def kv_wait(l):
        take(kv_all.at[l, core, pl.ds(0, PLANE - 1)], kv_recv.at[l])
        ref = kv_all.at[l, core]
        remote(ref, ref, kvd_send.at[l], kvd_recv.at[l], partner).start()
        take(kv_all.at[l, 1 - core], kvd_recv.at[l])

    def c_columns(z):
        return pl.ds(pl.multiple_of(z * hq, hq), hq)

    @scoped
    def attention(l):
        keys = 2 * PLANE * rows
        j = lax.broadcasted_iota(jnp.int32, (1, keys), 1)
        key_pos = ((j // seq_dev) % nz) * (2 * PLANE * seq_dev) + ((j // rows) % PLANE) * (2 * seq_dev) \
            + (j // (PLANE * rows)) * seq_dev + j % seq_dev
        i = lax.broadcasted_iota(jnp.int32, (hq // hd * rows, 1), 0) % rows
        q_pos = (i // seq_dev) * (2 * PLANE * seq_dev) + (mp * 2 + core) * seq_dev + i % seq_dev
        allowed = key_pos <= jnp.minimum(q_pos, len_s[0] - 1)
        kv = kv_all[l].reshape(keys, LANES)
        s = lax.dot_general(qbuf[...], kv, NT, preferred_element_type=F32)
        s = jnp.where(allowed, s, -1e30)
        e = jnp.exp(s - jnp.max(s, axis=-1, keepdims=True))
        p = (e * (1.0 / jnp.sum(e, axis=-1, keepdims=True))).astype(BF16)
        o = jnp.dot(p, kv, preferred_element_type=F32)
        for pair in range(hq // LANES):
            even, odd = (o[h * rows:(h + 1) * rows] for h in (2 * pair, 2 * pair + 1))
            c_mat[l, :, pl.ds(pl.multiple_of(mz * hq + pair * LANES, LANES), LANES)] = jnp.where(low_half, pltpu.roll(even, LANES - hd, 1), odd).astype(BF16)
        ref = c_mat.at[l, :, c_columns(mz)]
        for i in far_z:
            remote(ref, ref, c_send.at[l], c_recv.at[l, int(i in next_z)], z_peer(i)).start()

    @scoped
    def out_proj(l):
        with jax.named_scope('wo_wait'):
            wo_copy(l).wait()
        for i in [0] + far_z:
            if i and i in (far_z[0], far_z[-len(next_z)]):
                near = i in next_z
                n = len(next_z) if near else nz - 1 - len(next_z)
                with jax.named_scope('c_wait'):
                    take(c_mat.at[l, :, pl.ds(0, n * hq)], c_recv.at[l, int(near)])
            cols = c_columns((mz + nz - i) % nz)
            part = jnp.dot(c_mat[l, :, cols], wo_v[l, cols, :], preferred_element_type=F32)
            acc[...] = acc[...] + part if i else part

    group = CHUNK // units
    n_groups = len(GROUPS)
    assert group == 2 * len(GROUPS[0])

    def slab(l, places, first, cols):
        parts = [w_all[l, c, slot(0, px + dx, py + dy), pl.ds(first, units), cols] for dx, dy in places for c in range(2)]
        return jnp.concatenate(parts, axis=0)

    block = lax.broadcasted_iota(jnp.int32, (rows, CHUNK), 1) // units
    every = pl.ds(0, d_model)

    def units_of(l, places):
        gate = lax.dot_general(zb[...], slab(l, places, 0, every), NT, preferred_element_type=F32)
        up = lax.dot_general(zb[...], slab(l, places, units, every), NT, preferred_element_type=F32)
        return gate * (1.0 / (1.0 + jnp.exp(-gate))) * up

    def spread(g, act, blocks):
        for b in blocks:
            bd[g, pl.ds(b * rows, rows)] = jnp.where(block == b, act, 0.0).astype(BF16)

    @scoped
    def mlp_units(l, gs):
        for g in gs:
            spread(g, units_of(l, GROUPS[g]), range(group))

    @scoped
    def mlp_units_but_last(l, g):
        places = GROUPS[g][:-1] + GROUPS[g][:1]
        spread(g, units_of(l, places), range(group - 2))

    @scoped
    def mlp_units_last(l, g):
        act = units_of(l, GROUPS[g][-2:])
        spread(g, jnp.concatenate([jnp.zeros_like(act), act], axis=1), range(group - 2, group))

    two_step = nz == 8
    wide = min(2 * CHUNK, d_model)
    n_sums = d_model // wide

    def ps_of(l, n, i):
        return ps.at[l, n, (mz + i + nz) % nz]

    def rs_start(l, n):
        if not two_step:
            for k, i in enumerate(far_z):
                remote(ps_of(l, n, i), rs.at[l, n, k], rs_send.at[l], rs_recv.at[l, n], z_peer(i)).start()
            return
        for side, to in ((0, nz - 2), (1, 2)):
            cols = pl.ds(side * (wide // 2), wide // 2)
            remote(ps.at[l, n, (mz + 4) % nz, :, cols], ra.at[l, n, 2, :, cols], rs_send.at[l], ra_recv.at[l, n], z_peer(to)).start()
        for side, to in ((0, -1), (1, 1)):
            remote(ps_of(l, n, 3 * to), ra.at[l, n, side], rs_send.at[l], ra_recv.at[l, n], z_peer(nz + to)).start()

    @scoped
    def rs_middle(l):
        if not two_step:
            return
        for n in range(n_sums):
            for side, to in ((0, -1), (1, 1)):
                remote(ps_of(l, n, to), rs.at[l, n, side], rs_send.at[l], rs_recv.at[l, n], z_peer(nz + to)).start()

        @pl.loop(0, n_sums)
        def _(n):
            take(ra.at[l, n], ra_recv.at[l, n])
            for side, to in ((0, -2), (1, 2)):
                cols = pl.ds(side * (wide // 2), wide // 2)
                sb[l, n, side] = ps[l, n, (mz + nz + to) % nz] + ra[l, n, side]
                sb[l, n, side, :, cols] = sb[l, n, side, :, cols] + ra[l, n, 2, :, cols]
                remote(sb.at[l, n, side], rs.at[l, n, 2 + side], rs_send.at[l], rs_recv.at[l, n], z_peer(nz + to)).start()

    def down(l, n, gs):
        cols = pl.ds(pl.multiple_of(n * wide, wide), wide)
        total = jnp.zeros((rows, wide), F32)
        for g in gs:
            y = jnp.dot(bd[g], slab(l, GROUPS[g], 2 * units, cols), preferred_element_type=F32)
            y = y.astype(BF16).astype(F32)
            for b in range(group):
                total = total + y[b * rows:(b + 1) * rows]
        return total

    @scoped
    def mlp_down(l):
        @pl.loop(0, n_sums)
        def _(n):
            ps[l, n] = down(l, n, range(n_groups)).reshape(nz, seq_dev, wide)
            rs_start(l, n)

    n_in = 4 if two_step else nz - 1

    @scoped
    def rs_finish(l, store):
        mine = pl.ds(pl.multiple_of(mz * seq_dev, seq_dev), seq_dev)
        for n in range(n_sums):
            if n_in:
                take(rs.at[l, n], rs_recv.at[l, n])
            total = ps[l, n, mz]
            for k in range(n_in):
                total = total + rs[l, n, k]
            store(n, (hres[mine, n * wide:(n + 1) * wide] + total).astype(BF16))

    def store_next(l):
        def store(n, x):
            h_all[l + 1, mz, :, n * wide:(n + 1) * wide] = x
        return store

    with jax.named_scope('barrier'):
        pl.semaphore_wait(barrier, 1 + len(next_devices))
    round_start(0)
    p1(0)
    p3(0, (0,))
    with jax.named_scope('rounds'):
        small[0].wait()
        for r in range(4):
            if r:
                round_wait(r - 1)
                if r < 3:
                    round_start(r)
            h_start(0, 0, d_model, [i for i in far_z if min(i, nz - i) == r + 1])
    start_later_copies()
    with jax.named_scope('small'):
        for c in small[1:]:
            c.wait()
        rope_tables()
    p2(0)
    for l in range(layers):
        more = l + 1 < layers
        if l:
            kv_heads(l)
            h_start(l, 0, d_model, far_z)
            p3(l, (2,))
            kv_heads_wait(l)
            p4(l, (0, 1, 3))
        h_wait(l)
        norm_to_zb(l, ga)
        if l == 0:
            kv_first(l)
            p3(l, (1, 3, 2))
            p4(l, (0,))
        else:
            p4(l, (2,))
        q_first(l)
        kv_wait(l)
        attention(l)
        if l == 0:
            p4(0, (1, 3, 2))
            p5(0, (0,))
        else:
            p5(l, (0, 1, 3, 2))
        if more:
            p1(l + 1)
            p3(l + 1, (0,))
        out_proj(l)
        norm_to_zb(l, gm, True)
        if l == 0:
            w_done(l, (0,))
            mlp_units(l, (0,))
            w_done(l, (1,))
            mlp_units(l, (1,))
            p5(l, (1, 3))
            w_done(l, (2,))
            mlp_units(l, (2,))
            p5(l, (2,))
            w_done(l, (3,))
            mlp_units_but_last(l, 3)
            w_done(l, (4,))
            mlp_units_last(l, 3)
        else:
            w_done(l, range(n_groups + 1))
            mlp_units(l, range(n_groups))
        mlp_down(l)
        if more:
            p2(l + 1)
            p3(l + 1, (1, 3))
        rs_middle(l)
        if more:
            rs_finish(l, store_next(l))
    pieces = []
    rs_finish(layers - 1, lambda n, x: pieces.append(x.astype(F32)))
    x = jnp.concatenate(pieces, axis=1)
    inv = lax.rsqrt(jnp.mean(x * x, axis=-1, keepdims=True) + NORM_EPS)
    gain = gf[...].astype(F32)
    for i in range(d_model // LANES):
        cols = slice(i * LANES, (i + 1) * LANES)
        out_ref[:, cols] = x[:, cols] * inv * gain[i:i + 1]

    with jax.named_scope('drain'):
      for l in range(layers):
          ref = w_all.at[l, 0, pl.ds(0, PLANE - 1)]
          remote(ref, ref, w_send.at[l], w_recv.at[l, 0], me).wait_send()
          ref = w_all.at[l, 0]
          remote(ref, ref, d_send.at[l], d_recv.at[l, 0], me).wait_send()
          ref = kv_all.at[l, 0, pl.ds(0, PLANE - 1)]
          remote(ref, ref, kv_send.at[l], kv_recv.at[l], me).wait_send()
          ref = kv_all.at[l, 0]
          remote(ref, ref, kvd_send.at[l], kvd_recv.at[l], me).wait_send()
          if nz > 1 and l:
              ref = kv_rows.at[l - 1, pl.ds(0, nz - 1)]
              remote(ref, ref, kva_send.at[l - 1], kva_recv.at[l - 1], me).wait_send()
          if nz > 1:
              ref = h_all.at[l, pl.ds(0, nz - 1)]
              remote(ref, ref, h_send.at[l], h_recv.at[l], me).wait_send()
              ref = c_mat.at[l, :, pl.ds(0, (nz - 1) * hq)]
              remote(ref, ref, c_send.at[l], c_recv.at[l, 0], me).wait_send()
              ref = ps.at[l, :, pl.ds(0, nz - 1)]
              remote(ref, ref, rs_send.at[l], rs_recv.at[l, 0], me).wait_send()


def solution(mesh):
    nz = mesh.shape['tp'] // (2 * PLANE)

    def device_fn(hidden_in, lengths, attn_norm, w_query, w_key, w_value, w_out, mlp_norm, w_gate, w_up, w_down, final_norm):
        seq_dev, d_model = hidden_in.shape[1:]
        layers, _, heads, hd = w_query.shape
        kv_heads = w_key.shape[2]
        units = w_gate.shape[2]
        assert kv_heads == nz and 2 * hd == LANES and heads % nz == 0
        hq = heads // nz * hd
        rows = nz * seq_dev
        wide = min(2 * CHUNK, d_model)
        n_sums = d_model // wide
        n_groups = 2 * PLANE * units // CHUNK
        dev, row = np.arange(2 * PLANE)[:, None], np.arange(rows)[None, :]
        pos = (row // seq_dev) * (2 * PLANE * seq_dev) + dev * seq_dev + row % seq_dev
        freq = np.float32(ROPE_BASE) ** (np.float32(-2.0) * np.arange(hd // 2, dtype=np.float32) / np.float32(hd))
        angles = (pos[..., None].astype(np.float32) * freq).astype(np.float64)
        rope = np.tile(np.concatenate([np.cos(angles), np.sin(angles)], axis=-1), (1, 1, 2)).astype(np.float32)
        by_rows = lambda w: jnp.transpose(w, (0, 2, 3, 1)).reshape(layers, -1, d_model)
        units_first = lambda w: jnp.transpose(w, (0, 2, 1))
        pinned = lambda x: pltpu.with_memory_space_constraint(x, pltpu.HBM)
        hbm, vmem = (pl.BlockSpec(memory_space=s) for s in (pltpu.HBM, pltpu.VMEM))
        dma = pltpu.SemaphoreType.DMA
        out = pl.pallas_call(
            functools.partial(kernel, nz),
            name='decoder',
            out_shape=pltpu.VMEM((seq_dev, d_model), F32),
            in_specs=[hbm] * 13,
            out_specs=vmem,
            scratch_shapes=[
                pltpu.VMEM((layers, 2, PLANE, 3 * units, d_model), BF16),
                pltpu.VMEM((layers, heads * hd, d_model), BF16),
                pltpu.VMEM((layers, hq + 2 * hd, d_model), BF16),
                pltpu.VMEM((layers - 1, kv_heads * 2 * hd, d_model), BF16),
                pltpu.VMEM((layers - 1, kv_heads, seq_dev, LANES), BF16),
                pltpu.VMEM((layers, nz, seq_dev, d_model), BF16),
                pltpu.VMEM((layers, rows, heads * hd), BF16),
                pltpu.VMEM((layers, 2, PLANE, rows, LANES), BF16),
                pltpu.VMEM((layers, n_sums, 4 if nz == 8 else max(nz - 1, 1), seq_dev, wide), F32),
                pltpu.VMEM((layers, n_sums, 3, seq_dev, wide), F32),
                pltpu.VMEM((layers, n_sums, 2, seq_dev, wide), F32),
                pltpu.VMEM((layers, n_sums, nz, seq_dev, wide), F32),
                pltpu.VMEM((rows, d_model), F32),
                pltpu.VMEM((rows, d_model), F32),
                pltpu.VMEM((rows, d_model), BF16),
                pltpu.VMEM((hq // hd * rows, LANES), BF16),
                pltpu.VMEM((n_groups, CHUNK // units * rows, CHUNK), BF16),
                pltpu.VMEM((rows, LANES), F32), pltpu.VMEM((rows, LANES), F32), pltpu.VMEM((rows, LANES), F32),
                pltpu.VMEM((layers, d_model), BF16), pltpu.VMEM((layers, d_model), BF16),
                pltpu.VMEM((d_model // LANES, LANES), BF16),
                pltpu.SMEM((1,), jnp.int32),
                dma((layers, 4)), dma((6,)), dma((layers, 10)), dma((layers,)),
                dma((layers, n_groups + 1)), dma((layers,)),
                pltpu.SemaphoreType.REGULAR((3,)),
                dma((layers,)), dma((layers,)), dma((layers,)), dma((layers,)), dma((layers,)), dma((layers,)),
                dma((layers - 1,)), dma((layers - 1,)),
                dma((layers, 2)), dma((layers,)), dma((layers, n_sums)), dma((layers, n_sums)), dma((layers,)),
            ],
            compiler_params=pltpu.CompilerParams(
                collective_id=0, has_side_effects=True, vmem_limit_bytes=60_000_000),
        )(pinned(hidden_in[0]), lengths, *map(pinned, (
            jnp.asarray(rope), attn_norm, mlp_norm, final_norm.reshape(-1, LANES), by_rows(w_query), by_rows(w_key), by_rows(w_value),
            w_out.reshape(layers, heads * hd, d_model), units_first(w_gate), units_first(w_up), w_down)))
        return out.astype(BF16)[None]

    seq_part = P(None, 'tp', None)
    in_specs = (seq_part, P(), P(), P(), P(), P(), P(), P(), P(None, None, 'tp'), P(None, None, 'tp'), P(None, 'tp', None), P())
    return jax.shard_map(device_fn, mesh=mesh, in_specs=in_specs, out_specs=seq_part, check_vma=False)
```

```python
import functools

import jax
import jax.numpy as jnp
import numpy as np
from jax import lax
from jax.experimental import pallas as pl
from jax.experimental.pallas import tpu as pltpu
from jax.sharding import PartitionSpec as P

NORM_EPS = 1e-5
ROPE_BASE = 500000.0
NX = 4
PLANE = NX * NX
LANES = 128
CHUNK = 256
NT = (((1,), (1,)), ((), ()))
F32, BF16 = jnp.float32, jnp.bfloat16


def remote(src, dst, send_sem, recv_sem, device):
    return pltpu.make_async_remote_copy(
        src_ref=src, dst_ref=dst, send_sem=send_sem, recv_sem=recv_sem,
        device_id=(device,), device_id_type=pl.DeviceIdType.MESH)


def scoped(f):
    @functools.wraps(f)
    def wrapped(*args):
        with jax.named_scope(f.__name__ + ('#l=%d' % args[0])):
            return f(*args)
    return wrapped


def kernel(nz, h_ref, len_ref, rope_ref, ga_ref, gm_ref, gf_ref, wq_ref, wk_ref, wv_ref, wo_ref, wg_ref, wu_ref, wd_ref,
           out_ref, w_all, wo_v, wqkv, wkv, kv_rows, h_all, c_mat, kv_all, rs, ra, sb, ps, acc, hres, zb, qbuf, bd, rope, cos_t, sin_t, ga, gm, gf, len_s,
           local_sem, in_sem, w_recv, w_send, d_recv, d_send, rounds, h_recv, h_send, kv_recv, kv_send, kvd_recv, kvd_send, kva_recv, kva_send,
           c_recv, c_send, rs_recv, ra_recv, rs_send):
    layers = wo_ref.shape[0]
    seq_dev, d_model = h_ref.shape
    units = wg_ref.shape[1]
    pack = 3 * units
    half = pack // 2
    rows = nz * seq_dev
    hq = wq_ref.shape[1] // nz
    hd = wk_ref.shape[1] // nz
    me = lax.axis_index('tp')
    core = me % 2
    px = (me // 2) % NX
    py = (me // (2 * NX)) % NX
    mp = (me // 2) % PLANE
    mz = me // (2 * PLANE)
    base = mz * (2 * PLANE)
    partner = base + mp * 2 + (1 - core)

    def z_peer(i):
        return ((mz + i) % nz) * (2 * PLANE) + mp * 2 + core

    far_z = sorted(range(1, nz), key=lambda i: -min(i, nz - i))
    next_z = [i for i in far_z if min(i, nz - i) == 1]
    def plane_peer(dy, dx):
        return base + ((py + dy) % NX * NX + (px + dx) % NX) * 2 + core

    far_plane = sorted(((dy, dx) for dy in range(NX) for dx in range(NX) if dy or dx),
                       key=lambda d: -sum(min(i, NX - i) for i in d))

    barrier = pltpu.get_barrier_semaphore()
    next_devices = [plane_peer(0, 1), plane_peer(0, NX - 1), plane_peer(1, 0), plane_peer(NX - 1, 0)]
    next_devices += [z_peer(i) for i in next_z]

    def signal(sem, device):
        pl.semaphore_signal(sem, inc=1, device_id=(device,), device_id_type=pl.DeviceIdType.MESH)

    signal(barrier, partner)
    for d in next_devices:
        signal(barrier, d)

    def round_start(r):
        for d in next_devices:
            signal(rounds.at[r], d)

    def round_wait(r):
        pl.semaphore_wait(rounds.at[r], len(next_devices))

    def pack_copies(l):
        mine = w_all.at[l, core, mp]
        return [pltpu.make_async_copy(ref.at[l], mine.at[pl.ds(i * units, units)], local_sem.at[l, 0])
                for i, ref in enumerate((wg_ref, wu_ref, wd_ref))]

    def qkv_copies(l):
        mine = [(wq_ref, 0, hq), (wk_ref, hq, hd), (wv_ref, hq + hd, hd)]
        return [pltpu.make_async_copy(ref.at[l, pl.ds(mz * n, n)], wqkv.at[l, pl.ds(first, n)], local_sem.at[l, 1])
                for ref, first, n in (mine[:1] if l else mine)]

    def kv_weight_copies(l):
        return [pltpu.make_async_copy(ref.at[l, pl.ds(z * hd, hd)], wkv.at[l - 1, pl.ds((2 * z + i) * hd, hd)], local_sem.at[l, 3])
                for z in range(nz) for i, ref in enumerate((wk_ref, wv_ref))]

    def wo_copy(l):
        return pltpu.make_async_copy(wo_ref.at[l], wo_v.at[l], local_sem.at[l, 2])

    def take(ref, sem):
        remote(ref, ref, w_send.at[0], sem, me).wait_recv()

    def pack_wait(l):
        mine = w_all.at[l, core, mp]
        pltpu.make_async_copy(mine, mine, local_sem.at[l, 0]).wait()

    def qkv_wait(l):
        ref = wqkv.at[l, pl.ds(0, hq)] if l else wqkv.at[l]
        pltpu.make_async_copy(ref, ref, local_sem.at[l, 1]).wait()

    small = [pltpu.make_async_copy(src, dst, in_sem.at[i]) for i, (src, dst) in enumerate((
        (h_ref, h_all.at[0, mz]), (rope_ref.at[mp * 2 + core], rope), (ga_ref, ga), (gm_ref, gm), (gf_ref, gf), (len_ref, len_s)))]
    for c in pack_copies(0) + small + qkv_copies(0):
        c.start()

    def start_later_copies():
        wo_copy(0).start()
        for l in range(1, layers):
            for c in pack_copies(l) + qkv_copies(l) + kv_weight_copies(l):
                c.start()
            wo_copy(l).start()

    def slot(h, a1, a2):
        return a2 % NX * NX + a1 % NX if h == 0 else a1 % NX * NX + a2 % NX

    def where_am_i(h):
        return (px, py) if h == 0 else (py, px)

    def at(h, a1, a2):
        return base + slot(h, a1, a2) * 2 + core

    third = half // 3
    SPAN = ((0, half), (half, half))

    def from_minus(h, k):
        return (h * half, 2 * third if (k in (1, 2)) != (h == 1) else third)

    def from_plus(h, k):
        first, size = from_minus(h, k)
        return (first + size, half - size)

    def piece(l, c, p, span):
        return w_all.at[l, c, p, pl.ds(*span)]

    def w_start(l, p, span, idx, device):
        ref = piece(l, core, p, span)
        remote(ref, ref, w_send.at[l], w_recv.at[l, idx], device).start()

    def w_take(l, idx, packs):
        take(w_all.at[l, core, pl.ds(0, packs)], w_recv.at[l, idx])

    GROUPS = (((0, 0), (1, 0), (3, 0), (0, 1)), ((0, 3), (2, 0), (0, 2), (1, 1)),
              ((1, 3), (3, 1), (3, 3), (2, 1)), ((2, 3), (1, 2), (3, 2), (2, 2)))
    ARRIVALS = (*GROUPS[:-1], GROUPS[-1][:-1], GROUPS[-1][-1:])
    ARRIVAL_OF = {d: g for g, ds in enumerate(ARRIVALS) for d in ds}

    def to_partner(l, h, k1, k2, span):
        a1, a2 = where_am_i(h)
        ref = piece(l, core, slot(h, a1 + k1, a2 + k2), span)
        g = ARRIVAL_OF[(k1, k2) if h == 0 else (k2, k1)]
        remote(ref, ref, d_send.at[l], d_recv.at[l, g], partner).start()

    @scoped
    def p1(l):
        pack_wait(l)
        for h in range(2):
            a1, a2 = where_am_i(h)
            w_start(l, mp, SPAN[h], 0, at(h, a1 + 1, a2))
            w_start(l, mp, SPAN[h], 0, at(h, a1 + NX - 1, a2))
        to_partner(l, 0, 0, 0, (0, pack))

    @scoped
    def p2(l):
        w_take(l, 0, 2)
        for h in range(2):
            a1, a2 = where_am_i(h)
            w_start(l, slot(h, a1 + NX - 1, a2), from_minus(h, 0), 1, at(h, a1 + 1, a2))
            w_start(l, slot(h, a1 + 1, a2), from_plus(h, 0), 1, at(h, a1 + NX - 1, a2))
            to_partner(l, h, NX - 1, 0, SPAN[h])
            to_partner(l, h, 1, 0, SPAN[h])

    @scoped
    def p3(l, ks):
        for k in ks:
            if k == 2:
                w_take(l, 1, 1)
            for h in range(2):
                a1, a2 = where_am_i(h)
                p = slot(h, a1 + k, a2)
                w_start(l, p, SPAN[h], 2 + k, at(h, a1, a2 + 1))
                w_start(l, p, SPAN[h], 2 + k, at(h, a1, a2 + NX - 1))
                if k == 2:
                    to_partner(l, h, k, 0, SPAN[h])

    @scoped
    def p4(l, ks):
        for k in ks:
            w_take(l, 2 + k, 2)
            for h in range(2):
                a1, a2 = where_am_i(h)
                w_start(l, slot(h, a1 + k, a2 + NX - 1), from_minus(h, k), 6 + k, at(h, a1, a2 + 1))
                w_start(l, slot(h, a1 + k, a2 + 1), from_plus(h, k), 6 + k, at(h, a1, a2 + NX - 1))
                to_partner(l, h, k, NX - 1, SPAN[h])
                to_partner(l, h, k, 1, SPAN[h])

    @scoped
    def p5(l, ks):
        for k in ks:
            w_take(l, 6 + k, 1)
            for h in range(2):
                to_partner(l, h, k, 2, SPAN[h])

    @scoped
    def w_done(l, gs):
        for g in gs:
            take(w_all.at[l, 1 - core, pl.ds(0, len(ARRIVALS[g]))], d_recv.at[l, g])

    def h_start(l, first, size, peers):
        for i in peers:
            ref = h_all.at[l, mz, :, pl.ds(first, size)]
            remote(ref, ref, h_send.at[l], h_recv.at[l], z_peer(i)).start()

    @scoped
    def h_wait(l):
        if nz > 1:
            take(h_all.at[l, pl.ds(0, nz - 1)], h_recv.at[l])
        for i in range(nz):
            hres[pl.ds(i * seq_dev, seq_dev)] = h_all[l, i].astype(F32)

    @scoped
    def norm_to_zb(l, gains, residual=False):
        gain = gains[...].astype(F32)[l:l + 1]
        step = min(16, rows)
        for first in range(0, rows, step):
            r = pl.ds(first, step)
            x = hres[r]
            if residual:
                x = (x + acc[r]).astype(BF16).astype(F32)
                hres[r] = x
            inv = lax.rsqrt(jnp.mean(x * x, axis=-1, keepdims=True) + NORM_EPS)
            zb[r] = (x * inv * gain).astype(BF16)

    lane = lax.broadcasted_iota(jnp.int32, (rows, LANES), 1)
    low_half = lane < hd

    def rotate(x, cos, sin):
        first = (lane[:x.shape[0]] % hd) < hd // 2
        swapped = jnp.where(first, pltpu.roll(x, LANES - hd // 2, 1), pltpu.roll(x, hd // 2, 1))
        return x * cos + swapped * sin

    def rope_tables():
        first = (lane % hd) < hd // 2
        t = rope[...]
        cos_t[...] = jnp.where(first, t, pltpu.roll(t, hd // 2, 1))
        sin_t[...] = jnp.where(first, -pltpu.roll(t, LANES - hd // 2, 1), t)

    def kv_copy(l, device):
        ref = kv_all.at[l, core, mp]
        return remote(ref, ref, kv_send.at[l], kv_recv.at[l], device)

    def kv_start(l):
        for d in far_plane:
            kv_copy(l, plane_peer(*d)).start()

    @scoped
    def kv_first(l):
        qkv_wait(l)
        kv = lax.dot_general(zb[...], wqkv[l, pl.ds(hq, 2 * hd), :], NT, preferred_element_type=F32)
        kv_all[l, core, mp] = jnp.where(low_half, rotate(kv, cos_t[...], sin_t[...]), kv).astype(BF16)
        kv_start(l)

    def kv_own(l):
        return kv_all.at[l, core, mp, pl.ds(pl.multiple_of(mz * seq_dev, seq_dev), seq_dev)]

    @scoped
    def kv_heads(l):
        ref = wkv.at[l - 1]
        pltpu.make_async_copy(ref, ref, local_sem.at[l, 3]).wait()
        x = h_all[l, mz].astype(F32)
        inv = lax.rsqrt(jnp.mean(x * x, axis=-1, keepdims=True) + NORM_EPS)
        z = x * inv * ga[...].astype(F32)[l:l + 1]
        z = jnp.concatenate([z, z], axis=0).astype(BF16)
        kv = lax.dot_general(z, wkv[l - 1], NT, preferred_element_type=F32)[:seq_dev]
        mine = pl.ds(pl.multiple_of(mz * seq_dev, seq_dev), seq_dev)
        for head in range(nz):
            part = kv[:, head * LANES:(head + 1) * LANES]
            kv_rows[l - 1, head] = jnp.where(low_half[:seq_dev], rotate(part, cos_t[mine], sin_t[mine]), part).astype(BF16)
        pltpu.make_async_copy(kv_rows.at[l - 1, mz], kv_own(l), local_sem.at[l, 0]).start()
        for i in far_z:
            remote(kv_rows.at[l - 1, (mz + i) % nz], kv_own(l), kva_send.at[l - 1], kva_recv.at[l - 1], z_peer(i)).start()

    @scoped
    def kv_heads_wait(l):
        pltpu.make_async_copy(kv_rows.at[l - 1, mz], kv_own(l), local_sem.at[l, 0]).wait()
        if nz > 1:
            take(kv_rows.at[l - 1, pl.ds(0, nz - 1)], kva_recv.at[l - 1])
        kv_start(l)

    @scoped
    def q_first(l):
        if l:
            qkv_wait(l)
        proj = lax.dot_general(zb[...], wqkv[l, pl.ds(0, hq), :], NT, preferred_element_type=F32)
        for j in range(hq // LANES):
            q = rotate(proj[:, j * LANES:(j + 1) * LANES], cos_t[...], sin_t[...]) * (hd ** -0.5)
            for half_head, x in enumerate((q, pltpu.roll(q, LANES - hd, 1))):
                head = 2 * j + half_head
                qbuf[pl.ds(head * rows, rows)] = jnp.where(low_half, x, 0.0).astype(BF16)

    @scoped
    def kv_wait(l):
        take(kv_all.at[l, core, pl.ds(0, PLANE - 1)], kv_recv.at[l])
        ref = kv_all.at[l, core]
        remote(ref, ref, kvd_send.at[l], kvd_recv.at[l], partner).start()
        take(kv_all.at[l, 1 - core], kvd_recv.at[l])

    def c_columns(z):
        return pl.ds(pl.multiple_of(z * hq, hq), hq)

    @scoped
    def attention(l):
        keys = 2 * PLANE * rows
        j = lax.broadcasted_iota(jnp.int32, (1, keys), 1)
        key_pos = ((j // seq_dev) % nz) * (2 * PLANE * seq_dev) + ((j // rows) % PLANE) * (2 * seq_dev) \
            + (j // (PLANE * rows)) * seq_dev + j % seq_dev
        i = lax.broadcasted_iota(jnp.int32, (2 * rows, 1), 0) % rows
        q_pos = (i // seq_dev) * (2 * PLANE * seq_dev) + (mp * 2 + core) * seq_dev + i % seq_dev
        allowed = key_pos <= jnp.minimum(q_pos, len_s[0] - 1)
        kv = kv_all[l].reshape(keys, LANES)
        for pair in range(hq // LANES):
            s = lax.dot_general(qbuf[pl.ds(2 * pair * rows, 2 * rows)], kv, NT, preferred_element_type=F32)
            s = jnp.where(allowed, s, -1e30)
            e = jnp.exp(s - jnp.max(s, axis=-1, keepdims=True))
            p = (e * (1.0 / jnp.sum(e, axis=-1, keepdims=True))).astype(BF16)
            o = jnp.dot(p, kv, preferred_element_type=F32)
            cols = pl.ds(pl.multiple_of(mz * hq + pair * LANES, LANES), LANES)
            c_mat[l, :, cols] = jnp.where(low_half, pltpu.roll(o[:rows], LANES - hd, 1), o[rows:]).astype(BF16)
            ref = c_mat.at[l, :, cols]
            for i in far_z:
                remote(ref, ref, c_send.at[l], c_recv.at[l, int(i in next_z)], z_peer(i)).start()

    @scoped
    def out_proj(l):
        with jax.named_scope('wo_wait'):
            wo_copy(l).wait()
        for i in [0] + far_z:
            if i and i in (far_z[0], far_z[-len(next_z)]):
                near = i in next_z
                n = len(next_z) if near else nz - 1 - len(next_z)
                with jax.named_scope('c_wait'):
                    take(c_mat.at[l, :, pl.ds(0, n * hq)], c_recv.at[l, int(near)])
            cols = c_columns((mz + nz - i) % nz)
            part = jnp.dot(c_mat[l, :, cols], wo_v[l, cols, :], preferred_element_type=F32)
            acc[...] = acc[...] + part if i else part

    group = CHUNK // units
    n_groups = len(GROUPS)
    assert group == 2 * len(GROUPS[0])

    def slab(l, places, first, cols):
        parts = [w_all[l, c, slot(0, px + dx, py + dy), pl.ds(first, units), cols] for dx, dy in places for c in range(2)]
        return jnp.concatenate(parts, axis=0)

    block = lax.broadcasted_iota(jnp.int32, (rows, CHUNK), 1) // units
    every = pl.ds(0, d_model)

    def units_of(l, places):
        gate = lax.dot_general(zb[...], slab(l, places, 0, every), NT, preferred_element_type=F32)
        up = lax.dot_general(zb[...], slab(l, places, units, every), NT, preferred_element_type=F32)
        return gate * (1.0 / (1.0 + jnp.exp(-gate))) * up

    def spread(g, act, blocks):
        for b in blocks:
            bd[g, pl.ds(b * rows, rows)] = jnp.where(block == b, act, 0.0).astype(BF16)

    @scoped
    def mlp_units(l, gs):
        for g in gs:
            spread(g, units_of(l, GROUPS[g]), range(group))

    @scoped
    def mlp_units_but_last(l, g):
        places = GROUPS[g][:-1] + GROUPS[g][:1]
        spread(g, units_of(l, places), range(group - 2))

    @scoped
    def mlp_units_last(l, g):
        act = units_of(l, GROUPS[g][-2:])
        spread(g, jnp.concatenate([jnp.zeros_like(act), act], axis=1), range(group - 2, group))

    two_step = nz == 8
    wide = min(2 * CHUNK, d_model)
    n_sums = d_model // wide

    def ps_of(l, n, i):
        return ps.at[l, n, (mz + i + nz) % nz]

    def rs_start(l, n):
        if not two_step:
            for k, i in enumerate(far_z):
                remote(ps_of(l, n, i), rs.at[l, n, k], rs_send.at[l], rs_recv.at[l, n], z_peer(i)).start()
            return
        for side, to in ((0, nz - 2), (1, 2)):
            cols = pl.ds(side * (wide // 2), wide // 2)
            remote(ps.at[l, n, (mz + 4) % nz, :, cols], ra.at[l, n, 2, :, cols], rs_send.at[l], ra_recv.at[l, n], z_peer(to)).start()
        for side, to in ((0, -1), (1, 1)):
            remote(ps_of(l, n, 3 * to), ra.at[l, n, side], rs_send.at[l], ra_recv.at[l, n], z_peer(nz + to)).start()

    @scoped
    def rs_middle(l):
        if not two_step:
            return
        for n in range(n_sums):
            for side, to in ((0, -1), (1, 1)):
                remote(ps_of(l, n, to), rs.at[l, n, side], rs_send.at[l], rs_recv.at[l, n], z_peer(nz + to)).start()

        @pl.loop(0, n_sums)
        def _(n):
            take(ra.at[l, n], ra_recv.at[l, n])
            for side, to in ((0, -2), (1, 2)):
                cols = pl.ds(side * (wide // 2), wide // 2)
                sb[l, n, side] = ps[l, n, (mz + nz + to) % nz] + ra[l, n, side]
                sb[l, n, side, :, cols] = sb[l, n, side, :, cols] + ra[l, n, 2, :, cols]
                remote(sb.at[l, n, side], rs.at[l, n, 2 + side], rs_send.at[l], rs_recv.at[l, n], z_peer(nz + to)).start()

    def down(l, n, gs):
        cols = pl.ds(pl.multiple_of(n * wide, wide), wide)
        total = jnp.zeros((rows, wide), F32)
        for g in gs:
            y = jnp.dot(bd[g], slab(l, GROUPS[g], 2 * units, cols), preferred_element_type=F32)
            y = y.astype(BF16).astype(F32)
            for b in range(group):
                total = total + y[b * rows:(b + 1) * rows]
        return total

    @scoped
    def mlp_down(l):
        @pl.loop(0, n_sums)
        def _(n):
            ps[l, n] = down(l, n, range(n_groups)).reshape(nz, seq_dev, wide)
            rs_start(l, n)

    n_in = 4 if two_step else nz - 1

    @scoped
    def rs_finish(l, store):
        mine = pl.ds(pl.multiple_of(mz * seq_dev, seq_dev), seq_dev)
        for n in range(n_sums):
            if n_in:
                take(rs.at[l, n], rs_recv.at[l, n])
            total = ps[l, n, mz]
            for k in range(n_in):
                total = total + rs[l, n, k]
            store(n, (hres[mine, n * wide:(n + 1) * wide] + total).astype(BF16))

    def store_next(l):
        def store(n, x):
            h_all[l + 1, mz, :, n * wide:(n + 1) * wide] = x
        return store

    with jax.named_scope('barrier'):
        pl.semaphore_wait(barrier, 1 + len(next_devices))
    round_start(0)
    p1(0)
    p3(0, (0,))
    with jax.named_scope('rounds'):
        small[0].wait()
        for r in range(4):
            if r:
                round_wait(r - 1)
                if r < 3:
                    round_start(r)
            h_start(0, 0, d_model, [i for i in far_z if min(i, nz - i) == r + 1])
    start_later_copies()
    with jax.named_scope('small'):
        for c in small[1:]:
            c.wait()
        rope_tables()
    p2(0)
    for l in range(layers):
        more = l + 1 < layers
        if l:
            p4(l, (0,))
            kv_heads(l)
            h_start(l, 0, d_model, far_z)
            kv_heads_wait(l)
            p3(l, (2,))
            p4(l, (1, 3))
        h_wait(l)
        norm_to_zb(l, ga)
        if l == 0:
            kv_first(l)
            p3(l, (1, 3, 2))
            p4(l, (0,))
        q_first(l)
        kv_wait(l)
        attention(l)
        if l == 0:
            p4(0, (1, 3, 2))
            p5(0, (0,))
        else:
            p5(l, (0,))
            p4(l, (2,))
            p5(l, (1, 3, 2))
        if more:
            p1(l + 1)
            p3(l + 1, (0,))
        out_proj(l)
        norm_to_zb(l, gm, True)
        if l == 0:
            w_done(l, (0,))
            mlp_units(l, (0,))
            w_done(l, (1,))
            mlp_units(l, (1,))
            p5(l, (1, 3))
            w_done(l, (2,))
            mlp_units(l, (2,))
            p5(l, (2,))
            w_done(l, (3,))
            mlp_units_but_last(l, 3)
            w_done(l, (4,))
            mlp_units_last(l, 3)
        else:
            w_done(l, range(n_groups + 1))
            mlp_units(l, range(n_groups))
        mlp_down(l)
        if more:
            p2(l + 1)
            p3(l + 1, (1, 3))
        rs_middle(l)
        if more:
            rs_finish(l, store_next(l))
    pieces = []
    rs_finish(layers - 1, lambda n, x: pieces.append(x.astype(F32)))
    x = jnp.concatenate(pieces, axis=1)
    inv = lax.rsqrt(jnp.mean(x * x, axis=-1, keepdims=True) + NORM_EPS)
    gain = gf[...].astype(F32)
    for i in range(d_model // LANES):
        cols = slice(i * LANES, (i + 1) * LANES)
        out_ref[:, cols] = x[:, cols] * inv * gain[i:i + 1]

    with jax.named_scope('drain'):
      for l in range(layers):
          ref = w_all.at[l, 0, pl.ds(0, PLANE - 1)]
          remote(ref, ref, w_send.at[l], w_recv.at[l, 0], me).wait_send()
          ref = w_all.at[l, 0]
          remote(ref, ref, d_send.at[l], d_recv.at[l, 0], me).wait_send()
          ref = kv_all.at[l, 0, pl.ds(0, PLANE - 1)]
          remote(ref, ref, kv_send.at[l], kv_recv.at[l], me).wait_send()
          ref = kv_all.at[l, 0]
          remote(ref, ref, kvd_send.at[l], kvd_recv.at[l], me).wait_send()
          if nz > 1 and l:
              ref = kv_rows.at[l - 1, pl.ds(0, nz - 1)]
              remote(ref, ref, kva_send.at[l - 1], kva_recv.at[l - 1], me).wait_send()
          if nz > 1:
              ref = h_all.at[l, pl.ds(0, nz - 1)]
              remote(ref, ref, h_send.at[l], h_recv.at[l], me).wait_send()
              ref = c_mat.at[l, :, pl.ds(0, (nz - 1) * hq)]
              remote(ref, ref, c_send.at[l], c_recv.at[l, 0], me).wait_send()
              ref = ps.at[l, :, pl.ds(0, nz - 1)]
              remote(ref, ref, rs_send.at[l], rs_recv.at[l, 0], me).wait_send()


def solution(mesh):
    nz = mesh.shape['tp'] // (2 * PLANE)

    def device_fn(hidden_in, lengths, attn_norm, w_query, w_key, w_value, w_out, mlp_norm, w_gate, w_up, w_down, final_norm):
        seq_dev, d_model = hidden_in.shape[1:]
        layers, _, heads, hd = w_query.shape
        kv_heads = w_key.shape[2]
        units = w_gate.shape[2]
        assert kv_heads == nz and 2 * hd == LANES and heads % nz == 0
        hq = heads // nz * hd
        rows = nz * seq_dev
        wide = min(2 * CHUNK, d_model)
        n_sums = d_model // wide
        n_groups = 2 * PLANE * units // CHUNK
        dev, row = np.arange(2 * PLANE)[:, None], np.arange(rows)[None, :]
        pos = (row // seq_dev) * (2 * PLANE * seq_dev) + dev * seq_dev + row % seq_dev
        freq = np.float32(ROPE_BASE) ** (np.float32(-2.0) * np.arange(hd // 2, dtype=np.float32) / np.float32(hd))
        angles = (pos[..., None].astype(np.float32) * freq).astype(np.float64)
        rope = np.tile(np.concatenate([np.cos(angles), np.sin(angles)], axis=-1), (1, 1, 2)).astype(np.float32)
        by_rows = lambda w: jnp.transpose(w, (0, 2, 3, 1)).reshape(layers, -1, d_model)
        units_first = lambda w: jnp.transpose(w, (0, 2, 1))
        pinned = lambda x: pltpu.with_memory_space_constraint(x, pltpu.HBM)
        hbm, vmem = (pl.BlockSpec(memory_space=s) for s in (pltpu.HBM, pltpu.VMEM))
        dma = pltpu.SemaphoreType.DMA
        out = pl.pallas_call(
            functools.partial(kernel, nz),
            name='decoder',
            out_shape=pltpu.VMEM((seq_dev, d_model), F32),
            in_specs=[hbm] * 13,
            out_specs=vmem,
            scratch_shapes=[
                pltpu.VMEM((layers, 2, PLANE, 3 * units, d_model), BF16),
                pltpu.VMEM((layers, heads * hd, d_model), BF16),
                pltpu.VMEM((layers, hq + 2 * hd, d_model), BF16),
                pltpu.VMEM((layers - 1, kv_heads * 2 * hd, d_model), BF16),
                pltpu.VMEM((layers - 1, kv_heads, seq_dev, LANES), BF16),
                pltpu.VMEM((layers, nz, seq_dev, d_model), BF16),
                pltpu.VMEM((layers, rows, heads * hd), BF16),
                pltpu.VMEM((layers, 2, PLANE, rows, LANES), BF16),
                pltpu.VMEM((layers, n_sums, 4 if nz == 8 else max(nz - 1, 1), seq_dev, wide), F32),
                pltpu.VMEM((layers, n_sums, 3, seq_dev, wide), F32),
                pltpu.VMEM((layers, n_sums, 2, seq_dev, wide), F32),
                pltpu.VMEM((layers, n_sums, nz, seq_dev, wide), F32),
                pltpu.VMEM((rows, d_model), F32),
                pltpu.VMEM((rows, d_model), F32),
                pltpu.VMEM((rows, d_model), BF16),
                pltpu.VMEM((hq // hd * rows, LANES), BF16),
                pltpu.VMEM((n_groups, CHUNK // units * rows, CHUNK), BF16),
                pltpu.VMEM((rows, LANES), F32), pltpu.VMEM((rows, LANES), F32), pltpu.VMEM((rows, LANES), F32),
                pltpu.VMEM((layers, d_model), BF16), pltpu.VMEM((layers, d_model), BF16),
                pltpu.VMEM((d_model // LANES, LANES), BF16),
                pltpu.SMEM((1,), jnp.int32),
                dma((layers, 4)), dma((6,)), dma((layers, 10)), dma((layers,)),
                dma((layers, n_groups + 1)), dma((layers,)),
                pltpu.SemaphoreType.REGULAR((3,)),
                dma((layers,)), dma((layers,)), dma((layers,)), dma((layers,)), dma((layers,)), dma((layers,)),
                dma((layers - 1,)), dma((layers - 1,)),
                dma((layers, 2)), dma((layers,)), dma((layers, n_sums)), dma((layers, n_sums)), dma((layers,)),
            ],
            compiler_params=pltpu.CompilerParams(
                collective_id=0, has_side_effects=True, vmem_limit_bytes=60_000_000),
        )(pinned(hidden_in[0]), lengths, *map(pinned, (
            jnp.asarray(rope), attn_norm, mlp_norm, final_norm.reshape(-1, LANES), by_rows(w_query), by_rows(w_key), by_rows(w_value),
            w_out.reshape(layers, heads * hd, d_model), units_first(w_gate), units_first(w_up), w_down)))
        return out.astype(BF16)[None]

    seq_part = P(None, 'tp', None)
    in_specs = (seq_part, P(), P(), P(), P(), P(), P(), P(), P(None, None, 'tp'), P(None, None, 'tp'), P(None, 'tp', None), P())
    return jax.shard_map(device_fn, mesh=mesh, in_specs=in_specs, out_specs=seq_part, check_vma=False)
```

```python
import functools

import jax
import jax.numpy as jnp
import numpy as np
from jax import lax
from jax.experimental import pallas as pl
from jax.experimental.pallas import tpu as pltpu
from jax.sharding import PartitionSpec as P

NORM_EPS = 1e-5
ROPE_BASE = 500000.0
NX = 4
PLANE = NX * NX
LANES = 128
CHUNK = 256
NT = (((1,), (1,)), ((), ()))
F32, BF16 = jnp.float32, jnp.bfloat16


def remote(src, dst, send_sem, recv_sem, device):
    return pltpu.make_async_remote_copy(
        src_ref=src, dst_ref=dst, send_sem=send_sem, recv_sem=recv_sem,
        device_id=(device,), device_id_type=pl.DeviceIdType.MESH)


def scoped(f):
    @functools.wraps(f)
    def wrapped(*args):
        with jax.named_scope(f.__name__ + ('#l=%d' % args[0])):
            return f(*args)
    return wrapped


def kernel(nz, h_ref, len_ref, rope_ref, ga_ref, gm_ref, gf_ref, wq_ref, wk_ref, wv_ref, wo_ref, wg_ref, wu_ref, wd_ref,
           out_ref, w_all, wo_v, wqkv, wkv, kv_rows, h_all, c_mat, kv_all, rs, ra, sb, ps, acc, hres, zb, qbuf, bd, rope, cos_t, sin_t, ga, gm, gf, len_s,
           local_sem, in_sem, w_recv, w_send, d_recv, d_send, rounds, h_recv, h_send, kv_recv, kv_send, kvr_recv, kvd_recv, kvd_send, kva_recv, kva_send,
           c_recv, c_send, rs_recv, ra_recv, rs_send):
    layers = wo_ref.shape[0]
    seq_dev, d_model = h_ref.shape
    units = wg_ref.shape[1]
    pack = 3 * units
    half = pack // 2
    rows = nz * seq_dev
    hq = wq_ref.shape[1] // nz
    hd = wk_ref.shape[1] // nz
    me = lax.axis_index('tp')
    core = me % 2
    px = (me // 2) % NX
    py = (me // (2 * NX)) % NX
    mp = (me // 2) % PLANE
    mz = me // (2 * PLANE)
    base = mz * (2 * PLANE)
    partner = base + mp * 2 + (1 - core)

    def z_peer(i):
        return ((mz + i) % nz) * (2 * PLANE) + mp * 2 + core

    far_z = sorted(range(1, nz), key=lambda i: -min(i, nz - i))
    next_z = [i for i in far_z if min(i, nz - i) == 1]
    def plane_peer(dy, dx):
        return base + ((py + dy) % NX * NX + (px + dx) % NX) * 2 + core

    far_plane = sorted(((dy, dx) for dy in range(NX) for dx in range(NX) if dy or dx),
                       key=lambda d: -sum(min(i, NX - i) for i in d))

    barrier = pltpu.get_barrier_semaphore()
    next_devices = [plane_peer(0, 1), plane_peer(0, NX - 1), plane_peer(1, 0), plane_peer(NX - 1, 0)]
    next_devices += [z_peer(i) for i in next_z]

    def signal(sem, device):
        pl.semaphore_signal(sem, inc=1, device_id=(device,), device_id_type=pl.DeviceIdType.MESH)

    signal(barrier, partner)
    for d in next_devices:
        signal(barrier, d)

    def round_start(r):
        for d in next_devices:
            signal(rounds.at[r], d)

    def round_wait(r):
        pl.semaphore_wait(rounds.at[r], len(next_devices))

    def pack_copies(l):
        mine = w_all.at[l, core, mp]
        return [pltpu.make_async_copy(ref.at[l], mine.at[pl.ds(i * units, units)], local_sem.at[l, 0])
                for i, ref in enumerate((wg_ref, wu_ref, wd_ref))]

    def qkv_copies(l):
        mine = [(wq_ref, 0, hq), (wk_ref, hq, hd), (wv_ref, hq + hd, hd)]
        return [pltpu.make_async_copy(ref.at[l, pl.ds(mz * n, n)], wqkv.at[l, pl.ds(first, n)], local_sem.at[l, 1])
                for ref, first, n in (mine[:1] if l else mine)]

    def kv_weight_copies(l):
        return [pltpu.make_async_copy(ref.at[l, pl.ds(z * hd, hd)], wkv.at[l - 1, pl.ds((2 * z + i) * hd, hd)], local_sem.at[l, 3])
                for z in range(nz) for i, ref in enumerate((wk_ref, wv_ref))]

    def wo_copy(l):
        return pltpu.make_async_copy(wo_ref.at[l], wo_v.at[l], local_sem.at[l, 2])

    def take(ref, sem):
        remote(ref, ref, w_send.at[0], sem, me).wait_recv()

    def pack_wait(l):
        mine = w_all.at[l, core, mp]
        pltpu.make_async_copy(mine, mine, local_sem.at[l, 0]).wait()

    def qkv_wait(l):
        ref = wqkv.at[l, pl.ds(0, hq)] if l else wqkv.at[l]
        pltpu.make_async_copy(ref, ref, local_sem.at[l, 1]).wait()

    small = [pltpu.make_async_copy(src, dst, in_sem.at[i]) for i, (src, dst) in enumerate((
        (h_ref, h_all.at[0, mz]), (rope_ref.at[mp * 2 + core], rope), (ga_ref, ga), (gm_ref, gm), (gf_ref, gf), (len_ref, len_s)))]
    for c in pack_copies(0) + small + qkv_copies(0):
        c.start()

    def start_later_copies():
        wo_copy(0).start()
        for l in range(1, layers):
            for c in pack_copies(l) + qkv_copies(l) + kv_weight_copies(l):
                c.start()
            wo_copy(l).start()

    def slot(h, a1, a2):
        return a2 % NX * NX + a1 % NX if h == 0 else a1 % NX * NX + a2 % NX

    def where_am_i(h):
        return (px, py) if h == 0 else (py, px)

    def at(h, a1, a2):
        return base + slot(h, a1, a2) * 2 + core

    third = half // 3
    SPAN = ((0, half), (half, half))

    def from_minus(h, k):
        return (h * half, 2 * third if (k in (1, 2)) != (h == 1) else third)

    def from_plus(h, k):
        first, size = from_minus(h, k)
        return (first + size, half - size)

    def piece(l, c, p, span):
        return w_all.at[l, c, p, pl.ds(*span)]

    def w_start(l, p, span, idx, device):
        ref = piece(l, core, p, span)
        remote(ref, ref, w_send.at[l], w_recv.at[l, idx], device).start()

    def w_take(l, idx, packs):
        take(w_all.at[l, core, pl.ds(0, packs)], w_recv.at[l, idx])

    GROUPS = (((0, 0), (1, 0), (3, 0), (0, 1)), ((0, 3), (2, 0), (0, 2), (1, 1)),
              ((1, 3), (3, 1), (3, 3), (2, 1)), ((2, 3), (1, 2), (3, 2), (2, 2)))
    ARRIVALS = (*GROUPS[:-1], GROUPS[-1][:-1], GROUPS[-1][-1:])
    ARRIVAL_OF = {d: g for g, ds in enumerate(ARRIVALS) for d in ds}

    def to_partner(l, h, k1, k2, span):
        a1, a2 = where_am_i(h)
        ref = piece(l, core, slot(h, a1 + k1, a2 + k2), span)
        g = ARRIVAL_OF[(k1, k2) if h == 0 else (k2, k1)]
        remote(ref, ref, d_send.at[l], d_recv.at[l, g], partner).start()

    @scoped
    def p1(l):
        pack_wait(l)
        for h in range(2):
            a1, a2 = where_am_i(h)
            w_start(l, mp, SPAN[h], 0, at(h, a1 + 1, a2))
            w_start(l, mp, SPAN[h], 0, at(h, a1 + NX - 1, a2))
        to_partner(l, 0, 0, 0, (0, pack))

    @scoped
    def p2(l):
        w_take(l, 0, 2)
        for h in range(2):
            a1, a2 = where_am_i(h)
            w_start(l, slot(h, a1 + NX - 1, a2), from_minus(h, 0), 1, at(h, a1 + 1, a2))
            w_start(l, slot(h, a1 + 1, a2), from_plus(h, 0), 1, at(h, a1 + NX - 1, a2))
            to_partner(l, h, NX - 1, 0, SPAN[h])
            to_partner(l, h, 1, 0, SPAN[h])

    @scoped
    def p3(l, ks):
        for k in ks:
            if k == 2:
                w_take(l, 1, 1)
            for h in range(2):
                a1, a2 = where_am_i(h)
                p = slot(h, a1 + k, a2)
                w_start(l, p, SPAN[h], 2 + k, at(h, a1, a2 + 1))
                w_start(l, p, SPAN[h], 2 + k, at(h, a1, a2 + NX - 1))
                if k == 2:
                    to_partner(l, h, k, 0, SPAN[h])

    @scoped
    def p4(l, ks):
        for k in ks:
            w_take(l, 2 + k, 2)
            for h in range(2):
                a1, a2 = where_am_i(h)
                w_start(l, slot(h, a1 + k, a2 + NX - 1), from_minus(h, k), 6 + k, at(h, a1, a2 + 1))
                w_start(l, slot(h, a1 + k, a2 + 1), from_plus(h, k), 6 + k, at(h, a1, a2 + NX - 1))
                to_partner(l, h, k, NX - 1, SPAN[h])
                to_partner(l, h, k, 1, SPAN[h])

    @scoped
    def p5(l, ks):
        for k in ks:
            w_take(l, 6 + k, 1)
            for h in range(2):
                to_partner(l, h, k, 2, SPAN[h])

    @scoped
    def w_done(l, gs):
        for g in gs:
            take(w_all.at[l, 1 - core, pl.ds(0, len(ARRIVALS[g]))], d_recv.at[l, g])

    def h_start(l, first, size, peers):
        for i in peers:
            ref = h_all.at[l, mz, :, pl.ds(first, size)]
            remote(ref, ref, h_send.at[l], h_recv.at[l], z_peer(i)).start()

    @scoped
    def h_wait(l):
        if nz > 1:
            take(h_all.at[l, pl.ds(0, nz - 1)], h_recv.at[l])
        for i in range(nz):
            hres[pl.ds(i * seq_dev, seq_dev)] = h_all[l, i].astype(F32)

    @scoped
    def norm_to_zb(l, gains, residual=False):
        gain = gains[...].astype(F32)[l:l + 1]
        step = min(16, rows)
        for first in range(0, rows, step):
            r = pl.ds(first, step)
            x = hres[r]
            if residual:
                x = (x + acc[r]).astype(BF16).astype(F32)
                hres[r] = x
            inv = lax.rsqrt(jnp.mean(x * x, axis=-1, keepdims=True) + NORM_EPS)
            zb[r] = (x * inv * gain).astype(BF16)

    lane = lax.broadcasted_iota(jnp.int32, (rows, LANES), 1)
    low_half = lane < hd

    def rotate(x, cos, sin):
        first = (lane[:x.shape[0]] % hd) < hd // 2
        swapped = jnp.where(first, pltpu.roll(x, LANES - hd // 2, 1), pltpu.roll(x, hd // 2, 1))
        return x * cos + swapped * sin

    def rope_tables():
        first = (lane % hd) < hd // 2
        t = rope[...]
        cos_t[...] = jnp.where(first, t, pltpu.roll(t, hd // 2, 1))
        sin_t[...] = jnp.where(first, -pltpu.roll(t, LANES - hd // 2, 1), t)

    def kv_copy(l, device):
        ref = kv_all.at[l, core, mp]
        return remote(ref, ref, kv_send.at[l], kv_recv.at[l], device)

    def kv_start(l):
        for d in far_plane if l else ((0, 2), (0, 1), (0, 3)):
            kv_copy(l, plane_peer(*d)).start()

    @scoped
    def kv_row(l):
        take(kv_all.at[l, core, pl.ds(0, NX - 1)], kv_recv.at[l])
        ref = kv_all.at[l, core, pl.ds(py * NX, NX)]
        for dy in (2, 1, 3):
            remote(ref, ref, kv_send.at[l], kvr_recv.at[0], plane_peer(dy, 0)).start()

    @scoped
    def kv_first(l):
        qkv_wait(l)
        kv = lax.dot_general(zb[...], wqkv[l, pl.ds(hq, 2 * hd), :], NT, preferred_element_type=F32)
        kv_all[l, core, mp] = jnp.where(low_half, rotate(kv, cos_t[...], sin_t[...]), kv).astype(BF16)
        kv_start(l)

    def kv_own(l):
        return kv_all.at[l, core, mp, pl.ds(pl.multiple_of(mz * seq_dev, seq_dev), seq_dev)]

    @scoped
    def kv_heads(l):
        ref = wkv.at[l - 1]
        pltpu.make_async_copy(ref, ref, local_sem.at[l, 3]).wait()
        x = h_all[l, mz].astype(F32)
        inv = lax.rsqrt(jnp.mean(x * x, axis=-1, keepdims=True) + NORM_EPS)
        z = x * inv * ga[...].astype(F32)[l:l + 1]
        z = jnp.concatenate([z, z], axis=0).astype(BF16)
        kv = lax.dot_general(z, wkv[l - 1], NT, preferred_element_type=F32)[:seq_dev]
        mine = pl.ds(pl.multiple_of(mz * seq_dev, seq_dev), seq_dev)
        for head in range(nz):
            part = kv[:, head * LANES:(head + 1) * LANES]
            kv_rows[l - 1, head] = jnp.where(low_half[:seq_dev], rotate(part, cos_t[mine], sin_t[mine]), part).astype(BF16)
        pltpu.make_async_copy(kv_rows.at[l - 1, mz], kv_own(l), local_sem.at[l, 0]).start()
        for i in far_z:
            remote(kv_rows.at[l - 1, (mz + i) % nz], kv_own(l), kva_send.at[l - 1], kva_recv.at[l - 1], z_peer(i)).start()

    @scoped
    def kv_heads_wait(l):
        pltpu.make_async_copy(kv_rows.at[l - 1, mz], kv_own(l), local_sem.at[l, 0]).wait()
        if nz > 1:
            take(kv_rows.at[l - 1, pl.ds(0, nz - 1)], kva_recv.at[l - 1])
        kv_start(l)

    @scoped
    def q_first(l):
        if l:
            qkv_wait(l)
        proj = lax.dot_general(zb[...], wqkv[l, pl.ds(0, hq), :], NT, preferred_element_type=F32)
        for j in range(hq // LANES):
            q = rotate(proj[:, j * LANES:(j + 1) * LANES], cos_t[...], sin_t[...]) * (hd ** -0.5)
            for half_head, x in enumerate((q, pltpu.roll(q, LANES - hd, 1))):
                head = 2 * j + half_head
                qbuf[pl.ds(head * rows, rows)] = jnp.where(low_half, x, 0.0).astype(BF16)

    @scoped
    def kv_wait(l):
        if l:
            take(kv_all.at[l, core, pl.ds(0, PLANE - 1)], kv_recv.at[l])
        else:
            take(kv_all.at[l, core, pl.ds(0, PLANE - NX)], kvr_recv.at[0])
        ref = kv_all.at[l, core]
        remote(ref, ref, kvd_send.at[l], kvd_recv.at[l], partner).start()
        take(kv_all.at[l, 1 - core], kvd_recv.at[l])

    def c_columns(z):
        return pl.ds(pl.multiple_of(z * hq, hq), hq)

    @scoped
    def attention(l):
        keys = 2 * PLANE * rows
        j = lax.broadcasted_iota(jnp.int32, (1, keys), 1)
        key_pos = ((j // seq_dev) % nz) * (2 * PLANE * seq_dev) + ((j // rows) % PLANE) * (2 * seq_dev) \
            + (j // (PLANE * rows)) * seq_dev + j % seq_dev
        i = lax.broadcasted_iota(jnp.int32, (2 * rows, 1), 0) % rows
        q_pos = (i // seq_dev) * (2 * PLANE * seq_dev) + (mp * 2 + core) * seq_dev + i % seq_dev
        allowed = key_pos <= jnp.minimum(q_pos, len_s[0] - 1)
        kv = kv_all[l].reshape(keys, LANES)
        for pair in range(hq // LANES):
            s = lax.dot_general(qbuf[pl.ds(2 * pair * rows, 2 * rows)], kv, NT, preferred_element_type=F32)
            s = jnp.where(allowed, s, -1e30)
            e = jnp.exp(s - jnp.max(s, axis=-1, keepdims=True))
            p = (e * (1.0 / jnp.sum(e, axis=-1, keepdims=True))).astype(BF16)
            o = jnp.dot(p, kv, preferred_element_type=F32)
            cols = pl.ds(pl.multiple_of(mz * hq + pair * LANES, LANES), LANES)
            c_mat[l, :, cols] = jnp.where(low_half, pltpu.roll(o[:rows], LANES - hd, 1), o[rows:]).astype(BF16)
            ref = c_mat.at[l, :, cols]
            for i in far_z:
                remote(ref, ref, c_send.at[l], c_recv.at[l, int(i in next_z)], z_peer(i)).start()

    @scoped
    def out_proj(l):
        with jax.named_scope('wo_wait'):
            wo_copy(l).wait()
        for i in [0] + far_z:
            if i and i in (far_z[0], far_z[-len(next_z)]):
                near = i in next_z
                n = len(next_z) if near else nz - 1 - len(next_z)
                with jax.named_scope('c_wait'):
                    take(c_mat.at[l, :, pl.ds(0, n * hq)], c_recv.at[l, int(near)])
            cols = c_columns((mz + nz - i) % nz)
            part = jnp.dot(c_mat[l, :, cols], wo_v[l, cols, :], preferred_element_type=F32)
            acc[...] = acc[...] + part if i else part

    group = CHUNK // units
    n_groups = len(GROUPS)
    assert group == 2 * len(GROUPS[0])

    def slab(l, places, first, cols):
        parts = [w_all[l, c, slot(0, px + dx, py + dy), pl.ds(first, units), cols] for dx, dy in places for c in range(2)]
        return jnp.concatenate(parts, axis=0)

    block = lax.broadcasted_iota(jnp.int32, (rows, CHUNK), 1) // units
    every = pl.ds(0, d_model)

    def units_of(l, places):
        gate = lax.dot_general(zb[...], slab(l, places, 0, every), NT, preferred_element_type=F32)
        up = lax.dot_general(zb[...], slab(l, places, units, every), NT, preferred_element_type=F32)
        return gate * (1.0 / (1.0 + jnp.exp(-gate))) * up

    def spread(g, act, blocks):
        for b in blocks:
            bd[g, pl.ds(b * rows, rows)] = jnp.where(block == b, act, 0.0).astype(BF16)

    @scoped
    def mlp_units(l, gs):
        for g in gs:
            spread(g, units_of(l, GROUPS[g]), range(group))

    @scoped
    def mlp_units_but_last(l, g):
        places = GROUPS[g][:-1] + GROUPS[g][:1]
        spread(g, units_of(l, places), range(group - 2))

    @scoped
    def mlp_units_last(l, g):
        act = units_of(l, GROUPS[g][-2:])
        spread(g, jnp.concatenate([jnp.zeros_like(act), act], axis=1), range(group - 2, group))

    two_step = nz == 8
    wide = min(2 * CHUNK, d_model)
    n_sums = d_model // wide

    def ps_of(l, n, i):
        return ps.at[l, n, (mz + i + nz) % nz]

    def rs_start(l, n):
        if not two_step:
            for k, i in enumerate(far_z):
                remote(ps_of(l, n, i), rs.at[l, n, k], rs_send.at[l], rs_recv.at[l, n], z_peer(i)).start()
            return
        for side, to in ((0, nz - 2), (1, 2)):
            cols = pl.ds(side * (wide // 2), wide // 2)
            remote(ps.at[l, n, (mz + 4) % nz, :, cols], ra.at[l, n, 2, :, cols], rs_send.at[l], ra_recv.at[l, n], z_peer(to)).start()
        for side, to in ((0, -1), (1, 1)):
            remote(ps_of(l, n, 3 * to), ra.at[l, n, side], rs_send.at[l], ra_recv.at[l, n], z_peer(nz + to)).start()

    @scoped
    def rs_middle(l):
        if not two_step:
            return
        for n in range(n_sums):
            for side, to in ((0, -1), (1, 1)):
                remote(ps_of(l, n, to), rs.at[l, n, side], rs_send.at[l], rs_recv.at[l, n], z_peer(nz + to)).start()

        @pl.loop(0, n_sums)
        def _(n):
            take(ra.at[l, n], ra_recv.at[l, n])
            for side, to in ((0, -2), (1, 2)):
                cols = pl.ds(side * (wide // 2), wide // 2)
                sb[l, n, side] = ps[l, n, (mz + nz + to) % nz] + ra[l, n, side]
                sb[l, n, side, :, cols] = sb[l, n, side, :, cols] + ra[l, n, 2, :, cols]
                remote(sb.at[l, n, side], rs.at[l, n, 2 + side], rs_send.at[l], rs_recv.at[l, n], z_peer(nz + to)).start()

    def down(l, n, gs):
        cols = pl.ds(pl.multiple_of(n * wide, wide), wide)
        total = jnp.zeros((rows, wide), F32)
        for g in gs:
            y = jnp.dot(bd[g], slab(l, GROUPS[g], 2 * units, cols), preferred_element_type=F32)
            y = y.astype(BF16).astype(F32)
            for b in range(group):
                total = total + y[b * rows:(b + 1) * rows]
        return total

    @scoped
    def mlp_down(l):
        @pl.loop(0, n_sums)
        def _(n):
            ps[l, n] = down(l, n, range(n_groups)).reshape(nz, seq_dev, wide)
            rs_start(l, n)

    n_in = 4 if two_step else nz - 1

    @scoped
    def rs_finish(l, store):
        mine = pl.ds(pl.multiple_of(mz * seq_dev, seq_dev), seq_dev)
        for n in range(n_sums):
            if n_in:
                take(rs.at[l, n], rs_recv.at[l, n])
            total = ps[l, n, mz]
            for k in range(n_in):
                total = total + rs[l, n, k]
            store(n, (hres[mine, n * wide:(n + 1) * wide] + total).astype(BF16))

    def store_next(l):
        def store(n, x):
            h_all[l + 1, mz, :, n * wide:(n + 1) * wide] = x
        return store

    with jax.named_scope('barrier'):
        pl.semaphore_wait(barrier, 1 + len(next_devices))
    round_start(0)
    p1(0)
    p3(0, (0,))
    with jax.named_scope('rounds'):
        small[0].wait()
        for r in range(4):
            if r:
                round_wait(r - 1)
                if r < 3:
                    round_start(r)
            h_start(0, 0, d_model, [i for i in far_z if min(i, nz - i) == r + 1])
    start_later_copies()
    with jax.named_scope('small'):
        for c in small[1:]:
            c.wait()
        rope_tables()
    p2(0)
    for l in range(layers):
        more = l + 1 < layers
        if l:
            p4(l, (0,))
            kv_heads(l)
            h_start(l, 0, d_model, far_z)
            kv_heads_wait(l)
            p3(l, (2,))
            p4(l, (1, 3))
        h_wait(l)
        norm_to_zb(l, ga)
        if l == 0:
            kv_first(l)
            p3(l, (1,))
            q_first(l)
            kv_row(l)
            p3(l, (3, 2))
            p4(l, (0,))
        else:
            q_first(l)
        kv_wait(l)
        attention(l)
        if l == 0:
            p4(0, (1, 3, 2))
            p5(0, (0,))
        else:
            p5(l, (0,))
            p4(l, (2,))
            p5(l, (1, 3, 2))
        if more:
            p1(l + 1)
            p3(l + 1, (0,))
        out_proj(l)
        norm_to_zb(l, gm, True)
        if l == 0:
            w_done(l, (0,))
            mlp_units(l, (0,))
            w_done(l, (1,))
            mlp_units(l, (1,))
            p5(l, (1, 3))
            w_done(l, (2,))
            mlp_units(l, (2,))
            p5(l, (2,))
            w_done(l, (3,))
            mlp_units_but_last(l, 3)
            w_done(l, (4,))
            mlp_units_last(l, 3)
        else:
            for g in range(n_groups):
                w_done(l, (g,) if g + 1 < n_groups else (g, g + 1))
                mlp_units(l, (g,))
        mlp_down(l)
        if more:
            p2(l + 1)
            p3(l + 1, (1, 3))
        rs_middle(l)
        if more:
            rs_finish(l, store_next(l))
    pieces = []
    rs_finish(layers - 1, lambda n, x: pieces.append(x.astype(F32)))
    x = jnp.concatenate(pieces, axis=1)
    inv = lax.rsqrt(jnp.mean(x * x, axis=-1, keepdims=True) + NORM_EPS)
    gain = gf[...].astype(F32)
    for i in range(d_model // LANES):
        cols = slice(i * LANES, (i + 1) * LANES)
        out_ref[:, cols] = x[:, cols] * inv * gain[i:i + 1]

    with jax.named_scope('drain'):
      for l in range(layers):
          ref = w_all.at[l, 0, pl.ds(0, PLANE - 1)]
          remote(ref, ref, w_send.at[l], w_recv.at[l, 0], me).wait_send()
          ref = w_all.at[l, 0]
          remote(ref, ref, d_send.at[l], d_recv.at[l, 0], me).wait_send()
          ref = kv_all.at[l, 0, pl.ds(0, PLANE - 1)]
          remote(ref, ref, kv_send.at[l], kv_recv.at[l], me).wait_send()
          ref = kv_all.at[l, 0]
          remote(ref, ref, kvd_send.at[l], kvd_recv.at[l], me).wait_send()
          if nz > 1 and l:
              ref = kv_rows.at[l - 1, pl.ds(0, nz - 1)]
              remote(ref, ref, kva_send.at[l - 1], kva_recv.at[l - 1], me).wait_send()
          if nz > 1:
              ref = h_all.at[l, pl.ds(0, nz - 1)]
              remote(ref, ref, h_send.at[l], h_recv.at[l], me).wait_send()
              ref = c_mat.at[l, :, pl.ds(0, (nz - 1) * hq)]
              remote(ref, ref, c_send.at[l], c_recv.at[l, 0], me).wait_send()
              ref = ps.at[l, :, pl.ds(0, nz - 1)]
              remote(ref, ref, rs_send.at[l], rs_recv.at[l, 0], me).wait_send()


def solution(mesh):
    nz = mesh.shape['tp'] // (2 * PLANE)

    def device_fn(hidden_in, lengths, attn_norm, w_query, w_key, w_value, w_out, mlp_norm, w_gate, w_up, w_down, final_norm):
        seq_dev, d_model = hidden_in.shape[1:]
        layers, _, heads, hd = w_query.shape
        kv_heads = w_key.shape[2]
        units = w_gate.shape[2]
        assert kv_heads == nz and 2 * hd == LANES and heads % nz == 0
        hq = heads // nz * hd
        rows = nz * seq_dev
        wide = min(2 * CHUNK, d_model)
        n_sums = d_model // wide
        n_groups = 2 * PLANE * units // CHUNK
        dev, row = np.arange(2 * PLANE)[:, None], np.arange(rows)[None, :]
        pos = (row // seq_dev) * (2 * PLANE * seq_dev) + dev * seq_dev + row % seq_dev
        freq = np.float32(ROPE_BASE) ** (np.float32(-2.0) * np.arange(hd // 2, dtype=np.float32) / np.float32(hd))
        angles = (pos[..., None].astype(np.float32) * freq).astype(np.float64)
        rope = np.tile(np.concatenate([np.cos(angles), np.sin(angles)], axis=-1), (1, 1, 2)).astype(np.float32)
        by_rows = lambda w: jnp.transpose(w, (0, 2, 3, 1)).reshape(layers, -1, d_model)
        units_first = lambda w: jnp.transpose(w, (0, 2, 1))
        pinned = lambda x: pltpu.with_memory_space_constraint(x, pltpu.HBM)
        hbm, vmem = (pl.BlockSpec(memory_space=s) for s in (pltpu.HBM, pltpu.VMEM))
        dma = pltpu.SemaphoreType.DMA
        out = pl.pallas_call(
            functools.partial(kernel, nz),
            name='decoder',
            out_shape=pltpu.VMEM((seq_dev, d_model), F32),
            in_specs=[hbm] * 13,
            out_specs=vmem,
            scratch_shapes=[
                pltpu.VMEM((layers, 2, PLANE, 3 * units, d_model), BF16),
                pltpu.VMEM((layers, heads * hd, d_model), BF16),
                pltpu.VMEM((layers, hq + 2 * hd, d_model), BF16),
                pltpu.VMEM((layers - 1, kv_heads * 2 * hd, d_model), BF16),
                pltpu.VMEM((layers - 1, kv_heads, seq_dev, LANES), BF16),
                pltpu.VMEM((layers, nz, seq_dev, d_model), BF16),
                pltpu.VMEM((layers, rows, heads * hd), BF16),
                pltpu.VMEM((layers, 2, PLANE, rows, LANES), BF16),
                pltpu.VMEM((layers, n_sums, 4 if nz == 8 else max(nz - 1, 1), seq_dev, wide), F32),
                pltpu.VMEM((layers, n_sums, 3, seq_dev, wide), F32),
                pltpu.VMEM((layers, n_sums, 2, seq_dev, wide), F32),
                pltpu.VMEM((layers, n_sums, nz, seq_dev, wide), F32),
                pltpu.VMEM((rows, d_model), F32),
                pltpu.VMEM((rows, d_model), F32),
                pltpu.VMEM((rows, d_model), BF16),
                pltpu.VMEM((hq // hd * rows, LANES), BF16),
                pltpu.VMEM((n_groups, CHUNK // units * rows, CHUNK), BF16),
                pltpu.VMEM((rows, LANES), F32), pltpu.VMEM((rows, LANES), F32), pltpu.VMEM((rows, LANES), F32),
                pltpu.VMEM((layers, d_model), BF16), pltpu.VMEM((layers, d_model), BF16),
                pltpu.VMEM((d_model // LANES, LANES), BF16),
                pltpu.SMEM((1,), jnp.int32),
                dma((layers, 4)), dma((6,)), dma((layers, 10)), dma((layers,)),
                dma((layers, n_groups + 1)), dma((layers,)),
                pltpu.SemaphoreType.REGULAR((3,)),
                dma((layers,)), dma((layers,)), dma((layers,)), dma((layers,)), dma((1,)), dma((layers,)), dma((layers,)),
                dma((layers - 1,)), dma((layers - 1,)),
                dma((layers, 2)), dma((layers,)), dma((layers, n_sums)), dma((layers, n_sums)), dma((layers,)),
            ],
            compiler_params=pltpu.CompilerParams(
                collective_id=0, has_side_effects=True, vmem_limit_bytes=60_000_000),
        )(pinned(hidden_in[0]), lengths, *map(pinned, (
            jnp.asarray(rope), attn_norm, mlp_norm, final_norm.reshape(-1, LANES), by_rows(w_query), by_rows(w_key), by_rows(w_value),
            w_out.reshape(layers, heads * hd, d_model), units_first(w_gate), units_first(w_up), w_down)))
        return out.astype(BF16)[None]

    seq_part = P(None, 'tp', None)
    in_specs = (seq_part, P(), P(), P(), P(), P(), P(), P(), P(None, None, 'tp'), P(None, None, 'tp'), P(None, 'tp', None), P())
    return jax.shard_map(device_fn, mesh=mesh, in_specs=in_specs, out_specs=seq_part, check_vma=False)
```

```python
import functools

import jax
import jax.numpy as jnp
import numpy as np
from jax import lax
from jax.experimental import pallas as pl
from jax.experimental.pallas import tpu as pltpu
from jax.sharding import PartitionSpec as P

NORM_EPS = 1e-5
ROPE_BASE = 500000.0
NX = 4
PLANE = NX * NX
LANES = 128
CHUNK = 256
NT = (((1,), (1,)), ((), ()))
F32, BF16 = jnp.float32, jnp.bfloat16


def remote(src, dst, send_sem, recv_sem, device):
    return pltpu.make_async_remote_copy(
        src_ref=src, dst_ref=dst, send_sem=send_sem, recv_sem=recv_sem,
        device_id=(device,), device_id_type=pl.DeviceIdType.MESH)


def scoped(f):
    @functools.wraps(f)
    def wrapped(*args):
        with jax.named_scope(f.__name__ + ('#l=%d' % args[0])):
            return f(*args)
    return wrapped


def kernel(nz, h_ref, len_ref, rope_ref, ga_ref, gm_ref, gf_ref, wq_ref, wk_ref, wv_ref, wo_ref, wg_ref, wu_ref, wd_ref,
           out_ref, w_all, wo_v, wqkv, wkv, kv_rows, h_all, c_mat, kv_all, rs, ra, sb, ps, acc, hres, zb, qbuf, bd, rope, cos_t, sin_t, ga, gm, gf, len_s,
           local_sem, in_sem, w_recv, w_send, d_recv, d_send, rounds, h_recv, h_send, kv_recv, kv_send, kvd_recv, kvd_send, kva_recv, kva_send,
           c_recv, c_send, rs_recv, ra_recv, rs_send):
    layers = wo_ref.shape[0]
    seq_dev, d_model = h_ref.shape
    units = wg_ref.shape[1]
    pack = 3 * units
    half = pack // 2
    rows = nz * seq_dev
    hq = wq_ref.shape[1] // nz
    hd = wk_ref.shape[1] // nz
    me = lax.axis_index('tp')
    core = me % 2
    px = (me // 2) % NX
    py = (me // (2 * NX)) % NX
    mp = (me // 2) % PLANE
    mz = me // (2 * PLANE)
    base = mz * (2 * PLANE)
    partner = base + mp * 2 + (1 - core)

    def z_peer(i):
        return ((mz + i) % nz) * (2 * PLANE) + mp * 2 + core

    far_z = sorted(range(1, nz), key=lambda i: -min(i, nz - i))
    next_z = [i for i in far_z if min(i, nz - i) == 1]
    def plane_peer(dy, dx):
        return base + ((py + dy) % NX * NX + (px + dx) % NX) * 2 + core

    far_plane = sorted(((dy, dx) for dy in range(NX) for dx in range(NX) if dy or dx),
                       key=lambda d: -sum(min(i, NX - i) for i in d))

    barrier = pltpu.get_barrier_semaphore()
    next_devices = [plane_peer(0, 1), plane_peer(0, NX - 1), plane_peer(1, 0), plane_peer(NX - 1, 0)]
    next_devices += [z_peer(i) for i in next_z]

    def signal(sem, device):
        pl.semaphore_signal(sem, inc=1, device_id=(device,), device_id_type=pl.DeviceIdType.MESH)

    signal(barrier, partner)
    for d in next_devices:
        signal(barrier, d)

    def round_start(r):
        for d in next_devices:
            signal(rounds.at[r], d)

    def round_wait(r):
        pl.semaphore_wait(rounds.at[r], len(next_devices))

    def pack_copies(l):
        mine = w_all.at[l, core, mp]
        return [pltpu.make_async_copy(ref.at[l], mine.at[pl.ds(i * units, units)], local_sem.at[l, 0])
                for i, ref in enumerate((wg_ref, wu_ref, wd_ref))]

    def qkv_copies(l):
        mine = [(wq_ref, 0, hq), (wk_ref, hq, hd), (wv_ref, hq + hd, hd)]
        return [pltpu.make_async_copy(ref.at[l, pl.ds(mz * n, n)], wqkv.at[l, pl.ds(first, n)], local_sem.at[l, 1])
                for ref, first, n in (mine[:1] if l else mine)]

    def kv_weight_copies(l):
        return [pltpu.make_async_copy(ref.at[l, pl.ds(z * hd, hd)], wkv.at[l - 1, pl.ds((2 * z + i) * hd, hd)], local_sem.at[l, 3])
                for z in range(nz) for i, ref in enumerate((wk_ref, wv_ref))]

    def wo_copy(l):
        return pltpu.make_async_copy(wo_ref.at[l], wo_v.at[l], local_sem.at[l, 2])

    def take(ref, sem):
        remote(ref, ref, w_send.at[0], sem, me).wait_recv()

    def pack_wait(l):
        mine = w_all.at[l, core, mp]
        pltpu.make_async_copy(mine, mine, local_sem.at[l, 0]).wait()

    def qkv_wait(l):
        ref = wqkv.at[l, pl.ds(0, hq)] if l else wqkv.at[l]
        pltpu.make_async_copy(ref, ref, local_sem.at[l, 1]).wait()

    small = [pltpu.make_async_copy(src, dst, in_sem.at[i]) for i, (src, dst) in enumerate((
        (h_ref, h_all.at[0, mz]), (rope_ref.at[mp * 2 + core], rope), (ga_ref, ga), (gm_ref, gm), (gf_ref, gf), (len_ref, len_s)))]
    for c in pack_copies(0) + small + qkv_copies(0):
        c.start()

    def start_later_copies():
        wo_copy(0).start()
        for l in range(1, layers):
            for c in pack_copies(l) + qkv_copies(l) + kv_weight_copies(l):
                c.start()
            wo_copy(l).start()

    def slot(h, a1, a2):
        return a2 % NX * NX + a1 % NX if h == 0 else a1 % NX * NX + a2 % NX

    def where_am_i(h):
        return (px, py) if h == 0 else (py, px)

    def at(h, a1, a2):
        return base + slot(h, a1, a2) * 2 + core

    third = half // 3
    SPAN = ((0, half), (half, half))

    def from_minus(h, k):
        return (h * half, 2 * third if k == 2 else third)

    def from_plus(h, k):
        first, size = from_minus(h, k)
        return (first + size, half - size)

    def piece(l, c, p, span):
        return w_all.at[l, c, p, pl.ds(*span)]

    def w_start(l, p, span, idx, device):
        ref = piece(l, core, p, span)
        remote(ref, ref, w_send.at[l], w_recv.at[l, idx], device).start()

    def w_take(l, idx, packs):
        take(w_all.at[l, core, pl.ds(0, packs)], w_recv.at[l, idx])

    GROUPS = (((0, 0), (1, 0), (3, 0), (0, 1)), ((0, 3), (2, 0), (0, 2), (1, 1)),
              ((1, 3), (3, 1), (3, 3), (2, 1)), ((2, 3), (1, 2), (3, 2), (2, 2)))
    ARRIVALS = (*GROUPS[:-1], GROUPS[-1][:-1], GROUPS[-1][-1:])
    ARRIVAL_OF = {d: g for g, ds in enumerate(ARRIVALS) for d in ds}

    def to_partner(l, h, k1, k2, span):
        a1, a2 = where_am_i(h)
        ref = piece(l, core, slot(h, a1 + k1, a2 + k2), span)
        g = ARRIVAL_OF[(k1, k2) if h == 0 else (k2, k1)]
        remote(ref, ref, d_send.at[l], d_recv.at[l, g], partner).start()

    @scoped
    def p1(l):
        pack_wait(l)
        for h in range(2):
            a1, a2 = where_am_i(h)
            w_start(l, mp, SPAN[h], 0, at(h, a1 + 1, a2))
            w_start(l, mp, SPAN[h], 0, at(h, a1 + NX - 1, a2))
        to_partner(l, 0, 0, 0, (0, pack))

    @scoped
    def p2(l):
        w_take(l, 0, 2)
        for h in range(2):
            a1, a2 = where_am_i(h)
            w_start(l, slot(h, a1 + NX - 1, a2), from_minus(h, 0), 1, at(h, a1 + 1, a2))
            w_start(l, slot(h, a1 + 1, a2), from_plus(h, 0), 1, at(h, a1 + NX - 1, a2))
            to_partner(l, h, NX - 1, 0, SPAN[h])
            to_partner(l, h, 1, 0, SPAN[h])

    @scoped
    def p3(l, ks):
        for k in ks:
            if k == 2:
                w_take(l, 1, 1)
            for h in range(2):
                a1, a2 = where_am_i(h)
                p = slot(h, a1 + k, a2)
                w_start(l, p, SPAN[h], 2 + k, at(h, a1, a2 + 1))
                w_start(l, p, SPAN[h], 2 + k, at(h, a1, a2 + NX - 1))
                if k == 2:
                    to_partner(l, h, k, 0, SPAN[h])

    @scoped
    def p4(l, ks):
        for k in ks:
            w_take(l, 2 + k, 2)
            for h in range(2):
                a1, a2 = where_am_i(h)
                w_start(l, slot(h, a1 + k, a2 + NX - 1), from_minus(h, k), 6 + k, at(h, a1, a2 + 1))
                w_start(l, slot(h, a1 + k, a2 + 1), from_plus(h, k), 6 + k, at(h, a1, a2 + NX - 1))
                to_partner(l, h, k, NX - 1, SPAN[h])
                to_partner(l, h, k, 1, SPAN[h])

    @scoped
    def p5(l, ks):
        for k in ks:
            w_take(l, 6 + k, 1)
            for h in range(2):
                to_partner(l, h, k, 2, SPAN[h])

    @scoped
    def w_done(l, gs):
        for g in gs:
            take(w_all.at[l, 1 - core, pl.ds(0, len(ARRIVALS[g]))], d_recv.at[l, g])

    def h_start(l, first, size, peers):
        for i in peers:
            ref = h_all.at[l, mz, :, pl.ds(first, size)]
            remote(ref, ref, h_send.at[l], h_recv.at[l], z_peer(i)).start()

    @scoped
    def h_wait(l):
        if nz > 1:
            take(h_all.at[l, pl.ds(0, nz - 1)], h_recv.at[l])
        for i in range(nz):
            hres[pl.ds(i * seq_dev, seq_dev)] = h_all[l, i].astype(F32)

    @scoped
    def norm_to_zb(l, gains, residual=False):
        gain = gains[...].astype(F32)[l:l + 1]
        step = min(16, rows)
        for first in range(0, rows, step):
            r = pl.ds(first, step)
            x = hres[r]
            if residual:
                x = (x + acc[r]).astype(BF16).astype(F32)
                hres[r] = x
            inv = lax.rsqrt(jnp.mean(x * x, axis=-1, keepdims=True) + NORM_EPS)
            zb[r] = (x * inv * gain).astype(BF16)

    lane = lax.broadcasted_iota(jnp.int32, (rows, LANES), 1)
    low_half = lane < hd

    def rotate(x, cos, sin):
        first = (lane[:x.shape[0]] % hd) < hd // 2
        swapped = jnp.where(first, pltpu.roll(x, LANES - hd // 2, 1), pltpu.roll(x, hd // 2, 1))
        return x * cos + swapped * sin

    def rope_tables():
        first = (lane % hd) < hd // 2
        t = rope[...]
        cos_t[...] = jnp.where(first, t, pltpu.roll(t, hd // 2, 1))
        sin_t[...] = jnp.where(first, -pltpu.roll(t, LANES - hd // 2, 1), t)

    def kv_copy(l, device):
        ref = kv_all.at[l, core, mp]
        return remote(ref, ref, kv_send.at[l], kv_recv.at[l], device)

    def kv_start(l):
        for d in far_plane:
            kv_copy(l, plane_peer(*d)).start()

    @scoped
    def kv_first(l):
        qkv_wait(l)
        kv = lax.dot_general(zb[...], wqkv[l, pl.ds(hq, 2 * hd), :], NT, preferred_element_type=F32)
        kv_all[l, core, mp] = jnp.where(low_half, rotate(kv, cos_t[...], sin_t[...]), kv).astype(BF16)
        kv_start(l)

    def kv_own(l):
        return kv_all.at[l, core, mp, pl.ds(pl.multiple_of(mz * seq_dev, seq_dev), seq_dev)]

    @scoped
    def kv_heads(l):
        ref = wkv.at[l - 1]
        pltpu.make_async_copy(ref, ref, local_sem.at[l, 3]).wait()
        x = h_all[l, mz].astype(F32)
        inv = lax.rsqrt(jnp.mean(x * x, axis=-1, keepdims=True) + NORM_EPS)
        z = x * inv * ga[...].astype(F32)[l:l + 1]
        z = jnp.concatenate([z, z], axis=0).astype(BF16)
        kv = lax.dot_general(z, wkv[l - 1], NT, preferred_element_type=F32)[:seq_dev]
        mine = pl.ds(pl.multiple_of(mz * seq_dev, seq_dev), seq_dev)
        for head in range(nz):
            part = kv[:, head * LANES:(head + 1) * LANES]
            kv_rows[l - 1, head] = jnp.where(low_half[:seq_dev], rotate(part, cos_t[mine], sin_t[mine]), part).astype(BF16)
        pltpu.make_async_copy(kv_rows.at[l - 1, mz], kv_own(l), local_sem.at[l, 0]).start()
        for i in far_z:
            remote(kv_rows.at[l - 1, (mz + i) % nz], kv_own(l), kva_send.at[l - 1], kva_recv.at[l - 1], z_peer(i)).start()

    @scoped
    def kv_heads_wait(l):
        pltpu.make_async_copy(kv_rows.at[l - 1, mz], kv_own(l), local_sem.at[l, 0]).wait()
        if nz > 1:
            take(kv_rows.at[l - 1, pl.ds(0, nz - 1)], kva_recv.at[l - 1])
        kv_start(l)

    @scoped
    def q_first(l):
        if l:
            qkv_wait(l)
        proj = lax.dot_general(zb[...], wqkv[l, pl.ds(0, hq), :], NT, preferred_element_type=F32)
        for j in range(hq // LANES):
            q = rotate(proj[:, j * LANES:(j + 1) * LANES], cos_t[...], sin_t[...]) * (hd ** -0.5)
            for half_head, x in enumerate((q, pltpu.roll(q, LANES - hd, 1))):
                head = 2 * j + half_head
                qbuf[pl.ds(head * rows, rows)] = jnp.where(low_half, x, 0.0).astype(BF16)

    @scoped
    def kv_wait(l):
        take(kv_all.at[l, core, pl.ds(0, PLANE - 1)], kv_recv.at[l])
        ref = kv_all.at[l, core]
        remote(ref, ref, kvd_send.at[l], kvd_recv.at[l], partner).start()
        take(kv_all.at[l, 1 - core], kvd_recv.at[l])

    def c_columns(z):
        return pl.ds(pl.multiple_of(z * hq, hq), hq)

    @scoped
    def attention(l):
        keys = 2 * PLANE * rows
        j = lax.broadcasted_iota(jnp.int32, (1, keys), 1)
        key_pos = ((j // seq_dev) % nz) * (2 * PLANE * seq_dev) + ((j // rows) % PLANE) * (2 * seq_dev) \
            + (j // (PLANE * rows)) * seq_dev + j % seq_dev
        i = lax.broadcasted_iota(jnp.int32, (2 * rows, 1), 0) % rows
        q_pos = (i // seq_dev) * (2 * PLANE * seq_dev) + (mp * 2 + core) * seq_dev + i % seq_dev
        allowed = key_pos <= jnp.minimum(q_pos, len_s[0] - 1)
        kv = kv_all[l].reshape(keys, LANES)
        for pair in range(hq // LANES):
            s = lax.dot_general(qbuf[pl.ds(2 * pair * rows, 2 * rows)], kv, NT, preferred_element_type=F32)
            s = jnp.where(allowed, s, -1e30)
            e = jnp.exp(s - jnp.max(s, axis=-1, keepdims=True))
            p = (e * (1.0 / jnp.sum(e, axis=-1, keepdims=True))).astype(BF16)
            o = jnp.dot(p, kv, preferred_element_type=F32)
            cols = pl.ds(pl.multiple_of(mz * hq + pair * LANES, LANES), LANES)
            c_mat[l, :, cols] = jnp.where(low_half, pltpu.roll(o[:rows], LANES - hd, 1), o[rows:]).astype(BF16)
            ref = c_mat.at[l, :, cols]
            for i in far_z:
                remote(ref, ref, c_send.at[l], c_recv.at[l, int(i in next_z)], z_peer(i)).start()

    @scoped
    def out_proj(l):
        with jax.named_scope('wo_wait'):
            wo_copy(l).wait()
        for i in [0] + far_z:
            if i and i in (far_z[0], far_z[-len(next_z)]):
                near = i in next_z
                n = len(next_z) if near else nz - 1 - len(next_z)
                with jax.named_scope('c_wait'):
                    take(c_mat.at[l, :, pl.ds(0, n * hq)], c_recv.at[l, int(near)])
            cols = c_columns((mz + nz - i) % nz)
            part = jnp.dot(c_mat[l, :, cols], wo_v[l, cols, :], preferred_element_type=F32)
            acc[...] = acc[...] + part if i else part

    group = CHUNK // units
    n_groups = len(GROUPS)
    assert group == 2 * len(GROUPS[0])

    def slab(l, places, first, cols):
        parts = [w_all[l, c, slot(0, px + dx, py + dy), pl.ds(first, units), cols] for dx, dy in places for c in range(2)]
        return jnp.concatenate(parts, axis=0)

    block = lax.broadcasted_iota(jnp.int32, (rows, CHUNK), 1) // units
    every = pl.ds(0, d_model)

    def units_of(l, places):
        gate = lax.dot_general(zb[...], slab(l, places, 0, every), NT, preferred_element_type=F32)
        up = lax.dot_general(zb[...], slab(l, places, units, every), NT, preferred_element_type=F32)
        return gate * (1.0 / (1.0 + jnp.exp(-gate))) * up

    def spread(g, act, blocks):
        for b in blocks:
            bd[g, pl.ds(b * rows, rows)] = jnp.where(block == b, act, 0.0).astype(BF16)

    @scoped
    def mlp_units(l, gs):
        for g in gs:
            spread(g, units_of(l, GROUPS[g]), range(group))

    @scoped
    def mlp_units_but_last(l, g):
        places = GROUPS[g][:-1] + GROUPS[g][:1]
        spread(g, units_of(l, places), range(group - 2))

    @scoped
    def mlp_units_last(l, g):
        act = units_of(l, GROUPS[g][-2:])
        spread(g, jnp.concatenate([jnp.zeros_like(act), act], axis=1), range(group - 2, group))

    two_step = nz == 8
    wide = min(2 * CHUNK, d_model)
    n_sums = d_model // wide

    def ps_of(l, n, i):
        return ps.at[l, n, (mz + i + nz) % nz]

    def rs_start(l, n):
        if not two_step:
            for k, i in enumerate(far_z):
                remote(ps_of(l, n, i), rs.at[l, n, k], rs_send.at[l], rs_recv.at[l, n], z_peer(i)).start()
            return
        for side, to in ((0, nz - 2), (1, 2)):
            cols = pl.ds(side * (wide // 2), wide // 2)
            remote(ps.at[l, n, (mz + 4) % nz, :, cols], ra.at[l, n, 2, :, cols], rs_send.at[l], ra_recv.at[l, n], z_peer(to)).start()
        for side, to in ((0, -1), (1, 1)):
            remote(ps_of(l, n, 3 * to), ra.at[l, n, side], rs_send.at[l], ra_recv.at[l, n], z_peer(nz + to)).start()

    @scoped
    def rs_middle(l):
        if not two_step:
            return
        for n in range(n_sums):
            for side, to in ((0, -1), (1, 1)):
                remote(ps_of(l, n, to), rs.at[l, n, side], rs_send.at[l], rs_recv.at[l, n], z_peer(nz + to)).start()

        @pl.loop(0, n_sums)
        def _(n):
            take(ra.at[l, n], ra_recv.at[l, n])
            for side, to in ((0, -2), (1, 2)):
                cols = pl.ds(side * (wide // 2), wide // 2)
                sb[l, n, side] = ps[l, n, (mz + nz + to) % nz] + ra[l, n, side]
                sb[l, n, side, :, cols] = sb[l, n, side, :, cols] + ra[l, n, 2, :, cols]
                remote(sb.at[l, n, side], rs.at[l, n, 2 + side], rs_send.at[l], rs_recv.at[l, n], z_peer(nz + to)).start()

    def down(l, n, gs):
        cols = pl.ds(pl.multiple_of(n * wide, wide), wide)
        total = jnp.zeros((rows, wide), F32)
        for g in gs:
            y = jnp.dot(bd[g], slab(l, GROUPS[g], 2 * units, cols), preferred_element_type=F32)
            y = y.astype(BF16).astype(F32)
            for b in range(group):
                total = total + y[b * rows:(b + 1) * rows]
        return total

    @scoped
    def mlp_down(l):
        @pl.loop(0, n_sums)
        def _(n):
            ps[l, n] = down(l, n, range(n_groups)).reshape(nz, seq_dev, wide)
            rs_start(l, n)

    n_in = 4 if two_step else nz - 1

    @scoped
    def rs_finish(l, store):
        mine = pl.ds(pl.multiple_of(mz * seq_dev, seq_dev), seq_dev)
        for n in range(n_sums):
            if n_in:
                take(rs.at[l, n], rs_recv.at[l, n])
            total = ps[l, n, mz]
            for k in range(n_in):
                total = total + rs[l, n, k]
            store(n, (hres[mine, n * wide:(n + 1) * wide] + total).astype(BF16))

    def store_next(l):
        def store(n, x):
            h_all[l + 1, mz, :, n * wide:(n + 1) * wide] = x
        return store

    with jax.named_scope('barrier'):
        pl.semaphore_wait(barrier, 1 + len(next_devices))
    round_start(0)
    p1(0)
    p3(0, (0,))
    with jax.named_scope('rounds'):
        small[0].wait()
        for r in range(4):
            if r:
                round_wait(r - 1)
                if r < 3:
                    round_start(r)
            h_start(0, 0, d_model, [i for i in far_z if min(i, nz - i) == r + 1])
    start_later_copies()
    with jax.named_scope('small'):
        for c in small[1:]:
            c.wait()
        rope_tables()
    p2(0)
    for l in range(layers):
        more = l + 1 < layers
        if l:
            p4(l, (0,))
            kv_heads(l)
            h_start(l, 0, d_model, far_z)
            kv_heads_wait(l)
            p3(l, (2,))
            p4(l, (1, 3))
        h_wait(l)
        norm_to_zb(l, ga)
        if l == 0:
            kv_first(l)
            p3(l, (1, 3, 2))
            p4(l, (0,))
        q_first(l)
        kv_wait(l)
        attention(l)
        if l == 0:
            p4(0, (1, 3, 2))
            p5(0, (0,))
        else:
            p5(l, (0,))
            p4(l, (2,))
            p5(l, (1, 3, 2))
        if more:
            p1(l + 1)
            p3(l + 1, (0,))
        out_proj(l)
        norm_to_zb(l, gm, True)
        if l == 0:
            w_done(l, (0,))
            mlp_units(l, (0,))
            w_done(l, (1,))
            mlp_units(l, (1,))
            p5(l, (1, 3))
            w_done(l, (2,))
            mlp_units(l, (2,))
            p5(l, (2,))
            w_done(l, (3,))
            mlp_units_but_last(l, 3)
            w_done(l, (4,))
            mlp_units_last(l, 3)
        else:
            w_done(l, range(n_groups + 1))
            mlp_units(l, range(n_groups))
        mlp_down(l)
        if more:
            p2(l + 1)
            p3(l + 1, (1, 3))
        rs_middle(l)
        if more:
            rs_finish(l, store_next(l))
    pieces = []
    rs_finish(layers - 1, lambda n, x: pieces.append(x.astype(F32)))
    x = jnp.concatenate(pieces, axis=1)
    inv = lax.rsqrt(jnp.mean(x * x, axis=-1, keepdims=True) + NORM_EPS)
    gain = gf[...].astype(F32)
    for i in range(d_model // LANES):
        cols = slice(i * LANES, (i + 1) * LANES)
        out_ref[:, cols] = x[:, cols] * inv * gain[i:i + 1]

    with jax.named_scope('drain'):
      for l in range(layers):
          ref = w_all.at[l, 0, pl.ds(0, PLANE - 1)]
          remote(ref, ref, w_send.at[l], w_recv.at[l, 0], me).wait_send()
          ref = w_all.at[l, 0]
          remote(ref, ref, d_send.at[l], d_recv.at[l, 0], me).wait_send()
          ref = kv_all.at[l, 0, pl.ds(0, PLANE - 1)]
          remote(ref, ref, kv_send.at[l], kv_recv.at[l], me).wait_send()
          ref = kv_all.at[l, 0]
          remote(ref, ref, kvd_send.at[l], kvd_recv.at[l], me).wait_send()
          if nz > 1 and l:
              ref = kv_rows.at[l - 1, pl.ds(0, nz - 1)]
              remote(ref, ref, kva_send.at[l - 1], kva_recv.at[l - 1], me).wait_send()
          if nz > 1:
              ref = h_all.at[l, pl.ds(0, nz - 1)]
              remote(ref, ref, h_send.at[l], h_recv.at[l], me).wait_send()
              ref = c_mat.at[l, :, pl.ds(0, (nz - 1) * hq)]
              remote(ref, ref, c_send.at[l], c_recv.at[l, 0], me).wait_send()
              ref = ps.at[l, :, pl.ds(0, nz - 1)]
              remote(ref, ref, rs_send.at[l], rs_recv.at[l, 0], me).wait_send()


def solution(mesh):
    nz = mesh.shape['tp'] // (2 * PLANE)

    def device_fn(hidden_in, lengths, attn_norm, w_query, w_key, w_value, w_out, mlp_norm, w_gate, w_up, w_down, final_norm):
        seq_dev, d_model = hidden_in.shape[1:]
        layers, _, heads, hd = w_query.shape
        kv_heads = w_key.shape[2]
        units = w_gate.shape[2]
        assert kv_heads == nz and 2 * hd == LANES and heads % nz == 0
        hq = heads // nz * hd
        rows = nz * seq_dev
        wide = min(2 * CHUNK, d_model)
        n_sums = d_model // wide
        n_groups = 2 * PLANE * units // CHUNK
        dev, row = np.arange(2 * PLANE)[:, None], np.arange(rows)[None, :]
        pos = (row // seq_dev) * (2 * PLANE * seq_dev) + dev * seq_dev + row % seq_dev
        freq = np.float32(ROPE_BASE) ** (np.float32(-2.0) * np.arange(hd // 2, dtype=np.float32) / np.float32(hd))
        angles = (pos[..., None].astype(np.float32) * freq).astype(np.float64)
        rope = np.tile(np.concatenate([np.cos(angles), np.sin(angles)], axis=-1), (1, 1, 2)).astype(np.float32)
        by_rows = lambda w: jnp.transpose(w, (0, 2, 3, 1)).reshape(layers, -1, d_model)
        units_first = lambda w: jnp.transpose(w, (0, 2, 1))
        pinned = lambda x: pltpu.with_memory_space_constraint(x, pltpu.HBM)
        hbm, vmem = (pl.BlockSpec(memory_space=s) for s in (pltpu.HBM, pltpu.VMEM))
        dma = pltpu.SemaphoreType.DMA
        out = pl.pallas_call(
            functools.partial(kernel, nz),
            name='decoder',
            out_shape=pltpu.VMEM((seq_dev, d_model), F32),
            in_specs=[hbm] * 13,
            out_specs=vmem,
            scratch_shapes=[
                pltpu.VMEM((layers, 2, PLANE, 3 * units, d_model), BF16),
                pltpu.VMEM((layers, heads * hd, d_model), BF16),
                pltpu.VMEM((layers, hq + 2 * hd, d_model), BF16),
                pltpu.VMEM((layers - 1, kv_heads * 2 * hd, d_model), BF16),
                pltpu.VMEM((layers - 1, kv_heads, seq_dev, LANES), BF16),
                pltpu.VMEM((layers, nz, seq_dev, d_model), BF16),
                pltpu.VMEM((layers, rows, heads * hd), BF16),
                pltpu.VMEM((layers, 2, PLANE, rows, LANES), BF16),
                pltpu.VMEM((layers, n_sums, 4 if nz == 8 else max(nz - 1, 1), seq_dev, wide), F32),
                pltpu.VMEM((layers, n_sums, 3, seq_dev, wide), F32),
                pltpu.VMEM((layers, n_sums, 2, seq_dev, wide), F32),
                pltpu.VMEM((layers, n_sums, nz, seq_dev, wide), F32),
                pltpu.VMEM((rows, d_model), F32),
                pltpu.VMEM((rows, d_model), F32),
                pltpu.VMEM((rows, d_model), BF16),
                pltpu.VMEM((hq // hd * rows, LANES), BF16),
                pltpu.VMEM((n_groups, CHUNK // units * rows, CHUNK), BF16),
                pltpu.VMEM((rows, LANES), F32), pltpu.VMEM((rows, LANES), F32), pltpu.VMEM((rows, LANES), F32),
                pltpu.VMEM((layers, d_model), BF16), pltpu.VMEM((layers, d_model), BF16),
                pltpu.VMEM((d_model // LANES, LANES), BF16),
                pltpu.SMEM((1,), jnp.int32),
                dma((layers, 4)), dma((6,)), dma((layers, 10)), dma((layers,)),
                dma((layers, n_groups + 1)), dma((layers,)),
                pltpu.SemaphoreType.REGULAR((3,)),
                dma((layers,)), dma((layers,)), dma((layers,)), dma((layers,)), dma((layers,)), dma((layers,)),
                dma((layers - 1,)), dma((layers - 1,)),
                dma((layers, 2)), dma((layers,)), dma((layers, n_sums)), dma((layers, n_sums)), dma((layers,)),
            ],
            compiler_params=pltpu.CompilerParams(
                collective_id=0, has_side_effects=True, vmem_limit_bytes=60_000_000),
        )(pinned(hidden_in[0]), lengths, *map(pinned, (
            jnp.asarray(rope), attn_norm, mlp_norm, final_norm.reshape(-1, LANES), by_rows(w_query), by_rows(w_key), by_rows(w_value),
            w_out.reshape(layers, heads * hd, d_model), units_first(w_gate), units_first(w_up), w_down)))
        return out.astype(BF16)[None]

    seq_part = P(None, 'tp', None)
    in_specs = (seq_part, P(), P(), P(), P(), P(), P(), P(), P(None, None, 'tp'), P(None, None, 'tp'), P(None, 'tp', None), P())
    return jax.shard_map(device_fn, mesh=mesh, in_specs=in_specs, out_specs=seq_part, check_vma=False)
```

```python
import functools

import jax
import jax.numpy as jnp
import numpy as np
from jax import lax
from jax.experimental import pallas as pl
from jax.experimental.pallas import tpu as pltpu
from jax.sharding import PartitionSpec as P

NORM_EPS = 1e-5
ROPE_BASE = 500000.0
NX = 4
PLANE = NX * NX
LANES = 128
CHUNK = 256
NT = (((1,), (1,)), ((), ()))
F32, BF16 = jnp.float32, jnp.bfloat16


def remote(src, dst, send_sem, recv_sem, device):
    return pltpu.make_async_remote_copy(
        src_ref=src, dst_ref=dst, send_sem=send_sem, recv_sem=recv_sem,
        device_id=(device,), device_id_type=pl.DeviceIdType.MESH)


def scoped(f):
    @functools.wraps(f)
    def wrapped(*args):
        with jax.named_scope(f.__name__ + ('#l=%d' % args[0])):
            return f(*args)
    return wrapped


def kernel(nz, h_ref, len_ref, rope_ref, ga_ref, gm_ref, gf_ref, wq_ref, wk_ref, wv_ref, wo_ref, wg_ref, wu_ref, wd_ref,
           out_ref, w_all, wo_v, wqkv, wkv, kv_rows, h_all, c_mat, kv_all, rs, ra, sb, ps, acc, hres, zb, qbuf, bd, rope, cos_t, sin_t, ga, gm, gf, len_s,
           local_sem, in_sem, w_recv, w_send, d_recv, d_send, rounds, h_recv, h_send, kv_recv, kv_send, kvd_recv, kvd_send, kva_recv, kva_send,
           c_recv, c_send, rs_recv, ra_recv, rs_send):
    layers = wo_ref.shape[0]
    seq_dev, d_model = h_ref.shape
    units = wg_ref.shape[1]
    pack = 3 * units
    half = pack // 2
    rows = nz * seq_dev
    hq = wq_ref.shape[1] // nz
    hd = wk_ref.shape[1] // nz
    me = lax.axis_index('tp')
    core = me % 2
    px = (me // 2) % NX
    py = (me // (2 * NX)) % NX
    mp = (me // 2) % PLANE
    mz = me // (2 * PLANE)
    base = mz * (2 * PLANE)
    partner = base + mp * 2 + (1 - core)

    def z_peer(i):
        return ((mz + i) % nz) * (2 * PLANE) + mp * 2 + core

    far_z = sorted(range(1, nz), key=lambda i: -min(i, nz - i))
    next_z = [i for i in far_z if min(i, nz - i) == 1]
    def plane_peer(dy, dx):
        return base + ((py + dy) % NX * NX + (px + dx) % NX) * 2 + core

    far_plane = sorted(((dy, dx) for dy in range(NX) for dx in range(NX) if dy or dx),
                       key=lambda d: -sum(min(i, NX - i) for i in d))

    barrier = pltpu.get_barrier_semaphore()
    next_devices = [plane_peer(0, 1), plane_peer(0, NX - 1), plane_peer(1, 0), plane_peer(NX - 1, 0)]
    next_devices += [z_peer(i) for i in next_z]

    def signal(sem, device):
        pl.semaphore_signal(sem, inc=1, device_id=(device,), device_id_type=pl.DeviceIdType.MESH)

    signal(barrier, partner)
    for d in next_devices:
        signal(barrier, d)

    def round_start(r):
        for d in next_devices:
            signal(rounds.at[r], d)

    def round_wait(r):
        pl.semaphore_wait(rounds.at[r], len(next_devices))

    def pack_copies(l):
        mine = w_all.at[l, core, mp]
        return [pltpu.make_async_copy(ref.at[l], mine.at[pl.ds(i * units, units)], local_sem.at[l, 0])
                for i, ref in enumerate((wg_ref, wu_ref, wd_ref))]

    def qkv_copies(l):
        mine = [(wq_ref, 0, hq), (wk_ref, hq, hd), (wv_ref, hq + hd, hd)]
        return [pltpu.make_async_copy(ref.at[l, pl.ds(mz * n, n)], wqkv.at[l, pl.ds(first, n)], local_sem.at[l, 1])
                for ref, first, n in (mine[:1] if l else mine)]

    def kv_weight_copies(l):
        return [pltpu.make_async_copy(ref.at[l, pl.ds(z * hd, hd)], wkv.at[l - 1, pl.ds((2 * z + i) * hd, hd)], local_sem.at[l, 3])
                for z in range(nz) for i, ref in enumerate((wk_ref, wv_ref))]

    def wo_copy(l):
        return pltpu.make_async_copy(wo_ref.at[l], wo_v.at[l], local_sem.at[l, 2])

    def take(ref, sem):
        remote(ref, ref, w_send.at[0], sem, me).wait_recv()

    def pack_wait(l):
        mine = w_all.at[l, core, mp]
        pltpu.make_async_copy(mine, mine, local_sem.at[l, 0]).wait()

    def qkv_wait(l):
        ref = wqkv.at[l, pl.ds(0, hq)] if l else wqkv.at[l]
        pltpu.make_async_copy(ref, ref, local_sem.at[l, 1]).wait()

    small = [pltpu.make_async_copy(src, dst, in_sem.at[i]) for i, (src, dst) in enumerate((
        (h_ref, h_all.at[0, mz]), (rope_ref.at[mp * 2 + core], rope), (ga_ref, ga), (gm_ref, gm), (gf_ref, gf), (len_ref, len_s)))]
    for c in pack_copies(0) + small + qkv_copies(0):
        c.start()

    def start_later_copies():
        wo_copy(0).start()
        for l in range(1, layers):
            for c in pack_copies(l) + qkv_copies(l) + kv_weight_copies(l):
                c.start()
            wo_copy(l).start()

    def slot(h, a1, a2):
        return a2 % NX * NX + a1 % NX if h == 0 else a1 % NX * NX + a2 % NX

    def where_am_i(h):
        return (px, py) if h == 0 else (py, px)

    def at(h, a1, a2):
        return base + slot(h, a1, a2) * 2 + core

    third = half // 3
    SPAN = ((0, half), (half, half))

    def from_minus(h, k):
        return (h * half, third if k == 2 else 2 * third)

    def from_plus(h, k):
        first, size = from_minus(h, k)
        return (first + size, half - size)

    def piece(l, c, p, span):
        return w_all.at[l, c, p, pl.ds(*span)]

    def w_start(l, p, span, idx, device):
        ref = piece(l, core, p, span)
        remote(ref, ref, w_send.at[l], w_recv.at[l, idx], device).start()

    def w_take(l, idx, packs):
        take(w_all.at[l, core, pl.ds(0, packs)], w_recv.at[l, idx])

    GROUPS = (((0, 0), (1, 0), (3, 0), (0, 1)), ((0, 3), (2, 0), (0, 2), (1, 1)),
              ((1, 3), (3, 1), (3, 3), (2, 1)), ((2, 3), (1, 2), (3, 2), (2, 2)))
    ARRIVALS = (*GROUPS[:-1], GROUPS[-1][:-1], GROUPS[-1][-1:])
    ARRIVAL_OF = {d: g for g, ds in enumerate(ARRIVALS) for d in ds}

    def to_partner(l, h, k1, k2, span):
        a1, a2 = where_am_i(h)
        ref = piece(l, core, slot(h, a1 + k1, a2 + k2), span)
        g = ARRIVAL_OF[(k1, k2) if h == 0 else (k2, k1)]
        remote(ref, ref, d_send.at[l], d_recv.at[l, g], partner).start()

    @scoped
    def p1(l):
        pack_wait(l)
        for h in range(2):
            a1, a2 = where_am_i(h)
            w_start(l, mp, SPAN[h], 0, at(h, a1 + 1, a2))
            w_start(l, mp, SPAN[h], 0, at(h, a1 + NX - 1, a2))
        to_partner(l, 0, 0, 0, (0, pack))

    @scoped
    def p2(l):
        w_take(l, 0, 2)
        for h in range(2):
            a1, a2 = where_am_i(h)
            w_start(l, slot(h, a1 + NX - 1, a2), from_minus(h, 0), 1, at(h, a1 + 1, a2))
            w_start(l, slot(h, a1 + 1, a2), from_plus(h, 0), 1, at(h, a1 + NX - 1, a2))
            to_partner(l, h, NX - 1, 0, SPAN[h])
            to_partner(l, h, 1, 0, SPAN[h])

    @scoped
    def p3(l, ks):
        for k in ks:
            if k == 2:
                w_take(l, 1, 1)
            for h in range(2):
                a1, a2 = where_am_i(h)
                p = slot(h, a1 + k, a2)
                w_start(l, p, SPAN[h], 2 + k, at(h, a1, a2 + 1))
                w_start(l, p, SPAN[h], 2 + k, at(h, a1, a2 + NX - 1))
                if k == 2:
                    to_partner(l, h, k, 0, SPAN[h])

    @scoped
    def p4(l, ks):
        for k in ks:
            w_take(l, 2 + k, 2)
            for h in range(2):
                a1, a2 = where_am_i(h)
                w_start(l, slot(h, a1 + k, a2 + NX - 1), from_minus(h, k), 6 + k, at(h, a1, a2 + 1))
                w_start(l, slot(h, a1 + k, a2 + 1), from_plus(h, k), 6 + k, at(h, a1, a2 + NX - 1))
                to_partner(l, h, k, NX - 1, SPAN[h])
                to_partner(l, h, k, 1, SPAN[h])

    @scoped
    def p5(l, ks):
        for k in ks:
            w_take(l, 6 + k, 1)
            for h in range(2):
                to_partner(l, h, k, 2, SPAN[h])

    @scoped
    def w_done(l, gs):
        for g in gs:
            take(w_all.at[l, 1 - core, pl.ds(0, len(ARRIVALS[g]))], d_recv.at[l, g])

    def h_start(l, first, size, peers):
        for i in peers:
            ref = h_all.at[l, mz, :, pl.ds(first, size)]
            remote(ref, ref, h_send.at[l], h_recv.at[l], z_peer(i)).start()

    @scoped
    def h_wait(l):
        if nz > 1:
            take(h_all.at[l, pl.ds(0, nz - 1)], h_recv.at[l])
        for i in range(nz):
            hres[pl.ds(i * seq_dev, seq_dev)] = h_all[l, i].astype(F32)

    @scoped
    def norm_to_zb(l, gains, residual=False):
        gain = gains[...].astype(F32)[l:l + 1]
        step = min(16, rows)
        for first in range(0, rows, step):
            r = pl.ds(first, step)
            x = hres[r]
            if residual:
                x = (x + acc[r]).astype(BF16).astype(F32)
                hres[r] = x
            inv = lax.rsqrt(jnp.mean(x * x, axis=-1, keepdims=True) + NORM_EPS)
            zb[r] = (x * inv * gain).astype(BF16)

    lane = lax.broadcasted_iota(jnp.int32, (rows, LANES), 1)
    low_half = lane < hd

    def rotate(x, cos, sin):
        first = (lane[:x.shape[0]] % hd) < hd // 2
        swapped = jnp.where(first, pltpu.roll(x, LANES - hd // 2, 1), pltpu.roll(x, hd // 2, 1))
        return x * cos + swapped * sin

    def rope_tables():
        first = (lane % hd) < hd // 2
        t = rope[...]
        cos_t[...] = jnp.where(first, t, pltpu.roll(t, hd // 2, 1))
        sin_t[...] = jnp.where(first, -pltpu.roll(t, LANES - hd // 2, 1), t)

    def kv_copy(l, device):
        ref = kv_all.at[l, core, mp]
        return remote(ref, ref, kv_send.at[l], kv_recv.at[l], device)

    def kv_start(l):
        for d in far_plane:
            kv_copy(l, plane_peer(*d)).start()

    @scoped
    def kv_first(l):
        qkv_wait(l)
        kv = lax.dot_general(zb[...], wqkv[l, pl.ds(hq, 2 * hd), :], NT, preferred_element_type=F32)
        kv_all[l, core, mp] = jnp.where(low_half, rotate(kv, cos_t[...], sin_t[...]), kv).astype(BF16)
        kv_start(l)

    def kv_own(l):
        return kv_all.at[l, core, mp, pl.ds(pl.multiple_of(mz * seq_dev, seq_dev), seq_dev)]

    @scoped
    def kv_heads(l):
        ref = wkv.at[l - 1]
        pltpu.make_async_copy(ref, ref, local_sem.at[l, 3]).wait()
        x = h_all[l, mz].astype(F32)
        inv = lax.rsqrt(jnp.mean(x * x, axis=-1, keepdims=True) + NORM_EPS)
        z = x * inv * ga[...].astype(F32)[l:l + 1]
        z = jnp.concatenate([z, z], axis=0).astype(BF16)
        kv = lax.dot_general(z, wkv[l - 1], NT, preferred_element_type=F32)[:seq_dev]
        mine = pl.ds(pl.multiple_of(mz * seq_dev, seq_dev), seq_dev)
        for head in range(nz):
            part = kv[:, head * LANES:(head + 1) * LANES]
            kv_rows[l - 1, head] = jnp.where(low_half[:seq_dev], rotate(part, cos_t[mine], sin_t[mine]), part).astype(BF16)
        pltpu.make_async_copy(kv_rows.at[l - 1, mz], kv_own(l), local_sem.at[l, 0]).start()
        for i in far_z:
            remote(kv_rows.at[l - 1, (mz + i) % nz], kv_own(l), kva_send.at[l - 1], kva_recv.at[l - 1], z_peer(i)).start()

    @scoped
    def kv_heads_wait(l):
        pltpu.make_async_copy(kv_rows.at[l - 1, mz], kv_own(l), local_sem.at[l, 0]).wait()
        if nz > 1:
            take(kv_rows.at[l - 1, pl.ds(0, nz - 1)], kva_recv.at[l - 1])
        kv_start(l)

    @scoped
    def q_first(l):
        if l:
            qkv_wait(l)
        proj = lax.dot_general(zb[...], wqkv[l, pl.ds(0, hq), :], NT, preferred_element_type=F32)
        for j in range(hq // LANES):
            q = rotate(proj[:, j * LANES:(j + 1) * LANES], cos_t[...], sin_t[...]) * (hd ** -0.5)
            for half_head, x in enumerate((q, pltpu.roll(q, LANES - hd, 1))):
                head = 2 * j + half_head
                qbuf[pl.ds(head * rows, rows)] = jnp.where(low_half, x, 0.0).astype(BF16)

    @scoped
    def kv_wait(l):
        take(kv_all.at[l, core, pl.ds(0, PLANE - 1)], kv_recv.at[l])
        ref = kv_all.at[l, core]
        remote(ref, ref, kvd_send.at[l], kvd_recv.at[l], partner).start()
        take(kv_all.at[l, 1 - core], kvd_recv.at[l])

    def c_columns(z):
        return pl.ds(pl.multiple_of(z * hq, hq), hq)

    @scoped
    def attention(l):
        keys = 2 * PLANE * rows
        j = lax.broadcasted_iota(jnp.int32, (1, keys), 1)
        key_pos = ((j // seq_dev) % nz) * (2 * PLANE * seq_dev) + ((j // rows) % PLANE) * (2 * seq_dev) \
            + (j // (PLANE * rows)) * seq_dev + j % seq_dev
        i = lax.broadcasted_iota(jnp.int32, (2 * rows, 1), 0) % rows
        q_pos = (i // seq_dev) * (2 * PLANE * seq_dev) + (mp * 2 + core) * seq_dev + i % seq_dev
        allowed = key_pos <= jnp.minimum(q_pos, len_s[0] - 1)
        kv = kv_all[l].reshape(keys, LANES)
        for pair in range(hq // LANES):
            s = lax.dot_general(qbuf[pl.ds(2 * pair * rows, 2 * rows)], kv, NT, preferred_element_type=F32)
            s = jnp.where(allowed, s, -1e30)
            e = jnp.exp(s - jnp.max(s, axis=-1, keepdims=True))
            p = (e * (1.0 / jnp.sum(e, axis=-1, keepdims=True))).astype(BF16)
            o = jnp.dot(p, kv, preferred_element_type=F32)
            cols = pl.ds(pl.multiple_of(mz * hq + pair * LANES, LANES), LANES)
            c_mat[l, :, cols] = jnp.where(low_half, pltpu.roll(o[:rows], LANES - hd, 1), o[rows:]).astype(BF16)
            ref = c_mat.at[l, :, cols]
            for i in far_z:
                remote(ref, ref, c_send.at[l], c_recv.at[l, int(i in next_z)], z_peer(i)).start()

    @scoped
    def out_proj(l):
        with jax.named_scope('wo_wait'):
            wo_copy(l).wait()
        for i in [0] + far_z:
            if i and i in (far_z[0], far_z[-len(next_z)]):
                near = i in next_z
                n = len(next_z) if near else nz - 1 - len(next_z)
                with jax.named_scope('c_wait'):
                    take(c_mat.at[l, :, pl.ds(0, n * hq)], c_recv.at[l, int(near)])
            cols = c_columns((mz + nz - i) % nz)
            part = jnp.dot(c_mat[l, :, cols], wo_v[l, cols, :], preferred_element_type=F32)
            acc[...] = acc[...] + part if i else part

    group = CHUNK // units
    n_groups = len(GROUPS)
    assert group == 2 * len(GROUPS[0])

    def slab(l, places, first, cols):
        parts = [w_all[l, c, slot(0, px + dx, py + dy), pl.ds(first, units), cols] for dx, dy in places for c in range(2)]
        return jnp.concatenate(parts, axis=0)

    block = lax.broadcasted_iota(jnp.int32, (rows, CHUNK), 1) // units
    every = pl.ds(0, d_model)

    def units_of(l, places):
        gate = lax.dot_general(zb[...], slab(l, places, 0, every), NT, preferred_element_type=F32)
        up = lax.dot_general(zb[...], slab(l, places, units, every), NT, preferred_element_type=F32)
        return gate * (1.0 / (1.0 + jnp.exp(-gate))) * up

    def spread(g, act, blocks):
        for b in blocks:
            bd[g, pl.ds(b * rows, rows)] = jnp.where(block == b, act, 0.0).astype(BF16)

    @scoped
    def mlp_units(l, gs):
        for g in gs:
            spread(g, units_of(l, GROUPS[g]), range(group))

    @scoped
    def mlp_units_but_last(l, g):
        places = GROUPS[g][:-1] + GROUPS[g][:1]
        spread(g, units_of(l, places), range(group - 2))

    @scoped
    def mlp_units_last(l, g):
        act = units_of(l, GROUPS[g][-2:])
        spread(g, jnp.concatenate([jnp.zeros_like(act), act], axis=1), range(group - 2, group))

    two_step = nz == 8
    wide = min(2 * CHUNK, d_model)
    n_sums = d_model // wide

    def ps_of(l, n, i):
        return ps.at[l, n, (mz + i + nz) % nz]

    def rs_start(l, n):
        if not two_step:
            for k, i in enumerate(far_z):
                remote(ps_of(l, n, i), rs.at[l, n, k], rs_send.at[l], rs_recv.at[l, n], z_peer(i)).start()
            return
        for side, to in ((0, nz - 2), (1, 2)):
            cols = pl.ds(side * (wide // 2), wide // 2)
            remote(ps.at[l, n, (mz + 4) % nz, :, cols], ra.at[l, n, 2, :, cols], rs_send.at[l], ra_recv.at[l, n], z_peer(to)).start()
        for side, to in ((0, -1), (1, 1)):
            remote(ps_of(l, n, 3 * to), ra.at[l, n, side], rs_send.at[l], ra_recv.at[l, n], z_peer(nz + to)).start()

    @scoped
    def rs_middle(l):
        if not two_step:
            return
        for n in range(n_sums):
            for side, to in ((0, -1), (1, 1)):
                remote(ps_of(l, n, to), rs.at[l, n, side], rs_send.at[l], rs_recv.at[l, n], z_peer(nz + to)).start()

        @pl.loop(0, n_sums)
        def _(n):
            take(ra.at[l, n], ra_recv.at[l, n])
            for side, to in ((0, -2), (1, 2)):
                cols = pl.ds(side * (wide // 2), wide // 2)
                sb[l, n, side] = ps[l, n, (mz + nz + to) % nz] + ra[l, n, side]
                sb[l, n, side, :, cols] = sb[l, n, side, :, cols] + ra[l, n, 2, :, cols]
                remote(sb.at[l, n, side], rs.at[l, n, 2 + side], rs_send.at[l], rs_recv.at[l, n], z_peer(nz + to)).start()

    def down(l, n, gs):
        cols = pl.ds(pl.multiple_of(n * wide, wide), wide)
        total = jnp.zeros((rows, wide), F32)
        for g in gs:
            y = jnp.dot(bd[g], slab(l, GROUPS[g], 2 * units, cols), preferred_element_type=F32)
            y = y.astype(BF16).astype(F32)
            for b in range(group):
                total = total + y[b * rows:(b + 1) * rows]
        return total

    @scoped
    def mlp_down(l):
        @pl.loop(0, n_sums)
        def _(n):
            ps[l, n] = down(l, n, range(n_groups)).reshape(nz, seq_dev, wide)
            rs_start(l, n)

    n_in = 4 if two_step else nz - 1

    @scoped
    def rs_finish(l, store):
        mine = pl.ds(pl.multiple_of(mz * seq_dev, seq_dev), seq_dev)
        for n in range(n_sums):
            if n_in:
                take(rs.at[l, n], rs_recv.at[l, n])
            total = ps[l, n, mz]
            for k in range(n_in):
                total = total + rs[l, n, k]
            store(n, (hres[mine, n * wide:(n + 1) * wide] + total).astype(BF16))

    def store_next(l):
        def store(n, x):
            h_all[l + 1, mz, :, n * wide:(n + 1) * wide] = x
        return store

    with jax.named_scope('barrier'):
        pl.semaphore_wait(barrier, 1 + len(next_devices))
    round_start(0)
    p1(0)
    p3(0, (0,))
    with jax.named_scope('rounds'):
        small[0].wait()
        for r in range(4):
            if r:
                round_wait(r - 1)
                if r < 3:
                    round_start(r)
            h_start(0, 0, d_model, [i for i in far_z if min(i, nz - i) == r + 1])
    start_later_copies()
    with jax.named_scope('small'):
        for c in small[1:]:
            c.wait()
        rope_tables()
    p2(0)
    for l in range(layers):
        more = l + 1 < layers
        if l:
            p4(l, (0,))
            kv_heads(l)
            h_start(l, 0, d_model, far_z)
            kv_heads_wait(l)
            p3(l, (2,))
            p4(l, (1, 3))
        h_wait(l)
        norm_to_zb(l, ga)
        if l == 0:
            kv_first(l)
            p3(l, (1, 3, 2))
            p4(l, (0,))
        q_first(l)
        kv_wait(l)
        attention(l)
        if l == 0:
            p4(0, (1, 3, 2))
            p5(0, (0,))
        else:
            p5(l, (0,))
            p4(l, (2,))
            p5(l, (1, 3, 2))
        if more:
            p1(l + 1)
            p3(l + 1, (0,))
        out_proj(l)
        norm_to_zb(l, gm, True)
        if l == 0:
            w_done(l, (0,))
            mlp_units(l, (0,))
            w_done(l, (1,))
            mlp_units(l, (1,))
            p5(l, (1, 3))
            w_done(l, (2,))
            mlp_units(l, (2,))
            p5(l, (2,))
            w_done(l, (3,))
            mlp_units_but_last(l, 3)
            w_done(l, (4,))
            mlp_units_last(l, 3)
        else:
            w_done(l, range(n_groups + 1))
            mlp_units(l, range(n_groups))
        mlp_down(l)
        if more:
            p2(l + 1)
            p3(l + 1, (1, 3))
        rs_middle(l)
        if more:
            rs_finish(l, store_next(l))
    pieces = []
    rs_finish(layers - 1, lambda n, x: pieces.append(x.astype(F32)))
    x = jnp.concatenate(pieces, axis=1)
    inv = lax.rsqrt(jnp.mean(x * x, axis=-1, keepdims=True) + NORM_EPS)
    gain = gf[...].astype(F32)
    for i in range(d_model // LANES):
        cols = slice(i * LANES, (i + 1) * LANES)
        out_ref[:, cols] = x[:, cols] * inv * gain[i:i + 1]

    with jax.named_scope('drain'):
      for l in range(layers):
          ref = w_all.at[l, 0, pl.ds(0, PLANE - 1)]
          remote(ref, ref, w_send.at[l], w_recv.at[l, 0], me).wait_send()
          ref = w_all.at[l, 0]
          remote(ref, ref, d_send.at[l], d_recv.at[l, 0], me).wait_send()
          ref = kv_all.at[l, 0, pl.ds(0, PLANE - 1)]
          remote(ref, ref, kv_send.at[l], kv_recv.at[l], me).wait_send()
          ref = kv_all.at[l, 0]
          remote(ref, ref, kvd_send.at[l], kvd_recv.at[l], me).wait_send()
          if nz > 1 and l:
              ref = kv_rows.at[l - 1, pl.ds(0, nz - 1)]
              remote(ref, ref, kva_send.at[l - 1], kva_recv.at[l - 1], me).wait_send()
          if nz > 1:
              ref = h_all.at[l, pl.ds(0, nz - 1)]
              remote(ref, ref, h_send.at[l], h_recv.at[l], me).wait_send()
              ref = c_mat.at[l, :, pl.ds(0, (nz - 1) * hq)]
              remote(ref, ref, c_send.at[l], c_recv.at[l, 0], me).wait_send()
              ref = ps.at[l, :, pl.ds(0, nz - 1)]
              remote(ref, ref, rs_send.at[l], rs_recv.at[l, 0], me).wait_send()


def solution(mesh):
    nz = mesh.shape['tp'] // (2 * PLANE)

    def device_fn(hidden_in, lengths, attn_norm, w_query, w_key, w_value, w_out, mlp_norm, w_gate, w_up, w_down, final_norm):
        seq_dev, d_model = hidden_in.shape[1:]
        layers, _, heads, hd = w_query.shape
        kv_heads = w_key.shape[2]
        units = w_gate.shape[2]
        assert kv_heads == nz and 2 * hd == LANES and heads % nz == 0
        hq = heads // nz * hd
        rows = nz * seq_dev
        wide = min(2 * CHUNK, d_model)
        n_sums = d_model // wide
        n_groups = 2 * PLANE * units // CHUNK
        dev, row = np.arange(2 * PLANE)[:, None], np.arange(rows)[None, :]
        pos = (row // seq_dev) * (2 * PLANE * seq_dev) + dev * seq_dev + row % seq_dev
        freq = np.float32(ROPE_BASE) ** (np.float32(-2.0) * np.arange(hd // 2, dtype=np.float32) / np.float32(hd))
        angles = (pos[..., None].astype(np.float32) * freq).astype(np.float64)
        rope = np.tile(np.concatenate([np.cos(angles), np.sin(angles)], axis=-1), (1, 1, 2)).astype(np.float32)
        by_rows = lambda w: jnp.transpose(w, (0, 2, 3, 1)).reshape(layers, -1, d_model)
        units_first = lambda w: jnp.transpose(w, (0, 2, 1))
        pinned = lambda x: pltpu.with_memory_space_constraint(x, pltpu.HBM)
        hbm, vmem = (pl.BlockSpec(memory_space=s) for s in (pltpu.HBM, pltpu.VMEM))
        dma = pltpu.SemaphoreType.DMA
        out = pl.pallas_call(
            functools.partial(kernel, nz),
            name='decoder',
            out_shape=pltpu.VMEM((seq_dev, d_model), F32),
            in_specs=[hbm] * 13,
            out_specs=vmem,
            scratch_shapes=[
                pltpu.VMEM((layers, 2, PLANE, 3 * units, d_model), BF16),
                pltpu.VMEM((layers, heads * hd, d_model), BF16),
                pltpu.VMEM((layers, hq + 2 * hd, d_model), BF16),
                pltpu.VMEM((layers - 1, kv_heads * 2 * hd, d_model), BF16),
                pltpu.VMEM((layers - 1, kv_heads, seq_dev, LANES), BF16),
                pltpu.VMEM((layers, nz, seq_dev, d_model), BF16),
                pltpu.VMEM((layers, rows, heads * hd), BF16),
                pltpu.VMEM((layers, 2, PLANE, rows, LANES), BF16),
                pltpu.VMEM((layers, n_sums, 4 if nz == 8 else max(nz - 1, 1), seq_dev, wide), F32),
                pltpu.VMEM((layers, n_sums, 3, seq_dev, wide), F32),
                pltpu.VMEM((layers, n_sums, 2, seq_dev, wide), F32),
                pltpu.VMEM((layers, n_sums, nz, seq_dev, wide), F32),
                pltpu.VMEM((rows, d_model), F32),
                pltpu.VMEM((rows, d_model), F32),
                pltpu.VMEM((rows, d_model), BF16),
                pltpu.VMEM((hq // hd * rows, LANES), BF16),
                pltpu.VMEM((n_groups, CHUNK // units * rows, CHUNK), BF16),
                pltpu.VMEM((rows, LANES), F32), pltpu.VMEM((rows, LANES), F32), pltpu.VMEM((rows, LANES), F32),
                pltpu.VMEM((layers, d_model), BF16), pltpu.VMEM((layers, d_model), BF16),
                pltpu.VMEM((d_model // LANES, LANES), BF16),
                pltpu.SMEM((1,), jnp.int32),
                dma((layers, 4)), dma((6,)), dma((layers, 10)), dma((layers,)),
                dma((layers, n_groups + 1)), dma((layers,)),
                pltpu.SemaphoreType.REGULAR((3,)),
                dma((layers,)), dma((layers,)), dma((layers,)), dma((layers,)), dma((layers,)), dma((layers,)),
                dma((layers - 1,)), dma((layers - 1,)),
                dma((layers, 2)), dma((layers,)), dma((layers, n_sums)), dma((layers, n_sums)), dma((layers,)),
            ],
            compiler_params=pltpu.CompilerParams(
                collective_id=0, has_side_effects=True, vmem_limit_bytes=60_000_000),
        )(pinned(hidden_in[0]), lengths, *map(pinned, (
            jnp.asarray(rope), attn_norm, mlp_norm, final_norm.reshape(-1, LANES), by_rows(w_query), by_rows(w_key), by_rows(w_value),
            w_out.reshape(layers, heads * hd, d_model), units_first(w_gate), units_first(w_up), w_down)))
        return out.astype(BF16)[None]

    seq_part = P(None, 'tp', None)
    in_specs = (seq_part, P(), P(), P(), P(), P(), P(), P(), P(None, None, 'tp'), P(None, None, 'tp'), P(None, 'tp', None), P())
    return jax.shard_map(device_fn, mesh=mesh, in_specs=in_specs, out_specs=seq_part, check_vma=False)
```

```python
import functools

import jax
import jax.numpy as jnp
import numpy as np
from jax import lax
from jax.experimental import pallas as pl
from jax.experimental.pallas import tpu as pltpu
from jax.sharding import PartitionSpec as P

NORM_EPS = 1e-5
ROPE_BASE = 500000.0
NX = 4
PLANE = NX * NX
LANES = 128
CHUNK = 256
NT = (((1,), (1,)), ((), ()))
F32, BF16 = jnp.float32, jnp.bfloat16


def remote(src, dst, send_sem, recv_sem, device):
    return pltpu.make_async_remote_copy(
        src_ref=src, dst_ref=dst, send_sem=send_sem, recv_sem=recv_sem,
        device_id=(device,), device_id_type=pl.DeviceIdType.MESH)


def scoped(f):
    @functools.wraps(f)
    def wrapped(*args):
        with jax.named_scope(f.__name__ + ('#l=%d' % args[0])):
            return f(*args)
    return wrapped


def kernel(nz, h_ref, len_ref, rope_ref, ga_ref, gm_ref, gf_ref, wq_ref, wk_ref, wv_ref, wo_ref, wg_ref, wu_ref, wd_ref,
           out_ref, w_all, wo_v, wqkv, wkv, kv_rows, h_all, c_mat, kv_all, rs, ra, sb, ps, acc, hres, zb, qbuf, bd, rope, cos_t, sin_t, ga, gm, gf, len_s,
           local_sem, in_sem, w_recv, w_send, d_recv, d_send, rounds, h_recv, h_send, kv_recv, kv_send, kvd_recv, kvd_send, kva_recv, kva_send,
           c_recv, c_send, rs_recv, ra_recv, rs_send):
    layers = wo_ref.shape[0]
    seq_dev, d_model = h_ref.shape
    units = wg_ref.shape[1]
    pack = 3 * units
    half = pack // 2
    rows = nz * seq_dev
    hq = wq_ref.shape[1] // nz
    hd = wk_ref.shape[1] // nz
    me = lax.axis_index('tp')
    core = me % 2
    px = (me // 2) % NX
    py = (me // (2 * NX)) % NX
    mp = (me // 2) % PLANE
    mz = me // (2 * PLANE)
    base = mz * (2 * PLANE)
    partner = base + mp * 2 + (1 - core)

    def z_peer(i):
        return ((mz + i) % nz) * (2 * PLANE) + mp * 2 + core

    far_z = sorted(range(1, nz), key=lambda i: -min(i, nz - i))
    next_z = [i for i in far_z if min(i, nz - i) == 1]
    def plane_peer(dy, dx):
        return base + ((py + dy) % NX * NX + (px + dx) % NX) * 2 + core

    far_plane = sorted(((dy, dx) for dy in range(NX) for dx in range(NX) if dy or dx),
                       key=lambda d: -sum(min(i, NX - i) for i in d))

    barrier = pltpu.get_barrier_semaphore()
    next_devices = [plane_peer(0, 1), plane_peer(0, NX - 1), plane_peer(1, 0), plane_peer(NX - 1, 0)]
    next_devices += [z_peer(i) for i in next_z]

    def signal(sem, device):
        pl.semaphore_signal(sem, inc=1, device_id=(device,), device_id_type=pl.DeviceIdType.MESH)

    signal(barrier, partner)
    for d in next_devices:
        signal(barrier, d)

    def round_start(r):
        for d in next_devices:
            signal(rounds.at[r], d)

    def round_wait(r):
        pl.semaphore_wait(rounds.at[r], len(next_devices))

    def pack_copies(l):
        mine = w_all.at[l, core, mp]
        return [pltpu.make_async_copy(ref.at[l], mine.at[pl.ds(i * units, units)], local_sem.at[l, 0])
                for i, ref in enumerate((wg_ref, wu_ref, wd_ref))]

    def qkv_copies(l):
        mine = [(wq_ref, 0, hq), (wk_ref, hq, hd), (wv_ref, hq + hd, hd)]
        return [pltpu.make_async_copy(ref.at[l, pl.ds(mz * n, n)], wqkv.at[l, pl.ds(first, n)], local_sem.at[l, 1])
                for ref, first, n in (mine[:1] if l else mine)]

    def kv_weight_copies(l):
        return [pltpu.make_async_copy(ref.at[l, pl.ds(z * hd, hd)], wkv.at[l - 1, pl.ds((2 * z + i) * hd, hd)], local_sem.at[l, 3])
                for z in range(nz) for i, ref in enumerate((wk_ref, wv_ref))]

    def wo_copy(l):
        return pltpu.make_async_copy(wo_ref.at[l], wo_v.at[l], local_sem.at[l, 2])

    def take(ref, sem):
        remote(ref, ref, w_send.at[0], sem, me).wait_recv()

    def pack_wait(l):
        mine = w_all.at[l, core, mp]
        pltpu.make_async_copy(mine, mine, local_sem.at[l, 0]).wait()

    def qkv_wait(l):
        ref = wqkv.at[l, pl.ds(0, hq)] if l else wqkv.at[l]
        pltpu.make_async_copy(ref, ref, local_sem.at[l, 1]).wait()

    small = [pltpu.make_async_copy(src, dst, in_sem.at[i]) for i, (src, dst) in enumerate((
        (h_ref, h_all.at[0, 0]), (rope_ref.at[mp * 2 + core, pl.ds(mz * seq_dev, rows)], rope), (ga_ref, ga), (gm_ref, gm), (gf_ref, gf), (len_ref, len_s)))]
    for c in pack_copies(0) + small + qkv_copies(0):
        c.start()

    def start_later_copies():
        wo_copy(0).start()
        for l in range(1, layers):
            for c in pack_copies(l) + qkv_copies(l) + kv_weight_copies(l):
                c.start()
            wo_copy(l).start()

    def slot(h, a1, a2):
        return a2 % NX * NX + a1 % NX if h == 0 else a1 % NX * NX + a2 % NX

    def where_am_i(h):
        return (px, py) if h == 0 else (py, px)

    def at(h, a1, a2):
        return base + slot(h, a1, a2) * 2 + core

    SPAN = ((0, half), (half, half))

    FROM_MINUS = tuple((h * half, half // 2) for h in range(2))
    FROM_PLUS = tuple((h * half + half // 2, half // 2) for h in range(2))

    def piece(l, c, p, span):
        return w_all.at[l, c, p, pl.ds(*span)]

    def w_start(l, p, span, idx, device):
        ref = piece(l, core, p, span)
        remote(ref, ref, w_send.at[l], w_recv.at[l, idx], device).start()

    def w_take(l, idx, packs):
        take(w_all.at[l, core, pl.ds(0, packs)], w_recv.at[l, idx])

    GROUPS = (((0, 0), (1, 0), (3, 0), (0, 1)), ((0, 3), (2, 0), (0, 2), (1, 1)),
              ((1, 3), (3, 1), (3, 3), (2, 1)), ((2, 3), (1, 2), (3, 2), (2, 2)))
    ARRIVALS = (*GROUPS[:-1], GROUPS[-1][:-1], GROUPS[-1][-1:])
    ARRIVAL_OF = {d: g for g, ds in enumerate(ARRIVALS) for d in ds}

    def to_partner(l, h, k1, k2, span):
        a1, a2 = where_am_i(h)
        ref = piece(l, core, slot(h, a1 + k1, a2 + k2), span)
        g = ARRIVAL_OF[(k1, k2) if h == 0 else (k2, k1)]
        remote(ref, ref, d_send.at[l], d_recv.at[l, g], partner).start()

    @scoped
    def p1(l):
        pack_wait(l)
        for h in range(2):
            a1, a2 = where_am_i(h)
            w_start(l, mp, SPAN[h], 0, at(h, a1 + 1, a2))
            w_start(l, mp, SPAN[h], 0, at(h, a1 + NX - 1, a2))
        to_partner(l, 0, 0, 0, (0, pack))

    @scoped
    def p2(l):
        w_take(l, 0, 2)
        for h in range(2):
            a1, a2 = where_am_i(h)
            w_start(l, slot(h, a1 + NX - 1, a2), FROM_MINUS[h], 1, at(h, a1 + 1, a2))
            w_start(l, slot(h, a1 + 1, a2), FROM_PLUS[h], 1, at(h, a1 + NX - 1, a2))
            to_partner(l, h, NX - 1, 0, SPAN[h])
            to_partner(l, h, 1, 0, SPAN[h])

    @scoped
    def p3(l, ks):
        for k in ks:
            if k == 2:
                w_take(l, 1, 1)
            for h in range(2):
                a1, a2 = where_am_i(h)
                p = slot(h, a1 + k, a2)
                w_start(l, p, SPAN[h], 2 + k, at(h, a1, a2 + 1))
                w_start(l, p, SPAN[h], 2 + k, at(h, a1, a2 + NX - 1))
                if k == 2:
                    to_partner(l, h, k, 0, SPAN[h])

    @scoped
    def p4(l, ks):
        for k in ks:
            w_take(l, 2 + k, 2)
            for h in range(2):
                a1, a2 = where_am_i(h)
                w_start(l, slot(h, a1 + k, a2 + NX - 1), FROM_MINUS[h], 6 + k, at(h, a1, a2 + 1))
                w_start(l, slot(h, a1 + k, a2 + 1), FROM_PLUS[h], 6 + k, at(h, a1, a2 + NX - 1))
                to_partner(l, h, k, NX - 1, SPAN[h])
                to_partner(l, h, k, 1, SPAN[h])

    @scoped
    def p5(l, ks):
        for k in ks:
            w_take(l, 6 + k, 1)
            for h in range(2):
                to_partner(l, h, k, 2, SPAN[h])

    @scoped
    def w_done(l, gs):
        for g in gs:
            take(w_all.at[l, 1 - core, pl.ds(0, len(ARRIVALS[g]))], d_recv.at[l, g])

    def h_start(l, first, size, peers):
        for i in peers:
            cols = pl.ds(first, size)
            remote(h_all.at[l, 0, :, cols], h_all.at[l, nz - i, :, cols], h_send.at[l], h_recv.at[l], z_peer(i)).start()

    @scoped
    def h_wait(l):
        if nz > 1:
            take(h_all.at[l, pl.ds(0, nz - 1)], h_recv.at[l])
        for i in range(nz):
            hres[pl.ds(i * seq_dev, seq_dev)] = h_all[l, i].astype(F32)

    @scoped
    def norm_to_zb(l, gains, residual=False):
        gain = gains[...].astype(F32)[l:l + 1]
        step = min(16, rows)
        for first in range(0, rows, step):
            r = pl.ds(first, step)
            x = hres[r]
            if residual:
                x = (x + acc[r]).astype(BF16).astype(F32)
                hres[r] = x
            inv = lax.rsqrt(jnp.mean(x * x, axis=-1, keepdims=True) + NORM_EPS)
            zb[r] = (x * inv * gain).astype(BF16)

    lane = lax.broadcasted_iota(jnp.int32, (rows, LANES), 1)
    low_half = lane < hd

    def rotate(x, cos, sin):
        first = (lane[:x.shape[0]] % hd) < hd // 2
        swapped = jnp.where(first, pltpu.roll(x, LANES - hd // 2, 1), pltpu.roll(x, hd // 2, 1))
        return x * cos + swapped * sin

    def rope_tables():
        first = (lane % hd) < hd // 2
        t = rope[...]
        cos_t[...] = jnp.where(first, t, pltpu.roll(t, hd // 2, 1))
        sin_t[...] = jnp.where(first, -pltpu.roll(t, LANES - hd // 2, 1), t)

    def kv_copy(l, device):
        ref = kv_all.at[l, core, mp]
        return remote(ref, ref, kv_send.at[l], kv_recv.at[l], device)

    def kv_start(l):
        for d in far_plane:
            kv_copy(l, plane_peer(*d)).start()

    @scoped
    def kv_first(l):
        qkv_wait(l)
        kv = lax.dot_general(zb[...], wqkv[l, pl.ds(hq, 2 * hd), :], NT, preferred_element_type=F32)
        kv_all[l, core, mp] = jnp.where(low_half, rotate(kv, cos_t[...], sin_t[...]), kv).astype(BF16)
        kv_start(l)

    def kv_place(l, i):
        return kv_all.at[l, core, mp, pl.ds(i * seq_dev, seq_dev)]

    @scoped
    def kv_heads(l):
        ref = wkv.at[l - 1]
        pltpu.make_async_copy(ref, ref, local_sem.at[l, 3]).wait()
        x = h_all[l, 0].astype(F32)
        inv = lax.rsqrt(jnp.mean(x * x, axis=-1, keepdims=True) + NORM_EPS)
        z = x * inv * ga[...].astype(F32)[l:l + 1]
        z = jnp.concatenate([z, z], axis=0).astype(BF16)
        kv = lax.dot_general(z, wkv[l - 1], NT, preferred_element_type=F32)[:seq_dev]
        for head in range(nz):
            part = kv[:, head * LANES:(head + 1) * LANES]
            kv_rows[l - 1, head] = jnp.where(low_half[:seq_dev], rotate(part, cos_t[:seq_dev], sin_t[:seq_dev]), part).astype(BF16)
        pltpu.make_async_copy(kv_rows.at[l - 1, mz], kv_place(l, 0), local_sem.at[l, 0]).start()
        for i in far_z:
            remote(kv_rows.at[l - 1, (mz + i) % nz], kv_place(l, nz - i), kva_send.at[l - 1], kva_recv.at[l - 1], z_peer(i)).start()

    @scoped
    def kv_heads_wait(l):
        pltpu.make_async_copy(kv_rows.at[l - 1, mz], kv_place(l, 0), local_sem.at[l, 0]).wait()
        if nz > 1:
            take(kv_rows.at[l - 1, pl.ds(0, nz - 1)], kva_recv.at[l - 1])
        kv_start(l)

    @scoped
    def q_first(l):
        if l:
            qkv_wait(l)
        proj = lax.dot_general(zb[...], wqkv[l, pl.ds(0, hq), :], NT, preferred_element_type=F32)
        for j in range(hq // LANES):
            q = rotate(proj[:, j * LANES:(j + 1) * LANES], cos_t[...], sin_t[...]) * (hd ** -0.5)
            for half_head, x in enumerate((q, pltpu.roll(q, LANES - hd, 1))):
                head = 2 * j + half_head
                qbuf[pl.ds(head * rows, rows)] = jnp.where(low_half, x, 0.0).astype(BF16)

    @scoped
    def kv_wait(l):
        take(kv_all.at[l, core, pl.ds(0, PLANE - 1)], kv_recv.at[l])
        ref = kv_all.at[l, core]
        remote(ref, ref, kvd_send.at[l], kvd_recv.at[l], partner).start()
        take(kv_all.at[l, 1 - core], kvd_recv.at[l])

    def c_columns(z):
        return pl.ds(pl.multiple_of(z * hq, hq), hq)

    @scoped
    def attention(l):
        keys = 2 * PLANE * rows
        j = lax.broadcasted_iota(jnp.int32, (1, keys), 1)
        key_pos = ((mz + j // seq_dev) % nz) * (2 * PLANE * seq_dev) + ((j // rows) % PLANE) * (2 * seq_dev) \
            + (j // (PLANE * rows)) * seq_dev + j % seq_dev
        i = lax.broadcasted_iota(jnp.int32, (2 * rows, 1), 0) % rows
        q_pos = ((mz + i // seq_dev) % nz) * (2 * PLANE * seq_dev) + (mp * 2 + core) * seq_dev + i % seq_dev
        allowed = key_pos <= jnp.minimum(q_pos, len_s[0] - 1)
        kv = kv_all[l].reshape(keys, LANES)
        scores = [lax.dot_general(qbuf[pl.ds(2 * pair * rows, 2 * rows)], kv, NT, preferred_element_type=F32)
                  for pair in range(hq // LANES)]
        for pair, s in enumerate(scores):
            s = jnp.where(allowed, s, -1e30)
            e = jnp.exp(s - jnp.max(s, axis=-1, keepdims=True))
            p = (e * (1.0 / jnp.sum(e, axis=-1, keepdims=True))).astype(BF16)
            o = jnp.dot(p, kv, preferred_element_type=F32)
            cols = pl.ds(pl.multiple_of(mz * hq + pair * LANES, LANES), LANES)
            c_mat[l, :, cols] = jnp.where(low_half, pltpu.roll(o[:rows], LANES - hd, 1), o[rows:]).astype(BF16)
            for i in far_z:
                cut = i * seq_dev
                for src, dst, n in ((cut, 0, rows - cut), (0, rows - cut, cut)):
                    remote(c_mat.at[l, pl.ds(src, n), cols], c_mat.at[l, pl.ds(dst, n), cols], c_send.at[l],
                           c_recv.at[l, int(i in next_z)], z_peer(i)).start()

    @scoped
    def out_proj(l):
        with jax.named_scope('wo_wait'):
            wo_copy(l).wait()
        for i in [0] + far_z:
            if i and i in (far_z[0], far_z[-len(next_z)]):
                near = i in next_z
                n = len(next_z) if near else nz - 1 - len(next_z)
                with jax.named_scope('c_wait'):
                    take(c_mat.at[l, :, pl.ds(0, n * hq)], c_recv.at[l, int(near)])
            cols = c_columns((mz + nz - i) % nz)
            part = jnp.dot(c_mat[l, :, cols], wo_v[l, cols, :], preferred_element_type=F32)
            acc[...] = acc[...] + part if i else part

    group = CHUNK // units
    n_groups = len(GROUPS)
    assert group == 2 * len(GROUPS[0])

    def slab(l, places, first, cols):
        parts = [w_all[l, c, slot(0, px + dx, py + dy), pl.ds(first, units), cols] for dx, dy in places for c in range(2)]
        return jnp.concatenate(parts, axis=0)

    block = lax.broadcasted_iota(jnp.int32, (rows // (2 if nz == 8 else 1), CHUNK), 1) // units
    every = pl.ds(0, d_model)

    def units_of(l, places):
        gate = lax.dot_general(zb[...], slab(l, places, 0, every), NT, preferred_element_type=F32)
        up = lax.dot_general(zb[...], slab(l, places, units, every), NT, preferred_element_type=F32)
        return gate * (1.0 / (1.0 + jnp.exp(-gate))) * up

    PASSES = ((2, 3, 4, 5), (6, 7, 0, 1)) if nz == 8 else (tuple(range(nz)),)
    part = rows // len(PASSES)

    def spread(g, act, blocks):
        for n, places in enumerate(PASSES):
            halves = (places[:len(places) // 2], places[len(places) // 2:]) if nz > 1 else (places,)
            x = jnp.concatenate([act[p[0] * seq_dev:(p[-1] + 1) * seq_dev] for p in halves], axis=0)
            for b in blocks:
                bd[n, g, pl.ds(b * part, part)] = jnp.where(block == b, x, 0.0).astype(BF16)

    @scoped
    def mlp_units(l, gs):
        for g in gs:
            spread(g, units_of(l, GROUPS[g]), range(group))

    @scoped
    def mlp_units_but_last(l, g):
        places = GROUPS[g][:-1] + GROUPS[g][:1]
        spread(g, units_of(l, places), range(group - 2))

    @scoped
    def mlp_units_last(l, g):
        act = units_of(l, GROUPS[g][-2:])
        spread(g, jnp.concatenate([jnp.zeros_like(act), act], axis=1), range(group - 2, group))

    two_step = nz == 8
    wide = min(2 * CHUNK, d_model)
    n_sums = d_model // wide

    def ps_of(l, n, i):
        return ps.at[l, n, i % nz]

    def rs_start(l, n):
        if not two_step:
            for k, i in enumerate(far_z):
                remote(ps_of(l, n, i), rs.at[l, n, k], rs_send.at[l], rs_recv.at[l, n], z_peer(i)).start()
            return
        for side, to in ((0, nz - 2), (1, 2)):
            cols = pl.ds(side * (wide // 2), wide // 2)
            remote(ps.at[l, n, 4, :, cols], ra.at[l, n, 2, :, cols], rs_send.at[l], ra_recv.at[l, n], z_peer(to)).start()
        for side, to in ((0, -1), (1, 1)):
            remote(ps_of(l, n, 3 * to), ra.at[l, n, side], rs_send.at[l], ra_recv.at[l, n], z_peer(nz + to)).start()

    @scoped
    def rs_middle(l):
        if not two_step:
            return
        for n in range(n_sums):
            for side, to in ((0, -1), (1, 1)):
                remote(ps_of(l, n, to), rs.at[l, n, side], rs_send.at[l], rs_recv.at[l, n], z_peer(nz + to)).start()

        @pl.loop(0, n_sums)
        def _(n):
            take(ra.at[l, n], ra_recv.at[l, n])
            for side, to in ((0, -2), (1, 2)):
                cols = pl.ds(side * (wide // 2), wide // 2)
                sb[l, n, side] = ps[l, n, to % nz] + ra[l, n, side]
                sb[l, n, side, :, cols] = sb[l, n, side, :, cols] + ra[l, n, 2, :, cols]
                remote(sb.at[l, n, side], rs.at[l, n, 2 + side], rs_send.at[l], rs_recv.at[l, n], z_peer(nz + to)).start()

    def down(l, n, which):
        cols = pl.ds(pl.multiple_of(n * wide, wide), wide)
        total = jnp.zeros((part, wide), F32)
        for g in range(n_groups):
            y = jnp.dot(bd[which, g], slab(l, GROUPS[g], 2 * units, cols), preferred_element_type=F32)
            y = y.astype(BF16).astype(F32)
            for b in range(group):
                total = total + y[b * part:(b + 1) * part]
        for k, place in enumerate(PASSES[which]):
            ps[l, n, place] = total[k * seq_dev:(k + 1) * seq_dev]

    @scoped
    def mlp_down(l):
        for which in range(len(PASSES)):
            @pl.loop(0, n_sums)
            def _(n):
                down(l, n, which)
                if which == 0:
                    rs_start(l, n)

    n_in = 4 if two_step else nz - 1

    @scoped
    def rs_finish(l, store):
        for n in range(n_sums):
            if n_in:
                take(rs.at[l, n], rs_recv.at[l, n])
            total = ps[l, n, 0]
            for k in range(n_in):
                total = total + rs[l, n, k]
            store(n, (hres[:seq_dev, n * wide:(n + 1) * wide] + total).astype(BF16))

    def store_next(l):
        def store(n, x):
            h_all[l + 1, 0, :, n * wide:(n + 1) * wide] = x
        return store

    with jax.named_scope('barrier'):
        pl.semaphore_wait(barrier, 1 + len(next_devices))
    round_start(0)
    p1(0)
    p3(0, (0,))
    with jax.named_scope('rounds'):
        small[0].wait()
        for r in range(4):
            if r:
                round_wait(r - 1)
                if r < 3:
                    round_start(r)
            h_start(0, 0, d_model, [i for i in far_z if min(i, nz - i) == r + 1])
    start_later_copies()
    with jax.named_scope('small'):
        for c in small[1:]:
            c.wait()
        rope_tables()
    p2(0)
    for l in range(layers):
        more = l + 1 < layers
        if l:
            p4(l, (0,))
            kv_heads(l)
            h_start(l, 0, d_model, far_z)
            kv_heads_wait(l)
            p3(l, (2,))
            p4(l, (1, 3))
        h_wait(l)
        norm_to_zb(l, ga)
        if l == 0:
            kv_first(l)
            p3(l, (1, 3, 2))
            p4(l, (0,))
        q_first(l)
        kv_wait(l)
        attention(l)
        if l == 0:
            p4(0, (1, 3, 2))
            p5(0, (0,))
        else:
            p5(l, (0,))
            p4(l, (2,))
            p5(l, (1, 3, 2))
        out_proj(l)
        norm_to_zb(l, gm, True)
        if l == 0:
            w_done(l, (0,))
            mlp_units(l, (0,))
            w_done(l, (1,))
            mlp_units(l, (1,))
            p5(l, (1, 3))
            if more:
                p1(l + 1)
                p3(l + 1, (0,))
            w_done(l, (2,))
            mlp_units(l, (2,))
            p5(l, (2,))
            w_done(l, (3,))
            mlp_units_but_last(l, 3)
            w_done(l, (4,))
            mlp_units_last(l, 3)
        else:
            w_done(l, range(n_groups + 1))
            mlp_units(l, range(n_groups))
        mlp_down(l)
        if more:
            p2(l + 1)
            p3(l + 1, (1, 3))
        rs_middle(l)
        if more:
            rs_finish(l, store_next(l))
    pieces = []
    rs_finish(layers - 1, lambda n, x: pieces.append(x.astype(F32)))
    x = jnp.concatenate(pieces, axis=1)
    inv = lax.rsqrt(jnp.mean(x * x, axis=-1, keepdims=True) + NORM_EPS)
    gain = gf[...].astype(F32)
    for i in range(d_model // LANES):
        cols = slice(i * LANES, (i + 1) * LANES)
        out_ref[:, cols] = x[:, cols] * inv * gain[i:i + 1]

    with jax.named_scope('drain'):
      for l in range(layers):
          ref = w_all.at[l, 0, pl.ds(0, PLANE - 1)]
          remote(ref, ref, w_send.at[l], w_recv.at[l, 0], me).wait_send()
          ref = w_all.at[l, 0]
          remote(ref, ref, d_send.at[l], d_recv.at[l, 0], me).wait_send()
          ref = kv_all.at[l, 0, pl.ds(0, PLANE - 1)]
          remote(ref, ref, kv_send.at[l], kv_recv.at[l], me).wait_send()
          ref = kv_all.at[l, 0]
          remote(ref, ref, kvd_send.at[l], kvd_recv.at[l], me).wait_send()
          if nz > 1 and l:
              ref = kv_rows.at[l - 1, pl.ds(0, nz - 1)]
              remote(ref, ref, kva_send.at[l - 1], kva_recv.at[l - 1], me).wait_send()
          if nz > 1:
              ref = h_all.at[l, pl.ds(0, nz - 1)]
              remote(ref, ref, h_send.at[l], h_recv.at[l], me).wait_send()
              ref = c_mat.at[l, :, pl.ds(0, (nz - 1) * hq)]
              remote(ref, ref, c_send.at[l], c_recv.at[l, 0], me).wait_send()
              ref = ps.at[l, :, pl.ds(0, nz - 1)]
              remote(ref, ref, rs_send.at[l], rs_recv.at[l, 0], me).wait_send()


def solution(mesh):
    nz = mesh.shape['tp'] // (2 * PLANE)

    def device_fn(hidden_in, lengths, attn_norm, w_query, w_key, w_value, w_out, mlp_norm, w_gate, w_up, w_down, final_norm):
        seq_dev, d_model = hidden_in.shape[1:]
        layers, _, heads, hd = w_query.shape
        kv_heads = w_key.shape[2]
        units = w_gate.shape[2]
        assert kv_heads == nz and 2 * hd == LANES and heads % nz == 0
        hq = heads // nz * hd
        rows = nz * seq_dev
        wide = min(2 * CHUNK, d_model)
        n_sums = d_model // wide
        n_groups = 2 * PLANE * units // CHUNK
        dev, row = np.arange(2 * PLANE)[:, None], np.arange(2 * rows)[None, :] % rows
        pos = (row // seq_dev) * (2 * PLANE * seq_dev) + dev * seq_dev + row % seq_dev
        freq = np.float32(ROPE_BASE) ** (np.float32(-2.0) * np.arange(hd // 2, dtype=np.float32) / np.float32(hd))
        angles = (pos[..., None].astype(np.float32) * freq).astype(np.float64)
        rope = np.tile(np.concatenate([np.cos(angles), np.sin(angles)], axis=-1), (1, 1, 2)).astype(np.float32)
        by_rows = lambda w: jnp.transpose(w, (0, 2, 3, 1)).reshape(layers, -1, d_model)
        units_first = lambda w: jnp.transpose(w, (0, 2, 1))
        pinned = lambda x: pltpu.with_memory_space_constraint(x, pltpu.HBM)
        hbm, vmem = (pl.BlockSpec(memory_space=s) for s in (pltpu.HBM, pltpu.VMEM))
        dma = pltpu.SemaphoreType.DMA
        out = pl.pallas_call(
            functools.partial(kernel, nz),
            name='decoder',
            out_shape=pltpu.VMEM((seq_dev, d_model), F32),
            in_specs=[hbm] * 13,
            out_specs=vmem,
            scratch_shapes=[
                pltpu.VMEM((layers, 2, PLANE, 3 * units, d_model), BF16),
                pltpu.VMEM((layers, heads * hd, d_model), BF16),
                pltpu.VMEM((layers, hq + 2 * hd, d_model), BF16),
                pltpu.VMEM((layers - 1, kv_heads * 2 * hd, d_model), BF16),
                pltpu.VMEM((layers - 1, kv_heads, seq_dev, LANES), BF16),
                pltpu.VMEM((layers, nz, seq_dev, d_model), BF16),
                pltpu.VMEM((layers, rows, heads * hd), BF16),
                pltpu.VMEM((layers, 2, PLANE, rows, LANES), BF16),
                pltpu.VMEM((layers, n_sums, 4 if nz == 8 else max(nz - 1, 1), seq_dev, wide), F32),
                pltpu.VMEM((layers, n_sums, 3, seq_dev, wide), F32),
                pltpu.VMEM((layers, n_sums, 2, seq_dev, wide), F32),
                pltpu.VMEM((layers, n_sums, nz, seq_dev, wide), F32),
                pltpu.VMEM((rows, d_model), F32),
                pltpu.VMEM((rows, d_model), F32),
                pltpu.VMEM((rows, d_model), BF16),
                pltpu.VMEM((hq // hd * rows, LANES), BF16),
                pltpu.VMEM((2, n_groups, CHUNK // units * rows // 2, CHUNK) if nz == 8 else (1, n_groups, CHUNK // units * rows, CHUNK), BF16),
                pltpu.VMEM((rows, LANES), F32), pltpu.VMEM((rows, LANES), F32), pltpu.VMEM((rows, LANES), F32),
                pltpu.VMEM((layers, d_model), BF16), pltpu.VMEM((layers, d_model), BF16),
                pltpu.VMEM((d_model // LANES, LANES), BF16),
                pltpu.SMEM((1,), jnp.int32),
                dma((layers, 4)), dma((6,)), dma((layers, 10)), dma((layers,)),
                dma((layers, n_groups + 1)), dma((layers,)),
                pltpu.SemaphoreType.REGULAR((3,)),
                dma((layers,)), dma((layers,)), dma((layers,)), dma((layers,)), dma((layers,)), dma((layers,)),
                dma((layers - 1,)), dma((layers - 1,)),
                dma((layers, 2)), dma((layers,)), dma((layers, n_sums)), dma((layers, n_sums)), dma((layers,)),
            ],
            compiler_params=pltpu.CompilerParams(
                collective_id=0, has_side_effects=True, vmem_limit_bytes=60_000_000),
        )(pinned(hidden_in[0]), lengths, *map(pinned, (
            jnp.asarray(rope), attn_norm, mlp_norm, final_norm.reshape(-1, LANES), by_rows(w_query), by_rows(w_key), by_rows(w_value),
            w_out.reshape(layers, heads * hd, d_model), units_first(w_gate), units_first(w_up), w_down)))
        return out.astype(BF16)[None]

    seq_part = P(None, 'tp', None)
    in_specs = (seq_part, P(), P(), P(), P(), P(), P(), P(), P(None, None, 'tp'), P(None, None, 'tp'), P(None, 'tp', None), P())
    return jax.shard_map(device_fn, mesh=mesh, in_specs=in_specs, out_specs=seq_part, check_vma=False)
```

```python
import functools

import jax
import jax.numpy as jnp
import numpy as np
from jax import lax
from jax.experimental import pallas as pl
from jax.experimental.pallas import tpu as pltpu
from jax.sharding import PartitionSpec as P

NORM_EPS = 1e-5
ROPE_BASE = 500000.0
NX = 4
PLANE = NX * NX
LANES = 128
CHUNK = 256
NT = (((1,), (1,)), ((), ()))
F32, BF16 = jnp.float32, jnp.bfloat16


def remote(src, dst, send_sem, recv_sem, device):
    return pltpu.make_async_remote_copy(
        src_ref=src, dst_ref=dst, send_sem=send_sem, recv_sem=recv_sem,
        device_id=(device,), device_id_type=pl.DeviceIdType.MESH)


def scoped(f):
    @functools.wraps(f)
    def wrapped(*args):
        with jax.named_scope(f.__name__ + ('#l=%d' % args[0])):
            return f(*args)
    return wrapped


def kernel(nz, h_ref, len_ref, rope_ref, ga_ref, gm_ref, gf_ref, wq_ref, wk_ref, wv_ref, wo_ref, wg_ref, wu_ref, wd_ref,
           out_ref, w_all, wo_v, wqkv, wkv, kv_rows, h_all, c_all, kv_all, rs, ra, sb, ps, acc, hres, zb, qbuf, bd, rope, cos_t, sin_t, ga, gm, gf, len_s,
           local_sem, in_sem, w_recv, w_send, d_recv, d_send, rounds, h_recv, h_send, kv_recv, kv_send, kvd_recv, kvd_send, kva_recv, kva_send,
           c_recv, c_send, rs_recv, ra_recv, rs_send):
    layers = wo_ref.shape[0]
    seq_dev, d_model = h_ref.shape
    units = wg_ref.shape[1]
    pack = 3 * units
    half = pack // 2
    rows = nz * seq_dev
    hq = wq_ref.shape[1] // nz
    hd = wk_ref.shape[1] // nz
    me = lax.axis_index('tp')
    core = me % 2
    px = (me // 2) % NX
    py = (me // (2 * NX)) % NX
    mp = (me // 2) % PLANE
    mz = me // (2 * PLANE)
    base = mz * (2 * PLANE)
    partner = base + mp * 2 + (1 - core)

    def z_peer(i):
        return ((mz + i) % nz) * (2 * PLANE) + mp * 2 + core

    far_z = sorted(range(1, nz), key=lambda i: -min(i, nz - i))
    next_z = [i for i in far_z if min(i, nz - i) == 1]
    def plane_peer(dy, dx):
        return base + ((py + dy) % NX * NX + (px + dx) % NX) * 2 + core

    far_plane = sorted(((dy, dx) for dy in range(NX) for dx in range(NX) if dy or dx),
                       key=lambda d: -sum(min(i, NX - i) for i in d))

    barrier = pltpu.get_barrier_semaphore()
    next_devices = [plane_peer(0, 1), plane_peer(0, NX - 1), plane_peer(1, 0), plane_peer(NX - 1, 0)]
    next_devices += [z_peer(i) for i in next_z]

    def signal(sem, device):
        pl.semaphore_signal(sem, inc=1, device_id=(device,), device_id_type=pl.DeviceIdType.MESH)

    signal(barrier, partner)
    for d in next_devices:
        signal(barrier, d)

    def round_start(r):
        for d in next_devices:
            signal(rounds.at[r], d)

    def round_wait(r):
        pl.semaphore_wait(rounds.at[r], len(next_devices))

    def pack_copies(l):
        mine = w_all.at[l, core, mp]
        return [pltpu.make_async_copy(ref.at[l], mine.at[pl.ds(i * units, units)], local_sem.at[l, 0])
                for i, ref in enumerate((wg_ref, wu_ref, wd_ref))]

    def qkv_copies(l):
        mine = [(wq_ref, 0, hq), (wk_ref, hq, hd), (wv_ref, hq + hd, hd)]
        return [pltpu.make_async_copy(ref.at[l, pl.ds(mz * n, n)], wqkv.at[l, pl.ds(first, n)], local_sem.at[l, 1])
                for ref, first, n in (mine[:1] if l else mine)]

    def kv_weight_copies(l):
        return [pltpu.make_async_copy(ref.at[l, pl.ds(z * hd, hd)], wkv.at[l - 1, pl.ds((2 * z + i) * hd, hd)], local_sem.at[l, 3])
                for z in range(nz) for i, ref in enumerate((wk_ref, wv_ref))]

    def wo_copy(l):
        return pltpu.make_async_copy(wo_ref.at[l], wo_v.at[l], local_sem.at[l, 2])

    def take(ref, sem):
        remote(ref, ref, w_send.at[0], sem, me).wait_recv()

    def pack_wait(l):
        mine = w_all.at[l, core, mp]
        pltpu.make_async_copy(mine, mine, local_sem.at[l, 0]).wait()

    def qkv_wait(l):
        ref = wqkv.at[l, pl.ds(0, hq)] if l else wqkv.at[l]
        pltpu.make_async_copy(ref, ref, local_sem.at[l, 1]).wait()

    small = [pltpu.make_async_copy(src, dst, in_sem.at[i]) for i, (src, dst) in enumerate((
        (h_ref, h_all.at[0, mz]), (rope_ref.at[mp * 2 + core], rope), (ga_ref, ga), (gm_ref, gm), (gf_ref, gf), (len_ref, len_s)))]
    for c in pack_copies(0) + small + qkv_copies(0):
        c.start()

    def start_later_copies():
        wo_copy(0).start()
        for l in range(1, layers):
            for c in pack_copies(l) + qkv_copies(l) + kv_weight_copies(l):
                c.start()
            wo_copy(l).start()

    def slot(h, a1, a2):
        return a2 % NX * NX + a1 % NX if h == 0 else a1 % NX * NX + a2 % NX

    def where_am_i(h):
        return (px, py) if h == 0 else (py, px)

    def at(h, a1, a2):
        return base + slot(h, a1, a2) * 2 + core

    SPAN = ((0, half), (half, half))

    FROM_MINUS = tuple((h * half, half // 2) for h in range(2))
    FROM_PLUS = tuple((h * half + half // 2, half // 2) for h in range(2))

    def piece(l, c, p, span):
        return w_all.at[l, c, p, pl.ds(*span)]

    def w_start(l, p, span, idx, device):
        ref = piece(l, core, p, span)
        remote(ref, ref, w_send.at[l], w_recv.at[l, idx], device).start()

    def w_take(l, idx, packs):
        take(w_all.at[l, core, pl.ds(0, packs)], w_recv.at[l, idx])

    GROUPS = (((0, 0), (1, 0), (3, 0), (0, 1)), ((0, 3), (2, 0), (0, 2), (1, 1)),
              ((1, 3), (3, 1), (3, 3), (2, 1)), ((2, 3), (1, 2), (3, 2), (2, 2)))
    ARRIVALS = (*GROUPS[:-1], GROUPS[-1][:-1], GROUPS[-1][-1:])
    ARRIVAL_OF = {d: g for g, ds in enumerate(ARRIVALS) for d in ds}

    def to_partner(l, h, k1, k2, span):
        a1, a2 = where_am_i(h)
        ref = piece(l, core, slot(h, a1 + k1, a2 + k2), span)
        g = ARRIVAL_OF[(k1, k2) if h == 0 else (k2, k1)]
        remote(ref, ref, d_send.at[l], d_recv.at[l, g], partner).start()

    @scoped
    def p1(l):
        pack_wait(l)
        for h in range(2):
            a1, a2 = where_am_i(h)
            w_start(l, mp, SPAN[h], 0, at(h, a1 + 1, a2))
            w_start(l, mp, SPAN[h], 0, at(h, a1 + NX - 1, a2))
        to_partner(l, 0, 0, 0, (0, pack))

    @scoped
    def p2(l):
        w_take(l, 0, 2)
        for h in range(2):
            a1, a2 = where_am_i(h)
            w_start(l, slot(h, a1 + NX - 1, a2), FROM_MINUS[h], 1, at(h, a1 + 1, a2))
            w_start(l, slot(h, a1 + 1, a2), FROM_PLUS[h], 1, at(h, a1 + NX - 1, a2))
            to_partner(l, h, NX - 1, 0, SPAN[h])
            to_partner(l, h, 1, 0, SPAN[h])

    @scoped
    def p3(l, ks):
        for k in ks:
            if k == 2:
                w_take(l, 1, 1)
            for h in range(2):
                a1, a2 = where_am_i(h)
                p = slot(h, a1 + k, a2)
                w_start(l, p, SPAN[h], 2 + k, at(h, a1, a2 + 1))
                w_start(l, p, SPAN[h], 2 + k, at(h, a1, a2 + NX - 1))
                if k == 2:
                    to_partner(l, h, k, 0, SPAN[h])

    @scoped
    def p4(l, ks):
        for k in ks:
            w_take(l, 2 + k, 2)
            for h in range(2):
                a1, a2 = where_am_i(h)
                w_start(l, slot(h, a1 + k, a2 + NX - 1), FROM_MINUS[h], 6 + k, at(h, a1, a2 + 1))
                w_start(l, slot(h, a1 + k, a2 + 1), FROM_PLUS[h], 6 + k, at(h, a1, a2 + NX - 1))
                to_partner(l, h, k, NX - 1, SPAN[h])
                to_partner(l, h, k, 1, SPAN[h])

    @scoped
    def p5(l, ks):
        for k in ks:
            w_take(l, 6 + k, 1)
            for h in range(2):
                to_partner(l, h, k, 2, SPAN[h])

    @scoped
    def w_done(l, gs):
        for g in gs:
            take(w_all.at[l, 1 - core, pl.ds(0, len(ARRIVALS[g]))], d_recv.at[l, g])

    def h_start(l, first, size, peers):
        for i in peers:
            ref = h_all.at[l, mz, :, pl.ds(first, size)]
            remote(ref, ref, h_send.at[l], h_recv.at[l], z_peer(i)).start()

    @scoped
    def h_wait(l):
        if nz > 1:
            take(h_all.at[l, pl.ds(0, nz - 1)], h_recv.at[l])
        for i in range(nz):
            hres[pl.ds(i * seq_dev, seq_dev)] = h_all[l, i].astype(F32)

    @scoped
    def norm_to_zb(l, gains, residual=False):
        gain = gains[...].astype(F32)[l:l + 1]
        step = min(16, rows)
        for first in range(0, rows, step):
            r = pl.ds(first, step)
            x = hres[r]
            if residual:
                x = (x + acc[r]).astype(BF16).astype(F32)
                hres[r] = x
            inv = lax.rsqrt(jnp.mean(x * x, axis=-1, keepdims=True) + NORM_EPS)
            zb[r] = (x * inv * gain).astype(BF16)

    lane = lax.broadcasted_iota(jnp.int32, (rows, LANES), 1)
    low_half = lane < hd

    def rotate(x, cos, sin):
        first = (lane[:x.shape[0]] % hd) < hd // 2
        swapped = jnp.where(first, pltpu.roll(x, LANES - hd // 2, 1), pltpu.roll(x, hd // 2, 1))
        return x * cos + swapped * sin

    def rope_tables():
        first = (lane % hd) < hd // 2
        t = rope[...]
        cos_t[...] = jnp.where(first, t, pltpu.roll(t, hd // 2, 1))
        sin_t[...] = jnp.where(first, -pltpu.roll(t, LANES - hd // 2, 1), t)

    def kv_copy(l, device):
        ref = kv_all.at[l, core, mp]
        return remote(ref, ref, kv_send.at[l], kv_recv.at[l], device)

    def kv_start(l):
        for d in far_plane:
            kv_copy(l, plane_peer(*d)).start()

    @scoped
    def kv_first(l):
        qkv_wait(l)
        kv = lax.dot_general(zb[...], wqkv[l, pl.ds(hq, 2 * hd), :], NT, preferred_element_type=F32)
        kv_all[l, core, mp] = jnp.where(low_half, rotate(kv, cos_t[...], sin_t[...]), kv).astype(BF16)
        kv_start(l)

    def kv_own(l):
        return kv_all.at[l, core, mp, pl.ds(pl.multiple_of(mz * seq_dev, seq_dev), seq_dev)]

    @scoped
    def kv_heads(l):
        ref = wkv.at[l - 1]
        pltpu.make_async_copy(ref, ref, local_sem.at[l, 3]).wait()
        x = h_all[l, mz].astype(F32)
        inv = lax.rsqrt(jnp.mean(x * x, axis=-1, keepdims=True) + NORM_EPS)
        z = x * inv * ga[...].astype(F32)[l:l + 1]
        z = jnp.concatenate([z, z], axis=0).astype(BF16)
        kv = lax.dot_general(z, wkv[l - 1], NT, preferred_element_type=F32)[:seq_dev]
        mine = pl.ds(pl.multiple_of(mz * seq_dev, seq_dev), seq_dev)
        for head in range(nz):
            part = kv[:, head * LANES:(head + 1) * LANES]
            kv_rows[l - 1, head] = jnp.where(low_half[:seq_dev], rotate(part, cos_t[mine], sin_t[mine]), part).astype(BF16)
        pltpu.make_async_copy(kv_rows.at[l - 1, mz], kv_own(l), local_sem.at[l, 0]).start()
        for i in far_z:
            remote(kv_rows.at[l - 1, (mz + i) % nz], kv_own(l), kva_send.at[l - 1], kva_recv.at[l - 1], z_peer(i)).start()

    @scoped
    def kv_heads_wait(l):
        pltpu.make_async_copy(kv_rows.at[l - 1, mz], kv_own(l), local_sem.at[l, 0]).wait()
        if nz > 1:
            take(kv_rows.at[l - 1, pl.ds(0, nz - 1)], kva_recv.at[l - 1])
        kv_start(l)

    @scoped
    def q_first(l):
        if l:
            qkv_wait(l)
        proj = lax.dot_general(zb[...], wqkv[l, pl.ds(0, hq), :], NT, preferred_element_type=F32)
        for j in range(hq // LANES):
            q = rotate(proj[:, j * LANES:(j + 1) * LANES], cos_t[...], sin_t[...]) * (hd ** -0.5)
            for half_head, x in enumerate((q, pltpu.roll(q, LANES - hd, 1))):
                head = 2 * j + half_head
                qbuf[pl.ds(head * rows, rows)] = jnp.where(low_half, x, 0.0).astype(BF16)

    @scoped
    def kv_wait(l):
        take(kv_all.at[l, core, pl.ds(0, PLANE - 1)], kv_recv.at[l])
        ref = kv_all.at[l, core]
        remote(ref, ref, kvd_send.at[l], kvd_recv.at[l], partner).start()
        take(kv_all.at[l, 1 - core], kvd_recv.at[l])

    @scoped
    def attention(l):
        keys = 2 * PLANE * rows
        j = lax.broadcasted_iota(jnp.int32, (1, keys), 1)
        key_pos = ((j // seq_dev) % nz) * (2 * PLANE * seq_dev) + ((j // rows) % PLANE) * (2 * seq_dev) \
            + (j // (PLANE * rows)) * seq_dev + j % seq_dev
        i = lax.broadcasted_iota(jnp.int32, (2 * rows, 1), 0) % rows
        q_pos = (i // seq_dev) * (2 * PLANE * seq_dev) + (mp * 2 + core) * seq_dev + i % seq_dev
        allowed = key_pos <= jnp.minimum(q_pos, len_s[0] - 1)
        kv = kv_all[l].reshape(keys, LANES)
        scores = [lax.dot_general(qbuf[pl.ds(2 * pair * rows, 2 * rows)], kv, NT, preferred_element_type=F32)
                  for pair in range(hq // LANES)]
        for pair, s in enumerate(scores):
            s = jnp.where(allowed, s, -1e30)
            e = jnp.exp(s - jnp.max(s, axis=-1, keepdims=True))
            p = (e * (1.0 / jnp.sum(e, axis=-1, keepdims=True))).astype(BF16)
            o = jnp.dot(p, kv, preferred_element_type=F32)
            c_all[l, mz, pair] = jnp.where(low_half, pltpu.roll(o[:rows], LANES - hd, 1), o[rows:]).astype(BF16)
            ref = c_all.at[l, mz, pair]
            for i in far_z:
                remote(ref, ref, c_send.at[l], c_recv.at[l, int(i in next_z)], z_peer(i)).start()

    @scoped
    def out_proj(l):
        with jax.named_scope('wo_wait'):
            wo_copy(l).wait()
        for i in [0] + far_z:
            if i and i in (far_z[0], far_z[-len(next_z)]):
                near = i in next_z
                n = len(next_z) if near else nz - 1 - len(next_z)
                with jax.named_scope('c_wait'):
                    take(c_all.at[l, pl.ds(0, n)], c_recv.at[l, int(near)])
            src = (mz + nz - i) % nz
            c = jnp.concatenate([c_all[l, src, pair] for pair in range(hq // LANES)], axis=1)
            part = jnp.dot(c, wo_v[l, pl.ds(pl.multiple_of(src * hq, hq), hq), :], preferred_element_type=F32)
            acc[...] = acc[...] + part if i else part

    group = CHUNK // units
    n_groups = len(GROUPS)
    assert group == 2 * len(GROUPS[0])

    def slab(l, places, first, cols):
        parts = [w_all[l, c, slot(0, px + dx, py + dy), pl.ds(first, units), cols] for dx, dy in places for c in range(2)]
        return jnp.concatenate(parts, axis=0)

    block = lax.broadcasted_iota(jnp.int32, (rows, CHUNK), 1) // units
    every = pl.ds(0, d_model)

    def units_of(l, places):
        gate = lax.dot_general(zb[...], slab(l, places, 0, every), NT, preferred_element_type=F32)
        up = lax.dot_general(zb[...], slab(l, places, units, every), NT, preferred_element_type=F32)
        return gate * (1.0 / (1.0 + jnp.exp(-gate))) * up

    def spread(g, act, blocks):
        for b in blocks:
            bd[g, pl.ds(b * rows, rows)] = jnp.where(block == b, act, 0.0).astype(BF16)

    @scoped
    def mlp_units(l, gs):
        for g in gs:
            spread(g, units_of(l, GROUPS[g]), range(group))

    @scoped
    def mlp_units_but_last(l, g):
        places = GROUPS[g][:-1] + GROUPS[g][:1]
        spread(g, units_of(l, places), range(group - 2))

    @scoped
    def mlp_units_last(l, g):
        act = units_of(l, GROUPS[g][-2:])
        spread(g, jnp.concatenate([jnp.zeros_like(act), act], axis=1), range(group - 2, group))

    two_step = nz == 8
    wide = min(2 * CHUNK, d_model)
    n_sums = d_model // wide

    def ps_of(l, n, i):
        return ps.at[l, n, (mz + i + nz) % nz]

    def rs_start(l, n):
        if not two_step:
            for k, i in enumerate(far_z):
                remote(ps_of(l, n, i), rs.at[l, n, k], rs_send.at[l], rs_recv.at[l, n], z_peer(i)).start()
            return
        for side, to in ((0, nz - 2), (1, 2)):
            cols = pl.ds(side * (wide // 2), wide // 2)
            remote(ps.at[l, n, (mz + 4) % nz, :, cols], ra.at[l, n, 2, :, cols], rs_send.at[l], ra_recv.at[l, n], z_peer(to)).start()
        for side, to in ((0, -1), (1, 1)):
            remote(ps_of(l, n, 3 * to), ra.at[l, n, side], rs_send.at[l], ra_recv.at[l, n], z_peer(nz + to)).start()

    @scoped
    def rs_middle(l):
        if not two_step:
            return
        for n in range(n_sums):
            for side, to in ((0, -1), (1, 1)):
                remote(ps_of(l, n, to), rs.at[l, n, side], rs_send.at[l], rs_recv.at[l, n], z_peer(nz + to)).start()

        @pl.loop(0, n_sums)
        def _(n):
            take(ra.at[l, n], ra_recv.at[l, n])
            for side, to in ((0, -2), (1, 2)):
                cols = pl.ds(side * (wide // 2), wide // 2)
                sb[l, n, side] = ps[l, n, (mz + nz + to) % nz] + ra[l, n, side]
                sb[l, n, side, :, cols] = sb[l, n, side, :, cols] + ra[l, n, 2, :, cols]
                remote(sb.at[l, n, side], rs.at[l, n, 2 + side], rs_send.at[l], rs_recv.at[l, n], z_peer(nz + to)).start()

    def down(l, n, gs):
        cols = pl.ds(pl.multiple_of(n * wide, wide), wide)
        total = jnp.zeros((rows, wide), F32)
        for g in gs:
            y = jnp.dot(bd[g], slab(l, GROUPS[g], 2 * units, cols), preferred_element_type=F32)
            y = y.astype(BF16).astype(F32)
            for b in range(group):
                total = total + y[b * rows:(b + 1) * rows]
        return total

    @scoped
    def mlp_down(l):
        @pl.loop(0, n_sums)
        def _(n):
            ps[l, n] = down(l, n, range(n_groups)).reshape(nz, seq_dev, wide)
            rs_start(l, n)

    n_in = 4 if two_step else nz - 1

    @scoped
    def rs_finish(l, store):
        mine = pl.ds(pl.multiple_of(mz * seq_dev, seq_dev), seq_dev)
        for n in range(n_sums):
            if n_in:
                take(rs.at[l, n], rs_recv.at[l, n])
            total = ps[l, n, mz]
            for k in range(n_in):
                total = total + rs[l, n, k]
            store(n, (hres[mine, n * wide:(n + 1) * wide] + total).astype(BF16))

    def store_next(l):
        def store(n, x):
            h_all[l + 1, mz, :, n * wide:(n + 1) * wide] = x
        return store

    with jax.named_scope('barrier'):
        pl.semaphore_wait(barrier, 1 + len(next_devices))
    round_start(0)
    p1(0)
    p3(0, (0,))
    with jax.named_scope('rounds'):
        small[0].wait()
        for r in range(4):
            if r:
                round_wait(r - 1)
                if r < 3:
                    round_start(r)
            h_start(0, 0, d_model, [i for i in far_z if min(i, nz - i) == r + 1])
    start_later_copies()
    with jax.named_scope('small'):
        for c in small[1:]:
            c.wait()
        rope_tables()
    p2(0)
    for l in range(layers):
        more = l + 1 < layers
        if l:
            p4(l, (0,))
            kv_heads(l)
            h_start(l, 0, d_model, far_z)
            kv_heads_wait(l)
            p3(l, (2,))
            p4(l, (1, 3))
        h_wait(l)
        norm_to_zb(l, ga)
        if l == 0:
            kv_first(l)
            p3(l, (1, 3, 2))
            p4(l, (0,))
        q_first(l)
        kv_wait(l)
        attention(l)
        if l == 0:
            p4(0, (1, 3, 2))
            p5(0, (0,))
        else:
            p5(l, (0,))
            p4(l, (2,))
            p5(l, (1, 3))
        out_proj(l)
        norm_to_zb(l, gm, True)
        if l == 0:
            w_done(l, (0,))
            mlp_units(l, (0,))
            w_done(l, (1,))
            mlp_units(l, (1,))
            p5(l, (1, 3))
            if more:
                p1(l + 1)
                p3(l + 1, (0,))
            w_done(l, (2,))
            mlp_units(l, (2,))
            p5(l, (2,))
            w_done(l, (3,))
            mlp_units_but_last(l, 3)
            w_done(l, (4,))
            mlp_units_last(l, 3)
        else:
            p5(l, (2,))
            w_done(l, range(n_groups - 1))
            mlp_units(l, range(n_groups - 1))
            w_done(l, (n_groups - 1, n_groups))
            mlp_units(l, (n_groups - 1,))
        mlp_down(l)
        if more:
            p2(l + 1)
            p3(l + 1, (1, 3))
        rs_middle(l)
        if more:
            rs_finish(l, store_next(l))
    pieces = []
    rs_finish(layers - 1, lambda n, x: pieces.append(x.astype(F32)))
    x = jnp.concatenate(pieces, axis=1)
    inv = lax.rsqrt(jnp.mean(x * x, axis=-1, keepdims=True) + NORM_EPS)
    gain = gf[...].astype(F32)
    for i in range(d_model // LANES):
        cols = slice(i * LANES, (i + 1) * LANES)
        out_ref[:, cols] = x[:, cols] * inv * gain[i:i + 1]

    with jax.named_scope('drain'):
      for l in range(layers):
          ref = w_all.at[l, 0, pl.ds(0, PLANE - 1)]
          remote(ref, ref, w_send.at[l], w_recv.at[l, 0], me).wait_send()
          ref = w_all.at[l, 0]
          remote(ref, ref, d_send.at[l], d_recv.at[l, 0], me).wait_send()
          ref = kv_all.at[l, 0, pl.ds(0, PLANE - 1)]
          remote(ref, ref, kv_send.at[l], kv_recv.at[l], me).wait_send()
          ref = kv_all.at[l, 0]
          remote(ref, ref, kvd_send.at[l], kvd_recv.at[l], me).wait_send()
          if nz > 1 and l:
              ref = kv_rows.at[l - 1, pl.ds(0, nz - 1)]
              remote(ref, ref, kva_send.at[l - 1], kva_recv.at[l - 1], me).wait_send()
          if nz > 1:
              ref = h_all.at[l, pl.ds(0, nz - 1)]
              remote(ref, ref, h_send.at[l], h_recv.at[l], me).wait_send()
              ref = c_all.at[l, pl.ds(0, nz - 1)]
              remote(ref, ref, c_send.at[l], c_recv.at[l, 0], me).wait_send()
              ref = ps.at[l, :, pl.ds(0, nz - 1)]
              remote(ref, ref, rs_send.at[l], rs_recv.at[l, 0], me).wait_send()


def solution(mesh):
    nz = mesh.shape['tp'] // (2 * PLANE)

    def device_fn(hidden_in, lengths, attn_norm, w_query, w_key, w_value, w_out, mlp_norm, w_gate, w_up, w_down, final_norm):
        seq_dev, d_model = hidden_in.shape[1:]
        layers, _, heads, hd = w_query.shape
        kv_heads = w_key.shape[2]
        units = w_gate.shape[2]
        assert kv_heads == nz and 2 * hd == LANES and heads % nz == 0
        hq = heads // nz * hd
        rows = nz * seq_dev
        wide = min(2 * CHUNK, d_model)
        n_sums = d_model // wide
        n_groups = 2 * PLANE * units // CHUNK
        dev, row = np.arange(2 * PLANE)[:, None], np.arange(rows)[None, :]
        pos = (row // seq_dev) * (2 * PLANE * seq_dev) + dev * seq_dev + row % seq_dev
        freq = np.float32(ROPE_BASE) ** (np.float32(-2.0) * np.arange(hd // 2, dtype=np.float32) / np.float32(hd))
        angles = (pos[..., None].astype(np.float32) * freq).astype(np.float64)
        rope = np.tile(np.concatenate([np.cos(angles), np.sin(angles)], axis=-1), (1, 1, 2)).astype(np.float32)
        by_rows = lambda w: jnp.transpose(w, (0, 2, 3, 1)).reshape(layers, -1, d_model)
        units_first = lambda w: jnp.transpose(w, (0, 2, 1))
        pinned = lambda x: pltpu.with_memory_space_constraint(x, pltpu.HBM)
        hbm, vmem = (pl.BlockSpec(memory_space=s) for s in (pltpu.HBM, pltpu.VMEM))
        dma = pltpu.SemaphoreType.DMA
        out = pl.pallas_call(
            functools.partial(kernel, nz),
            name='decoder',
            out_shape=pltpu.VMEM((seq_dev, d_model), F32),
            in_specs=[hbm] * 13,
            out_specs=vmem,
            scratch_shapes=[
                pltpu.VMEM((layers, 2, PLANE, 3 * units, d_model), BF16),
                pltpu.VMEM((layers, heads * hd, d_model), BF16),
                pltpu.VMEM((layers, hq + 2 * hd, d_model), BF16),
                pltpu.VMEM((layers - 1, kv_heads * 2 * hd, d_model), BF16),
                pltpu.VMEM((layers - 1, kv_heads, seq_dev, LANES), BF16),
                pltpu.VMEM((layers, nz, seq_dev, d_model), BF16),
                pltpu.VMEM((layers, nz, hq // LANES, rows, LANES), BF16),
                pltpu.VMEM((layers, 2, PLANE, rows, LANES), BF16),
                pltpu.VMEM((layers, n_sums, 4 if nz == 8 else max(nz - 1, 1), seq_dev, wide), F32),
                pltpu.VMEM((layers, n_sums, 3, seq_dev, wide), F32),
                pltpu.VMEM((layers, n_sums, 2, seq_dev, wide), F32),
                pltpu.VMEM((layers, n_sums, nz, seq_dev, wide), F32),
                pltpu.VMEM((rows, d_model), F32),
                pltpu.VMEM((rows, d_model), F32),
                pltpu.VMEM((rows, d_model), BF16),
                pltpu.VMEM((hq // hd * rows, LANES), BF16),
                pltpu.VMEM((n_groups, CHUNK // units * rows, CHUNK), BF16),
                pltpu.VMEM((rows, LANES), F32), pltpu.VMEM((rows, LANES), F32), pltpu.VMEM((rows, LANES), F32),
                pltpu.VMEM((layers, d_model), BF16), pltpu.VMEM((layers, d_model), BF16),
                pltpu.VMEM((d_model // LANES, LANES), BF16),
                pltpu.SMEM((1,), jnp.int32),
                dma((layers, 4)), dma((6,)), dma((layers, 10)), dma((layers,)),
                dma((layers, n_groups + 1)), dma((layers,)),
                pltpu.SemaphoreType.REGULAR((3,)),
                dma((layers,)), dma((layers,)), dma((layers,)), dma((layers,)), dma((layers,)), dma((layers,)),
                dma((layers - 1,)), dma((layers - 1,)),
                dma((layers, 2)), dma((layers,)), dma((layers, n_sums)), dma((layers, n_sums)), dma((layers,)),
            ],
            compiler_params=pltpu.CompilerParams(
                collective_id=0, has_side_effects=True, vmem_limit_bytes=60_000_000),
        )(pinned(hidden_in[0]), lengths, *map(pinned, (
            jnp.asarray(rope), attn_norm, mlp_norm, final_norm.reshape(-1, LANES), by_rows(w_query), by_rows(w_key), by_rows(w_value),
            w_out.reshape(layers, heads * hd, d_model), units_first(w_gate), units_first(w_up), w_down)))
        return out.astype(BF16)[None]

    seq_part = P(None, 'tp', None)
    in_specs = (seq_part, P(), P(), P(), P(), P(), P(), P(), P(None, None, 'tp'), P(None, None, 'tp'), P(None, 'tp', None), P())
    return jax.shard_map(device_fn, mesh=mesh, in_specs=in_specs, out_specs=seq_part, check_vma=False)
```
